32 devices in a mesh: dp: 4 (over z), exp: 8 (over y, x, core).
Axes of the slice: x: 2, y: 2, z: 4, core: 2. Of those that a mesh axis runs over, the one named last changes fastest.
Arguments:
- tokens: bfloat16 [16384, 1536], P(('dp', 'exp')), may hold values from -6 to 6
- targets: bfloat16 [16384, 1536], P(('dp', 'exp')), may hold values from -6 to 6
- valid_count: int32 [1], replicated, may hold values from 8192 to 16384
- segments: int32 [16384], P(('dp', 'exp')), may hold values from 0 to 2, as said below
- routes: int32 [16384, 4], P(('dp', 'exp')), may hold values from 0 to 7, all different within a row; in each aligned block of 512 rows (0 to 511, 512 to 1023, ...) at most 320 rows name the same one
- gain_attn: bfloat16 [1536], P(('dp', 'exp')), may hold values from 0.5 to 1.5
- w_query: bfloat16 [1536, 1536], P(('dp', 'exp')), may hold values from -0.15625 to 0.15625
- w_key: bfloat16 [1536, 256], P(('dp', 'exp')), may hold values from -0.15625 to 0.15625
- w_value: bfloat16 [1536, 256], P(('dp', 'exp')), may hold values from -0.15625 to 0.15625
- w_out: bfloat16 [1536, 1536], P(('dp', 'exp')), may hold values from -1.5 to 1.5
- gain_moe: bfloat16 [1536], P(('dp', 'exp')), may hold values from 0.5 to 1.5
- w_router: bfloat16 [1536, 8], P(('dp', 'exp')), may hold values from -0.15625 to 0.15625
- w_gate: bfloat16 [8, 1536, 768], P('exp', 'dp'), may hold values from -0.15625 to 0.15625
- w_up: bfloat16 [8, 1536, 768], P('exp', 'dp'), may hold values from -0.15625 to 0.15625
- w_down: bfloat16 [8, 768, 1536], P('exp', 'dp'), may hold values from -0.4375 to 0.4375
Outputs:
- layer_out: bfloat16 [16384, 1536], P(('dp', 'exp'))
- grad_tokens: float32 [16384, 1536], P(('dp', 'exp'))
- grad_gain_attn: float32 [1536], P(('dp', 'exp'))
- grad_w_query: float32 [1536, 1536], P(('dp', 'exp'))
- grad_w_key: float32 [1536, 256], P(('dp', 'exp'))
- grad_w_value: float32 [1536, 256], P(('dp', 'exp'))
- grad_w_out: float32 [1536, 1536], P(('dp', 'exp'))
- grad_gain_moe: float32 [1536], P(('dp', 'exp'))
- grad_w_router: float32 [1536, 8], P(('dp', 'exp'))
- grad_w_gate: float32 [8, 1536, 768], P('exp', 'dp')
- grad_w_up: float32 [8, 1536, 768], P('exp', 'dp')
- grad_w_down: float32 [8, 768, 1536], P('exp', 'dp')
The draws below stay inside these ranges and needn't reach their ends.
Inputs may be any that keep to these rules, and one draw needn't show every extreme that they name: `segments`: in each group of 512 rows the first 256 are 0 and the rest rise from 1 to 2 without falling, each continuation nonempty. `routes`: the 4 experts of a token differ; in the rows of one device no expert is named more than 320 times.
All inputs are finite; a program needn't handle non-finite values.
Results may differ from the reference program's by a relative error of at most 0.04.
Values may be sent and summed in bfloat16 or wider, within the bound.
A program may use at most 256 MiB of HBM per device.

```python
import math
import jax
import jax.numpy as jnp
import numpy as np
from jax import lax

D = 1536
H = 12
KV = 2
HD = 128
FF = 768
TOPK = 4
PROMPT = 256
CLEN = 128
NCONT = 2
TOK_DEV = 512
TOKENS = 16384
EXPERTS = 8
CAP = 320


def draw_segments(key, part):
    groups = TOKENS // TOK_DEV
    offsets = jax.random.randint(key, (groups, NCONT - 1), -(CLEN // 2), CLEN // 2 + 1).astype(jnp.int32)
    cuts = PROMPT + (jnp.arange(1, NCONT, dtype=jnp.int32) * CLEN)[None, :] + offsets
    row_ids = jnp.arange(TOK_DEV, dtype=jnp.int32)
    labels = 1 + jnp.sum((row_ids[None, :, None] >= cuts[:, None, :]).astype(jnp.int32), axis=2)
    labels = jnp.where(row_ids[None, :] < PROMPT, 0, labels)
    return labels.reshape(TOKENS).astype(jnp.int32)


def levels(key, shape, shards, least, largest):
    def one(position, parts):
        steps = jax.random.uniform(jax.random.fold_in(jax.random.fold_in(key, 6), position), (parts,), jnp.float32, least / len(shards), largest / len(shards))
        return jnp.repeat(jnp.exp(steps), shape[position] // parts).reshape((-1,) + (1,) * (len(shape) - position - 1))

    level = one(*shards[0])
    for cut in shards[1:]:
        level = level * one(*cut)
    return level


def deal_out(key, own, number, rows, number_of, top, most, slope):
    sequence = jax.random.permutation(key, number_of)
    crowded, ordinary = shares(number_of, rows * top, most, slope, True), shares(number_of, rows * top, most, slope, False)
    places = jnp.arange(number_of)

    def named(lengths, turn):
        used = int((lengths > 0).sum())
        fixed = max(1, used // 4)
        moved = fixed + (places - fixed + turn * (used - fixed)) % max(1, number_of - fixed)
        return jnp.zeros((number_of,), jnp.int32).at[sequence[jnp.where(places < fixed, places, moved)]].set(jnp.asarray(lengths, jnp.int32))

    lengths = jnp.where(number % 4 == 0, named(crowded, number // 4), named(ordinary, number - number // 4 - 1))
    mixed = jax.random.permutation(jax.random.fold_in(own, 3), number_of)
    donor, sink = mixed[0:number_of // 2 * 2:2], mixed[1:number_of // 2 * 2:2]
    room = jnp.minimum(lengths[donor] - 1, most - lengths[sink]) // 2
    room = jnp.where((donor == sequence[0]) | (sink == sequence[0]) | (lengths[sink] == 0), 0, jnp.maximum(room, 0))
    moved = jax.random.randint(jax.random.fold_in(own, 4), (number_of // 2,), 0, 1 << 20) % (room + 1)
    lengths = lengths.at[donor].add(-moved).at[sink].add(moved)
    items = jnp.searchsorted(jnp.cumsum(lengths), jnp.arange(rows * top), side="right").astype(jnp.int32)
    table = items.reshape(top, rows).T
    table = table[jax.random.permutation(jax.random.fold_in(own, 1), rows)]
    turn = jax.random.randint(jax.random.fold_in(own, 2), (rows, 1), 0, top)
    return jnp.take_along_axis(table, (jnp.arange(top)[None, :] + turn) % top, axis=1)


def shares(amount, total, reach, slope, full):
    loads = [(1 << 20) // math.isqrt(standing ** slope) + 1 for standing in range(1, amount + 1)]
    largest = reach if full else min(reach, max(-(-total // amount), total * loads[0] // sum(loads)))
    least = 1 if total - largest >= amount - 1 else 0
    counts, spare = [largest] + [least] * (amount - 1), total - largest - least * (amount - 1)
    while spare > 0:
        candidates = [i for i in range(1, amount) if counts[i] < largest] or [i for i in range(1, amount) if counts[i] < reach]
        whole, remaining = sum([loads[i] for i in candidates]), spare
        for i in candidates:
            extra = min(reach - counts[i], max(1, remaining * loads[i] // whole), spare)
            counts[i] = counts[i] + extra
            spare = spare - extra
    return np.array(counts)


def normal_values(key, dims, width, reach, split=(), held_as=jnp.bfloat16):
    array = jax.random.normal(key, dims, jnp.float32) * width
    if len(split) > 0:
        array = levels(key, dims, split, -0.22, 0.18) * array
    return jnp.clip(array, min=-reach, max=reach).astype(held_as)


def setup_inputs(seed: int = 0) -> dict:
    splits = jax.random.split(jax.random.key(seed), 16)
    tokens = normal_values(splits[0], (TOKENS, D), 1.0, 6.0, ((0, 32),))
    targets = normal_values(splits[1], (TOKENS, D), 1.0, 6.0, ((0, 32),))
    valid_count = jax.random.randint(splits[2], (1,), TOKENS // 2, TOKENS + 1).astype(jnp.int32)
    segments = draw_segments(jax.random.fold_in(splits[15], 71), 0)
    routes_keys = jax.random.split(jax.random.fold_in(splits[4], 1), TOKENS // TOK_DEV)
    routes_turns = jax.random.permutation(jax.random.fold_in(splits[4], 3), TOKENS // TOK_DEV)
    routes = jax.vmap(lambda own, number: deal_out(jax.random.fold_in(splits[4], 2), own, number, TOK_DEV, EXPERTS, TOPK, CAP, 1))(routes_keys, routes_turns).reshape((TOKENS, TOPK))
    gain_attn = jnp.clip(1.0 + 0.1 * jax.random.normal(splits[5], (D,), jnp.float32), 0.5, 1.5).astype(jnp.bfloat16)
    w_query = normal_values(splits[6], (D, H * HD), D ** -0.5, 0.15625, ((0, 32),))
    w_key = normal_values(splits[7], (D, KV * HD), D ** -0.5, 0.15625, ((0, 32),))
    w_value = normal_values(splits[8], (D, KV * HD), D ** -0.5, 0.15625, ((0, 32),))
    w_out = normal_values(splits[9], (H * HD, D), (max(H * HD // 96, 8)) ** -0.5, 1.5, ((0, 32),))
    gain_moe = jnp.clip(1.0 + 0.1 * jax.random.normal(splits[10], (D,), jnp.float32), 0.5, 1.5).astype(jnp.bfloat16)
    w_router = normal_values(splits[11], (D, EXPERTS), D ** -0.5, 0.15625, ((0, 32),))
    w_gate = normal_values(splits[12], (EXPERTS, D, FF), D ** -0.5, 0.15625, ((0, 8), (1, 4)))
    w_up = normal_values(splits[13], (EXPERTS, D, FF), D ** -0.5, 0.15625, ((0, 8), (1, 4)))
    w_down = normal_values(splits[14], (EXPERTS, FF, D), (FF // 4) ** -0.5, 0.4375, ((0, 8), (1, 4)))
    return {"tokens": tokens, "targets": targets, "valid_count": valid_count, "segments": segments, "routes": routes, "gain_attn": gain_attn, "w_query": w_query, "w_key": w_key, "w_value": w_value, "w_out": w_out, "gain_moe": gain_moe, "w_router": w_router, "w_gate": w_gate, "w_up": w_up, "w_down": w_down}


EPS = 1e-06
THETA = 10000.0
HIGH = lax.Precision.HIGHEST
NEG_BIG = -1e+30

@jax.custom_vjp
def low(v):
    return lax.optimization_barrier(v.astype(jnp.bfloat16)).astype(jnp.float32)

@jax.custom_vjp
def low_back(v):
    return v

def low_keep(v):
    return (low(v), None)

def low_pass(kept, grad):
    return (grad,)

def back_keep(v):
    return (v, None)

def back_low(kept, grad):
    return (low(grad),)
low.defvjp(low_keep, low_pass)
low_back.defvjp(back_keep, back_low)

def matmul_high(left, right):
    return jnp.dot(left, right, precision=HIGH, preferred_element_type=jnp.float32)

def rms_norm(values, gain):
    return values * lax.rsqrt(lax.optimization_barrier(jnp.mean(values * values, axis=-1, keepdims=True)) + EPS) * gain

def positions(segments):
    count_rows = segments.shape[0]
    row_ids = jnp.arange(count_rows, dtype=jnp.int32)
    labels = jnp.arange(NCONT + 1, dtype=jnp.int32)
    member = segments[:, None] == labels[None, :]
    first_row = lax.optimization_barrier(jnp.min(jnp.where(member, row_ids[:, None], count_rows), axis=0)).astype(jnp.int32)
    start_row = lax.optimization_barrier(jnp.sum(jnp.where(member, first_row[None, :], 0), axis=1)).astype(jnp.int32)
    return jnp.where(segments == 0, row_ids, PROMPT + row_ids - start_row).astype(jnp.int32)

def key_mask(segments):
    row_ids = jnp.arange(segments.shape[0], dtype=jnp.int32)
    causal = row_ids[None, :] <= row_ids[:, None]
    visible = (segments[None, :] == 0) | (segments[None, :] == segments[:, None])
    return causal & visible

def rotate(values, pos_rows, sign_value):
    half_size = HD // 2
    freq = THETA ** (-2.0 * jnp.arange(half_size, dtype=jnp.float32) / HD)
    angle = pos_rows.astype(jnp.float32)[:, None] * freq[None, :]
    cosine = jnp.cos(angle)[:, None, :]
    sine_part = sign_value * jnp.sin(angle)[:, None, :]
    first_half = values[..., :half_size]
    second = values[..., half_size:]
    return jnp.concatenate([first_half * cosine - second * sine_part, second * cosine + first_half * sine_part], axis=-1)

def attend_group(items):
    query_g, key_g, value_g, segs_g = items
    logits = jnp.einsum('qkgd,pkd->kgqp', query_g, key_g, precision=HIGH) * HD ** (-0.5)
    logits = low_back(logits)
    logits = jnp.where(key_mask(segs_g)[None, None], logits, NEG_BIG)
    weights = low(jax.nn.softmax(logits, axis=-1))
    mixed = jnp.einsum('kgqp,pkd->qkgd', weights, value_g, precision=HIGH)
    return mixed.reshape(mixed.shape[0], H * HD)

def layer_forward(tokens_f, gain_attn, w_query, w_key, w_value, w_out, gain_moe, w_router, w_gate, w_up, w_down, routes, segments):
    total_rows = tokens_f.shape[0]
    groups = total_rows // TOK_DEV
    seg_groups = segments.reshape(groups, TOK_DEV)
    pos_all = jax.vmap(positions)(seg_groups).reshape(total_rows)
    hidden_one = low(rms_norm(tokens_f, gain_attn))
    query_raw = low_back(matmul_high(hidden_one, w_query))
    key_raw = low_back(matmul_high(hidden_one, w_key))
    value_all = low_back(low(matmul_high(hidden_one, w_value)))
    query_rot = low(rotate(query_raw.reshape(total_rows, H, HD), pos_all, 1.0))
    key_rot = low(rotate(key_raw.reshape(total_rows, KV, HD), pos_all, 1.0))
    mixed = lax.map(jax.checkpoint(attend_group), (query_rot.reshape(groups, TOK_DEV, KV, H // KV, HD), key_rot.reshape(groups, TOK_DEV, KV, HD), value_all.reshape(groups, TOK_DEV, KV, HD), seg_groups))
    mixed = low_back(low(mixed.reshape(total_rows, H * HD)))
    resid_mid = tokens_f + low_back(matmul_high(mixed, w_out))
    hidden_two = low(rms_norm(resid_mid, gain_moe))
    router_prob = jax.nn.softmax(matmul_high(hidden_two, w_router), axis=-1)
    chosen = jnp.take_along_axis(router_prob, routes, axis=1)
    combine = chosen / lax.optimization_barrier(jnp.sum(chosen, axis=1, keepdims=True))
    expert_ids = jnp.arange(EXPERTS, dtype=jnp.int32)
    weight_full = lax.optimization_barrier(jnp.sum(jnp.where(routes[:, :, None] == expert_ids[None, None, :], combine[:, :, None], 0.0), axis=1))

    def expert_step(carry, items):
        gate_e, up_e, down_e, weight_e = items
        rows_in = low_back(hidden_two)
        gate_val = low_back(matmul_high(rows_in, gate_e))
        up_val = low_back(matmul_high(rows_in, up_e))
        act_val = low(jax.nn.relu(gate_val) * up_val)
        out_val = low_back(low(matmul_high(act_val, down_e)))
        return (carry + weight_e[:, None] * out_val, None)
    moe_out, unused_out = lax.scan(jax.checkpoint(expert_step), jnp.zeros_like(tokens_f), (w_gate, w_up, w_down, weight_full.T))
    return resid_mid + moe_out

def reference(tokens, targets, valid_count, segments, routes, gain_attn, w_query, w_key, w_value, w_out, gain_moe, w_router, w_gate, w_up, w_down):
    params = tuple((weight.astype(jnp.float32) for weight in (tokens, gain_attn, w_query, w_key, w_value, w_out, gain_moe, w_router, w_gate, w_up, w_down)))

    def forward_fn(*inputs):
        return layer_forward(*inputs, routes, segments)
    output, pullback = jax.vjp(forward_fn, *params)
    count_now = valid_count[0]
    row_ids = jnp.arange(output.shape[0], dtype=jnp.int32)
    loss_scale = output.shape[0] / count_now.astype(jnp.float32)
    cotangent = jnp.where((row_ids < count_now)[:, None], (output - targets.astype(jnp.float32)) * loss_scale, 0.0)
    grads = pullback(cotangent)
    return (output.astype(jnp.bfloat16), grads[0], grads[1], grads[2], grads[3], grads[4], grads[5], grads[6], grads[7], grads[8], grads[9], grads[10])
```

```python
import functools

import jax
import jax.numpy as jnp
from jax import lax
from jax.experimental import pallas as pl
from jax.experimental.pallas import tpu as pltpu
from jax.sharding import PartitionSpec as P

HD = 128
PROMPT = 256
NCONT = 2


EPS = 1e-06
THETA = 10000.0
HIGH = lax.Precision.HIGHEST
NEG_BIG = -1e30


def positions(segments):
    count_rows = segments.shape[0]
    row_ids = jnp.arange(count_rows, dtype=jnp.int32)
    labels = jnp.arange(NCONT + 1, dtype=jnp.int32)
    member = segments[:, None] == labels[None, :]
    first_row = jnp.min(jnp.where(member, row_ids[:, None], count_rows), axis=0)
    start_row = jnp.sum(jnp.where(member, first_row[None, :], 0), axis=1)
    return jnp.where(segments == 0, row_ids, PROMPT + row_ids - start_row)


def key_mask(segments):
    row_ids = jnp.arange(segments.shape[0], dtype=jnp.int32)
    causal = row_ids[None, :] <= row_ids[:, None]
    visible = (segments[None, :] == 0) | (segments[None, :] == segments[:, None])
    return causal & visible


def rotate(values, pos_rows, sign_value):
    half_size = HD // 2
    freq = THETA ** (-2.0 * jnp.arange(half_size, dtype=jnp.float32) / HD)
    angle = pos_rows.astype(jnp.float32)[:, None] * freq[None, :]
    cosine = jnp.cos(angle)[:, None, :]
    sine_part = sign_value * jnp.sin(angle)[:, None, :]
    first_half = values[..., :half_size]
    second = values[..., half_size:]
    return jnp.concatenate(
        [first_half * cosine - second * sine_part, second * cosine + first_half * sine_part],
        axis=-1,
    )


def attention_scores(query_b, key_b, allowed):
    logits = jnp.einsum(
        "qkgd,pkd->kgqp", query_b, key_b, preferred_element_type=jnp.float32
    ) * HD ** (-0.5)
    return jnp.where(allowed[None, None], logits, NEG_BIG)


def expert_gates(rows_in, gate_w, up_w):
    gate_val = jnp.einsum("sacd,adf->sacf", rows_in, gate_w, preferred_element_type=jnp.float32)
    up_val = jnp.einsum("sacd,adf->sacf", rows_in, up_w, preferred_element_type=jnp.float32)
    return (gate_val, up_val)


def body_general(
    tokens,
    targets,
    valid_count,
    segments,
    routes,
    gain_attn,
    w_query,
    w_key,
    w_value,
    w_out,
    gain_moe,
    w_router,
    w_gate,
    w_up,
    w_down,
):
    gain_one, query_w, key_w, value_w, out_w, gain_two, router_w = (
        lax.all_gather(gain_attn, ("dp", "exp"), axis=0, tiled=True),
        lax.all_gather(w_query, ("dp", "exp"), axis=0, tiled=True),
        lax.all_gather(w_key, ("dp", "exp"), axis=0, tiled=True),
        lax.all_gather(w_value, ("dp", "exp"), axis=0, tiled=True),
        lax.all_gather(w_out, ("dp", "exp"), axis=0, tiled=True),
        lax.all_gather(gain_moe, ("dp", "exp"), axis=0, tiled=True),
        lax.all_gather(w_router, ("dp", "exp"), axis=0, tiled=True),
    )
    gate_w, up_w, down_w = (
        lax.all_gather(w_gate, "dp", axis=1, tiled=True),
        lax.all_gather(w_up, "dp", axis=1, tiled=True),
        lax.all_gather(w_down, "dp", axis=1, tiled=True),
    )
    num_rows = tokens.shape[0]
    width = tokens.shape[1]
    num_heads = query_w.shape[1] // HD
    kv_heads = key_w.shape[1] // HD
    group_size = num_heads // kv_heads
    num_experts = router_w.shape[1]
    top_count = routes.shape[1]
    exp_local = gate_w.shape[0]
    exp_ranks = lax.axis_size("exp")
    capacity = 5 * num_rows * top_count // (4 * num_experts)
    tok_pos = positions(segments)
    allowed = key_mask(segments)
    resid_in = tokens.astype(jnp.float32)
    inv_one = lax.rsqrt(jnp.mean(resid_in * resid_in, axis=-1, keepdims=True) + EPS)
    normed_one = resid_in * inv_one
    hidden_one = (normed_one * gain_one.astype(jnp.float32)).astype(jnp.bfloat16)
    query_raw = jnp.dot(hidden_one, query_w, preferred_element_type=jnp.float32)
    key_raw = jnp.dot(hidden_one, key_w, preferred_element_type=jnp.float32)
    value_b = jnp.dot(hidden_one, value_w, preferred_element_type=jnp.float32).astype(jnp.bfloat16)
    query_b = rotate(query_raw.reshape(num_rows, num_heads, HD), tok_pos, 1.0).astype(jnp.bfloat16)
    query_b = query_b.reshape(num_rows, kv_heads, group_size, HD)
    key_b = rotate(key_raw.reshape(num_rows, kv_heads, HD), tok_pos, 1.0).astype(jnp.bfloat16)
    value_h = value_b.reshape(num_rows, kv_heads, HD)
    logit_att = attention_scores(query_b, key_b, allowed)
    row_max = jnp.max(logit_att, axis=-1, keepdims=True)
    log_total = row_max + jnp.log(jnp.sum(jnp.exp(logit_att - row_max), axis=-1, keepdims=True))
    probs_b = jnp.exp(logit_att - log_total).astype(jnp.bfloat16)
    attn_vals = jnp.einsum("kgqp,pkd->qkgd", probs_b, value_h, preferred_element_type=jnp.float32)
    attn_vals = attn_vals.reshape(num_rows, num_heads * HD).astype(jnp.bfloat16)
    resid_mid = resid_in + jnp.dot(attn_vals, out_w, preferred_element_type=jnp.float32)
    inv_two = lax.rsqrt(jnp.mean(resid_mid * resid_mid, axis=-1, keepdims=True) + EPS)
    normed_two = resid_mid * inv_two
    gain_two_f = gain_two.astype(jnp.float32)
    hidden_two = (normed_two * gain_two_f).astype(jnp.bfloat16)
    router_prob = jax.nn.softmax(
        jnp.dot(hidden_two, router_w, preferred_element_type=jnp.float32), axis=-1
    )
    expert_ids = jnp.arange(num_experts, dtype=jnp.int32)
    route_hot = routes[:, :, None] == expert_ids[None, None, :]
    chosen = jnp.sum(jnp.where(route_hot, router_prob[:, None, :], 0.0), axis=-1)
    weight_sum = jnp.sum(chosen, axis=1, keepdims=True)
    combine = chosen / weight_sum
    flat_hot = route_hot.reshape(num_rows * top_count, num_experts).astype(jnp.int32)
    slot_index = jnp.sum((jnp.cumsum(flat_hot, axis=0) - flat_hot) * flat_hot, axis=1)
    dest_index = routes.reshape(-1) * capacity + slot_index
    send_shape = (exp_ranks, exp_local, capacity, width)
    send_rows = jnp.zeros((num_experts * capacity, width), jnp.bfloat16)
    send_rows = (
        send_rows.at[dest_index].set(jnp.repeat(hidden_two, top_count, axis=0)).reshape(send_shape)
    )
    gate_val, up_val = expert_gates(
        lax.all_to_all(send_rows, "exp", split_axis=0, concat_axis=0, tiled=True), gate_w, up_w
    )
    act_b = (jax.nn.relu(gate_val) * up_val).astype(jnp.bfloat16)
    out_b = jnp.einsum("sacf,afd->sacd", act_b, down_w, preferred_element_type=jnp.float32).astype(
        jnp.bfloat16
    )
    returned = lax.all_to_all(out_b, "exp", split_axis=0, concat_axis=0, tiled=True)
    route_out = returned.reshape(num_experts * capacity, width)[dest_index].reshape(
        num_rows, top_count, width
    )
    route_out_f = route_out.astype(jnp.float32)
    resid_out = resid_mid + jnp.sum(combine[:, :, None] * route_out_f, axis=1)
    layer_out = resid_out.astype(jnp.bfloat16)
    total_rows = num_rows * lax.axis_size(("dp", "exp"))
    global_row = lax.axis_index(("dp", "exp")) * num_rows + jnp.arange(num_rows, dtype=jnp.int32)
    loss_scale = total_rows / valid_count[0].astype(jnp.float32)
    grad_out = jnp.where(
        (global_row < valid_count[0])[:, None],
        (resid_out - targets.astype(jnp.float32)) * loss_scale,
        0.0,
    )
    gain_one, query_w, key_w, value_w, out_w, gain_two, router_w = (
        lax.all_gather(gain_attn, ("dp", "exp"), axis=0, tiled=True),
        lax.all_gather(w_query, ("dp", "exp"), axis=0, tiled=True),
        lax.all_gather(w_key, ("dp", "exp"), axis=0, tiled=True),
        lax.all_gather(w_value, ("dp", "exp"), axis=0, tiled=True),
        lax.all_gather(w_out, ("dp", "exp"), axis=0, tiled=True),
        lax.all_gather(gain_moe, ("dp", "exp"), axis=0, tiled=True),
        lax.all_gather(w_router, ("dp", "exp"), axis=0, tiled=True),
    )
    gain_two_f = gain_two.astype(jnp.float32)
    grad_route = (combine[:, :, None] * grad_out[:, None, :]).astype(jnp.bfloat16)
    grad_comb = jnp.sum(grad_out[:, None, :] * route_out_f, axis=-1)
    grad_send = jnp.zeros((num_experts * capacity, width), jnp.bfloat16)
    grad_send = (
        grad_send.at[dest_index]
        .set(grad_route.reshape(num_rows * top_count, width))
        .reshape(send_shape)
    )
    expert_rows, grad_recv = (
        lax.all_to_all(send_rows, "exp", split_axis=0, concat_axis=0, tiled=True),
        lax.all_to_all(grad_send, "exp", split_axis=0, concat_axis=0, tiled=True),
    )
    gate_val, up_val = expert_gates(expert_rows, gate_w, up_w)
    gate_relu = jax.nn.relu(gate_val)
    act_b = (gate_relu * up_val).astype(jnp.bfloat16)
    grad_act = jnp.einsum("sacd,afd->sacf", grad_recv, down_w, preferred_element_type=jnp.float32)
    grad_down_w = jnp.einsum("sacf,sacd->afd", act_b, grad_recv, preferred_element_type=jnp.float32)
    grad_gate_b = jnp.where(gate_val > 0, grad_act * up_val, 0.0).astype(jnp.bfloat16)
    grad_up_b = (grad_act * gate_relu).astype(jnp.bfloat16)
    grad_gate_w = jnp.einsum(
        "sacd,sacf->adf", expert_rows, grad_gate_b, preferred_element_type=jnp.float32
    )
    grad_up_w = jnp.einsum(
        "sacd,sacf->adf", expert_rows, grad_up_b, preferred_element_type=jnp.float32
    )
    grad_rows = (
        jnp.einsum("sacf,adf->sacd", grad_gate_b, gate_w, preferred_element_type=jnp.float32)
        + jnp.einsum("sacf,adf->sacd", grad_up_b, up_w, preferred_element_type=jnp.float32)
    ).astype(jnp.bfloat16)
    grad_back = lax.all_to_all(grad_rows, "exp", split_axis=0, concat_axis=0, tiled=True)
    grad_copies = grad_back.reshape(num_experts * capacity, width)[dest_index].reshape(
        num_rows, top_count, width
    )
    grad_hidden_two = jnp.sum(grad_copies.astype(jnp.float32), axis=1)
    grad_chosen = (grad_comb - jnp.sum(grad_comb * combine, axis=1, keepdims=True)) / weight_sum
    grad_prob = jnp.sum(jnp.where(route_hot, grad_chosen[:, :, None], 0.0), axis=1)
    grad_logit = router_prob * (
        grad_prob - jnp.sum(router_prob * grad_prob, axis=-1, keepdims=True)
    )
    router_f = router_w.astype(jnp.float32)
    grad_hidden_two = grad_hidden_two + jnp.einsum(
        "re,de->rd", grad_logit, router_f, precision=HIGH
    )
    grad_router = jnp.einsum(
        "rd,re->de", hidden_two.astype(jnp.float32), grad_logit, precision=HIGH
    )
    grad_gain_two = jnp.sum(grad_hidden_two * normed_two, axis=0)
    grad_norm_two = grad_hidden_two * gain_two_f
    grad_mid = grad_out + inv_two * (
        grad_norm_two - normed_two * jnp.mean(grad_norm_two * normed_two, axis=-1, keepdims=True)
    )
    grad_proj_b = grad_mid.astype(jnp.bfloat16)
    grad_out_w = jnp.einsum("rh,rd->hd", attn_vals, grad_proj_b, preferred_element_type=jnp.float32)
    grad_vals_b = jnp.einsum(
        "rd,hd->rh", grad_proj_b, out_w, preferred_element_type=jnp.float32
    ).astype(jnp.bfloat16)
    grad_vals_b = grad_vals_b.reshape(num_rows, kv_heads, group_size, HD)
    logit_att = attention_scores(query_b, key_b, allowed)
    probs = jnp.exp(logit_att - log_total)
    probs_b = probs.astype(jnp.bfloat16)
    grad_value = jnp.einsum(
        "kgqp,qkgd->pkd", probs_b, grad_vals_b, preferred_element_type=jnp.float32
    )
    grad_prob_att = jnp.einsum(
        "qkgd,pkd->kgqp", grad_vals_b, value_h, preferred_element_type=jnp.float32
    )
    delta_row = jnp.sum(probs * grad_prob_att, axis=-1, keepdims=True)
    grad_score_b = (probs * (grad_prob_att - delta_row)).astype(jnp.bfloat16)
    grad_query = jnp.einsum(
        "kgqp,pkd->qkgd", grad_score_b, key_b, preferred_element_type=jnp.float32
    ) * HD ** (-0.5)
    grad_key = jnp.einsum(
        "kgqp,qkgd->pkd", grad_score_b, query_b, preferred_element_type=jnp.float32
    ) * HD ** (-0.5)
    grad_query_b = rotate(grad_query.reshape(num_rows, num_heads, HD), tok_pos, -1.0).astype(
        jnp.bfloat16
    )
    grad_query_b = grad_query_b.reshape(num_rows, num_heads * HD)
    grad_key_b = (
        rotate(grad_key, tok_pos, -1.0).astype(jnp.bfloat16).reshape(num_rows, kv_heads * HD)
    )
    grad_value_b = grad_value.astype(jnp.bfloat16).reshape(num_rows, kv_heads * HD)
    grad_query_w = jnp.einsum(
        "rd,rh->dh", hidden_one, grad_query_b, preferred_element_type=jnp.float32
    )
    grad_key_w = jnp.einsum("rd,rh->dh", hidden_one, grad_key_b, preferred_element_type=jnp.float32)
    grad_value_w = jnp.einsum(
        "rd,rh->dh", hidden_one, grad_value_b, preferred_element_type=jnp.float32
    )
    grad_hidden_one = (
        jnp.einsum("rh,dh->rd", grad_query_b, query_w, preferred_element_type=jnp.float32)
        + jnp.einsum("rh,dh->rd", grad_key_b, key_w, preferred_element_type=jnp.float32)
        + jnp.einsum("rh,dh->rd", grad_value_b, value_w, preferred_element_type=jnp.float32)
    )
    grad_gain_one = jnp.sum(grad_hidden_one * normed_one, axis=0)
    grad_norm_one = grad_hidden_one * gain_one.astype(jnp.float32)
    grad_in = grad_mid + inv_one * (
        grad_norm_one - normed_one * jnp.mean(grad_norm_one * normed_one, axis=-1, keepdims=True)
    )
    dense_sums = (
        lax.psum_scatter(grad_gain_one, ("dp", "exp"), scatter_dimension=0, tiled=True),
        lax.psum_scatter(grad_query_w, ("dp", "exp"), scatter_dimension=0, tiled=True),
        lax.psum_scatter(grad_key_w, ("dp", "exp"), scatter_dimension=0, tiled=True),
        lax.psum_scatter(grad_value_w, ("dp", "exp"), scatter_dimension=0, tiled=True),
        lax.psum_scatter(grad_out_w, ("dp", "exp"), scatter_dimension=0, tiled=True),
        lax.psum_scatter(grad_gain_two, ("dp", "exp"), scatter_dimension=0, tiled=True),
        lax.psum_scatter(grad_router, ("dp", "exp"), scatter_dimension=0, tiled=True),
    )
    expert_sums = (
        lax.psum_scatter(
            grad_gate_w.astype(jnp.bfloat16), "dp", scatter_dimension=1, tiled=True
        ).astype(jnp.float32),
        lax.psum_scatter(
            grad_up_w.astype(jnp.bfloat16), "dp", scatter_dimension=1, tiled=True
        ).astype(jnp.float32),
        lax.psum_scatter(
            grad_down_w.astype(jnp.bfloat16), "dp", scatter_dimension=1, tiled=True
        ).astype(jnp.float32),
    )
    return (
        layer_out,
        grad_in,
        dense_sums[0],
        dense_sums[1],
        dense_sums[2],
        dense_sums[3],
        dense_sums[4],
        dense_sums[5],
        dense_sums[6],
        expert_sums[0],
        expert_sums[1],
        expert_sums[2],
    )


MESH = pl.DeviceIdType.MESH
ANY = pl.BlockSpec(memory_space=pl.ANY)
VMEM_BYTES = 62 * 2**20


def nn_dot(left, right):
    return jnp.dot(left, right, preferred_element_type=jnp.float32)


def nt_dot(left, right):
    return lax.dot_general(
        left, right, (((1,), (1,)), ((), ())), preferred_element_type=jnp.float32
    )


def plane_peers():
    me = lax.axis_index("exp")
    core = lax.rem(me, 2)
    x_pos = lax.rem(lax.div(me, 2), 2)
    y_pos = lax.div(me, 4)
    return me, me + 1 - 2 * core, me + 2 - 4 * x_pos, me + 4 - 8 * y_pos


def remote(src, dst, send_sem, recv_sem, peer):
    return pltpu.make_async_remote_copy(
        src_ref=src,
        dst_ref=dst,
        send_sem=send_sem,
        recv_sem=recv_sem,
        device_id={"exp": peer},
        device_id_type=MESH,
    )


def plane_barrier(peers):
    barrier = pltpu.get_barrier_semaphore()
    for peer in peers:
        pl.semaphore_signal(barrier, inc=1, device_id={"exp": peer}, device_id_type=MESH)
    pl.semaphore_wait(barrier, len(peers))


def step_place(step, quad):
    odd = lax.rem(step, 2)
    last = lax.div(quad, 3)
    mid = lax.rem(lax.div(quad + 1, 2), 2)
    return mid * (1 - odd) + last, mid * odd + last


class Gather:
    def __init__(self, own, buf, send, recv):
        self.own, self.buf, self.send, self.recv = own, buf, send, recv
        self.me, self.sib, self.xn, self.yn = plane_peers()
        self.diag = self.xn + self.yn - self.me

    def own_copy(self, half, peer, sem):
        return remote(
            self.own.at[half],
            self.buf.at[self.me, half],
            self.send.at[sem],
            self.recv.at[self.me, half],
            peer,
        )

    def pass_copy(self, slot, half, peer, sem):
        return remote(
            self.buf.at[slot, half],
            self.buf.at[slot, half],
            self.send.at[sem],
            self.recv.at[slot, half],
            peer,
        )

    def own_copies(self):
        return (
            self.own_copy(0, self.xn, 0),
            self.own_copy(1, self.yn, 1),
            self.own_copy(0, self.sib, 2),
            self.own_copy(1, self.sib, 3),
            self.own_copy(1, self.xn, 4),
            self.own_copy(0, self.yn, 5),
        )

    def near_copies(self):
        return (
            self.pass_copy(self.xn, 0, self.yn, 6),
            self.pass_copy(self.yn, 1, self.xn, 7),
            self.pass_copy(self.xn, 0, self.sib, 8),
            self.pass_copy(self.yn, 1, self.sib, 9),
        )

    def late_copies(self):
        return (
            self.pass_copy(self.xn, 1, self.sib, 10),
            self.pass_copy(self.yn, 0, self.sib, 11),
        )

    def far_copies(self):
        return (
            self.pass_copy(self.diag, 0, self.sib, 12),
            self.pass_copy(self.diag, 1, self.sib, 13),
        )

    def wait_block(self, slot, half):
        self.pass_copy(slot, half, self.sib, 0).wait_recv()

    def begin(self):
        plane_barrier((self.sib, self.xn, self.yn))
        for copy in self.own_copies():
            copy.start()

    def place(self, step):
        quad = lax.div(step, 4)
        far_x, far_y = step_place(step, quad)
        odd = lax.rem(step, 2)
        third = lax.div(quad, 2) * (1 - lax.div(quad, 3))
        other = lax.div(lax.rem(step, 4), 2)
        slot = (
            self.me
            + far_x * (self.xn - self.me)
            + far_y * (self.yn - self.me)
            + other * (self.sib - self.me)
        )
        return slot, odd + third * (1 - 2 * odd), other

    def arrive(self, step):
        @pl.when(step == 4)
        def _():
            self.wait_block(self.xn, 0)
            self.wait_block(self.yn, 1)
            for copy in self.near_copies():
                copy.start()

        @pl.when(step == 8)
        def _():
            self.wait_block(self.xn, 1)
            self.wait_block(self.yn, 0)
            for copy in self.late_copies():
                copy.start()

        @pl.when(step == 12)
        def _():
            self.wait_block(self.diag, 0)
            self.wait_block(self.diag, 1)
            for copy in self.far_copies():
                copy.start()

        slot, half, other = self.place(step)

        @pl.when(other == 1)
        def _():
            self.wait_block(slot, half)

        return slot, half

    def finish(self):
        for copies in (self.own_copies(), self.near_copies(), self.late_copies(), self.far_copies()):
            for copy in copies:
                copy.wait_send()


def expert_in_kernel(own, gate_hbm, up_hbm, rows_out, gua_out, buf, gua, gate_w, up_w, send, recv, load, store_a, store_b):
    width, hidden = gate_w.shape
    gather = Gather(own, buf, send, recv)
    loads = (
        pltpu.make_async_copy(gate_hbm, gate_w, load.at[0]),
        pltpu.make_async_copy(up_hbm, up_w, load.at[1]),
        pltpu.make_async_copy(own.at[0], buf.at[gather.me, 0], load.at[2]),
        pltpu.make_async_copy(own.at[1], buf.at[gather.me, 1], load.at[3]),
    )
    for copy in loads:
        copy.start()
    gather.begin()
    for copy in loads:
        copy.wait()

    def row_store(slot, half, step):
        return pltpu.make_async_copy(buf.at[slot, half], rows_out.at[slot, half], store_a.at[step])

    def gua_store(slot, half, step):
        return pltpu.make_async_copy(gua.at[slot, half], gua_out.at[slot, half], store_b.at[step])

    def one(step, carry):
        slot, half = gather.arrive(step)
        row_store(slot, half, step).start()
        rows = buf[slot, half, :, :width]
        lanes = lax.broadcasted_iota(jnp.int32, (buf.shape[2], 128), 1)
        tail = buf[slot, half, :, width:].astype(jnp.float32)
        weight = jnp.sum(jnp.where(lanes == gather.me, tail, 0.0), axis=1, keepdims=True)
        gate_val = nn_dot(rows, gate_w[...])
        up_val = nn_dot(rows, up_w[...])
        gua[slot, half, :, :hidden] = gate_val.astype(jnp.bfloat16)
        gua[slot, half, :, hidden : 2 * hidden] = up_val.astype(jnp.bfloat16)
        act_val = jnp.maximum(gate_val, 0.0) * up_val * weight
        gua[slot, half, :, 2 * hidden :] = act_val.astype(jnp.bfloat16)
        gua_store(slot, half, step).start()
        return carry

    lax.fori_loop(0, 16, one, 0)
    gather.finish()

    def drain(step, carry):
        slot, half, _ = gather.place(step)
        row_store(slot, half, step).wait()
        gua_store(slot, half, step).wait()
        return carry

    lax.fori_loop(0, 16, drain, 0)


def expert_in(own, gate_w, up_w):
    _, half, columns = own.shape
    width, hidden = gate_w.shape
    bf = jnp.bfloat16
    return pl.pallas_call(
        expert_in_kernel,
        out_shape=(
            jax.ShapeDtypeStruct((8, 2, half, columns), bf),
            jax.ShapeDtypeStruct((8, 2, half, 3 * hidden), bf),
        ),
        in_specs=[ANY] * 3,
        out_specs=(ANY, ANY),
        scratch_shapes=[
            pltpu.VMEM((8, 2, half, columns), bf),
            pltpu.VMEM((8, 2, half, 3 * hidden), bf),
            pltpu.VMEM((width, hidden), bf),
            pltpu.VMEM((width, hidden), bf),
            pltpu.SemaphoreType.DMA((14,)),
            pltpu.SemaphoreType.DMA((8, 2)),
            pltpu.SemaphoreType.DMA((4,)),
            pltpu.SemaphoreType.DMA((16,)),
            pltpu.SemaphoreType.DMA((16,)),
        ],
        compiler_params=pltpu.CompilerParams(
            collective_id=1, has_side_effects=True, vmem_limit_bytes=VMEM_BYTES
        ),
        name="expert_in",
    )(own, gate_w, up_w)


def add_rows(target, others, chunk=64):
    def one(index, carry):
        rows = pl.ds(pl.multiple_of(index * chunk, chunk), chunk)
        total = target[rows, :].astype(jnp.float32)
        for other in others:
            total = total + other[rows, :].astype(jnp.float32)
        target[rows, :] = total.astype(target.dtype)
        return carry

    lax.fori_loop(0, target.shape[0] // chunk, one, 0)


class Scatter:
    def __init__(self, part, side, relay, final, send, side_sem, relay_sem, final_sem):
        self.part, self.side, self.relay, self.final = part, side, relay, final
        self.send, self.side_sem = send, side_sem
        self.relay_sem, self.final_sem = relay_sem, final_sem
        self.me, self.sib, self.xn, self.yn = plane_peers()
        self.diag = self.xn + self.yn - self.me

    def begin(self):
        plane_barrier((self.sib, self.xn, self.yn))

    def place(self, step):
        quad = lax.div(step, 4)
        far_x, far_y = step_place(step, 3 - quad)
        odd = lax.rem(step, 2)
        third = lax.div(quad, 2) * (1 - lax.div(quad, 3))
        other = 1 - lax.div(lax.rem(step, 4), 2)
        slot = (
            self.me
            + far_x * (self.xn - self.me)
            + far_y * (self.yn - self.me)
            + other * (self.sib - self.me)
        )
        return slot, odd + third * (1 - 2 * odd), other, far_x + 2 * far_y

    def side_copy(self, step):
        slot, half, _, place = self.place(step)
        return remote(
            self.part.at[slot, half],
            self.side.at[place, half],
            self.send.at[step],
            self.side_sem.at[place, half],
            self.sib,
        )

    def side_wait(self, place, half):
        remote(
            self.side.at[place, half],
            self.side.at[place, half],
            self.send.at[0],
            self.side_sem.at[place, half],
            self.sib,
        ).wait_recv()

    def relay_copy(self, step, way):
        return remote(
            self.part.at[self.diag, way],
            self.relay.at[way],
            self.send.at[step],
            self.relay_sem.at[way],
            (self.xn, self.yn)[way],
        )

    def final_copy(self, step, way, half):
        return remote(
            self.part.at[(self.xn, self.yn)[way], half],
            self.final.at[way, half],
            self.send.at[step],
            self.final_sem.at[way, half],
            (self.xn, self.yn)[way],
        )

    def depart(self, step):
        slot, half, other, place = self.place(step)

        @pl.when(other == 1)
        def _():
            self.side_copy(step).start()

        for way in (0, 1):

            @pl.when(step == 2 + way)
            def _():
                self.side_wait(3, way)
                add_rows(self.part.at[self.diag, way], (self.side.at[3, way],))
                self.relay_copy(2 + way, way).start()

            peer = (self.xn, self.yn)[way]

            @pl.when(step == 6 + way)
            def _():
                self.side_wait(1 + way, way)
                add_rows(self.part.at[peer, way], (self.side.at[1 + way, way],))
                self.final_copy(6 + way, way, way).start()

            @pl.when(step == 15)
            def _():
                self.side_wait(1 + way, 1 - way)
                self.relay_copy(3 - way, 1 - way).wait_recv()
                add_rows(
                    self.part.at[peer, 1 - way], (self.side.at[1 + way, 1 - way], self.relay.at[1 - way])
                )
                self.final_copy(10 + way, way, 1 - way).start()

    def finish(self, out):
        half_rows = out.shape[1]
        chunk = 64
        for half in (0, 1):
            self.side_wait(0, half)
            self.final_copy(0, 0, half).wait_recv()
            self.final_copy(0, 1, half).wait_recv()

            def one(index, carry):
                rows = pl.ds(pl.multiple_of(index * chunk, chunk), chunk)
                total = self.part[self.me, half, rows, :].astype(jnp.float32)
                total = total + self.side[0, half, rows, :].astype(jnp.float32)
                total = total + self.final[0, half, rows, :].astype(jnp.float32)
                total = total + self.final[1, half, rows, :].astype(jnp.float32)
                out[half, rows, :] = total
                return carry

            lax.fori_loop(0, half_rows // chunk, one, 0)
        for way in (0, 1):
            self.relay_copy(2 + way, way).wait_send()
            self.final_copy(6 + way, way, way).wait_send()
            self.final_copy(10 + way, way, 1 - way).wait_send()

        def drain(step, carry):
            @pl.when(self.place(step)[2] == 1)
            def _():
                self.side_copy(step).wait_send()

            return carry

        lax.fori_loop(0, 16, drain, 0)


def scatter_scratch(half, columns):
    bf = jnp.bfloat16
    return [
        pltpu.VMEM((8, 2, half, columns), bf),
        pltpu.VMEM((4, 2, half, columns), bf),
        pltpu.VMEM((2, half, columns), bf),
        pltpu.VMEM((2, 2, half, columns), bf),
        pltpu.SemaphoreType.DMA((16,)),
        pltpu.SemaphoreType.DMA((4, 2)),
        pltpu.SemaphoreType.DMA((2,)),
        pltpu.SemaphoreType.DMA((2, 2)),
    ]


def expert_out_kernel(gua_hbm, down_hbm, out, act, down_w, load, part, side, relay, final, send, side_sem, relay_sem, final_sem):
    hidden = down_w.shape[0]
    scatter = Scatter(part, side, relay, final, send, side_sem, relay_sem, final_sem)
    down_load = pltpu.make_async_copy(down_hbm, down_w, load.at[16])
    down_load.start()

    def act_load(step):
        slot, half, _, _ = scatter.place(step)
        return pltpu.make_async_copy(
            gua_hbm.at[slot, half, :, pl.ds(2 * hidden, hidden)], act.at[slot, half], load.at[step]
        )

    def fetch(step, carry):
        act_load(step).start()
        return carry

    lax.fori_loop(0, 16, fetch, 0)
    scatter.begin()
    down_load.wait()

    def one(step, carry):
        slot, half, _, _ = scatter.place(step)
        act_load(step).wait()
        part[slot, half] = nn_dot(act[slot, half], down_w[...]).astype(jnp.bfloat16)
        scatter.depart(step)
        return carry

    lax.fori_loop(0, 16, one, 0)
    scatter.finish(out)


def expert_out(gua, down_w):
    half = gua.shape[2]
    hidden, width = down_w.shape
    return pl.pallas_call(
        expert_out_kernel,
        out_shape=jax.ShapeDtypeStruct((2, half, width), jnp.float32),
        in_specs=[ANY] * 2,
        out_specs=pl.BlockSpec(memory_space=pltpu.VMEM),
        scratch_shapes=[
            pltpu.VMEM((8, 2, half, hidden), jnp.bfloat16),
            pltpu.VMEM((hidden, width), jnp.bfloat16),
            pltpu.SemaphoreType.DMA((17,)),
        ]
        + scatter_scratch(half, width),
        compiler_params=pltpu.CompilerParams(
            collective_id=2, has_side_effects=True, vmem_limit_bytes=VMEM_BYTES
        ),
        name="expert_out",
    )(gua, down_w)


def expert_back_kernel(own, rows_hbm, gua_hbm, gate_hbm, up_hbm, down_hbm, grads_out, dgu_out, part_out, buf, gu, tails, part, gate_w, up_w, down_w, send, recv, load, load_gu, load_tail, store_a, store_b, store_c):
    width, hidden = gate_w.shape
    gather = Gather(own, buf, send, recv)
    loads = (
        pltpu.make_async_copy(down_hbm, down_w, load.at[0]),
        pltpu.make_async_copy(own.at[0], buf.at[gather.me, 0], load.at[1]),
        pltpu.make_async_copy(own.at[1], buf.at[gather.me, 1], load.at[2]),
        pltpu.make_async_copy(gate_hbm, gate_w, load.at[3]),
        pltpu.make_async_copy(up_hbm, up_w, load.at[4]),
    )
    for copy in loads:
        copy.start()

    def block_loads(step):
        slot, half, _ = gather.place(step)
        return (
            pltpu.make_async_copy(
                gua_hbm.at[slot, half, :, pl.ds(0, 2 * hidden)], gu.at[slot, half], load_gu.at[step]
            ),
            pltpu.make_async_copy(
                rows_hbm.at[slot, half, :, pl.ds(width, 128)], tails.at[slot, half], load_tail.at[step]
            ),
        )

    def fetch(step, carry):
        for copy in block_loads(step):
            copy.start()
        return carry

    lax.fori_loop(0, 16, fetch, 0)
    gather.begin()
    for copy in loads:
        copy.wait()

    def stores(step):
        slot, half, _ = gather.place(step)
        return (
            pltpu.make_async_copy(buf.at[slot, half], grads_out.at[slot, half], store_a.at[step]),
            pltpu.make_async_copy(gu.at[slot, half], dgu_out.at[slot, half], store_b.at[step]),
            pltpu.make_async_copy(part.at[slot, half], part_out.at[slot, half], store_c.at[step]),
        )

    def one(step, carry):
        slot, half = gather.arrive(step)
        store_rows, store_dgu, store_part = stores(step)
        store_rows.start()
        for copy in block_loads(step):
            copy.wait()
        lanes = lax.broadcasted_iota(jnp.int32, (buf.shape[2], 128), 1)
        tail = tails[slot, half].astype(jnp.float32)
        weight = jnp.sum(jnp.where(lanes == gather.me, tail, 0.0), axis=1, keepdims=True)
        grad_act = nt_dot(buf[slot, half], down_w[...])
        gate_val = gu[slot, half, :, :hidden].astype(jnp.float32)
        up_val = gu[slot, half, :, hidden:].astype(jnp.float32)
        gate_relu = jnp.maximum(gate_val, 0.0)
        grad_comb = jnp.sum(gate_relu * up_val * grad_act, axis=1, keepdims=True)
        grad_act = grad_act * weight
        grad_gate = jnp.where(gate_val > 0, grad_act * up_val, 0.0).astype(jnp.bfloat16)
        grad_up = (grad_act * gate_relu).astype(jnp.bfloat16)
        gu[slot, half, :, :hidden] = grad_gate
        gu[slot, half, :, hidden:] = grad_up
        store_dgu.start()
        part[slot, half, :, :width] = (
            nt_dot(grad_gate, gate_w[...]) + nt_dot(grad_up, up_w[...])
        ).astype(jnp.bfloat16)
        part[slot, half, :, width:] = jnp.where(lanes == gather.me, grad_comb, 0.0).astype(
            jnp.bfloat16
        )
        store_part.start()
        return carry

    lax.fori_loop(0, 16, one, 0)
    gather.finish()

    def drain(step, carry):
        for copy in stores(step):
            copy.wait()
        return carry

    lax.fori_loop(0, 16, drain, 0)


def expert_back(own, rows_all, gua, gate_w, up_w, down_w):
    _, half, columns = rows_all.shape[1:]
    width, hidden = gate_w.shape
    bf = jnp.bfloat16
    return pl.pallas_call(
        expert_back_kernel,
        out_shape=(
            jax.ShapeDtypeStruct((8, 2, half, width), bf),
            jax.ShapeDtypeStruct((8, 2, half, 2 * hidden), bf),
            jax.ShapeDtypeStruct((8, 2, half, columns), bf),
        ),
        in_specs=[ANY] * 6,
        out_specs=(ANY,) * 3,
        scratch_shapes=[
            pltpu.VMEM((8, 2, half, width), bf),
            pltpu.VMEM((8, 2, half, 2 * hidden), bf),
            pltpu.VMEM((8, 2, half, 128), bf),
            pltpu.VMEM((8, 2, half, columns), bf),
            pltpu.VMEM((width, hidden), bf),
            pltpu.VMEM((width, hidden), bf),
            pltpu.VMEM((hidden, width), bf),
            pltpu.SemaphoreType.DMA((14,)),
            pltpu.SemaphoreType.DMA((8, 2)),
            pltpu.SemaphoreType.DMA((5,)),
        ]
        + [pltpu.SemaphoreType.DMA((16,))] * 5,
        compiler_params=pltpu.CompilerParams(
            collective_id=3, has_side_effects=True, vmem_limit_bytes=VMEM_BYTES
        ),
        name="expert_back",
    )(own, rows_all, gua, gate_w, up_w, down_w)


def scatter_kernel(part_hbm, out, load, part, side, relay, final, send, side_sem, relay_sem, final_sem):
    scatter = Scatter(part, side, relay, final, send, side_sem, relay_sem, final_sem)

    def part_load(step):
        slot, half, _, _ = scatter.place(step)
        return pltpu.make_async_copy(part_hbm.at[slot, half], part.at[slot, half], load.at[step])

    def fetch(step, carry):
        part_load(step).start()
        return carry

    lax.fori_loop(0, 16, fetch, 0)
    scatter.begin()

    def one(step, carry):
        part_load(step).wait()
        scatter.depart(step)
        return carry

    lax.fori_loop(0, 16, one, 0)
    scatter.finish(out)


def plane_scatter(part, ident):
    _, _, half, columns = part.shape
    return pl.pallas_call(
        scatter_kernel,
        out_shape=jax.ShapeDtypeStruct((2, half, columns), jnp.float32),
        in_specs=[ANY],
        out_specs=pl.BlockSpec(memory_space=pltpu.VMEM),
        scratch_shapes=[pltpu.SemaphoreType.DMA((16,))] + scatter_scratch(half, columns),
        compiler_params=pltpu.CompilerParams(
            collective_id=ident, has_side_effects=True, vmem_limit_bytes=VMEM_BYTES
        ),
        name="plane_scatter",
    )(part)


def body_plane(
    tokens,
    targets,
    valid_count,
    segments,
    routes,
    gain_attn,
    w_query,
    w_key,
    w_value,
    w_out,
    gain_moe,
    w_router,
    w_gate,
    w_up,
    w_down,
):
    bf = jnp.bfloat16
    num_rows, width = tokens.shape
    half = num_rows // 2
    q_cols, k_cols = w_query.shape[1], w_key.shape[1]
    qkv_cols = q_cols + 2 * k_cols
    dense_cols = qkv_cols + w_out.shape[1]
    num_experts = w_router.shape[1]
    num_heads = q_cols // HD
    kv_heads = k_cols // HD
    group_size = num_heads // kv_heads
    pad_cols = 128 - 2 - num_experts
    dense_own = jnp.concatenate(
        [
            w_query,
            w_key,
            w_value,
            w_out,
            gain_attn[:, None],
            gain_moe[:, None],
            w_router,
            jnp.zeros((gain_attn.shape[0], pad_cols), bf),
        ],
        axis=1,
    )
    dense_w = lax.all_gather(dense_own, ("dp", "exp"), axis=0, tiled=True)
    gate_w = lax.all_gather(w_gate, "dp", axis=1, tiled=True)[0]
    up_w = lax.all_gather(w_up, "dp", axis=1, tiled=True)[0]
    down_w = lax.all_gather(w_down, "dp", axis=1, tiled=True)[0]
    qkv_w = dense_w[:, :qkv_cols]
    out_w = dense_w[:, qkv_cols:dense_cols]
    gain_one = dense_w[:, dense_cols].astype(jnp.float32)
    gain_two = dense_w[:, dense_cols + 1].astype(jnp.float32)
    router_w = dense_w[:, dense_cols + 2 : dense_cols + 2 + num_experts]
    tok_pos = positions(segments)
    allowed = key_mask(segments)
    resid_in = tokens.astype(jnp.float32)
    inv_one = lax.rsqrt(jnp.mean(resid_in * resid_in, axis=-1, keepdims=True) + EPS)
    normed_one = resid_in * inv_one
    hidden_one = (normed_one * gain_one).astype(bf)
    qkv_raw = jnp.dot(hidden_one, qkv_w, preferred_element_type=jnp.float32)
    value_b = qkv_raw[:, q_cols + k_cols :].astype(bf)
    query_b = rotate(qkv_raw[:, :q_cols].reshape(num_rows, num_heads, HD), tok_pos, 1.0).astype(bf)
    query_b = query_b.reshape(num_rows, kv_heads, group_size, HD)
    key_b = rotate(
        qkv_raw[:, q_cols : q_cols + k_cols].reshape(num_rows, kv_heads, HD), tok_pos, 1.0
    ).astype(bf)
    value_h = value_b.reshape(num_rows, kv_heads, HD)
    logit_att = attention_scores(query_b, key_b, allowed)
    row_max = jnp.max(logit_att, axis=-1, keepdims=True)
    log_total = row_max + jnp.log(jnp.sum(jnp.exp(logit_att - row_max), axis=-1, keepdims=True))
    probs_b = jnp.exp(logit_att - log_total).astype(bf)
    attn_vals = jnp.einsum("kgqp,pkd->qkgd", probs_b, value_h, preferred_element_type=jnp.float32)
    attn_vals = attn_vals.reshape(num_rows, q_cols).astype(bf)
    resid_mid = resid_in + jnp.dot(attn_vals, out_w, preferred_element_type=jnp.float32)
    inv_two = lax.rsqrt(jnp.mean(resid_mid * resid_mid, axis=-1, keepdims=True) + EPS)
    normed_two = resid_mid * inv_two
    hidden_two = (normed_two * gain_two).astype(bf)
    router_prob = jax.nn.softmax(
        jnp.dot(hidden_two, router_w, preferred_element_type=jnp.float32), axis=-1
    )
    expert_ids = jnp.arange(num_experts, dtype=jnp.int32)
    route_hot = routes[:, :, None] == expert_ids[None, None, :]
    chosen = jnp.sum(jnp.where(route_hot, router_prob[:, None, :], 0.0), axis=-1)
    weight_sum = jnp.sum(chosen, axis=1, keepdims=True)
    combine = chosen / weight_sum
    weight_full = jnp.sum(jnp.where(route_hot, combine[:, :, None], 0.0), axis=1)
    rows_own = jnp.concatenate(
        [hidden_two, jnp.pad(weight_full.astype(bf), ((0, 0), (0, 128 - num_experts)))], axis=1
    )
    rows_all, gua = expert_in(rows_own.reshape(2, half, width + 128), gate_w, up_w)
    moe_out = expert_out(gua, down_w).reshape(num_rows, width)
    resid_out = resid_mid + moe_out
    layer_out = resid_out.astype(bf)
    total_rows = num_rows * lax.axis_size(("dp", "exp"))
    global_row = lax.axis_index(("dp", "exp")) * num_rows + jnp.arange(num_rows, dtype=jnp.int32)
    loss_scale = total_rows / valid_count[0].astype(jnp.float32)
    grad_out = jnp.where(
        (global_row < valid_count[0])[:, None],
        (resid_out - targets.astype(jnp.float32)) * loss_scale,
        0.0,
    )
    grads_all, dgu, part = expert_back(
        grad_out.astype(bf).reshape(2, half, width), rows_all, gua, gate_w, up_w, down_w
    )
    back = plane_scatter(part, 4).reshape(num_rows, width + 128)
    hidden = gate_w.shape[1]
    flat_rows = rows_all.reshape(-1, width + 128)[:, :width]
    flat_grads = grads_all.reshape(-1, width)
    grad_gate_up = jnp.einsum(
        "rd,rf->df", flat_rows, dgu.reshape(-1, 2 * hidden), preferred_element_type=jnp.float32
    ).astype(bf)
    grad_down_w = jnp.einsum(
        "rf,rd->fd",
        gua.reshape(-1, 3 * hidden)[:, 2 * hidden :],
        flat_grads,
        preferred_element_type=jnp.float32,
    ).astype(bf)
    expert_sums = tuple(
        lax.psum_scatter(grad[None], "dp", scatter_dimension=1, tiled=True).astype(jnp.float32)
        for grad in (grad_gate_up[:, :hidden], grad_gate_up[:, hidden:], grad_down_w)
    )
    grad_hidden_two = back[:, :width]
    grad_comb = jnp.sum(
        jnp.where(route_hot, back[:, None, width : width + num_experts], 0.0), axis=-1
    )
    grad_chosen = (grad_comb - jnp.sum(grad_comb * combine, axis=1, keepdims=True)) / weight_sum
    grad_prob = jnp.sum(jnp.where(route_hot, grad_chosen[:, :, None], 0.0), axis=1)
    grad_logit = router_prob * (
        grad_prob - jnp.sum(router_prob * grad_prob, axis=-1, keepdims=True)
    )
    grad_hidden_two = grad_hidden_two + jnp.einsum(
        "re,de->rd", grad_logit, router_w.astype(jnp.float32), precision=HIGH
    )
    grad_router = jnp.einsum(
        "rd,re->de", hidden_two.astype(jnp.float32), grad_logit, precision=HIGH
    )
    grad_gain_two = jnp.sum(grad_hidden_two * normed_two, axis=0)
    grad_norm_two = grad_hidden_two * gain_two
    grad_mid = grad_out + inv_two * (
        grad_norm_two - normed_two * jnp.mean(grad_norm_two * normed_two, axis=-1, keepdims=True)
    )
    grad_proj_b = grad_mid.astype(bf)
    grad_out_w = jnp.einsum("rh,rd->hd", attn_vals, grad_proj_b, preferred_element_type=jnp.float32)
    grad_vals_b = jnp.einsum(
        "rd,hd->rh", grad_proj_b, out_w, preferred_element_type=jnp.float32
    ).astype(bf)
    grad_vals_b = grad_vals_b.reshape(num_rows, kv_heads, group_size, HD)
    logit_att = attention_scores(query_b, key_b, allowed)
    probs = jnp.exp(logit_att - log_total)
    probs_b = probs.astype(bf)
    grad_value = jnp.einsum(
        "kgqp,qkgd->pkd", probs_b, grad_vals_b, preferred_element_type=jnp.float32
    )
    grad_prob_att = jnp.einsum(
        "qkgd,pkd->kgqp", grad_vals_b, value_h, preferred_element_type=jnp.float32
    )
    delta_row = jnp.sum(probs * grad_prob_att, axis=-1, keepdims=True)
    grad_score_b = (probs * (grad_prob_att - delta_row)).astype(bf)
    grad_query = jnp.einsum(
        "kgqp,pkd->qkgd", grad_score_b, key_b, preferred_element_type=jnp.float32
    ) * HD ** (-0.5)
    grad_key = jnp.einsum(
        "kgqp,qkgd->pkd", grad_score_b, query_b, preferred_element_type=jnp.float32
    ) * HD ** (-0.5)
    grad_query_b = rotate(grad_query.reshape(num_rows, num_heads, HD), tok_pos, -1.0).astype(bf)
    grad_key_b = rotate(grad_key, tok_pos, -1.0).astype(bf)
    grad_qkv_b = jnp.concatenate(
        [
            grad_query_b.reshape(num_rows, q_cols),
            grad_key_b.reshape(num_rows, k_cols),
            grad_value.astype(bf).reshape(num_rows, k_cols),
        ],
        axis=1,
    )
    grad_qkv_w = jnp.einsum("rd,rh->dh", hidden_one, grad_qkv_b, preferred_element_type=jnp.float32)
    grad_hidden_one = jnp.einsum("rh,dh->rd", grad_qkv_b, qkv_w, preferred_element_type=jnp.float32)
    grad_gain_one = jnp.sum(grad_hidden_one * normed_one, axis=0)
    grad_norm_one = grad_hidden_one * gain_one
    grad_in = grad_mid + inv_one * (
        grad_norm_one - normed_one * jnp.mean(grad_norm_one * normed_one, axis=-1, keepdims=True)
    )
    dense_grad = jnp.concatenate(
        [
            grad_qkv_w.astype(bf),
            grad_out_w.astype(bf),
            jnp.pad(
                jnp.concatenate([grad_gain_one[:, None], grad_gain_two[:, None], grad_router], axis=1),
                ((0, 0), (0, pad_cols)),
            ).astype(bf),
        ],
        axis=1,
    )
    dense_sum = lax.psum_scatter(
        dense_grad, ("dp", "exp"), scatter_dimension=0, tiled=True
    ).astype(jnp.float32)
    return (
        layer_out,
        grad_in,
        dense_sum[:, dense_cols],
        dense_sum[:, :q_cols],
        dense_sum[:, q_cols : q_cols + k_cols],
        dense_sum[:, q_cols + k_cols : qkv_cols],
        dense_sum[:, qkv_cols:dense_cols],
        dense_sum[:, dense_cols + 1],
        dense_sum[:, dense_cols + 2 : dense_cols + 2 + num_experts],
        *expert_sums,
    )


def solution(mesh):
    in_specs = (
        P(("dp", "exp"), None),
        P(("dp", "exp"), None),
        P(),
        P(("dp", "exp")),
        P(("dp", "exp"), None),
        P(("dp", "exp")),
        P(("dp", "exp"), None),
        P(("dp", "exp"), None),
        P(("dp", "exp"), None),
        P(("dp", "exp"), None),
        P(("dp", "exp")),
        P(("dp", "exp"), None),
        P("exp", "dp", None),
        P("exp", "dp", None),
        P("exp", "dp", None),
    )
    out_specs = (
        P(("dp", "exp"), None),
        P(("dp", "exp"), None),
        P(("dp", "exp")),
        P(("dp", "exp"), None),
        P(("dp", "exp"), None),
        P(("dp", "exp"), None),
        P(("dp", "exp"), None),
        P(("dp", "exp")),
        P(("dp", "exp"), None),
        P("exp", "dp", None),
        P("exp", "dp", None),
        P("exp", "dp", None),
    )
    body = body_plane if mesh.shape["exp"] == 8 else body_general
    return jax.shard_map(body, mesh=mesh, in_specs=in_specs, out_specs=out_specs, check_vma=False)
```

```python
import functools

import jax
import jax.numpy as jnp
from jax import lax
from jax.experimental import pallas as pl
from jax.experimental.pallas import tpu as pltpu
from jax.sharding import PartitionSpec as P

HD = 128
PROMPT = 256
NCONT = 2


EPS = 1e-06
THETA = 10000.0
HIGH = lax.Precision.HIGHEST
NEG_BIG = -1e30


def positions(segments):
    count_rows = segments.shape[0]
    row_ids = jnp.arange(count_rows, dtype=jnp.int32)
    labels = jnp.arange(NCONT + 1, dtype=jnp.int32)
    member = segments[:, None] == labels[None, :]
    first_row = jnp.min(jnp.where(member, row_ids[:, None], count_rows), axis=0)
    start_row = jnp.sum(jnp.where(member, first_row[None, :], 0), axis=1)
    return jnp.where(segments == 0, row_ids, PROMPT + row_ids - start_row)


def key_mask(segments):
    row_ids = jnp.arange(segments.shape[0], dtype=jnp.int32)
    causal = row_ids[None, :] <= row_ids[:, None]
    visible = (segments[None, :] == 0) | (segments[None, :] == segments[:, None])
    return causal & visible


def rotate(values, pos_rows, sign_value):
    half_size = HD // 2
    freq = THETA ** (-2.0 * jnp.arange(half_size, dtype=jnp.float32) / HD)
    angle = pos_rows.astype(jnp.float32)[:, None] * freq[None, :]
    cosine = jnp.cos(angle)[:, None, :]
    sine_part = sign_value * jnp.sin(angle)[:, None, :]
    first_half = values[..., :half_size]
    second = values[..., half_size:]
    return jnp.concatenate(
        [first_half * cosine - second * sine_part, second * cosine + first_half * sine_part],
        axis=-1,
    )


def attention_scores(query_b, key_b, allowed):
    logits = jnp.einsum(
        "qkgd,pkd->kgqp", query_b, key_b, preferred_element_type=jnp.float32
    ) * HD ** (-0.5)
    return jnp.where(allowed[None, None], logits, NEG_BIG)


def expert_gates(rows_in, gate_w, up_w):
    gate_val = jnp.einsum("sacd,adf->sacf", rows_in, gate_w, preferred_element_type=jnp.float32)
    up_val = jnp.einsum("sacd,adf->sacf", rows_in, up_w, preferred_element_type=jnp.float32)
    return (gate_val, up_val)


def body_general(
    tokens,
    targets,
    valid_count,
    segments,
    routes,
    gain_attn,
    w_query,
    w_key,
    w_value,
    w_out,
    gain_moe,
    w_router,
    w_gate,
    w_up,
    w_down,
):
    gain_one, query_w, key_w, value_w, out_w, gain_two, router_w = (
        lax.all_gather(gain_attn, ("dp", "exp"), axis=0, tiled=True),
        lax.all_gather(w_query, ("dp", "exp"), axis=0, tiled=True),
        lax.all_gather(w_key, ("dp", "exp"), axis=0, tiled=True),
        lax.all_gather(w_value, ("dp", "exp"), axis=0, tiled=True),
        lax.all_gather(w_out, ("dp", "exp"), axis=0, tiled=True),
        lax.all_gather(gain_moe, ("dp", "exp"), axis=0, tiled=True),
        lax.all_gather(w_router, ("dp", "exp"), axis=0, tiled=True),
    )
    gate_w, up_w, down_w = (
        lax.all_gather(w_gate, "dp", axis=1, tiled=True),
        lax.all_gather(w_up, "dp", axis=1, tiled=True),
        lax.all_gather(w_down, "dp", axis=1, tiled=True),
    )
    num_rows = tokens.shape[0]
    width = tokens.shape[1]
    num_heads = query_w.shape[1] // HD
    kv_heads = key_w.shape[1] // HD
    group_size = num_heads // kv_heads
    num_experts = router_w.shape[1]
    top_count = routes.shape[1]
    exp_local = gate_w.shape[0]
    exp_ranks = lax.axis_size("exp")
    capacity = 5 * num_rows * top_count // (4 * num_experts)
    tok_pos = positions(segments)
    allowed = key_mask(segments)
    resid_in = tokens.astype(jnp.float32)
    inv_one = lax.rsqrt(jnp.mean(resid_in * resid_in, axis=-1, keepdims=True) + EPS)
    normed_one = resid_in * inv_one
    hidden_one = (normed_one * gain_one.astype(jnp.float32)).astype(jnp.bfloat16)
    query_raw = jnp.dot(hidden_one, query_w, preferred_element_type=jnp.float32)
    key_raw = jnp.dot(hidden_one, key_w, preferred_element_type=jnp.float32)
    value_b = jnp.dot(hidden_one, value_w, preferred_element_type=jnp.float32).astype(jnp.bfloat16)
    query_b = rotate(query_raw.reshape(num_rows, num_heads, HD), tok_pos, 1.0).astype(jnp.bfloat16)
    query_b = query_b.reshape(num_rows, kv_heads, group_size, HD)
    key_b = rotate(key_raw.reshape(num_rows, kv_heads, HD), tok_pos, 1.0).astype(jnp.bfloat16)
    value_h = value_b.reshape(num_rows, kv_heads, HD)
    logit_att = attention_scores(query_b, key_b, allowed)
    row_max = jnp.max(logit_att, axis=-1, keepdims=True)
    log_total = row_max + jnp.log(jnp.sum(jnp.exp(logit_att - row_max), axis=-1, keepdims=True))
    probs_b = jnp.exp(logit_att - log_total).astype(jnp.bfloat16)
    attn_vals = jnp.einsum("kgqp,pkd->qkgd", probs_b, value_h, preferred_element_type=jnp.float32)
    attn_vals = attn_vals.reshape(num_rows, num_heads * HD).astype(jnp.bfloat16)
    resid_mid = resid_in + jnp.dot(attn_vals, out_w, preferred_element_type=jnp.float32)
    inv_two = lax.rsqrt(jnp.mean(resid_mid * resid_mid, axis=-1, keepdims=True) + EPS)
    normed_two = resid_mid * inv_two
    gain_two_f = gain_two.astype(jnp.float32)
    hidden_two = (normed_two * gain_two_f).astype(jnp.bfloat16)
    router_prob = jax.nn.softmax(
        jnp.dot(hidden_two, router_w, preferred_element_type=jnp.float32), axis=-1
    )
    expert_ids = jnp.arange(num_experts, dtype=jnp.int32)
    route_hot = routes[:, :, None] == expert_ids[None, None, :]
    chosen = jnp.sum(jnp.where(route_hot, router_prob[:, None, :], 0.0), axis=-1)
    weight_sum = jnp.sum(chosen, axis=1, keepdims=True)
    combine = chosen / weight_sum
    flat_hot = route_hot.reshape(num_rows * top_count, num_experts).astype(jnp.int32)
    slot_index = jnp.sum((jnp.cumsum(flat_hot, axis=0) - flat_hot) * flat_hot, axis=1)
    dest_index = routes.reshape(-1) * capacity + slot_index
    send_shape = (exp_ranks, exp_local, capacity, width)
    send_rows = jnp.zeros((num_experts * capacity, width), jnp.bfloat16)
    send_rows = (
        send_rows.at[dest_index].set(jnp.repeat(hidden_two, top_count, axis=0)).reshape(send_shape)
    )
    gate_val, up_val = expert_gates(
        lax.all_to_all(send_rows, "exp", split_axis=0, concat_axis=0, tiled=True), gate_w, up_w
    )
    act_b = (jax.nn.relu(gate_val) * up_val).astype(jnp.bfloat16)
    out_b = jnp.einsum("sacf,afd->sacd", act_b, down_w, preferred_element_type=jnp.float32).astype(
        jnp.bfloat16
    )
    returned = lax.all_to_all(out_b, "exp", split_axis=0, concat_axis=0, tiled=True)
    route_out = returned.reshape(num_experts * capacity, width)[dest_index].reshape(
        num_rows, top_count, width
    )
    route_out_f = route_out.astype(jnp.float32)
    resid_out = resid_mid + jnp.sum(combine[:, :, None] * route_out_f, axis=1)
    layer_out = resid_out.astype(jnp.bfloat16)
    total_rows = num_rows * lax.axis_size(("dp", "exp"))
    global_row = lax.axis_index(("dp", "exp")) * num_rows + jnp.arange(num_rows, dtype=jnp.int32)
    loss_scale = total_rows / valid_count[0].astype(jnp.float32)
    grad_out = jnp.where(
        (global_row < valid_count[0])[:, None],
        (resid_out - targets.astype(jnp.float32)) * loss_scale,
        0.0,
    )
    gain_one, query_w, key_w, value_w, out_w, gain_two, router_w = (
        lax.all_gather(gain_attn, ("dp", "exp"), axis=0, tiled=True),
        lax.all_gather(w_query, ("dp", "exp"), axis=0, tiled=True),
        lax.all_gather(w_key, ("dp", "exp"), axis=0, tiled=True),
        lax.all_gather(w_value, ("dp", "exp"), axis=0, tiled=True),
        lax.all_gather(w_out, ("dp", "exp"), axis=0, tiled=True),
        lax.all_gather(gain_moe, ("dp", "exp"), axis=0, tiled=True),
        lax.all_gather(w_router, ("dp", "exp"), axis=0, tiled=True),
    )
    gain_two_f = gain_two.astype(jnp.float32)
    grad_route = (combine[:, :, None] * grad_out[:, None, :]).astype(jnp.bfloat16)
    grad_comb = jnp.sum(grad_out[:, None, :] * route_out_f, axis=-1)
    grad_send = jnp.zeros((num_experts * capacity, width), jnp.bfloat16)
    grad_send = (
        grad_send.at[dest_index]
        .set(grad_route.reshape(num_rows * top_count, width))
        .reshape(send_shape)
    )
    expert_rows, grad_recv = (
        lax.all_to_all(send_rows, "exp", split_axis=0, concat_axis=0, tiled=True),
        lax.all_to_all(grad_send, "exp", split_axis=0, concat_axis=0, tiled=True),
    )
    gate_val, up_val = expert_gates(expert_rows, gate_w, up_w)
    gate_relu = jax.nn.relu(gate_val)
    act_b = (gate_relu * up_val).astype(jnp.bfloat16)
    grad_act = jnp.einsum("sacd,afd->sacf", grad_recv, down_w, preferred_element_type=jnp.float32)
    grad_down_w = jnp.einsum("sacf,sacd->afd", act_b, grad_recv, preferred_element_type=jnp.float32)
    grad_gate_b = jnp.where(gate_val > 0, grad_act * up_val, 0.0).astype(jnp.bfloat16)
    grad_up_b = (grad_act * gate_relu).astype(jnp.bfloat16)
    grad_gate_w = jnp.einsum(
        "sacd,sacf->adf", expert_rows, grad_gate_b, preferred_element_type=jnp.float32
    )
    grad_up_w = jnp.einsum(
        "sacd,sacf->adf", expert_rows, grad_up_b, preferred_element_type=jnp.float32
    )
    grad_rows = (
        jnp.einsum("sacf,adf->sacd", grad_gate_b, gate_w, preferred_element_type=jnp.float32)
        + jnp.einsum("sacf,adf->sacd", grad_up_b, up_w, preferred_element_type=jnp.float32)
    ).astype(jnp.bfloat16)
    grad_back = lax.all_to_all(grad_rows, "exp", split_axis=0, concat_axis=0, tiled=True)
    grad_copies = grad_back.reshape(num_experts * capacity, width)[dest_index].reshape(
        num_rows, top_count, width
    )
    grad_hidden_two = jnp.sum(grad_copies.astype(jnp.float32), axis=1)
    grad_chosen = (grad_comb - jnp.sum(grad_comb * combine, axis=1, keepdims=True)) / weight_sum
    grad_prob = jnp.sum(jnp.where(route_hot, grad_chosen[:, :, None], 0.0), axis=1)
    grad_logit = router_prob * (
        grad_prob - jnp.sum(router_prob * grad_prob, axis=-1, keepdims=True)
    )
    router_f = router_w.astype(jnp.float32)
    grad_hidden_two = grad_hidden_two + jnp.einsum(
        "re,de->rd", grad_logit, router_f, precision=HIGH
    )
    grad_router = jnp.einsum(
        "rd,re->de", hidden_two.astype(jnp.float32), grad_logit, precision=HIGH
    )
    grad_gain_two = jnp.sum(grad_hidden_two * normed_two, axis=0)
    grad_norm_two = grad_hidden_two * gain_two_f
    grad_mid = grad_out + inv_two * (
        grad_norm_two - normed_two * jnp.mean(grad_norm_two * normed_two, axis=-1, keepdims=True)
    )
    grad_proj_b = grad_mid.astype(jnp.bfloat16)
    grad_out_w = jnp.einsum("rh,rd->hd", attn_vals, grad_proj_b, preferred_element_type=jnp.float32)
    grad_vals_b = jnp.einsum(
        "rd,hd->rh", grad_proj_b, out_w, preferred_element_type=jnp.float32
    ).astype(jnp.bfloat16)
    grad_vals_b = grad_vals_b.reshape(num_rows, kv_heads, group_size, HD)
    logit_att = attention_scores(query_b, key_b, allowed)
    probs = jnp.exp(logit_att - log_total)
    probs_b = probs.astype(jnp.bfloat16)
    grad_value = jnp.einsum(
        "kgqp,qkgd->pkd", probs_b, grad_vals_b, preferred_element_type=jnp.float32
    )
    grad_prob_att = jnp.einsum(
        "qkgd,pkd->kgqp", grad_vals_b, value_h, preferred_element_type=jnp.float32
    )
    delta_row = jnp.sum(probs * grad_prob_att, axis=-1, keepdims=True)
    grad_score_b = (probs * (grad_prob_att - delta_row)).astype(jnp.bfloat16)
    grad_query = jnp.einsum(
        "kgqp,pkd->qkgd", grad_score_b, key_b, preferred_element_type=jnp.float32
    ) * HD ** (-0.5)
    grad_key = jnp.einsum(
        "kgqp,qkgd->pkd", grad_score_b, query_b, preferred_element_type=jnp.float32
    ) * HD ** (-0.5)
    grad_query_b = rotate(grad_query.reshape(num_rows, num_heads, HD), tok_pos, -1.0).astype(
        jnp.bfloat16
    )
    grad_query_b = grad_query_b.reshape(num_rows, num_heads * HD)
    grad_key_b = (
        rotate(grad_key, tok_pos, -1.0).astype(jnp.bfloat16).reshape(num_rows, kv_heads * HD)
    )
    grad_value_b = grad_value.astype(jnp.bfloat16).reshape(num_rows, kv_heads * HD)
    grad_query_w = jnp.einsum(
        "rd,rh->dh", hidden_one, grad_query_b, preferred_element_type=jnp.float32
    )
    grad_key_w = jnp.einsum("rd,rh->dh", hidden_one, grad_key_b, preferred_element_type=jnp.float32)
    grad_value_w = jnp.einsum(
        "rd,rh->dh", hidden_one, grad_value_b, preferred_element_type=jnp.float32
    )
    grad_hidden_one = (
        jnp.einsum("rh,dh->rd", grad_query_b, query_w, preferred_element_type=jnp.float32)
        + jnp.einsum("rh,dh->rd", grad_key_b, key_w, preferred_element_type=jnp.float32)
        + jnp.einsum("rh,dh->rd", grad_value_b, value_w, preferred_element_type=jnp.float32)
    )
    grad_gain_one = jnp.sum(grad_hidden_one * normed_one, axis=0)
    grad_norm_one = grad_hidden_one * gain_one.astype(jnp.float32)
    grad_in = grad_mid + inv_one * (
        grad_norm_one - normed_one * jnp.mean(grad_norm_one * normed_one, axis=-1, keepdims=True)
    )
    dense_sums = (
        lax.psum_scatter(grad_gain_one, ("dp", "exp"), scatter_dimension=0, tiled=True),
        lax.psum_scatter(grad_query_w, ("dp", "exp"), scatter_dimension=0, tiled=True),
        lax.psum_scatter(grad_key_w, ("dp", "exp"), scatter_dimension=0, tiled=True),
        lax.psum_scatter(grad_value_w, ("dp", "exp"), scatter_dimension=0, tiled=True),
        lax.psum_scatter(grad_out_w, ("dp", "exp"), scatter_dimension=0, tiled=True),
        lax.psum_scatter(grad_gain_two, ("dp", "exp"), scatter_dimension=0, tiled=True),
        lax.psum_scatter(grad_router, ("dp", "exp"), scatter_dimension=0, tiled=True),
    )
    expert_sums = (
        lax.psum_scatter(
            grad_gate_w.astype(jnp.bfloat16), "dp", scatter_dimension=1, tiled=True
        ).astype(jnp.float32),
        lax.psum_scatter(
            grad_up_w.astype(jnp.bfloat16), "dp", scatter_dimension=1, tiled=True
        ).astype(jnp.float32),
        lax.psum_scatter(
            grad_down_w.astype(jnp.bfloat16), "dp", scatter_dimension=1, tiled=True
        ).astype(jnp.float32),
    )
    return (
        layer_out,
        grad_in,
        dense_sums[0],
        dense_sums[1],
        dense_sums[2],
        dense_sums[3],
        dense_sums[4],
        dense_sums[5],
        dense_sums[6],
        expert_sums[0],
        expert_sums[1],
        expert_sums[2],
    )


MESH = pl.DeviceIdType.MESH
ANY = pl.BlockSpec(memory_space=pl.ANY)
VMEM = pl.BlockSpec(memory_space=pltpu.VMEM)
VMEM_BYTES = 62 * 2**20


def nn_dot(left, right):
    return jnp.dot(left, right, preferred_element_type=jnp.float32)


def nt_dot(left, right):
    return lax.dot_general(
        left, right, (((1,), (1,)), ((), ())), preferred_element_type=jnp.float32
    )


def tn_dot(left, right):
    return lax.dot_general(
        left, right, (((0,), (0,)), ((), ())), preferred_element_type=jnp.float32
    )


def plane_peers():
    me = lax.axis_index("exp")
    core = lax.rem(me, 2)
    x_pos = lax.rem(lax.div(me, 2), 2)
    y_pos = lax.div(me, 4)
    return me, me + 1 - 2 * core, me + 2 - 4 * x_pos, me + 4 - 8 * y_pos


def remote(src, dst, send_sem, recv_sem, peer):
    return pltpu.make_async_remote_copy(
        src_ref=src,
        dst_ref=dst,
        send_sem=send_sem,
        recv_sem=recv_sem,
        device_id={"exp": peer},
        device_id_type=MESH,
    )


def plane_barrier(peers):
    barrier = pltpu.get_barrier_semaphore()
    for peer in peers:
        pl.semaphore_signal(barrier, inc=1, device_id={"exp": peer}, device_id_type=MESH)
    pl.semaphore_wait(barrier, len(peers))


def step_place(step, quad):
    odd = lax.rem(step, 2)
    last = lax.div(quad, 3)
    mid = lax.rem(lax.div(quad + 1, 2), 2)
    return mid * (1 - odd) + last, mid * odd + last


class Gather:
    def __init__(self, own, buf, send, recv):
        self.own, self.buf, self.send, self.recv = own, buf, send, recv
        self.me, self.sib, self.xn, self.yn = plane_peers()
        self.diag = self.xn + self.yn - self.me

    def own_copy(self, half, peer, sem):
        return remote(
            self.own.at[half],
            self.buf.at[self.me, half],
            self.send.at[sem],
            self.recv.at[self.me, half],
            peer,
        )

    def pass_copy(self, slot, half, peer, sem):
        return remote(
            self.buf.at[slot, half],
            self.buf.at[slot, half],
            self.send.at[sem],
            self.recv.at[slot, half],
            peer,
        )

    def own_copies(self):
        return (
            self.own_copy(0, self.xn, 0),
            self.own_copy(1, self.yn, 1),
            self.own_copy(0, self.sib, 2),
            self.own_copy(1, self.sib, 3),
            self.own_copy(1, self.xn, 4),
            self.own_copy(0, self.yn, 5),
        )

    def near_copies(self):
        return (
            self.pass_copy(self.xn, 0, self.yn, 6),
            self.pass_copy(self.yn, 1, self.xn, 7),
            self.pass_copy(self.xn, 0, self.sib, 8),
            self.pass_copy(self.yn, 1, self.sib, 9),
        )

    def late_copies(self):
        return (
            self.pass_copy(self.xn, 1, self.sib, 10),
            self.pass_copy(self.yn, 0, self.sib, 11),
        )

    def far_copies(self):
        return (
            self.pass_copy(self.diag, 0, self.sib, 12),
            self.pass_copy(self.diag, 1, self.sib, 13),
        )

    def wait_block(self, slot, half):
        self.pass_copy(slot, half, self.sib, 0).wait_recv()

    def begin(self):
        plane_barrier((self.sib, self.xn, self.yn))
        for copy in self.own_copies():
            copy.start()

    def place(self, step):
        quad = lax.div(step, 4)
        far_x, far_y = step_place(step, quad)
        odd = lax.rem(step, 2)
        third = lax.div(quad, 2) * (1 - lax.div(quad, 3))
        other = lax.div(lax.rem(step, 4), 2)
        slot = (
            self.me
            + far_x * (self.xn - self.me)
            + far_y * (self.yn - self.me)
            + other * (self.sib - self.me)
        )
        return slot, odd + third * (1 - 2 * odd), other

    def arrive(self, step):
        @pl.when(step == 4)
        def _():
            self.wait_block(self.xn, 0)
            self.wait_block(self.yn, 1)
            for copy in self.near_copies():
                copy.start()

        @pl.when(step == 8)
        def _():
            self.wait_block(self.xn, 1)
            self.wait_block(self.yn, 0)
            for copy in self.late_copies():
                copy.start()

        @pl.when(step == 12)
        def _():
            self.wait_block(self.diag, 0)
            self.wait_block(self.diag, 1)
            for copy in self.far_copies():
                copy.start()

        slot, half, other = self.place(step)

        @pl.when(other == 1)
        def _():
            self.wait_block(slot, half)

        return slot, half

    def finish(self):
        for copies in (self.own_copies(), self.near_copies(), self.late_copies(), self.far_copies()):
            for copy in copies:
                copy.wait_send()


def expert_in_kernel(own, gate_hbm, up_hbm, rows_out, gua_out, buf, gua, gate_w, up_w, send, recv, load, store_a, store_b):
    width, hidden = gate_w.shape
    gather = Gather(own, buf, send, recv)
    loads = (
        pltpu.make_async_copy(gate_hbm, gate_w, load.at[0]),
        pltpu.make_async_copy(up_hbm, up_w, load.at[1]),
        pltpu.make_async_copy(own.at[0], buf.at[gather.me, 0], load.at[2]),
        pltpu.make_async_copy(own.at[1], buf.at[gather.me, 1], load.at[3]),
    )
    for copy in loads:
        copy.start()
    gather.begin()
    for copy in loads:
        copy.wait()

    def row_store(slot, half, step):
        return pltpu.make_async_copy(buf.at[slot, half], rows_out.at[slot, half], store_a.at[step])

    def gua_store(slot, half, step):
        return pltpu.make_async_copy(gua.at[slot, half], gua_out.at[slot, half], store_b.at[step])

    def one(step, carry):
        slot, half = gather.arrive(step)
        row_store(slot, half, step).start()
        rows = buf[slot, half, :, :width]
        lanes = lax.broadcasted_iota(jnp.int32, (buf.shape[2], 128), 1)
        tail = buf[slot, half, :, width:].astype(jnp.float32)
        weight = jnp.sum(jnp.where(lanes == gather.me, tail, 0.0), axis=1, keepdims=True)
        gate_val = nn_dot(rows, gate_w[...])
        up_val = nn_dot(rows, up_w[...])
        gua[slot, half, :, :hidden] = gate_val.astype(jnp.bfloat16)
        gua[slot, half, :, hidden : 2 * hidden] = up_val.astype(jnp.bfloat16)
        act_val = jnp.maximum(gate_val, 0.0) * up_val * weight
        gua[slot, half, :, 2 * hidden :] = act_val.astype(jnp.bfloat16)
        gua_store(slot, half, step).start()
        return carry

    lax.fori_loop(0, 16, one, 0)
    gather.finish()

    def drain(step, carry):
        slot, half, _ = gather.place(step)
        row_store(slot, half, step).wait()
        gua_store(slot, half, step).wait()
        return carry

    lax.fori_loop(0, 16, drain, 0)


def expert_in(own, gate_w, up_w):
    _, half, columns = own.shape
    width, hidden = gate_w.shape
    bf = jnp.bfloat16
    return pl.pallas_call(
        expert_in_kernel,
        out_shape=(
            jax.ShapeDtypeStruct((8, 2, half, columns), bf),
            jax.ShapeDtypeStruct((8, 2, half, 3 * hidden), bf),
        ),
        in_specs=[ANY] * 3,
        out_specs=(ANY, ANY),
        scratch_shapes=[
            pltpu.VMEM((8, 2, half, columns), bf),
            pltpu.VMEM((8, 2, half, 3 * hidden), bf),
            pltpu.VMEM((width, hidden), bf),
            pltpu.VMEM((width, hidden), bf),
            pltpu.SemaphoreType.DMA((14,)),
            pltpu.SemaphoreType.DMA((8, 2)),
            pltpu.SemaphoreType.DMA((4,)),
            pltpu.SemaphoreType.DMA((16,)),
            pltpu.SemaphoreType.DMA((16,)),
        ],
        compiler_params=pltpu.CompilerParams(
            collective_id=1, has_side_effects=True, vmem_limit_bytes=VMEM_BYTES
        ),
        name="expert_in",
    )(own, gate_w, up_w)


def row_chunk(rows):
    return 64 if rows % 64 == 0 else 16


def add_rows(target, others):
    parts, rows_all, _ = target.shape
    chunk = row_chunk(rows_all)
    for part in range(parts):

        def one(index, carry):
            rows = pl.ds(pl.multiple_of(index * chunk, chunk), chunk)
            total = target[part, rows, :].astype(jnp.float32)
            for other in others:
                total = total + other[part, rows, :].astype(jnp.float32)
            target[part, rows, :] = total.astype(target.dtype)
            return carry

        lax.fori_loop(0, rows_all // chunk, one, 0)


class Scatter:
    def __init__(self, theirs, scratch):
        self.theirs = theirs
        self.mine, self.side, self.relay, self.final = scratch[:4]
        self.send, self.side_sem, self.relay_sem, self.final_sem = scratch[4:]
        self.me, self.sib, self.xn, self.yn = plane_peers()

    def peers(self):
        return self.sib, self.xn, self.yn

    def place(self, step):
        quad = lax.div(step, 4)
        far_x, far_y = step_place(step, 3 - quad)
        odd = lax.rem(step, 2)
        third = lax.div(quad, 2) * (1 - lax.div(quad, 3))
        other = 1 - lax.div(lax.rem(step, 4), 2)
        slot = (
            self.me
            + far_x * (self.xn - self.me)
            + far_y * (self.yn - self.me)
            + other * (self.sib - self.me)
        )
        return slot, odd + third * (1 - 2 * odd), other, far_x + 2 * far_y

    def side_copy(self, step):
        slot, half, _, place = self.place(step)
        return remote(
            self.theirs(place, slot, half),
            self.side.at[place, half],
            self.send.at[step],
            self.side_sem.at[place, half],
            self.sib,
        )

    def side_wait(self, place, half):
        remote(
            self.side.at[place, half],
            self.side.at[place, half],
            self.send.at[0],
            self.side_sem.at[place, half],
            self.sib,
        ).wait_recv()

    def relay_copy(self, step, way):
        return remote(
            self.mine.at[3, way],
            self.relay.at[way],
            self.send.at[step],
            self.relay_sem.at[way],
            (self.xn, self.yn)[way],
        )

    def final_copy(self, step, way, half):
        return remote(
            self.mine.at[1 + way, half],
            self.final.at[way, half],
            self.send.at[step],
            self.final_sem.at[way, half],
            (self.xn, self.yn)[way],
        )

    def depart(self, step):
        @pl.when(self.place(step)[2] == 1)
        def _():
            self.side_copy(step).start()

        for way in (0, 1):

            @pl.when(step == 2 + way)
            def _():
                self.side_wait(3, way)
                add_rows(self.mine.at[3, way], (self.side.at[3, way],))
                self.relay_copy(2 + way, way).start()

            @pl.when(step == 6 + way)
            def _():
                self.side_wait(1 + way, way)
                add_rows(self.mine.at[1 + way, way], (self.side.at[1 + way, way],))
                self.final_copy(6 + way, way, way).start()

    def forward(self):
        for way in (0, 1):
            self.side_wait(1 + way, 1 - way)
            self.relay_copy(3 - way, 1 - way).wait_recv()
            add_rows(
                self.mine.at[1 + way, 1 - way],
                (self.side.at[1 + way, 1 - way], self.relay.at[1 - way]),
            )
            self.final_copy(10 + way, way, 1 - way).start()

    def finish(self, write):
        parts, rows_all = self.mine.shape[2:4]
        chunk = row_chunk(rows_all)
        for half in (0, 1):
            self.side_wait(0, half)
            self.final_copy(0, 0, half).wait_recv()
            self.final_copy(0, 1, half).wait_recv()
            for part in range(parts):

                def one(index, carry):
                    rows = pl.ds(pl.multiple_of(index * chunk, chunk), chunk)
                    total = self.mine[0, half, part, rows, :].astype(jnp.float32)
                    total = total + self.side[0, half, part, rows, :].astype(jnp.float32)
                    total = total + self.final[0, half, part, rows, :].astype(jnp.float32)
                    total = total + self.final[1, half, part, rows, :].astype(jnp.float32)
                    write(half, part, rows, total)
                    return carry

                lax.fori_loop(0, rows_all // chunk, one, 0)

    def drain(self):
        for way in (0, 1):
            self.relay_copy(2 + way, way).wait_send()
            self.final_copy(6 + way, way, way).wait_send()
            self.final_copy(10 + way, way, 1 - way).wait_send()

        def one(step, carry):
            @pl.when(self.place(step)[2] == 1)
            def _():
                self.side_copy(step).wait_send()

            return carry

        lax.fori_loop(0, 16, one, 0)


SCATTER_REFS = 8


def scatter_scratch(parts, rows, columns):
    bf = jnp.bfloat16
    return [
        pltpu.VMEM((4, 2, parts, rows, columns), bf),
        pltpu.VMEM((4, 2, parts, rows, columns), bf),
        pltpu.VMEM((2, parts, rows, columns), bf),
        pltpu.VMEM((2, 2, parts, rows, columns), bf),
        pltpu.SemaphoreType.DMA((16,)),
        pltpu.SemaphoreType.DMA((4, 2)),
        pltpu.SemaphoreType.DMA((2,)),
        pltpu.SemaphoreType.DMA((2, 2)),
    ]


def expert_out_kernel(gua_hbm, down_hbm, out, act, down_w, away, load, *scratch):
    hidden = down_w.shape[0]
    scatter = Scatter(lambda place, slot, half: away.at[place, half], scratch)
    mine = scatter.mine
    down_load = pltpu.make_async_copy(down_hbm, down_w, load.at[16])
    down_load.start()

    def act_load(step):
        slot, half, _, _ = scatter.place(step)
        return pltpu.make_async_copy(
            gua_hbm.at[slot, half, :, pl.ds(2 * hidden, hidden)], act.at[slot, half], load.at[step]
        )

    def fetch(step, carry):
        act_load(step).start()
        return carry

    lax.fori_loop(0, 16, fetch, 0)
    plane_barrier(scatter.peers())
    down_load.wait()

    def one(step, carry):
        slot, half, other, place = scatter.place(step)
        act_load(step).wait()
        partial = nn_dot(act[slot, half], down_w[...]).astype(jnp.bfloat16)

        @pl.when(other == 1)
        def _():
            away[place, half, 0] = partial

        @pl.when(other == 0)
        def _():
            mine[place, half, 0] = partial

        scatter.depart(step)
        return carry

    lax.fori_loop(0, 16, one, 0)
    scatter.forward()

    def write(half, part, rows, total):
        out[half, rows, :] = total

    scatter.finish(write)
    scatter.drain()


def expert_out(gua, down_w):
    half = gua.shape[2]
    hidden, width = down_w.shape
    return pl.pallas_call(
        expert_out_kernel,
        out_shape=jax.ShapeDtypeStruct((2, half, width), jnp.float32),
        in_specs=[ANY] * 2,
        out_specs=VMEM,
        scratch_shapes=[
            pltpu.VMEM((8, 2, half, hidden), jnp.bfloat16),
            pltpu.VMEM((hidden, width), jnp.bfloat16),
            pltpu.VMEM((4, 2, 1, half, width), jnp.bfloat16),
            pltpu.SemaphoreType.DMA((17,)),
        ]
        + scatter_scratch(1, half, width),
        compiler_params=pltpu.CompilerParams(
            collective_id=2, has_side_effects=True, vmem_limit_bytes=VMEM_BYTES
        ),
        name="expert_out",
    )(gua, down_w)


def expert_back_kernel(own, rows_hbm, gua_hbm, gate_hbm, up_hbm, down_hbm, grads_out, dgu_out, part_out, buf, gu, tails, part, gate_w, up_w, down_w, send, recv, load, load_gu, load_tail, store_a, store_b, store_c):
    width, hidden = gate_w.shape
    gather = Gather(own, buf, send, recv)
    loads = (
        pltpu.make_async_copy(down_hbm, down_w, load.at[0]),
        pltpu.make_async_copy(own.at[0], buf.at[gather.me, 0], load.at[1]),
        pltpu.make_async_copy(own.at[1], buf.at[gather.me, 1], load.at[2]),
        pltpu.make_async_copy(gate_hbm, gate_w, load.at[3]),
        pltpu.make_async_copy(up_hbm, up_w, load.at[4]),
    )
    for copy in loads:
        copy.start()

    def block_loads(step):
        slot, half, _ = gather.place(step)
        return (
            pltpu.make_async_copy(
                gua_hbm.at[slot, half, :, pl.ds(0, 2 * hidden)], gu.at[slot, half], load_gu.at[step]
            ),
            pltpu.make_async_copy(
                rows_hbm.at[slot, half, :, pl.ds(width, 128)], tails.at[slot, half], load_tail.at[step]
            ),
        )

    def fetch(step, carry):
        for copy in block_loads(step):
            copy.start()
        return carry

    lax.fori_loop(0, 16, fetch, 0)
    gather.begin()
    for copy in loads:
        copy.wait()

    def stores(step):
        slot, half, _ = gather.place(step)
        return (
            pltpu.make_async_copy(buf.at[slot, half], grads_out.at[slot, half], store_a.at[step]),
            pltpu.make_async_copy(gu.at[slot, half], dgu_out.at[slot, half], store_b.at[step]),
            pltpu.make_async_copy(part.at[slot, half], part_out.at[slot, half], store_c.at[step]),
        )

    def one(step, carry):
        slot, half = gather.arrive(step)
        store_rows, store_dgu, store_part = stores(step)
        store_rows.start()
        for copy in block_loads(step):
            copy.wait()
        lanes = lax.broadcasted_iota(jnp.int32, (buf.shape[2], 128), 1)
        tail = tails[slot, half].astype(jnp.float32)
        weight = jnp.sum(jnp.where(lanes == gather.me, tail, 0.0), axis=1, keepdims=True)
        grad_act = nt_dot(buf[slot, half], down_w[...])
        gate_val = gu[slot, half, :, :hidden].astype(jnp.float32)
        up_val = gu[slot, half, :, hidden:].astype(jnp.float32)
        gate_relu = jnp.maximum(gate_val, 0.0)
        grad_comb = jnp.sum(gate_relu * up_val * grad_act, axis=1, keepdims=True)
        grad_act = grad_act * weight
        grad_gate = jnp.where(gate_val > 0, grad_act * up_val, 0.0).astype(jnp.bfloat16)
        grad_up = (grad_act * gate_relu).astype(jnp.bfloat16)
        gu[slot, half, :, :hidden] = grad_gate
        gu[slot, half, :, hidden:] = grad_up
        store_dgu.start()
        part[slot, half, :, :width] = (
            nt_dot(grad_gate, gate_w[...]) + nt_dot(grad_up, up_w[...])
        ).astype(jnp.bfloat16)
        part[slot, half, :, width:] = jnp.where(lanes == gather.me, grad_comb, 0.0).astype(
            jnp.bfloat16
        )
        store_part.start()
        return carry

    lax.fori_loop(0, 16, one, 0)
    gather.finish()

    def drain(step, carry):
        for copy in stores(step):
            copy.wait()
        return carry

    lax.fori_loop(0, 16, drain, 0)


def expert_back(own, rows_all, gua, gate_w, up_w, down_w):
    _, half, columns = rows_all.shape[1:]
    width, hidden = gate_w.shape
    bf = jnp.bfloat16
    return pl.pallas_call(
        expert_back_kernel,
        out_shape=(
            jax.ShapeDtypeStruct((8, 2, half, width), bf),
            jax.ShapeDtypeStruct((8, 2, half, 2 * hidden), bf),
            jax.ShapeDtypeStruct((8, 2, half, columns), bf),
        ),
        in_specs=[ANY] * 6,
        out_specs=(ANY,) * 3,
        scratch_shapes=[
            pltpu.VMEM((8, 2, half, width), bf),
            pltpu.VMEM((8, 2, half, 2 * hidden), bf),
            pltpu.VMEM((8, 2, half, 128), bf),
            pltpu.VMEM((8, 2, half, columns), bf),
            pltpu.VMEM((width, hidden), bf),
            pltpu.VMEM((width, hidden), bf),
            pltpu.VMEM((hidden, width), bf),
            pltpu.SemaphoreType.DMA((14,)),
            pltpu.SemaphoreType.DMA((8, 2)),
            pltpu.SemaphoreType.DMA((5,)),
        ]
        + [pltpu.SemaphoreType.DMA((16,))] * 5,
        compiler_params=pltpu.CompilerParams(
            collective_id=3, has_side_effects=True, vmem_limit_bytes=VMEM_BYTES
        ),
        name="expert_back",
    )(own, rows_all, gua, gate_w, up_w, down_w)


def expert_grads_kernel(part_hbm, rows_hbm, dgu_hbm, gua_hbm, grads_hbm, out, gate_out, up_out, down_out, rows, dgu, act, grads, gate_up_acc, down_acc, load, block_load, *scratch):
    hidden, width = down_acc.shape
    scatter = Scatter(lambda place, slot, half: part_hbm.at[slot, half], scratch)

    def part_load(step):
        slot, half, _, place = scatter.place(step)
        return pltpu.make_async_copy(
            part_hbm.at[slot, half], scatter.mine.at[place, half], load.at[step]
        )

    def fetch(step, carry):
        @pl.when(scatter.place(step)[2] == 0)
        def _():
            part_load(step).start()

        return carry

    def block_copies(block):
        slot = lax.rem(block, 2)
        return (
            pltpu.make_async_copy(
                rows_hbm.at[block, :, :, pl.ds(0, width)], rows.at[slot], block_load.at[slot, 0]
            ),
            pltpu.make_async_copy(dgu_hbm.at[block], dgu.at[slot], block_load.at[slot, 1]),
            pltpu.make_async_copy(
                gua_hbm.at[block, :, :, pl.ds(2 * hidden, hidden)], act.at[slot], block_load.at[slot, 2]
            ),
            pltpu.make_async_copy(grads_hbm.at[block], grads.at[slot], block_load.at[slot, 3]),
        )

    lax.fori_loop(0, 16, fetch, 0)
    plane_barrier(scatter.peers())

    def one(step, carry):
        @pl.when(scatter.place(step)[2] == 0)
        def _():
            part_load(step).wait()

        scatter.depart(step)
        return carry

    lax.fori_loop(0, 16, one, 0)
    for copy in block_copies(0):
        copy.start()
    tile = 256

    def accumulate(block, carry):
        for copy in block_copies(block):
            copy.wait()

        @pl.when(block < 7)
        def _():
            for copy in block_copies(block + 1):
                copy.start()

        slot = lax.rem(block, 2)

        def add_tile(acc, left, right, index):
            cols = pl.ds(pl.multiple_of(index * tile, tile), tile)
            total = tn_dot(
                left[slot, :, :, cols].reshape(-1, tile), right[slot].reshape(-1, width)
            )

            @pl.when(block == 0)
            def _():
                acc[cols, :] = total

            @pl.when(block > 0)
            def _():
                acc[cols, :] = acc[cols, :] + total

        def gate_up_tile(index, carry):
            add_tile(gate_up_acc, rows, dgu, index)
            return carry

        def down_tile(index, carry):
            add_tile(down_acc, act, grads, index)
            return carry

        lax.fori_loop(0, width // tile, gate_up_tile, 0)
        lax.fori_loop(0, hidden // tile, down_tile, 0)
        return carry

    def blocks(index, carry):
        @pl.when(index == 3)
        def _():
            scatter.forward()

        return accumulate(index, carry)

    lax.fori_loop(0, 8, blocks, 0)

    def round_tile(index, carry):
        cols = pl.ds(pl.multiple_of(index * 64, 64), 64)
        gate_out[cols, :] = gate_up_acc[cols, :hidden].astype(jnp.bfloat16)
        up_out[cols, :] = gate_up_acc[cols, hidden:].astype(jnp.bfloat16)
        return carry

    lax.fori_loop(0, width // 64, round_tile, 0)

    def round_down(index, carry):
        cols = pl.ds(pl.multiple_of(index * 64, 64), 64)
        down_out[cols, :] = down_acc[cols, :].astype(jnp.bfloat16)
        return carry

    lax.fori_loop(0, hidden // 64, round_down, 0)

    def write(half, part, rows, total):
        out[half, rows, :] = total

    scatter.finish(write)
    scatter.drain()


def expert_grads(part, rows_all, dgu, gua, grads_all):
    _, _, half, columns = part.shape
    width = grads_all.shape[3]
    hidden = dgu.shape[3] // 2
    bf = jnp.bfloat16
    return pl.pallas_call(
        expert_grads_kernel,
        out_shape=(
            jax.ShapeDtypeStruct((2, half, columns), jnp.float32),
            jax.ShapeDtypeStruct((width, hidden), bf),
            jax.ShapeDtypeStruct((width, hidden), bf),
            jax.ShapeDtypeStruct((hidden, width), bf),
        ),
        in_specs=[ANY] * 5,
        out_specs=(VMEM,) * 4,
        scratch_shapes=[
            pltpu.VMEM((2, 2, half, width), bf),
            pltpu.VMEM((2, 2, half, 2 * hidden), bf),
            pltpu.VMEM((2, 2, half, hidden), bf),
            pltpu.VMEM((2, 2, half, width), bf),
            pltpu.VMEM((width, 2 * hidden), jnp.float32),
            pltpu.VMEM((hidden, width), jnp.float32),
            pltpu.SemaphoreType.DMA((16,)),
            pltpu.SemaphoreType.DMA((2, 4)),
        ]
        + scatter_scratch(1, half, columns),
        compiler_params=pltpu.CompilerParams(
            collective_id=4, has_side_effects=True, vmem_limit_bytes=VMEM_BYTES
        ),
        name="expert_grads",
    )(part.reshape(8, 2, 1, half, columns), rows_all, dgu, gua, grads_all)


def line_peers():
    line = lax.axis_index("dp")
    return (
        line,
        line + 1 - 2 * lax.rem(line, 2),
        line + 2 - 4 * lax.div(line, 2),
        3 - line,
    )


def line_remote(src, dst, send_sem, recv_sem, peer):
    return pltpu.make_async_remote_copy(
        src_ref=src,
        dst_ref=dst,
        send_sem=send_sem,
        recv_sem=recv_sem,
        device_id={"dp": peer},
        device_id_type=MESH,
    )


def full_barrier(plane, line):
    barrier = pltpu.get_barrier_semaphore()
    for peer in plane:
        pl.semaphore_signal(barrier, inc=1, device_id={"exp": peer}, device_id_type=MESH)
    for peer in line:
        pl.semaphore_signal(barrier, inc=1, device_id={"dp": peer}, device_id_type=MESH)
    pl.semaphore_wait(barrier, len(plane) + len(line))


def dense_gather_kernel(own, everything, stage, send, recv, local):
    me, sib, xn, yn = plane_peers()
    diag = xn + yn - me
    line = line_peers()
    into = pltpu.make_async_copy(own, stage, local.at[0])
    into.start()
    full_barrier((sib, xn, yn), line[1:])
    started = []

    def put(src, slot, turn, peer):
        copy = remote(
            src, everything.at[line[turn], slot], send.at[len(started)], recv.at[line[turn], slot], peer
        )
        copy.start()
        started.append(copy)

    def pass_on(slot, turn, peer):
        put(everything.at[line[turn], slot], slot, turn, peer)

    def wait(slot, turn):
        ref = everything.at[line[turn], slot]
        remote(ref, ref, send.at[0], recv.at[line[turn], slot], sib).wait_recv()

    put(own, me, 0, xn)
    put(own, me, 0, yn)
    for turn in (1, 2, 3):
        copy = line_remote(
            own, everything.at[line[0], me], send.at[len(started)], recv.at[line[0], me], line[turn]
        )
        copy.start()
        started.append(copy)
    put(own, me, 0, sib)
    into.wait()
    out = pltpu.make_async_copy(stage, everything.at[line[0], me], local.at[1])
    out.start()
    for turn in (0, 1, 2, 3):
        if turn > 0:
            wait(me, turn)
            for peer in (xn, yn, sib):
                pass_on(me, turn, peer)
        wait(xn, turn)
        if turn % 2 == 0:
            pass_on(xn, turn, yn)
        pass_on(xn, turn, sib)
        wait(yn, turn)
        if turn % 2 == 1:
            pass_on(yn, turn, xn)
        pass_on(yn, turn, sib)
        if turn > 0:
            wait(diag, turn - 1)
            pass_on(diag, turn - 1, sib)
    wait(diag, 3)
    pass_on(diag, 3, sib)
    for turn in (0, 1, 2, 3):
        for slot in (sib, xn + sib - me, yn + sib - me, diag + sib - me):
            wait(slot, turn)
    out.wait()
    for copy in started:
        copy.wait_send()


def dense_gather(own):
    rows, columns = own.shape
    return pl.pallas_call(
        dense_gather_kernel,
        out_shape=jax.ShapeDtypeStruct((4, 8, rows, columns), own.dtype),
        in_specs=[ANY],
        out_specs=ANY,
        scratch_shapes=[
            pltpu.VMEM((rows, columns), own.dtype),
            pltpu.SemaphoreType.DMA((32,)),
            pltpu.SemaphoreType.DMA((4, 8)),
            pltpu.SemaphoreType.DMA((2,)),
        ],
        compiler_params=pltpu.CompilerParams(
            collective_id=5, has_side_effects=True, vmem_limit_bytes=48 * 2**20
        ),
        name="dense_gather",
    )(own).reshape(32 * rows, columns)


class LineScatter:
    def __init__(self, scratch):
        self.sums, self.other, self.send, self.recv = scratch
        self.line = line_peers()

    def copy(self, turn):
        target = self.line[turn]
        return line_remote(
            self.sums.at[target],
            self.other.at[turn - 1],
            self.send.at[turn - 1],
            self.recv.at[turn - 1],
            target,
        )

    def write(self, half, part, rows, total):
        self.sums[2 * half + part, rows, :] = total.astype(self.sums.dtype)

    def begin(self):
        for turn in (1, 2, 3):
            self.copy(turn).start()

    def finish(self, out, first):
        rows_all, columns = out.shape[0], self.sums.shape[2]
        for turn in (1, 2, 3):
            self.copy(turn).wait_recv()

        def one(index, carry):
            rows = pl.ds(pl.multiple_of(index * 16, 16), 16)
            total = self.sums[self.line[0], rows, :].astype(jnp.float32)
            for turn in (0, 1, 2):
                total = total + self.other[turn, rows, :].astype(jnp.float32)
            out[rows, pl.ds(first, columns)] = total
            return carry

        lax.fori_loop(0, rows_all // 16, one, 0)
        for turn in (1, 2, 3):
            self.copy(turn).wait_send()


LINE_REFS = 4


def line_scratch(rows, columns):
    bf = jnp.bfloat16
    return [
        pltpu.VMEM((4, rows, columns), bf),
        pltpu.VMEM((3, rows, columns), bf),
        pltpu.SemaphoreType.DMA((3,)),
        pltpu.SemaphoreType.DMA((3,)),
    ]


def dense_scatter_kernel(groups, *refs):
    parts, out, refs = refs[:groups], refs[groups], refs[groups + 1 :]
    step_refs = 1 + SCATTER_REFS + LINE_REFS
    loads, planes, lines = [], [], []
    for index, part in enumerate(parts):
        some = refs[index * step_refs : (index + 1) * step_refs]
        plane = Scatter(
            lambda place, slot, half, part=part: part.at[half, :, slot], some[1 : 1 + SCATTER_REFS]
        )

        def load(step, part=part, plane=plane, sem=some[0]):
            slot, half, _, place = plane.place(step)
            return pltpu.make_async_copy(
                part.at[half, :, slot], plane.mine.at[place, half], sem.at[step]
            )

        loads.append(load)
        planes.append(plane)
        lines.append(LineScatter(some[1 + SCATTER_REFS :]))

    for plane, load in zip(planes, loads):

        def fetch(step, carry, plane=plane, load=load):
            @pl.when(plane.place(step)[2] == 0)
            def _():
                load(step).start()

            return carry

        lax.fori_loop(0, 16, fetch, 0)
    full_barrier(planes[0].peers(), lines[0].line[1:])
    for plane, load in zip(planes, loads):

        def one(step, carry, plane=plane, load=load):
            @pl.when(plane.place(step)[2] == 0)
            def _():
                load(step).wait()

            plane.depart(step)
            return carry

        lax.fori_loop(0, 16, one, 0)
    for plane in planes:
        plane.forward()
    for plane, line in zip(planes, lines):
        plane.finish(line.write)
        line.begin()
    first = 0
    for plane, line in zip(planes, lines):
        line.finish(out, first)
        first += line.sums.shape[2]
        plane.drain()


def dense_scatter(parts):
    rows = parts[0].shape[0] // 32
    scratch = []
    for part in parts:
        scratch += [pltpu.SemaphoreType.DMA((16,))]
        scratch += scatter_scratch(2, rows, part.shape[1]) + line_scratch(rows, part.shape[1])
    columns = sum(part.shape[1] for part in parts)
    return pl.pallas_call(
        functools.partial(dense_scatter_kernel, len(parts)),
        out_shape=jax.ShapeDtypeStruct((rows, columns), jnp.float32),
        in_specs=[ANY] * len(parts),
        out_specs=VMEM,
        scratch_shapes=scratch,
        compiler_params=pltpu.CompilerParams(
            collective_id=6, has_side_effects=True, vmem_limit_bytes=VMEM_BYTES
        ),
        name="dense_scatter",
    )(*(part.reshape(2, 2, 8, rows, part.shape[1]) for part in parts))


def body_plane(
    tokens,
    targets,
    valid_count,
    segments,
    routes,
    gain_attn,
    w_query,
    w_key,
    w_value,
    w_out,
    gain_moe,
    w_router,
    w_gate,
    w_up,
    w_down,
):
    bf = jnp.bfloat16
    num_rows, width = tokens.shape
    half = num_rows // 2
    q_cols, k_cols = w_query.shape[1], w_key.shape[1]
    qkv_cols = q_cols + 2 * k_cols
    dense_cols = qkv_cols + w_out.shape[1]
    num_experts = w_router.shape[1]
    num_heads = q_cols // HD
    kv_heads = k_cols // HD
    group_size = num_heads // kv_heads
    pad_cols = 128 - 2 - num_experts
    dense_own = jnp.concatenate(
        [
            w_query,
            w_key,
            w_value,
            w_out,
            gain_attn[:, None],
            gain_moe[:, None],
            w_router,
            jnp.zeros((gain_attn.shape[0], pad_cols), bf),
        ],
        axis=1,
    )
    dense_w = dense_gather(dense_own)
    gate_w = lax.all_gather(w_gate, "dp", axis=1, tiled=True)[0]
    up_w = lax.all_gather(w_up, "dp", axis=1, tiled=True)[0]
    down_w = lax.all_gather(w_down, "dp", axis=1, tiled=True)[0]
    qkv_w = dense_w[:, :qkv_cols]
    out_w = dense_w[:, qkv_cols:dense_cols]
    gain_one = dense_w[:, dense_cols].astype(jnp.float32)
    gain_two = dense_w[:, dense_cols + 1].astype(jnp.float32)
    router_w = dense_w[:, dense_cols + 2 : dense_cols + 2 + num_experts]
    tok_pos = positions(segments)
    allowed = key_mask(segments)
    resid_in = tokens.astype(jnp.float32)
    inv_one = lax.rsqrt(jnp.mean(resid_in * resid_in, axis=-1, keepdims=True) + EPS)
    normed_one = resid_in * inv_one
    hidden_one = (normed_one * gain_one).astype(bf)
    qkv_raw = jnp.dot(hidden_one, qkv_w, preferred_element_type=jnp.float32)
    value_b = qkv_raw[:, q_cols + k_cols :].astype(bf)
    query_b = rotate(qkv_raw[:, :q_cols].reshape(num_rows, num_heads, HD), tok_pos, 1.0).astype(bf)
    query_b = query_b.reshape(num_rows, kv_heads, group_size, HD)
    key_b = rotate(
        qkv_raw[:, q_cols : q_cols + k_cols].reshape(num_rows, kv_heads, HD), tok_pos, 1.0
    ).astype(bf)
    value_h = value_b.reshape(num_rows, kv_heads, HD)
    logit_att = attention_scores(query_b, key_b, allowed)
    row_max = jnp.max(logit_att, axis=-1, keepdims=True)
    log_total = row_max + jnp.log(jnp.sum(jnp.exp(logit_att - row_max), axis=-1, keepdims=True))
    probs_b = jnp.exp(logit_att - log_total).astype(bf)
    attn_vals = jnp.einsum("kgqp,pkd->qkgd", probs_b, value_h, preferred_element_type=jnp.float32)
    attn_vals = attn_vals.reshape(num_rows, q_cols).astype(bf)
    resid_mid = resid_in + jnp.dot(attn_vals, out_w, preferred_element_type=jnp.float32)
    inv_two = lax.rsqrt(jnp.mean(resid_mid * resid_mid, axis=-1, keepdims=True) + EPS)
    normed_two = resid_mid * inv_two
    hidden_two = (normed_two * gain_two).astype(bf)
    router_prob = jax.nn.softmax(
        jnp.dot(hidden_two, router_w, preferred_element_type=jnp.float32), axis=-1
    )
    expert_ids = jnp.arange(num_experts, dtype=jnp.int32)
    route_hot = routes[:, :, None] == expert_ids[None, None, :]
    chosen = jnp.sum(jnp.where(route_hot, router_prob[:, None, :], 0.0), axis=-1)
    weight_sum = jnp.sum(chosen, axis=1, keepdims=True)
    combine = chosen / weight_sum
    weight_full = jnp.sum(jnp.where(route_hot, combine[:, :, None], 0.0), axis=1)
    rows_own = jnp.concatenate(
        [hidden_two, jnp.pad(weight_full.astype(bf), ((0, 0), (0, 128 - num_experts)))], axis=1
    )
    rows_all, gua = expert_in(rows_own.reshape(2, half, width + 128), gate_w, up_w)
    moe_out = expert_out(gua, down_w).reshape(num_rows, width)
    resid_out = resid_mid + moe_out
    layer_out = resid_out.astype(bf)
    total_rows = num_rows * lax.axis_size(("dp", "exp"))
    global_row = lax.axis_index(("dp", "exp")) * num_rows + jnp.arange(num_rows, dtype=jnp.int32)
    loss_scale = total_rows / valid_count[0].astype(jnp.float32)
    grad_out = jnp.where(
        (global_row < valid_count[0])[:, None],
        (resid_out - targets.astype(jnp.float32)) * loss_scale,
        0.0,
    )
    grads_all, dgu, part = expert_back(
        grad_out.astype(bf).reshape(2, half, width), rows_all, gua, gate_w, up_w, down_w
    )
    back, *expert_parts = expert_grads(part, rows_all, dgu, gua, grads_all)
    back = back.reshape(num_rows, width + 128)
    expert_sums = tuple(
        lax.psum_scatter(grad[None], "dp", scatter_dimension=1, tiled=True).astype(jnp.float32)
        for grad in expert_parts
    )
    grad_hidden_two = back[:, :width]
    grad_comb = jnp.sum(
        jnp.where(route_hot, back[:, None, width : width + num_experts], 0.0), axis=-1
    )
    grad_chosen = (grad_comb - jnp.sum(grad_comb * combine, axis=1, keepdims=True)) / weight_sum
    grad_prob = jnp.sum(jnp.where(route_hot, grad_chosen[:, :, None], 0.0), axis=1)
    grad_logit = router_prob * (
        grad_prob - jnp.sum(router_prob * grad_prob, axis=-1, keepdims=True)
    )
    grad_hidden_two = grad_hidden_two + jnp.einsum(
        "re,de->rd", grad_logit, router_w.astype(jnp.float32), precision=HIGH
    )
    grad_router = jnp.einsum(
        "rd,re->de", hidden_two.astype(jnp.float32), grad_logit, precision=HIGH
    )
    grad_gain_two = jnp.sum(grad_hidden_two * normed_two, axis=0)
    grad_norm_two = grad_hidden_two * gain_two
    grad_mid = grad_out + inv_two * (
        grad_norm_two - normed_two * jnp.mean(grad_norm_two * normed_two, axis=-1, keepdims=True)
    )
    grad_proj_b = grad_mid.astype(bf)
    grad_out_w = jnp.einsum("rh,rd->hd", attn_vals, grad_proj_b, preferred_element_type=jnp.float32)
    grad_vals_b = jnp.einsum(
        "rd,hd->rh", grad_proj_b, out_w, preferred_element_type=jnp.float32
    ).astype(bf)
    grad_vals_b = grad_vals_b.reshape(num_rows, kv_heads, group_size, HD)
    logit_att = attention_scores(query_b, key_b, allowed)
    probs = jnp.exp(logit_att - log_total)
    probs_b = probs.astype(bf)
    grad_value = jnp.einsum(
        "kgqp,qkgd->pkd", probs_b, grad_vals_b, preferred_element_type=jnp.float32
    )
    grad_prob_att = jnp.einsum(
        "qkgd,pkd->kgqp", grad_vals_b, value_h, preferred_element_type=jnp.float32
    )
    delta_row = jnp.sum(probs * grad_prob_att, axis=-1, keepdims=True)
    grad_score_b = (probs * (grad_prob_att - delta_row)).astype(bf)
    grad_query = jnp.einsum(
        "kgqp,pkd->qkgd", grad_score_b, key_b, preferred_element_type=jnp.float32
    ) * HD ** (-0.5)
    grad_key = jnp.einsum(
        "kgqp,qkgd->pkd", grad_score_b, query_b, preferred_element_type=jnp.float32
    ) * HD ** (-0.5)
    grad_query_b = rotate(grad_query.reshape(num_rows, num_heads, HD), tok_pos, -1.0).astype(bf)
    grad_key_b = rotate(grad_key, tok_pos, -1.0).astype(bf)
    grad_qkv_b = jnp.concatenate(
        [
            grad_query_b.reshape(num_rows, q_cols),
            grad_key_b.reshape(num_rows, k_cols),
            grad_value.astype(bf).reshape(num_rows, k_cols),
        ],
        axis=1,
    )
    grad_qkv_w = jnp.einsum("rd,rh->dh", hidden_one, grad_qkv_b, preferred_element_type=jnp.float32)
    grad_hidden_one = jnp.einsum("rh,dh->rd", grad_qkv_b, qkv_w, preferred_element_type=jnp.float32)
    grad_gain_one = jnp.sum(grad_hidden_one * normed_one, axis=0)
    grad_norm_one = grad_hidden_one * gain_one
    grad_in = grad_mid + inv_one * (
        grad_norm_one - normed_one * jnp.mean(grad_norm_one * normed_one, axis=-1, keepdims=True)
    )
    qkv_part = jnp.concatenate(
        [
            grad_qkv_w.astype(bf),
            jnp.pad(
                jnp.concatenate([grad_gain_one[:, None], grad_gain_two[:, None], grad_router], axis=1),
                ((0, 0), (0, pad_cols)),
            ).astype(bf),
        ],
        axis=1,
    )
    dense_sum = dense_scatter((grad_out_w.astype(bf), qkv_part))
    out_sum, qkv_sum = dense_sum[:, :width], dense_sum[:, width:]
    return (
        layer_out,
        grad_in,
        qkv_sum[:, qkv_cols],
        qkv_sum[:, :q_cols],
        qkv_sum[:, q_cols : q_cols + k_cols],
        qkv_sum[:, q_cols + k_cols : qkv_cols],
        out_sum,
        qkv_sum[:, qkv_cols + 1],
        qkv_sum[:, qkv_cols + 2 : qkv_cols + 2 + num_experts],
        *expert_sums,
    )


def solution(mesh):
    in_specs = (
        P(("dp", "exp"), None),
        P(("dp", "exp"), None),
        P(),
        P(("dp", "exp")),
        P(("dp", "exp"), None),
        P(("dp", "exp")),
        P(("dp", "exp"), None),
        P(("dp", "exp"), None),
        P(("dp", "exp"), None),
        P(("dp", "exp"), None),
        P(("dp", "exp")),
        P(("dp", "exp"), None),
        P("exp", "dp", None),
        P("exp", "dp", None),
        P("exp", "dp", None),
    )
    out_specs = (
        P(("dp", "exp"), None),
        P(("dp", "exp"), None),
        P(("dp", "exp")),
        P(("dp", "exp"), None),
        P(("dp", "exp"), None),
        P(("dp", "exp"), None),
        P(("dp", "exp"), None),
        P(("dp", "exp")),
        P(("dp", "exp"), None),
        P("exp", "dp", None),
        P("exp", "dp", None),
        P("exp", "dp", None),
    )
    body = body_plane if (mesh.shape["dp"], mesh.shape["exp"]) == (4, 8) else body_general
    return jax.shard_map(body, mesh=mesh, in_specs=in_specs, out_specs=out_specs, check_vma=False)
```

```python
import functools

import jax
import jax.numpy as jnp
from jax import lax
from jax.experimental import pallas as pl
from jax.experimental.pallas import tpu as pltpu
from jax.sharding import PartitionSpec as P

HD = 128
PROMPT = 256
NCONT = 2


EPS = 1e-06
THETA = 10000.0
HIGH = lax.Precision.HIGHEST
NEG_BIG = -1e30


def positions(segments):
    count_rows = segments.shape[0]
    row_ids = jnp.arange(count_rows, dtype=jnp.int32)
    labels = jnp.arange(NCONT + 1, dtype=jnp.int32)
    member = segments[:, None] == labels[None, :]
    first_row = jnp.min(jnp.where(member, row_ids[:, None], count_rows), axis=0)
    start_row = jnp.sum(jnp.where(member, first_row[None, :], 0), axis=1)
    return jnp.where(segments == 0, row_ids, PROMPT + row_ids - start_row)


def key_mask(segments):
    row_ids = jnp.arange(segments.shape[0], dtype=jnp.int32)
    causal = row_ids[None, :] <= row_ids[:, None]
    visible = (segments[None, :] == 0) | (segments[None, :] == segments[:, None])
    return causal & visible


def rotate(values, pos_rows, sign_value):
    half_size = HD // 2
    freq = THETA ** (-2.0 * jnp.arange(half_size, dtype=jnp.float32) / HD)
    angle = pos_rows.astype(jnp.float32)[:, None] * freq[None, :]
    cosine = jnp.cos(angle)[:, None, :]
    sine_part = sign_value * jnp.sin(angle)[:, None, :]
    first_half = values[..., :half_size]
    second = values[..., half_size:]
    return jnp.concatenate(
        [first_half * cosine - second * sine_part, second * cosine + first_half * sine_part],
        axis=-1,
    )


def attention_scores(query_b, key_b, allowed):
    logits = jnp.einsum(
        "qkgd,pkd->kgqp", query_b, key_b, preferred_element_type=jnp.float32
    ) * HD ** (-0.5)
    return jnp.where(allowed[None, None], logits, NEG_BIG)


def expert_gates(rows_in, gate_w, up_w):
    gate_val = jnp.einsum("sacd,adf->sacf", rows_in, gate_w, preferred_element_type=jnp.float32)
    up_val = jnp.einsum("sacd,adf->sacf", rows_in, up_w, preferred_element_type=jnp.float32)
    return (gate_val, up_val)


def body_general(
    tokens,
    targets,
    valid_count,
    segments,
    routes,
    gain_attn,
    w_query,
    w_key,
    w_value,
    w_out,
    gain_moe,
    w_router,
    w_gate,
    w_up,
    w_down,
):
    gain_one, query_w, key_w, value_w, out_w, gain_two, router_w = (
        lax.all_gather(gain_attn, ("dp", "exp"), axis=0, tiled=True),
        lax.all_gather(w_query, ("dp", "exp"), axis=0, tiled=True),
        lax.all_gather(w_key, ("dp", "exp"), axis=0, tiled=True),
        lax.all_gather(w_value, ("dp", "exp"), axis=0, tiled=True),
        lax.all_gather(w_out, ("dp", "exp"), axis=0, tiled=True),
        lax.all_gather(gain_moe, ("dp", "exp"), axis=0, tiled=True),
        lax.all_gather(w_router, ("dp", "exp"), axis=0, tiled=True),
    )
    gate_w, up_w, down_w = (
        lax.all_gather(w_gate, "dp", axis=1, tiled=True),
        lax.all_gather(w_up, "dp", axis=1, tiled=True),
        lax.all_gather(w_down, "dp", axis=1, tiled=True),
    )
    num_rows = tokens.shape[0]
    width = tokens.shape[1]
    num_heads = query_w.shape[1] // HD
    kv_heads = key_w.shape[1] // HD
    group_size = num_heads // kv_heads
    num_experts = router_w.shape[1]
    top_count = routes.shape[1]
    exp_local = gate_w.shape[0]
    exp_ranks = lax.axis_size("exp")
    capacity = 5 * num_rows * top_count // (4 * num_experts)
    tok_pos = positions(segments)
    allowed = key_mask(segments)
    resid_in = tokens.astype(jnp.float32)
    inv_one = lax.rsqrt(jnp.mean(resid_in * resid_in, axis=-1, keepdims=True) + EPS)
    normed_one = resid_in * inv_one
    hidden_one = (normed_one * gain_one.astype(jnp.float32)).astype(jnp.bfloat16)
    query_raw = jnp.dot(hidden_one, query_w, preferred_element_type=jnp.float32)
    key_raw = jnp.dot(hidden_one, key_w, preferred_element_type=jnp.float32)
    value_b = jnp.dot(hidden_one, value_w, preferred_element_type=jnp.float32).astype(jnp.bfloat16)
    query_b = rotate(query_raw.reshape(num_rows, num_heads, HD), tok_pos, 1.0).astype(jnp.bfloat16)
    query_b = query_b.reshape(num_rows, kv_heads, group_size, HD)
    key_b = rotate(key_raw.reshape(num_rows, kv_heads, HD), tok_pos, 1.0).astype(jnp.bfloat16)
    value_h = value_b.reshape(num_rows, kv_heads, HD)
    logit_att = attention_scores(query_b, key_b, allowed)
    row_max = jnp.max(logit_att, axis=-1, keepdims=True)
    log_total = row_max + jnp.log(jnp.sum(jnp.exp(logit_att - row_max), axis=-1, keepdims=True))
    probs_b = jnp.exp(logit_att - log_total).astype(jnp.bfloat16)
    attn_vals = jnp.einsum("kgqp,pkd->qkgd", probs_b, value_h, preferred_element_type=jnp.float32)
    attn_vals = attn_vals.reshape(num_rows, num_heads * HD).astype(jnp.bfloat16)
    resid_mid = resid_in + jnp.dot(attn_vals, out_w, preferred_element_type=jnp.float32)
    inv_two = lax.rsqrt(jnp.mean(resid_mid * resid_mid, axis=-1, keepdims=True) + EPS)
    normed_two = resid_mid * inv_two
    gain_two_f = gain_two.astype(jnp.float32)
    hidden_two = (normed_two * gain_two_f).astype(jnp.bfloat16)
    router_prob = jax.nn.softmax(
        jnp.dot(hidden_two, router_w, preferred_element_type=jnp.float32), axis=-1
    )
    expert_ids = jnp.arange(num_experts, dtype=jnp.int32)
    route_hot = routes[:, :, None] == expert_ids[None, None, :]
    chosen = jnp.sum(jnp.where(route_hot, router_prob[:, None, :], 0.0), axis=-1)
    weight_sum = jnp.sum(chosen, axis=1, keepdims=True)
    combine = chosen / weight_sum
    flat_hot = route_hot.reshape(num_rows * top_count, num_experts).astype(jnp.int32)
    slot_index = jnp.sum((jnp.cumsum(flat_hot, axis=0) - flat_hot) * flat_hot, axis=1)
    dest_index = routes.reshape(-1) * capacity + slot_index
    send_shape = (exp_ranks, exp_local, capacity, width)
    send_rows = jnp.zeros((num_experts * capacity, width), jnp.bfloat16)
    send_rows = (
        send_rows.at[dest_index].set(jnp.repeat(hidden_two, top_count, axis=0)).reshape(send_shape)
    )
    gate_val, up_val = expert_gates(
        lax.all_to_all(send_rows, "exp", split_axis=0, concat_axis=0, tiled=True), gate_w, up_w
    )
    act_b = (jax.nn.relu(gate_val) * up_val).astype(jnp.bfloat16)
    out_b = jnp.einsum("sacf,afd->sacd", act_b, down_w, preferred_element_type=jnp.float32).astype(
        jnp.bfloat16
    )
    returned = lax.all_to_all(out_b, "exp", split_axis=0, concat_axis=0, tiled=True)
    route_out = returned.reshape(num_experts * capacity, width)[dest_index].reshape(
        num_rows, top_count, width
    )
    route_out_f = route_out.astype(jnp.float32)
    resid_out = resid_mid + jnp.sum(combine[:, :, None] * route_out_f, axis=1)
    layer_out = resid_out.astype(jnp.bfloat16)
    total_rows = num_rows * lax.axis_size(("dp", "exp"))
    global_row = lax.axis_index(("dp", "exp")) * num_rows + jnp.arange(num_rows, dtype=jnp.int32)
    loss_scale = total_rows / valid_count[0].astype(jnp.float32)
    grad_out = jnp.where(
        (global_row < valid_count[0])[:, None],
        (resid_out - targets.astype(jnp.float32)) * loss_scale,
        0.0,
    )
    gain_one, query_w, key_w, value_w, out_w, gain_two, router_w = (
        lax.all_gather(gain_attn, ("dp", "exp"), axis=0, tiled=True),
        lax.all_gather(w_query, ("dp", "exp"), axis=0, tiled=True),
        lax.all_gather(w_key, ("dp", "exp"), axis=0, tiled=True),
        lax.all_gather(w_value, ("dp", "exp"), axis=0, tiled=True),
        lax.all_gather(w_out, ("dp", "exp"), axis=0, tiled=True),
        lax.all_gather(gain_moe, ("dp", "exp"), axis=0, tiled=True),
        lax.all_gather(w_router, ("dp", "exp"), axis=0, tiled=True),
    )
    gain_two_f = gain_two.astype(jnp.float32)
    grad_route = (combine[:, :, None] * grad_out[:, None, :]).astype(jnp.bfloat16)
    grad_comb = jnp.sum(grad_out[:, None, :] * route_out_f, axis=-1)
    grad_send = jnp.zeros((num_experts * capacity, width), jnp.bfloat16)
    grad_send = (
        grad_send.at[dest_index]
        .set(grad_route.reshape(num_rows * top_count, width))
        .reshape(send_shape)
    )
    expert_rows, grad_recv = (
        lax.all_to_all(send_rows, "exp", split_axis=0, concat_axis=0, tiled=True),
        lax.all_to_all(grad_send, "exp", split_axis=0, concat_axis=0, tiled=True),
    )
    gate_val, up_val = expert_gates(expert_rows, gate_w, up_w)
    gate_relu = jax.nn.relu(gate_val)
    act_b = (gate_relu * up_val).astype(jnp.bfloat16)
    grad_act = jnp.einsum("sacd,afd->sacf", grad_recv, down_w, preferred_element_type=jnp.float32)
    grad_down_w = jnp.einsum("sacf,sacd->afd", act_b, grad_recv, preferred_element_type=jnp.float32)
    grad_gate_b = jnp.where(gate_val > 0, grad_act * up_val, 0.0).astype(jnp.bfloat16)
    grad_up_b = (grad_act * gate_relu).astype(jnp.bfloat16)
    grad_gate_w = jnp.einsum(
        "sacd,sacf->adf", expert_rows, grad_gate_b, preferred_element_type=jnp.float32
    )
    grad_up_w = jnp.einsum(
        "sacd,sacf->adf", expert_rows, grad_up_b, preferred_element_type=jnp.float32
    )
    grad_rows = (
        jnp.einsum("sacf,adf->sacd", grad_gate_b, gate_w, preferred_element_type=jnp.float32)
        + jnp.einsum("sacf,adf->sacd", grad_up_b, up_w, preferred_element_type=jnp.float32)
    ).astype(jnp.bfloat16)
    grad_back = lax.all_to_all(grad_rows, "exp", split_axis=0, concat_axis=0, tiled=True)
    grad_copies = grad_back.reshape(num_experts * capacity, width)[dest_index].reshape(
        num_rows, top_count, width
    )
    grad_hidden_two = jnp.sum(grad_copies.astype(jnp.float32), axis=1)
    grad_chosen = (grad_comb - jnp.sum(grad_comb * combine, axis=1, keepdims=True)) / weight_sum
    grad_prob = jnp.sum(jnp.where(route_hot, grad_chosen[:, :, None], 0.0), axis=1)
    grad_logit = router_prob * (
        grad_prob - jnp.sum(router_prob * grad_prob, axis=-1, keepdims=True)
    )
    router_f = router_w.astype(jnp.float32)
    grad_hidden_two = grad_hidden_two + jnp.einsum(
        "re,de->rd", grad_logit, router_f, precision=HIGH
    )
    grad_router = jnp.einsum(
        "rd,re->de", hidden_two.astype(jnp.float32), grad_logit, precision=HIGH
    )
    grad_gain_two = jnp.sum(grad_hidden_two * normed_two, axis=0)
    grad_norm_two = grad_hidden_two * gain_two_f
    grad_mid = grad_out + inv_two * (
        grad_norm_two - normed_two * jnp.mean(grad_norm_two * normed_two, axis=-1, keepdims=True)
    )
    grad_proj_b = grad_mid.astype(jnp.bfloat16)
    grad_out_w = jnp.einsum("rh,rd->hd", attn_vals, grad_proj_b, preferred_element_type=jnp.float32)
    grad_vals_b = jnp.einsum(
        "rd,hd->rh", grad_proj_b, out_w, preferred_element_type=jnp.float32
    ).astype(jnp.bfloat16)
    grad_vals_b = grad_vals_b.reshape(num_rows, kv_heads, group_size, HD)
    logit_att = attention_scores(query_b, key_b, allowed)
    probs = jnp.exp(logit_att - log_total)
    probs_b = probs.astype(jnp.bfloat16)
    grad_value = jnp.einsum(
        "kgqp,qkgd->pkd", probs_b, grad_vals_b, preferred_element_type=jnp.float32
    )
    grad_prob_att = jnp.einsum(
        "qkgd,pkd->kgqp", grad_vals_b, value_h, preferred_element_type=jnp.float32
    )
    delta_row = jnp.sum(probs * grad_prob_att, axis=-1, keepdims=True)
    grad_score_b = (probs * (grad_prob_att - delta_row)).astype(jnp.bfloat16)
    grad_query = jnp.einsum(
        "kgqp,pkd->qkgd", grad_score_b, key_b, preferred_element_type=jnp.float32
    ) * HD ** (-0.5)
    grad_key = jnp.einsum(
        "kgqp,qkgd->pkd", grad_score_b, query_b, preferred_element_type=jnp.float32
    ) * HD ** (-0.5)
    grad_query_b = rotate(grad_query.reshape(num_rows, num_heads, HD), tok_pos, -1.0).astype(
        jnp.bfloat16
    )
    grad_query_b = grad_query_b.reshape(num_rows, num_heads * HD)
    grad_key_b = (
        rotate(grad_key, tok_pos, -1.0).astype(jnp.bfloat16).reshape(num_rows, kv_heads * HD)
    )
    grad_value_b = grad_value.astype(jnp.bfloat16).reshape(num_rows, kv_heads * HD)
    grad_query_w = jnp.einsum(
        "rd,rh->dh", hidden_one, grad_query_b, preferred_element_type=jnp.float32
    )
    grad_key_w = jnp.einsum("rd,rh->dh", hidden_one, grad_key_b, preferred_element_type=jnp.float32)
    grad_value_w = jnp.einsum(
        "rd,rh->dh", hidden_one, grad_value_b, preferred_element_type=jnp.float32
    )
    grad_hidden_one = (
        jnp.einsum("rh,dh->rd", grad_query_b, query_w, preferred_element_type=jnp.float32)
        + jnp.einsum("rh,dh->rd", grad_key_b, key_w, preferred_element_type=jnp.float32)
        + jnp.einsum("rh,dh->rd", grad_value_b, value_w, preferred_element_type=jnp.float32)
    )
    grad_gain_one = jnp.sum(grad_hidden_one * normed_one, axis=0)
    grad_norm_one = grad_hidden_one * gain_one.astype(jnp.float32)
    grad_in = grad_mid + inv_one * (
        grad_norm_one - normed_one * jnp.mean(grad_norm_one * normed_one, axis=-1, keepdims=True)
    )
    dense_sums = (
        lax.psum_scatter(grad_gain_one, ("dp", "exp"), scatter_dimension=0, tiled=True),
        lax.psum_scatter(grad_query_w, ("dp", "exp"), scatter_dimension=0, tiled=True),
        lax.psum_scatter(grad_key_w, ("dp", "exp"), scatter_dimension=0, tiled=True),
        lax.psum_scatter(grad_value_w, ("dp", "exp"), scatter_dimension=0, tiled=True),
        lax.psum_scatter(grad_out_w, ("dp", "exp"), scatter_dimension=0, tiled=True),
        lax.psum_scatter(grad_gain_two, ("dp", "exp"), scatter_dimension=0, tiled=True),
        lax.psum_scatter(grad_router, ("dp", "exp"), scatter_dimension=0, tiled=True),
    )
    expert_sums = (
        lax.psum_scatter(
            grad_gate_w.astype(jnp.bfloat16), "dp", scatter_dimension=1, tiled=True
        ).astype(jnp.float32),
        lax.psum_scatter(
            grad_up_w.astype(jnp.bfloat16), "dp", scatter_dimension=1, tiled=True
        ).astype(jnp.float32),
        lax.psum_scatter(
            grad_down_w.astype(jnp.bfloat16), "dp", scatter_dimension=1, tiled=True
        ).astype(jnp.float32),
    )
    return (
        layer_out,
        grad_in,
        dense_sums[0],
        dense_sums[1],
        dense_sums[2],
        dense_sums[3],
        dense_sums[4],
        dense_sums[5],
        dense_sums[6],
        expert_sums[0],
        expert_sums[1],
        expert_sums[2],
    )


MESH = pl.DeviceIdType.MESH
ANY = pl.BlockSpec(memory_space=pl.ANY)
VMEM = pl.BlockSpec(memory_space=pltpu.VMEM)
VMEM_BYTES = 62 * 2**20


def nn_dot(left, right):
    return jnp.dot(left, right, preferred_element_type=jnp.float32)


def nt_dot(left, right):
    return lax.dot_general(
        left, right, (((1,), (1,)), ((), ())), preferred_element_type=jnp.float32
    )


def tn_dot(left, right):
    return lax.dot_general(
        left, right, (((0,), (0,)), ((), ())), preferred_element_type=jnp.float32
    )


def plane_peers():
    me = lax.axis_index("exp")
    core = lax.rem(me, 2)
    x_pos = lax.rem(lax.div(me, 2), 2)
    y_pos = lax.div(me, 4)
    return me, me + 1 - 2 * core, me + 2 - 4 * x_pos, me + 4 - 8 * y_pos


def remote(src, dst, send_sem, recv_sem, peer):
    return pltpu.make_async_remote_copy(
        src_ref=src,
        dst_ref=dst,
        send_sem=send_sem,
        recv_sem=recv_sem,
        device_id={"exp": peer},
        device_id_type=MESH,
    )


def plane_barrier(peers):
    barrier = pltpu.get_barrier_semaphore()
    for peer in peers:
        pl.semaphore_signal(barrier, inc=1, device_id={"exp": peer}, device_id_type=MESH)
    pl.semaphore_wait(barrier, len(peers))


def step_place(step, quad):
    odd = lax.rem(step, 2)
    last = lax.div(quad, 3)
    mid = lax.rem(lax.div(quad + 1, 2), 2)
    return mid * (1 - odd) + last, mid * odd + last


class Gather:
    def __init__(self, own, buf, send, recv):
        self.own, self.buf, self.send, self.recv = own, buf, send, recv
        self.me, self.sib, self.xn, self.yn = plane_peers()
        self.diag = self.xn + self.yn - self.me

    def own_copy(self, half, peer, sem):
        return remote(
            self.own.at[half],
            self.buf.at[self.me, half],
            self.send.at[sem],
            self.recv.at[self.me, half],
            peer,
        )

    def pass_copy(self, slot, half, peer, sem):
        return remote(
            self.buf.at[slot, half],
            self.buf.at[slot, half],
            self.send.at[sem],
            self.recv.at[slot, half],
            peer,
        )

    def own_copies(self):
        return (
            self.own_copy(0, self.xn, 0),
            self.own_copy(1, self.yn, 1),
            self.own_copy(0, self.sib, 2),
            self.own_copy(1, self.sib, 3),
            self.own_copy(1, self.xn, 4),
            self.own_copy(0, self.yn, 5),
        )

    def near_copies(self):
        return (
            self.pass_copy(self.xn, 0, self.yn, 6),
            self.pass_copy(self.yn, 1, self.xn, 7),
            self.pass_copy(self.xn, 0, self.sib, 8),
            self.pass_copy(self.yn, 1, self.sib, 9),
        )

    def late_copies(self):
        return (
            self.pass_copy(self.xn, 1, self.sib, 10),
            self.pass_copy(self.yn, 0, self.sib, 11),
        )

    def far_copies(self):
        return (
            self.pass_copy(self.diag, 0, self.sib, 12),
            self.pass_copy(self.diag, 1, self.sib, 13),
        )

    def wait_block(self, slot, half):
        self.pass_copy(slot, half, self.sib, 0).wait_recv()

    def begin(self):
        plane_barrier((self.sib, self.xn, self.yn))
        for copy in self.own_copies():
            copy.start()

    def place(self, step):
        quad = lax.div(step, 4)
        far_x, far_y = step_place(step, quad)
        odd = lax.rem(step, 2)
        third = lax.div(quad, 2) * (1 - lax.div(quad, 3))
        other = lax.div(lax.rem(step, 4), 2)
        slot = (
            self.me
            + far_x * (self.xn - self.me)
            + far_y * (self.yn - self.me)
            + other * (self.sib - self.me)
        )
        return slot, odd + third * (1 - 2 * odd), other

    def arrive(self, step):
        @pl.when(step == 4)
        def _():
            self.wait_block(self.xn, 0)
            self.wait_block(self.yn, 1)
            for copy in self.near_copies():
                copy.start()

        @pl.when(step == 8)
        def _():
            self.wait_block(self.xn, 1)
            self.wait_block(self.yn, 0)
            for copy in self.late_copies():
                copy.start()

        @pl.when(step == 12)
        def _():
            self.wait_block(self.diag, 0)
            self.wait_block(self.diag, 1)
            for copy in self.far_copies():
                copy.start()

        slot, half, other = self.place(step)

        @pl.when(other == 1)
        def _():
            self.wait_block(slot, half)

        return slot, half

    def finish(self):
        for copies in (self.own_copies(), self.near_copies(), self.late_copies(), self.far_copies()):
            for copy in copies:
                copy.wait_send()


def expert_in_kernel(own, gate_hbm, up_hbm, rows_out, gua_out, buf, gua, gate_w, up_w, send, recv, load, store_a, store_b):
    width, hidden = gate_w.shape
    gather = Gather(own, buf, send, recv)
    loads = (
        pltpu.make_async_copy(gate_hbm, gate_w, load.at[0]),
        pltpu.make_async_copy(up_hbm, up_w, load.at[1]),
        pltpu.make_async_copy(own.at[0], buf.at[gather.me, 0], load.at[2]),
        pltpu.make_async_copy(own.at[1], buf.at[gather.me, 1], load.at[3]),
    )
    for copy in loads:
        copy.start()
    gather.begin()
    for copy in loads:
        copy.wait()

    def row_store(slot, half, step):
        return pltpu.make_async_copy(buf.at[slot, half], rows_out.at[slot, half], store_a.at[step])

    def gua_store(slot, half, step):
        return pltpu.make_async_copy(gua.at[slot, half], gua_out.at[slot, half], store_b.at[step])

    def one(step, carry):
        slot, half = gather.arrive(step)
        row_store(slot, half, step).start()
        rows = buf[slot, half, :, :width]
        lanes = lax.broadcasted_iota(jnp.int32, (buf.shape[2], 128), 1)
        tail = buf[slot, half, :, width:].astype(jnp.float32)
        weight = jnp.sum(jnp.where(lanes == gather.me, tail, 0.0), axis=1, keepdims=True)
        gate_val = nn_dot(rows, gate_w[...])
        up_val = nn_dot(rows, up_w[...])
        gua[slot, half, :, :hidden] = gate_val.astype(jnp.bfloat16)
        gua[slot, half, :, hidden : 2 * hidden] = up_val.astype(jnp.bfloat16)
        act_val = jnp.maximum(gate_val, 0.0) * up_val * weight
        gua[slot, half, :, 2 * hidden :] = act_val.astype(jnp.bfloat16)
        gua_store(slot, half, step).start()
        return carry

    lax.fori_loop(0, 16, one, 0)
    gather.finish()

    def drain(step, carry):
        slot, half, _ = gather.place(step)
        row_store(slot, half, step).wait()
        gua_store(slot, half, step).wait()
        return carry

    lax.fori_loop(0, 16, drain, 0)


def expert_in(own, gate_w, up_w):
    _, half, columns = own.shape
    width, hidden = gate_w.shape
    bf = jnp.bfloat16
    return pl.pallas_call(
        expert_in_kernel,
        out_shape=(
            jax.ShapeDtypeStruct((8, 2, half, columns), bf),
            jax.ShapeDtypeStruct((8, 2, half, 3 * hidden), bf),
        ),
        in_specs=[ANY] * 3,
        out_specs=(ANY, ANY),
        scratch_shapes=[
            pltpu.VMEM((8, 2, half, columns), bf),
            pltpu.VMEM((8, 2, half, 3 * hidden), bf),
            pltpu.VMEM((width, hidden), bf),
            pltpu.VMEM((width, hidden), bf),
            pltpu.SemaphoreType.DMA((14,)),
            pltpu.SemaphoreType.DMA((8, 2)),
            pltpu.SemaphoreType.DMA((4,)),
            pltpu.SemaphoreType.DMA((16,)),
            pltpu.SemaphoreType.DMA((16,)),
        ],
        compiler_params=pltpu.CompilerParams(
            collective_id=1, has_side_effects=True, vmem_limit_bytes=VMEM_BYTES
        ),
        name="expert_in",
    )(own, gate_w, up_w)


def row_chunk(rows):
    return 64 if rows % 64 == 0 else 16


def add_rows(target, others):
    parts, rows_all, _ = target.shape
    chunk = row_chunk(rows_all)
    for part in range(parts):

        def one(index, carry):
            rows = pl.ds(pl.multiple_of(index * chunk, chunk), chunk)
            total = target[part, rows, :].astype(jnp.float32)
            for other in others:
                total = total + other[part, rows, :].astype(jnp.float32)
            target[part, rows, :] = total.astype(target.dtype)
            return carry

        lax.fori_loop(0, rows_all // chunk, one, 0)


class Scatter:
    def __init__(self, theirs, scratch):
        self.theirs = theirs
        self.mine, self.side, self.relay, self.final = scratch[:4]
        self.send, self.side_sem, self.relay_sem, self.final_sem = scratch[4:]
        self.me, self.sib, self.xn, self.yn = plane_peers()

    def peers(self):
        return self.sib, self.xn, self.yn

    def place(self, step):
        quad = lax.div(step, 4)
        far_x, far_y = step_place(step, 3 - quad)
        odd = lax.rem(step, 2)
        third = lax.div(quad, 2) * (1 - lax.div(quad, 3))
        other = 1 - lax.div(lax.rem(step, 4), 2)
        slot = (
            self.me
            + far_x * (self.xn - self.me)
            + far_y * (self.yn - self.me)
            + other * (self.sib - self.me)
        )
        return slot, odd + third * (1 - 2 * odd), other, far_x + 2 * far_y

    def side_copy(self, step):
        slot, half, _, place = self.place(step)
        return remote(
            self.theirs(place, slot, half),
            self.side.at[place, half],
            self.send.at[step],
            self.side_sem.at[place, half],
            self.sib,
        )

    def side_wait(self, place, half):
        remote(
            self.side.at[place, half],
            self.side.at[place, half],
            self.send.at[0],
            self.side_sem.at[place, half],
            self.sib,
        ).wait_recv()

    def relay_copy(self, step, way):
        return remote(
            self.mine.at[3, way],
            self.relay.at[way],
            self.send.at[step],
            self.relay_sem.at[way],
            (self.xn, self.yn)[way],
        )

    def final_copy(self, step, way, half):
        return remote(
            self.mine.at[1 + way, half],
            self.final.at[way, half],
            self.send.at[step],
            self.final_sem.at[way, half],
            (self.xn, self.yn)[way],
        )

    def depart(self, step):
        @pl.when(self.place(step)[2] == 1)
        def _():
            self.side_copy(step).start()

        for way in (0, 1):

            @pl.when(step == 2 + way)
            def _():
                self.side_wait(3, way)
                add_rows(self.mine.at[3, way], (self.side.at[3, way],))
                self.relay_copy(2 + way, way).start()

            @pl.when(step == 6 + way)
            def _():
                self.side_wait(1 + way, way)
                add_rows(self.mine.at[1 + way, way], (self.side.at[1 + way, way],))
                self.final_copy(6 + way, way, way).start()

    def forward(self):
        for way in (0, 1):
            self.side_wait(1 + way, 1 - way)
            self.relay_copy(3 - way, 1 - way).wait_recv()
            add_rows(
                self.mine.at[1 + way, 1 - way],
                (self.side.at[1 + way, 1 - way], self.relay.at[1 - way]),
            )
            self.final_copy(10 + way, way, 1 - way).start()

    def finish(self, write):
        parts, rows_all = self.mine.shape[2:4]
        chunk = row_chunk(rows_all)
        for half in (0, 1):
            self.side_wait(0, half)
            self.final_copy(0, 0, half).wait_recv()
            self.final_copy(0, 1, half).wait_recv()
            for part in range(parts):

                def one(index, carry):
                    rows = pl.ds(pl.multiple_of(index * chunk, chunk), chunk)
                    total = self.mine[0, half, part, rows, :].astype(jnp.float32)
                    total = total + self.side[0, half, part, rows, :].astype(jnp.float32)
                    total = total + self.final[0, half, part, rows, :].astype(jnp.float32)
                    total = total + self.final[1, half, part, rows, :].astype(jnp.float32)
                    write(half, part, rows, total)
                    return carry

                lax.fori_loop(0, rows_all // chunk, one, 0)

    def drain(self):
        for way in (0, 1):
            self.relay_copy(2 + way, way).wait_send()
            self.final_copy(6 + way, way, way).wait_send()
            self.final_copy(10 + way, way, 1 - way).wait_send()

        def one(step, carry):
            @pl.when(self.place(step)[2] == 1)
            def _():
                self.side_copy(step).wait_send()

            return carry

        lax.fori_loop(0, 16, one, 0)


SCATTER_REFS = 8


def scatter_scratch(parts, rows, columns):
    bf = jnp.bfloat16
    return [
        pltpu.VMEM((4, 2, parts, rows, columns), bf),
        pltpu.VMEM((4, 2, parts, rows, columns), bf),
        pltpu.VMEM((2, parts, rows, columns), bf),
        pltpu.VMEM((2, 2, parts, rows, columns), bf),
        pltpu.SemaphoreType.DMA((16,)),
        pltpu.SemaphoreType.DMA((4, 2)),
        pltpu.SemaphoreType.DMA((2,)),
        pltpu.SemaphoreType.DMA((2, 2)),
    ]


def expert_out_kernel(gua_hbm, down_hbm, resid, targets, scales, layer, grad, grad_b, act, down_w, away, load, *scratch):
    hidden = down_w.shape[0]
    scatter = Scatter(lambda place, slot, half: away.at[place, half], scratch)
    mine = scatter.mine
    down_load = pltpu.make_async_copy(down_hbm, down_w, load.at[16])
    down_load.start()

    def act_load(step):
        slot, half, _, _ = scatter.place(step)
        return pltpu.make_async_copy(
            gua_hbm.at[slot, half, :, pl.ds(2 * hidden, hidden)], act.at[slot, half], load.at[step]
        )

    def fetch(step, carry):
        act_load(step).start()
        return carry

    lax.fori_loop(0, 16, fetch, 0)
    plane_barrier(scatter.peers())
    down_load.wait()

    def one(step, carry):
        slot, half, other, place = scatter.place(step)
        act_load(step).wait()
        partial = nn_dot(act[slot, half], down_w[...]).astype(jnp.bfloat16)

        @pl.when(other == 1)
        def _():
            away[place, half, 0] = partial

        @pl.when(other == 0)
        def _():
            mine[place, half, 0] = partial

        scatter.depart(step)
        return carry

    lax.fori_loop(0, 16, one, 0)
    scatter.forward()

    def write(half, part, rows, total):
        value = resid[half, rows, :] + total
        layer[half, rows, :] = value.astype(layer.dtype)
        error = (value - targets[half, rows, :].astype(jnp.float32)) * scales[half, rows, 0:1]
        grad[half, rows, :] = error
        grad_b[half, rows, :] = error.astype(grad_b.dtype)

    scatter.finish(write)
    scatter.drain()


def expert_out(gua, down_w, resid, targets, scales):
    half = gua.shape[2]
    hidden, width = down_w.shape
    return pl.pallas_call(
        expert_out_kernel,
        out_shape=(
            jax.ShapeDtypeStruct((2, half, width), jnp.bfloat16),
            jax.ShapeDtypeStruct((2, half, width), jnp.float32),
            jax.ShapeDtypeStruct((2, half, width), jnp.bfloat16),
        ),
        in_specs=[ANY] * 2 + [VMEM] * 3,
        out_specs=(VMEM,) * 3,
        scratch_shapes=[
            pltpu.VMEM((8, 2, half, hidden), jnp.bfloat16),
            pltpu.VMEM((hidden, width), jnp.bfloat16),
            pltpu.VMEM((4, 2, 1, half, width), jnp.bfloat16),
            pltpu.SemaphoreType.DMA((17,)),
        ]
        + scatter_scratch(1, half, width),
        compiler_params=pltpu.CompilerParams(
            collective_id=2, has_side_effects=True, vmem_limit_bytes=VMEM_BYTES
        ),
        name="expert_out",
    )(
        gua,
        down_w,
        resid.reshape(2, half, width),
        targets.reshape(2, half, width),
        scales.reshape(2, half, 128),
    )


def expert_back_kernel(own, rows_hbm, gua_hbm, gate_hbm, up_hbm, down_hbm, grads_out, dgu_out, part_out, buf, gu, tails, part, gate_w, up_w, down_w, send, recv, load, load_gu, load_tail, store_a, store_b, store_c):
    width, hidden = gate_w.shape
    gather = Gather(own, buf, send, recv)
    loads = (
        pltpu.make_async_copy(down_hbm, down_w, load.at[0]),
        pltpu.make_async_copy(own.at[0], buf.at[gather.me, 0], load.at[1]),
        pltpu.make_async_copy(own.at[1], buf.at[gather.me, 1], load.at[2]),
        pltpu.make_async_copy(gate_hbm, gate_w, load.at[3]),
        pltpu.make_async_copy(up_hbm, up_w, load.at[4]),
    )
    for copy in loads:
        copy.start()

    def block_loads(step):
        slot, half, _ = gather.place(step)
        return (
            pltpu.make_async_copy(
                gua_hbm.at[slot, half, :, pl.ds(0, 2 * hidden)], gu.at[slot, half], load_gu.at[step]
            ),
            pltpu.make_async_copy(
                rows_hbm.at[slot, half, :, pl.ds(width, 128)], tails.at[slot, half], load_tail.at[step]
            ),
        )

    def fetch(step, carry):
        for copy in block_loads(step):
            copy.start()
        return carry

    lax.fori_loop(0, 16, fetch, 0)
    gather.begin()
    for copy in loads:
        copy.wait()

    def stores(step):
        slot, half, _ = gather.place(step)
        return (
            pltpu.make_async_copy(buf.at[slot, half], grads_out.at[slot, half], store_a.at[step]),
            pltpu.make_async_copy(gu.at[slot, half], dgu_out.at[slot, half], store_b.at[step]),
            pltpu.make_async_copy(part.at[slot, half], part_out.at[slot, half], store_c.at[step]),
        )

    def one(step, carry):
        slot, half = gather.arrive(step)
        store_rows, store_dgu, store_part = stores(step)
        store_rows.start()
        for copy in block_loads(step):
            copy.wait()
        lanes = lax.broadcasted_iota(jnp.int32, (buf.shape[2], 128), 1)
        tail = tails[slot, half].astype(jnp.float32)
        weight = jnp.sum(jnp.where(lanes == gather.me, tail, 0.0), axis=1, keepdims=True)
        grad_act = nt_dot(buf[slot, half], down_w[...])
        gate_val = gu[slot, half, :, :hidden].astype(jnp.float32)
        up_val = gu[slot, half, :, hidden:].astype(jnp.float32)
        gate_relu = jnp.maximum(gate_val, 0.0)
        grad_comb = jnp.sum(gate_relu * up_val * grad_act, axis=1, keepdims=True)
        grad_act = grad_act * weight
        grad_gate = jnp.where(gate_val > 0, grad_act * up_val, 0.0).astype(jnp.bfloat16)
        grad_up = (grad_act * gate_relu).astype(jnp.bfloat16)
        gu[slot, half, :, :hidden] = grad_gate
        gu[slot, half, :, hidden:] = grad_up
        store_dgu.start()
        part[slot, half, :, :width] = (
            nt_dot(grad_gate, gate_w[...]) + nt_dot(grad_up, up_w[...])
        ).astype(jnp.bfloat16)
        part[slot, half, :, width:] = jnp.where(lanes == gather.me, grad_comb, 0.0).astype(
            jnp.bfloat16
        )
        store_part.start()
        return carry

    lax.fori_loop(0, 16, one, 0)
    gather.finish()

    def drain(step, carry):
        for copy in stores(step):
            copy.wait()
        return carry

    lax.fori_loop(0, 16, drain, 0)


def expert_back(own, rows_all, gua, gate_w, up_w, down_w):
    _, half, columns = rows_all.shape[1:]
    width, hidden = gate_w.shape
    bf = jnp.bfloat16
    return pl.pallas_call(
        expert_back_kernel,
        out_shape=(
            jax.ShapeDtypeStruct((8, 2, half, width), bf),
            jax.ShapeDtypeStruct((8, 2, half, 2 * hidden), bf),
            jax.ShapeDtypeStruct((8, 2, half, columns), bf),
        ),
        in_specs=[ANY] * 6,
        out_specs=(ANY,) * 3,
        scratch_shapes=[
            pltpu.VMEM((8, 2, half, width), bf),
            pltpu.VMEM((8, 2, half, 2 * hidden), bf),
            pltpu.VMEM((8, 2, half, 128), bf),
            pltpu.VMEM((8, 2, half, columns), bf),
            pltpu.VMEM((width, hidden), bf),
            pltpu.VMEM((width, hidden), bf),
            pltpu.VMEM((hidden, width), bf),
            pltpu.SemaphoreType.DMA((14,)),
            pltpu.SemaphoreType.DMA((8, 2)),
            pltpu.SemaphoreType.DMA((5,)),
        ]
        + [pltpu.SemaphoreType.DMA((16,))] * 5,
        compiler_params=pltpu.CompilerParams(
            collective_id=3, has_side_effects=True, vmem_limit_bytes=VMEM_BYTES
        ),
        name="expert_back",
    )(own, rows_all, gua, gate_w, up_w, down_w)


def expert_grads_kernel(part_hbm, rows_hbm, dgu_hbm, gua_hbm, grads_hbm, out, gate_out, up_out, down_out, rows, dgu, act, grads, gate_up_acc, down_acc, load, block_load, *scratch):
    hidden, width = down_acc.shape
    scatter = Scatter(lambda place, slot, half: part_hbm.at[slot, half], scratch)

    def part_load(step):
        slot, half, _, place = scatter.place(step)
        return pltpu.make_async_copy(
            part_hbm.at[slot, half], scatter.mine.at[place, half], load.at[step]
        )

    def fetch(step, carry):
        @pl.when(scatter.place(step)[2] == 0)
        def _():
            part_load(step).start()

        return carry

    def block_copies(block):
        slot = lax.rem(block, 2)
        return (
            pltpu.make_async_copy(
                rows_hbm.at[block, :, :, pl.ds(0, width)], rows.at[slot], block_load.at[slot, 0]
            ),
            pltpu.make_async_copy(dgu_hbm.at[block], dgu.at[slot], block_load.at[slot, 1]),
            pltpu.make_async_copy(
                gua_hbm.at[block, :, :, pl.ds(2 * hidden, hidden)], act.at[slot], block_load.at[slot, 2]
            ),
            pltpu.make_async_copy(grads_hbm.at[block], grads.at[slot], block_load.at[slot, 3]),
        )

    lax.fori_loop(0, 16, fetch, 0)
    plane_barrier(scatter.peers())

    def one(step, carry):
        @pl.when(scatter.place(step)[2] == 0)
        def _():
            part_load(step).wait()

        scatter.depart(step)
        return carry

    lax.fori_loop(0, 16, one, 0)
    for copy in block_copies(0):
        copy.start()
    tile = 256

    def accumulate(block, carry):
        for copy in block_copies(block):
            copy.wait()

        @pl.when(block < 7)
        def _():
            for copy in block_copies(block + 1):
                copy.start()

        slot = lax.rem(block, 2)

        def add_tile(acc, left, right, index):
            cols = pl.ds(pl.multiple_of(index * tile, tile), tile)
            total = tn_dot(
                left[slot, :, :, cols].reshape(-1, tile), right[slot].reshape(-1, width)
            )

            @pl.when(block == 0)
            def _():
                acc[cols, :] = total

            @pl.when(block > 0)
            def _():
                acc[cols, :] = acc[cols, :] + total

        def gate_up_tile(index, carry):
            add_tile(gate_up_acc, rows, dgu, index)
            return carry

        def down_tile(index, carry):
            add_tile(down_acc, act, grads, index)
            return carry

        lax.fori_loop(0, width // tile, gate_up_tile, 0)
        lax.fori_loop(0, hidden // tile, down_tile, 0)
        return carry

    def blocks(index, carry):
        @pl.when(index == 3)
        def _():
            scatter.forward()

        return accumulate(index, carry)

    lax.fori_loop(0, 8, blocks, 0)

    def round_tile(index, carry):
        cols = pl.ds(pl.multiple_of(index * 64, 64), 64)
        gate_out[cols, :] = gate_up_acc[cols, :hidden].astype(jnp.bfloat16)
        up_out[cols, :] = gate_up_acc[cols, hidden:].astype(jnp.bfloat16)
        return carry

    lax.fori_loop(0, width // 64, round_tile, 0)

    def round_down(index, carry):
        cols = pl.ds(pl.multiple_of(index * 64, 64), 64)
        down_out[cols, :] = down_acc[cols, :].astype(jnp.bfloat16)
        return carry

    lax.fori_loop(0, hidden // 64, round_down, 0)

    def write(half, part, rows, total):
        out[half, rows, :] = total

    scatter.finish(write)
    scatter.drain()


def expert_grads(part, rows_all, dgu, gua, grads_all):
    _, _, half, columns = part.shape
    width = grads_all.shape[3]
    hidden = dgu.shape[3] // 2
    bf = jnp.bfloat16
    return pl.pallas_call(
        expert_grads_kernel,
        out_shape=(
            jax.ShapeDtypeStruct((2, half, columns), jnp.float32),
            jax.ShapeDtypeStruct((width, hidden), bf),
            jax.ShapeDtypeStruct((width, hidden), bf),
            jax.ShapeDtypeStruct((hidden, width), bf),
        ),
        in_specs=[ANY] * 5,
        out_specs=(VMEM,) * 4,
        scratch_shapes=[
            pltpu.VMEM((2, 2, half, width), bf),
            pltpu.VMEM((2, 2, half, 2 * hidden), bf),
            pltpu.VMEM((2, 2, half, hidden), bf),
            pltpu.VMEM((2, 2, half, width), bf),
            pltpu.VMEM((width, 2 * hidden), jnp.float32),
            pltpu.VMEM((hidden, width), jnp.float32),
            pltpu.SemaphoreType.DMA((16,)),
            pltpu.SemaphoreType.DMA((2, 4)),
        ]
        + scatter_scratch(1, half, columns),
        compiler_params=pltpu.CompilerParams(
            collective_id=4, has_side_effects=True, vmem_limit_bytes=VMEM_BYTES
        ),
        name="expert_grads",
    )(part.reshape(8, 2, 1, half, columns), rows_all, dgu, gua, grads_all)


def line_peers():
    line = lax.axis_index("dp")
    return (
        line,
        line + 1 - 2 * lax.rem(line, 2),
        line + 2 - 4 * lax.div(line, 2),
        3 - line,
    )


def line_remote(src, dst, send_sem, recv_sem, peer):
    return pltpu.make_async_remote_copy(
        src_ref=src,
        dst_ref=dst,
        send_sem=send_sem,
        recv_sem=recv_sem,
        device_id={"dp": peer},
        device_id_type=MESH,
    )


def full_barrier(plane, line):
    barrier = pltpu.get_barrier_semaphore()
    for peer in plane:
        pl.semaphore_signal(barrier, inc=1, device_id={"exp": peer}, device_id_type=MESH)
    for peer in line:
        pl.semaphore_signal(barrier, inc=1, device_id={"dp": peer}, device_id_type=MESH)
    pl.semaphore_wait(barrier, len(plane) + len(line))


def dense_gather_kernel(own, everything, stage, send, recv, local):
    me, sib, xn, yn = plane_peers()
    diag = xn + yn - me
    line = line_peers()
    into = pltpu.make_async_copy(own, stage, local.at[0])
    into.start()
    full_barrier((sib, xn, yn), line[1:])
    started = []

    def put(src, slot, turn, peer):
        copy = remote(
            src, everything.at[line[turn], slot], send.at[len(started)], recv.at[line[turn], slot], peer
        )
        copy.start()
        started.append(copy)

    def pass_on(slot, turn, peer):
        put(everything.at[line[turn], slot], slot, turn, peer)

    def wait(slot, turn):
        ref = everything.at[line[turn], slot]
        remote(ref, ref, send.at[0], recv.at[line[turn], slot], sib).wait_recv()

    put(own, me, 0, xn)
    put(own, me, 0, yn)
    for turn in (1, 2, 3):
        copy = line_remote(
            own, everything.at[line[0], me], send.at[len(started)], recv.at[line[0], me], line[turn]
        )
        copy.start()
        started.append(copy)
    put(own, me, 0, sib)
    into.wait()
    out = pltpu.make_async_copy(stage, everything.at[line[0], me], local.at[1])
    out.start()
    for turn in (0, 1, 2, 3):
        if turn > 0:
            wait(me, turn)
            for peer in (xn, yn, sib):
                pass_on(me, turn, peer)
        wait(xn, turn)
        if turn % 2 == 0:
            pass_on(xn, turn, yn)
        pass_on(xn, turn, sib)
        wait(yn, turn)
        if turn % 2 == 1:
            pass_on(yn, turn, xn)
        pass_on(yn, turn, sib)
        if turn > 0:
            wait(diag, turn - 1)
            pass_on(diag, turn - 1, sib)
    wait(diag, 3)
    pass_on(diag, 3, sib)
    for turn in (0, 1, 2, 3):
        for slot in (sib, xn + sib - me, yn + sib - me, diag + sib - me):
            wait(slot, turn)
    out.wait()
    for copy in started:
        copy.wait_send()


def dense_gather(own):
    rows, columns = own.shape
    return pl.pallas_call(
        dense_gather_kernel,
        out_shape=jax.ShapeDtypeStruct((4, 8, rows, columns), own.dtype),
        in_specs=[ANY],
        out_specs=ANY,
        scratch_shapes=[
            pltpu.VMEM((rows, columns), own.dtype),
            pltpu.SemaphoreType.DMA((32,)),
            pltpu.SemaphoreType.DMA((4, 8)),
            pltpu.SemaphoreType.DMA((2,)),
        ],
        compiler_params=pltpu.CompilerParams(
            collective_id=5, has_side_effects=True, vmem_limit_bytes=48 * 2**20
        ),
        name="dense_gather",
    )(own).reshape(32 * rows, columns)


class LineScatter:
    def __init__(self, scratch):
        self.sums, self.other, self.send, self.recv = scratch
        self.line = line_peers()

    def copy(self, turn):
        target = self.line[turn]
        return line_remote(
            self.sums.at[target],
            self.other.at[turn - 1],
            self.send.at[turn - 1],
            self.recv.at[turn - 1],
            target,
        )

    def write(self, half, part, rows, total):
        self.sums[2 * half + part, rows, :] = total.astype(self.sums.dtype)

    def begin(self):
        for turn in (1, 2, 3):
            self.copy(turn).start()

    def finish(self, outs):
        rows_all = outs[0].shape[0]
        for turn in (1, 2, 3):
            self.copy(turn).wait_recv()

        def one(index, carry):
            rows = pl.ds(pl.multiple_of(index * 16, 16), 16)
            total = self.sums[self.line[0], rows, :].astype(jnp.float32)
            for turn in (0, 1, 2):
                total = total + self.other[turn, rows, :].astype(jnp.float32)
            first = 0
            for out in outs:
                out[rows, :] = total[:, first : first + out.shape[1]]
                first += out.shape[1]
            return carry

        lax.fori_loop(0, rows_all // 16, one, 0)
        for turn in (1, 2, 3):
            self.copy(turn).wait_send()


LINE_REFS = 4


def line_scratch(rows, columns):
    bf = jnp.bfloat16
    return [
        pltpu.VMEM((4, rows, columns), bf),
        pltpu.VMEM((3, rows, columns), bf),
        pltpu.SemaphoreType.DMA((3,)),
        pltpu.SemaphoreType.DMA((3,)),
    ]


def dense_scatter_kernel(splits, *refs):
    groups, count = len(splits), sum(len(split) for split in splits)
    parts, outs, refs = refs[:groups], refs[groups : groups + count], refs[groups + count :]
    step_refs = 1 + SCATTER_REFS + LINE_REFS
    loads, planes, lines = [], [], []
    for index, part in enumerate(parts):
        some = refs[index * step_refs : (index + 1) * step_refs]
        plane = Scatter(
            lambda place, slot, half, part=part: part.at[half, :, slot], some[1 : 1 + SCATTER_REFS]
        )

        def load(step, part=part, plane=plane, sem=some[0]):
            slot, half, _, place = plane.place(step)
            return pltpu.make_async_copy(
                part.at[half, :, slot], plane.mine.at[place, half], sem.at[step]
            )

        loads.append(load)
        planes.append(plane)
        lines.append(LineScatter(some[1 + SCATTER_REFS :]))

    for plane, load in zip(planes, loads):

        def fetch(step, carry, plane=plane, load=load):
            @pl.when(plane.place(step)[2] == 0)
            def _():
                load(step).start()

            return carry

        lax.fori_loop(0, 16, fetch, 0)
    full_barrier(planes[0].peers(), lines[0].line[1:])
    for plane, load in zip(planes, loads):

        def one(step, carry, plane=plane, load=load):
            @pl.when(plane.place(step)[2] == 0)
            def _():
                load(step).wait()

            plane.depart(step)
            return carry

        lax.fori_loop(0, 16, one, 0)
    for plane in planes:
        plane.forward()
    for plane, line in zip(planes, lines):
        plane.finish(line.write)
        line.begin()
    for plane, line, split in zip(planes, lines, splits):
        line.finish(outs[: len(split)])
        outs = outs[len(split) :]
        plane.drain()


def dense_scatter(parts, splits):
    rows = parts[0].shape[0] // 32
    scratch = []
    for part in parts:
        scratch += [pltpu.SemaphoreType.DMA((16,))]
        scratch += scatter_scratch(2, rows, part.shape[1]) + line_scratch(rows, part.shape[1])
    shapes = [
        jax.ShapeDtypeStruct((rows, columns), jnp.float32) for split in splits for columns in split
    ]
    return pl.pallas_call(
        functools.partial(dense_scatter_kernel, splits),
        out_shape=shapes,
        in_specs=[ANY] * len(parts),
        out_specs=[VMEM] * len(shapes),
        scratch_shapes=scratch,
        compiler_params=pltpu.CompilerParams(
            collective_id=6, has_side_effects=True, vmem_limit_bytes=VMEM_BYTES
        ),
        name="dense_scatter",
    )(*(part.reshape(2, 2, 8, rows, part.shape[1]) for part in parts))


def rope(values, cosine, sine):
    return values * cosine + pltpu.roll(values, HD // 2, 1) * sine


def gain_rows(misc, out):
    for index in range(misc.shape[0] // 128):
        rows = pl.ds(index * 128, 128)
        out[:, rows] = jnp.transpose(misc[rows, :].astype(jnp.float32))


def inverse_rms(values):
    return lax.rsqrt(jnp.mean(values * values, axis=1, keepdims=True) + EPS)


def row_loop(count, chunk, body):
    def one(index, carry):
        body(pl.ds(pl.multiple_of(index * chunk, chunk), chunk))
        return carry

    lax.fori_loop(0, count // chunk, one, 0)


def tile_loop(count, tile, body):
    row_loop(count, tile, body)


ROW_CHUNK = 16
TILE = 256


def attend_kernel(q_heads, kv_heads, experts, tokens, dense_hbm, cosine, sine, bias, picked, rows_out, resid, heads, mixed, lse, prob, qkv_w, rest_w, gains, hidden, load):
    num_rows, width = tokens.shape
    group = q_heads // kv_heads
    q_cols = q_heads * HD
    loads = (
        pltpu.make_async_copy(dense_hbm.at[:, pl.ds(0, qkv_w.shape[1])], qkv_w, load.at[0]),
        pltpu.make_async_copy(
            dense_hbm.at[:, pl.ds(qkv_w.shape[1], rest_w.shape[1])], rest_w, load.at[1]
        ),
    )
    for copy in loads:
        copy.start()
    loads[1].wait()
    misc = rest_w.at[:, pl.ds(width, 128)]
    gain_rows(misc, gains)

    def norm_one(rows):
        value = tokens[rows, :].astype(jnp.float32)
        normed = value * inverse_rms(value)
        hidden[rows, :] = (normed * gains[experts : experts + 1, :]).astype(jnp.bfloat16)

    row_loop(num_rows, ROW_CHUNK, norm_one)
    loads[0].wait()

    def project(index, carry):
        cols = pl.ds(pl.multiple_of(index * TILE, TILE), TILE)
        raw = nn_dot(hidden[...], qkv_w[:, cols])
        turned = index < (q_heads + kv_heads) // 2
        cos_now = jnp.where(turned, cosine[...], 1.0)
        sin_now = jnp.where(turned, sine[...], 0.0)
        for part in (0, 1):
            value = rope(raw[:, part * HD : (part + 1) * HD], cos_now, sin_now)
            heads[2 * index + part] = value.astype(jnp.bfloat16)
        return carry

    lax.fori_loop(0, (q_heads + 2 * kv_heads) // 2, project, 0)
    lse[...] = jnp.zeros_like(lse)

    def head_step(head, carry):
        kv_head = q_heads + lax.div(head, group)
        cols = pl.ds(pl.multiple_of(head * HD, HD), HD)
        for first, keys in ((0, PROMPT), (PROMPT, num_rows)):
            rows = pl.ds(first, keys - first)
            query = heads[head, rows, :]
            score = nt_dot(query, heads[kv_head, :keys, :]) * HD ** (-0.5) + bias[rows, :keys]
            top = jnp.max(score, axis=1, keepdims=True)
            weight = jnp.exp(score - top)
            total = jnp.sum(weight, axis=1, keepdims=True)
            value = nn_dot(weight.astype(jnp.bfloat16), heads[kv_head + kv_heads, :keys, :])
            mixed[rows, cols] = (value / total).astype(jnp.bfloat16)
            lanes = lax.broadcasted_iota(jnp.int32, (keys - first, 128), 1)
            lse[rows, :] = jnp.where(lanes == head, top + jnp.log(total), lse[rows, :])
        return carry

    lax.fori_loop(0, q_heads, head_step, 0)

    def out_tile(cols):
        resid[:, cols] = tokens[:, cols].astype(jnp.float32) + nn_dot(mixed[...], rest_w[:, cols])

    tile_loop(width, TILE, out_tile)

    def norm_two(rows):
        value = resid[rows, :]
        normed = value * inverse_rms(value)
        rows_out[rows, :width] = (normed * gains[experts + 1 : experts + 2, :]).astype(jnp.bfloat16)

    row_loop(num_rows, ROW_CHUNK, norm_two)
    logits = nn_dot(rows_out[:, :width], misc[...])
    lanes = lax.broadcasted_iota(jnp.int32, logits.shape, 1)
    logits = jnp.where(lanes < experts, logits, NEG_BIG)
    weight = jnp.exp(logits - jnp.max(logits, axis=1, keepdims=True))
    value = weight / jnp.sum(weight, axis=1, keepdims=True)
    prob[...] = value
    chosen = value * picked[...]
    rows_out[:, width:] = (chosen / jnp.sum(chosen, axis=1, keepdims=True)).astype(jnp.bfloat16)


def attend(tokens, dense_w, cosine, sine, bias, picked, q_heads, kv_heads, experts):
    num_rows, width = tokens.shape
    bf = jnp.bfloat16
    all_heads = q_heads + 2 * kv_heads
    return pl.pallas_call(
        functools.partial(attend_kernel, q_heads, kv_heads, experts),
        out_shape=(
            jax.ShapeDtypeStruct((num_rows, width + 128), bf),
            jax.ShapeDtypeStruct((num_rows, width), jnp.float32),
            jax.ShapeDtypeStruct((all_heads, num_rows, HD), bf),
            jax.ShapeDtypeStruct((num_rows, q_heads * HD), bf),
            jax.ShapeDtypeStruct((num_rows, 128), jnp.float32),
            jax.ShapeDtypeStruct((num_rows, 128), jnp.float32),
        ),
        in_specs=[VMEM, ANY] + [VMEM] * 4,
        out_specs=(VMEM,) * 6,
        scratch_shapes=[
            pltpu.VMEM((width, all_heads * HD), bf),
            pltpu.VMEM((q_heads * HD, width + 128), bf),
            pltpu.VMEM((128, width), jnp.float32),
            pltpu.VMEM((num_rows, width), bf),
            pltpu.SemaphoreType.DMA((2,)),
        ],
        compiler_params=pltpu.CompilerParams(vmem_limit_bytes=VMEM_BYTES),
        name="attend",
    )(tokens, dense_w, cosine, sine, bias, picked)


def attend_back_kernel(q_heads, kv_heads, experts, back_hbm, grad_hbm, resid_hbm, rows_hbm, prob_hbm, picked_hbm, dense_hbm, mixed_hbm, heads_hbm, lse_hbm, bias_hbm, cos_hbm, sin_hbm, tokens_hbm, grad_in, out_part, qkv_part, back, grad, resid, hidden_two, prob, picked, dense, mixed, heads, lse, bias, cosine, sine, tokens, gains, gain_sums, grad_logit, grad_proj, grad_mixed, grad_qkv, grad_kv, load):
    num_rows, width = tokens.shape
    group = q_heads // kv_heads
    q_cols = q_heads * HD
    qkv_cols = q_cols + 2 * kv_heads * HD
    bf = jnp.bfloat16
    pairs = (
        (prob_hbm, prob),
        (picked_hbm, picked),
        (back_hbm, back),
        (dense_hbm, dense),
        (resid_hbm, resid),
        (grad_hbm, grad),
        (rows_hbm, hidden_two),
        (mixed_hbm, mixed),
        (heads_hbm, heads),
        (lse_hbm, lse),
        (bias_hbm, bias),
        (cos_hbm, cosine),
        (sin_hbm, sine),
        (tokens_hbm, tokens),
    )
    loads = [pltpu.make_async_copy(src, dst, load.at[i]) for i, (src, dst) in enumerate(pairs)]
    for copy in loads:
        copy.start()
    for copy in loads[:3]:
        copy.wait()
    gain_sums[...] = jnp.zeros_like(gain_sums)

    def router_rows(rows):
        value = prob[rows, :]
        chosen = value * picked[rows, :]
        total = jnp.sum(chosen, axis=1, keepdims=True)
        comb = chosen / total
        grad_comb = back[rows, width:]
        grad_chosen = (
            picked[rows, :] * (grad_comb - jnp.sum(grad_comb * comb, axis=1, keepdims=True)) / total
        )
        logit = value * (grad_chosen - jnp.sum(value * grad_chosen, axis=1, keepdims=True))
        grad_logit[rows, :] = logit.astype(bf)

    row_loop(num_rows, 64, router_rows)
    loads[3].wait()
    misc = dense.at[:, pl.ds(qkv_cols + width, 128)]
    gain_rows(misc, gains)
    lanes = lax.broadcasted_iota(jnp.int32, (TILE, 128), 1)

    def hidden_tile(cols):
        router = jnp.where(lanes < experts, misc[cols, :], jnp.zeros((), bf))
        back[:, cols] = back[:, cols] + nt_dot(grad_logit[...], router)

    tile_loop(width, TILE, hidden_tile)
    for copy in loads[4:]:
        copy.wait()

    def fold(values):
        return jnp.sum(values.reshape(-1, 8, width), axis=0)

    def norm_two(rows):
        value = resid[rows, :]
        inverse = inverse_rms(value)
        normed = value * inverse
        grad_hidden = back[rows, :width]
        gain_sums[8:16, :] = gain_sums[8:16, :] + fold(grad_hidden * normed)
        grad_norm = grad_hidden * gains[experts + 1 : experts + 2, :]
        mean = jnp.mean(grad_norm * normed, axis=1, keepdims=True)
        total = grad[rows, :] + inverse * (grad_norm - normed * mean)
        grad[rows, :] = total
        grad_proj[rows, :] = total.astype(bf)

    row_loop(num_rows, ROW_CHUNK, norm_two)

    def out_tile(cols):
        out_part[cols, :] = tn_dot(mixed[:, cols], grad_proj[...]).astype(bf)
        grad_mixed[:, cols] = nt_dot(
            grad_proj[...], dense[cols, pl.ds(qkv_cols, width)]
        ).astype(bf)

    tile_loop(q_cols, TILE, out_tile)
    scale = HD ** (-0.5)

    def head_step(head, carry):
        kv_head = lax.div(head, group)
        cols = pl.ds(pl.multiple_of(head * HD, HD), HD)

        @pl.when(lax.rem(head, group) == 0)
        def _():
            grad_kv[...] = jnp.zeros_like(grad_kv)

        for first, keys in ((0, PROMPT), (PROMPT, num_rows)):
            rows = pl.ds(first, keys - first)
            key = heads[q_heads + kv_head, :keys, :]
            query = heads[head, rows, :]
            up = grad_mixed[rows, cols]
            lane = lax.broadcasted_iota(jnp.int32, (keys - first, 128), 1)
            total = jnp.sum(jnp.where(lane == head, lse[rows, :], 0.0), axis=1, keepdims=True)
            weight = jnp.exp(nt_dot(query, key) * scale + bias[rows, :keys] - total)
            grad_weight = nt_dot(up, heads[q_heads + kv_heads + kv_head, :keys, :])
            delta = jnp.sum(weight * grad_weight, axis=1, keepdims=True)
            score = (weight * (grad_weight - delta)).astype(bf)
            grad_kv[1, :keys, :] = grad_kv[1, :keys, :] + tn_dot(weight.astype(bf), up)
            grad_kv[0, :keys, :] = grad_kv[0, :keys, :] + tn_dot(score, query) * scale
            value = rope(nn_dot(score, key) * scale, cosine[rows, :], -sine[rows, :])
            grad_qkv[rows, cols] = value.astype(bf)

        @pl.when(lax.rem(head, group) == group - 1)
        def _():
            key_cols = pl.ds(pl.multiple_of(q_cols + kv_head * HD, HD), HD)
            value_cols = pl.ds(pl.multiple_of(q_cols + (kv_heads + kv_head) * HD, HD), HD)
            grad_qkv[:, key_cols] = rope(grad_kv[0], cosine[...], -sine[...]).astype(bf)
            grad_qkv[:, value_cols] = grad_kv[1].astype(bf)

        return carry

    lax.fori_loop(0, q_heads, head_step, 0)
    hidden = grad_mixed

    def norm_one(rows):
        value = tokens[rows, :].astype(jnp.float32)
        normed = value * inverse_rms(value)
        hidden[rows, :] = (normed * gains[experts : experts + 1, :]).astype(bf)

    row_loop(num_rows, ROW_CHUNK, norm_one)

    def hidden_back_tile(cols):
        back[:, cols] = nt_dot(grad_qkv[...], dense[cols, pl.ds(0, qkv_cols)])

    tile_loop(width, TILE, hidden_back_tile)

    def last_rows(rows):
        value = tokens[rows, :].astype(jnp.float32)
        inverse = inverse_rms(value)
        normed = value * inverse
        grad_hidden = back[rows, :width]
        gain_sums[0:8, :] = gain_sums[0:8, :] + fold(grad_hidden * normed)
        grad_norm = grad_hidden * gains[experts : experts + 1, :]
        mean = jnp.mean(grad_norm * normed, axis=1, keepdims=True)
        grad_in[rows, :] = grad[rows, :] + inverse * (grad_norm - normed * mean)

    row_loop(num_rows, ROW_CHUNK, last_rows)
    gains[0:16, :] = gain_sums[...]

    def weight_tile(cols):
        qkv_part[cols, :qkv_cols] = tn_dot(hidden[:, cols], grad_qkv[...]).astype(bf)
        router = tn_dot(hidden_two[:, cols], grad_logit[...])
        one = jnp.sum(gains[0:8, cols], axis=0, keepdims=True)
        two = jnp.sum(gains[8:16, cols], axis=0, keepdims=True)
        place = lax.broadcasted_iota(jnp.int32, (128, TILE), 0)
        block = jnp.where(place == experts, one, jnp.where(place == experts + 1, two, 0.0))
        qkv_part[cols, qkv_cols:] = (router + jnp.transpose(block)).astype(bf)

    tile_loop(width, TILE, weight_tile)


def attend_back(back, grad, resid, rows_own, prob, picked, dense_w, mixed, heads, lse, bias, cosine, sine, tokens, q_heads, kv_heads, experts):
    num_rows, width = tokens.shape
    bf = jnp.bfloat16
    arrays = (back, grad, resid, rows_own, prob, picked, dense_w, mixed, heads, lse, bias, cosine, sine, tokens)
    qkv_cols = (q_heads + 2 * kv_heads) * HD
    q_cols = q_heads * HD
    return pl.pallas_call(
        functools.partial(attend_back_kernel, q_heads, kv_heads, experts),
        out_shape=(
            jax.ShapeDtypeStruct((num_rows, width), jnp.float32),
            jax.ShapeDtypeStruct((q_cols, width), bf),
            jax.ShapeDtypeStruct((width, qkv_cols + 128), bf),
        ),
        in_specs=[ANY] * len(arrays),
        out_specs=(VMEM,) * 3,
        scratch_shapes=[pltpu.VMEM(array.shape, array.dtype) for array in arrays]
        + [
            pltpu.VMEM((128, width), jnp.float32),
            pltpu.VMEM((16, width), jnp.float32),
            pltpu.VMEM((num_rows, 128), bf),
            pltpu.VMEM((num_rows, width), bf),
            pltpu.VMEM((num_rows, q_cols), bf),
            pltpu.VMEM((num_rows, qkv_cols), bf),
            pltpu.VMEM((2, num_rows, HD), jnp.float32),
            pltpu.SemaphoreType.DMA((len(arrays),)),
        ],
        compiler_params=pltpu.CompilerParams(vmem_limit_bytes=63 * 2**20),
        name="attend_back",
    )(*arrays)


def body_plane(
    tokens,
    targets,
    valid_count,
    segments,
    routes,
    gain_attn,
    w_query,
    w_key,
    w_value,
    w_out,
    gain_moe,
    w_router,
    w_gate,
    w_up,
    w_down,
):
    bf = jnp.bfloat16
    num_rows, width = tokens.shape
    half = num_rows // 2
    q_cols, k_cols = w_query.shape[1], w_key.shape[1]
    num_experts = w_router.shape[1]
    num_heads = q_cols // HD
    kv_heads = k_cols // HD
    pad_cols = 128 - 2 - num_experts
    dense_own = jnp.concatenate(
        [
            w_query,
            w_key,
            w_value,
            w_out,
            w_router,
            gain_attn[:, None],
            gain_moe[:, None],
            jnp.zeros((gain_attn.shape[0], pad_cols), bf),
        ],
        axis=1,
    )
    dense_w = dense_gather(dense_own)
    gate_w = lax.all_gather(w_gate, "dp", axis=1, tiled=True)[0]
    up_w = lax.all_gather(w_up, "dp", axis=1, tiled=True)[0]
    down_w = lax.all_gather(w_down, "dp", axis=1, tiled=True)[0]
    tok_pos = positions(segments)
    bias = jnp.where(key_mask(segments), 0.0, NEG_BIG)
    freq = THETA ** (-2.0 * jnp.arange(HD // 2, dtype=jnp.float32) / HD)
    angle = tok_pos.astype(jnp.float32)[:, None] * freq[None, :]
    cosine, sine_part = jnp.cos(angle), jnp.sin(angle)
    cosine = jnp.concatenate([cosine, cosine], axis=1)
    sine = jnp.concatenate([-sine_part, sine_part], axis=1)
    lane_ids = jnp.arange(128, dtype=jnp.int32)
    picked = jnp.sum((routes[:, :, None] == lane_ids[None, None, :]).astype(jnp.float32), axis=1)
    rows_own, resid_mid, heads, mixed, lse, prob = attend(
        tokens, dense_w, cosine, sine, bias, picked, num_heads, kv_heads, num_experts
    )
    rows_all, gua = expert_in(rows_own.reshape(2, half, width + 128), gate_w, up_w)
    total_rows = num_rows * lax.axis_size(("dp", "exp"))
    global_row = lax.axis_index(("dp", "exp")) * num_rows + jnp.arange(num_rows, dtype=jnp.int32)
    loss_scale = total_rows / valid_count[0].astype(jnp.float32)
    scales = jnp.broadcast_to(
        jnp.where(global_row < valid_count[0], loss_scale, 0.0)[:, None], (num_rows, 128)
    )
    layer_out, grad_out, grad_out_b = expert_out(gua, down_w, resid_mid, targets, scales)
    layer_out = layer_out.reshape(num_rows, width)
    grads_all, dgu, part = expert_back(grad_out_b, rows_all, gua, gate_w, up_w, down_w)
    back, *expert_parts = expert_grads(part, rows_all, dgu, gua, grads_all)
    expert_sums = tuple(
        lax.psum_scatter(grad[None], "dp", scatter_dimension=1, tiled=True).astype(jnp.float32)
        for grad in expert_parts
    )
    grad_in, out_part, qkv_part = attend_back(
        back.reshape(num_rows, width + 128),
        grad_out.reshape(num_rows, width),
        resid_mid,
        rows_own,
        prob,
        picked,
        dense_w,
        mixed,
        heads,
        lse,
        bias,
        cosine,
        sine,
        tokens,
        num_heads,
        kv_heads,
        num_experts,
    )
    out_sum, q_sum, k_sum, v_sum, misc_sum = dense_scatter(
        (out_part, qkv_part), ((width,), (q_cols, k_cols, k_cols, 128))
    )
    return (
        layer_out,
        grad_in,
        misc_sum[:, num_experts],
        q_sum,
        k_sum,
        v_sum,
        out_sum,
        misc_sum[:, num_experts + 1],
        misc_sum[:, :num_experts],
        *expert_sums,
    )


def solution(mesh):
    in_specs = (
        P(("dp", "exp"), None),
        P(("dp", "exp"), None),
        P(),
        P(("dp", "exp")),
        P(("dp", "exp"), None),
        P(("dp", "exp")),
        P(("dp", "exp"), None),
        P(("dp", "exp"), None),
        P(("dp", "exp"), None),
        P(("dp", "exp"), None),
        P(("dp", "exp")),
        P(("dp", "exp"), None),
        P("exp", "dp", None),
        P("exp", "dp", None),
        P("exp", "dp", None),
    )
    out_specs = (
        P(("dp", "exp"), None),
        P(("dp", "exp"), None),
        P(("dp", "exp")),
        P(("dp", "exp"), None),
        P(("dp", "exp"), None),
        P(("dp", "exp"), None),
        P(("dp", "exp"), None),
        P(("dp", "exp")),
        P(("dp", "exp"), None),
        P("exp", "dp", None),
        P("exp", "dp", None),
        P("exp", "dp", None),
    )
    body = body_plane if (mesh.shape["dp"], mesh.shape["exp"]) == (4, 8) else body_general
    return jax.shard_map(body, mesh=mesh, in_specs=in_specs, out_specs=out_specs, check_vma=False)
```

```python
import functools

import jax
import jax.numpy as jnp
from jax import lax
from jax.experimental import pallas as pl
from jax.experimental.pallas import tpu as pltpu
from jax.sharding import PartitionSpec as P

HD = 128
PROMPT = 256
NCONT = 2


EPS = 1e-06
THETA = 10000.0
HIGH = lax.Precision.HIGHEST
NEG_BIG = -1e30


def positions(segments):
    count_rows = segments.shape[0]
    row_ids = jnp.arange(count_rows, dtype=jnp.int32)
    labels = jnp.arange(NCONT + 1, dtype=jnp.int32)
    member = segments[:, None] == labels[None, :]
    first_row = jnp.min(jnp.where(member, row_ids[:, None], count_rows), axis=0)
    start_row = jnp.sum(jnp.where(member, first_row[None, :], 0), axis=1)
    return jnp.where(segments == 0, row_ids, PROMPT + row_ids - start_row)


def key_mask(segments):
    row_ids = jnp.arange(segments.shape[0], dtype=jnp.int32)
    causal = row_ids[None, :] <= row_ids[:, None]
    visible = (segments[None, :] == 0) | (segments[None, :] == segments[:, None])
    return causal & visible


def rotate(values, pos_rows, sign_value):
    half_size = HD // 2
    freq = THETA ** (-2.0 * jnp.arange(half_size, dtype=jnp.float32) / HD)
    angle = pos_rows.astype(jnp.float32)[:, None] * freq[None, :]
    cosine = jnp.cos(angle)[:, None, :]
    sine_part = sign_value * jnp.sin(angle)[:, None, :]
    first_half = values[..., :half_size]
    second = values[..., half_size:]
    return jnp.concatenate(
        [first_half * cosine - second * sine_part, second * cosine + first_half * sine_part],
        axis=-1,
    )


def attention_scores(query_b, key_b, allowed):
    logits = jnp.einsum(
        "qkgd,pkd->kgqp", query_b, key_b, preferred_element_type=jnp.float32
    ) * HD ** (-0.5)
    return jnp.where(allowed[None, None], logits, NEG_BIG)


def expert_gates(rows_in, gate_w, up_w):
    gate_val = jnp.einsum("sacd,adf->sacf", rows_in, gate_w, preferred_element_type=jnp.float32)
    up_val = jnp.einsum("sacd,adf->sacf", rows_in, up_w, preferred_element_type=jnp.float32)
    return (gate_val, up_val)


def body_general(
    tokens,
    targets,
    valid_count,
    segments,
    routes,
    gain_attn,
    w_query,
    w_key,
    w_value,
    w_out,
    gain_moe,
    w_router,
    w_gate,
    w_up,
    w_down,
):
    gain_one, query_w, key_w, value_w, out_w, gain_two, router_w = (
        lax.all_gather(gain_attn, ("dp", "exp"), axis=0, tiled=True),
        lax.all_gather(w_query, ("dp", "exp"), axis=0, tiled=True),
        lax.all_gather(w_key, ("dp", "exp"), axis=0, tiled=True),
        lax.all_gather(w_value, ("dp", "exp"), axis=0, tiled=True),
        lax.all_gather(w_out, ("dp", "exp"), axis=0, tiled=True),
        lax.all_gather(gain_moe, ("dp", "exp"), axis=0, tiled=True),
        lax.all_gather(w_router, ("dp", "exp"), axis=0, tiled=True),
    )
    gate_w, up_w, down_w = (
        lax.all_gather(w_gate, "dp", axis=1, tiled=True),
        lax.all_gather(w_up, "dp", axis=1, tiled=True),
        lax.all_gather(w_down, "dp", axis=1, tiled=True),
    )
    num_rows = tokens.shape[0]
    width = tokens.shape[1]
    num_heads = query_w.shape[1] // HD
    kv_heads = key_w.shape[1] // HD
    group_size = num_heads // kv_heads
    num_experts = router_w.shape[1]
    top_count = routes.shape[1]
    exp_local = gate_w.shape[0]
    exp_ranks = lax.axis_size("exp")
    capacity = 5 * num_rows * top_count // (4 * num_experts)
    tok_pos = positions(segments)
    allowed = key_mask(segments)
    resid_in = tokens.astype(jnp.float32)
    inv_one = lax.rsqrt(jnp.mean(resid_in * resid_in, axis=-1, keepdims=True) + EPS)
    normed_one = resid_in * inv_one
    hidden_one = (normed_one * gain_one.astype(jnp.float32)).astype(jnp.bfloat16)
    query_raw = jnp.dot(hidden_one, query_w, preferred_element_type=jnp.float32)
    key_raw = jnp.dot(hidden_one, key_w, preferred_element_type=jnp.float32)
    value_b = jnp.dot(hidden_one, value_w, preferred_element_type=jnp.float32).astype(jnp.bfloat16)
    query_b = rotate(query_raw.reshape(num_rows, num_heads, HD), tok_pos, 1.0).astype(jnp.bfloat16)
    query_b = query_b.reshape(num_rows, kv_heads, group_size, HD)
    key_b = rotate(key_raw.reshape(num_rows, kv_heads, HD), tok_pos, 1.0).astype(jnp.bfloat16)
    value_h = value_b.reshape(num_rows, kv_heads, HD)
    logit_att = attention_scores(query_b, key_b, allowed)
    row_max = jnp.max(logit_att, axis=-1, keepdims=True)
    log_total = row_max + jnp.log(jnp.sum(jnp.exp(logit_att - row_max), axis=-1, keepdims=True))
    probs_b = jnp.exp(logit_att - log_total).astype(jnp.bfloat16)
    attn_vals = jnp.einsum("kgqp,pkd->qkgd", probs_b, value_h, preferred_element_type=jnp.float32)
    attn_vals = attn_vals.reshape(num_rows, num_heads * HD).astype(jnp.bfloat16)
    resid_mid = resid_in + jnp.dot(attn_vals, out_w, preferred_element_type=jnp.float32)
    inv_two = lax.rsqrt(jnp.mean(resid_mid * resid_mid, axis=-1, keepdims=True) + EPS)
    normed_two = resid_mid * inv_two
    gain_two_f = gain_two.astype(jnp.float32)
    hidden_two = (normed_two * gain_two_f).astype(jnp.bfloat16)
    router_prob = jax.nn.softmax(
        jnp.dot(hidden_two, router_w, preferred_element_type=jnp.float32), axis=-1
    )
    expert_ids = jnp.arange(num_experts, dtype=jnp.int32)
    route_hot = routes[:, :, None] == expert_ids[None, None, :]
    chosen = jnp.sum(jnp.where(route_hot, router_prob[:, None, :], 0.0), axis=-1)
    weight_sum = jnp.sum(chosen, axis=1, keepdims=True)
    combine = chosen / weight_sum
    flat_hot = route_hot.reshape(num_rows * top_count, num_experts).astype(jnp.int32)
    slot_index = jnp.sum((jnp.cumsum(flat_hot, axis=0) - flat_hot) * flat_hot, axis=1)
    dest_index = routes.reshape(-1) * capacity + slot_index
    send_shape = (exp_ranks, exp_local, capacity, width)
    send_rows = jnp.zeros((num_experts * capacity, width), jnp.bfloat16)
    send_rows = (
        send_rows.at[dest_index].set(jnp.repeat(hidden_two, top_count, axis=0)).reshape(send_shape)
    )
    gate_val, up_val = expert_gates(
        lax.all_to_all(send_rows, "exp", split_axis=0, concat_axis=0, tiled=True), gate_w, up_w
    )
    act_b = (jax.nn.relu(gate_val) * up_val).astype(jnp.bfloat16)
    out_b = jnp.einsum("sacf,afd->sacd", act_b, down_w, preferred_element_type=jnp.float32).astype(
        jnp.bfloat16
    )
    returned = lax.all_to_all(out_b, "exp", split_axis=0, concat_axis=0, tiled=True)
    route_out = returned.reshape(num_experts * capacity, width)[dest_index].reshape(
        num_rows, top_count, width
    )
    route_out_f = route_out.astype(jnp.float32)
    resid_out = resid_mid + jnp.sum(combine[:, :, None] * route_out_f, axis=1)
    layer_out = resid_out.astype(jnp.bfloat16)
    total_rows = num_rows * lax.axis_size(("dp", "exp"))
    global_row = lax.axis_index(("dp", "exp")) * num_rows + jnp.arange(num_rows, dtype=jnp.int32)
    loss_scale = total_rows / valid_count[0].astype(jnp.float32)
    grad_out = jnp.where(
        (global_row < valid_count[0])[:, None],
        (resid_out - targets.astype(jnp.float32)) * loss_scale,
        0.0,
    )
    gain_one, query_w, key_w, value_w, out_w, gain_two, router_w = (
        lax.all_gather(gain_attn, ("dp", "exp"), axis=0, tiled=True),
        lax.all_gather(w_query, ("dp", "exp"), axis=0, tiled=True),
        lax.all_gather(w_key, ("dp", "exp"), axis=0, tiled=True),
        lax.all_gather(w_value, ("dp", "exp"), axis=0, tiled=True),
        lax.all_gather(w_out, ("dp", "exp"), axis=0, tiled=True),
        lax.all_gather(gain_moe, ("dp", "exp"), axis=0, tiled=True),
        lax.all_gather(w_router, ("dp", "exp"), axis=0, tiled=True),
    )
    gain_two_f = gain_two.astype(jnp.float32)
    grad_route = (combine[:, :, None] * grad_out[:, None, :]).astype(jnp.bfloat16)
    grad_comb = jnp.sum(grad_out[:, None, :] * route_out_f, axis=-1)
    grad_send = jnp.zeros((num_experts * capacity, width), jnp.bfloat16)
    grad_send = (
        grad_send.at[dest_index]
        .set(grad_route.reshape(num_rows * top_count, width))
        .reshape(send_shape)
    )
    expert_rows, grad_recv = (
        lax.all_to_all(send_rows, "exp", split_axis=0, concat_axis=0, tiled=True),
        lax.all_to_all(grad_send, "exp", split_axis=0, concat_axis=0, tiled=True),
    )
    gate_val, up_val = expert_gates(expert_rows, gate_w, up_w)
    gate_relu = jax.nn.relu(gate_val)
    act_b = (gate_relu * up_val).astype(jnp.bfloat16)
    grad_act = jnp.einsum("sacd,afd->sacf", grad_recv, down_w, preferred_element_type=jnp.float32)
    grad_down_w = jnp.einsum("sacf,sacd->afd", act_b, grad_recv, preferred_element_type=jnp.float32)
    grad_gate_b = jnp.where(gate_val > 0, grad_act * up_val, 0.0).astype(jnp.bfloat16)
    grad_up_b = (grad_act * gate_relu).astype(jnp.bfloat16)
    grad_gate_w = jnp.einsum(
        "sacd,sacf->adf", expert_rows, grad_gate_b, preferred_element_type=jnp.float32
    )
    grad_up_w = jnp.einsum(
        "sacd,sacf->adf", expert_rows, grad_up_b, preferred_element_type=jnp.float32
    )
    grad_rows = (
        jnp.einsum("sacf,adf->sacd", grad_gate_b, gate_w, preferred_element_type=jnp.float32)
        + jnp.einsum("sacf,adf->sacd", grad_up_b, up_w, preferred_element_type=jnp.float32)
    ).astype(jnp.bfloat16)
    grad_back = lax.all_to_all(grad_rows, "exp", split_axis=0, concat_axis=0, tiled=True)
    grad_copies = grad_back.reshape(num_experts * capacity, width)[dest_index].reshape(
        num_rows, top_count, width
    )
    grad_hidden_two = jnp.sum(grad_copies.astype(jnp.float32), axis=1)
    grad_chosen = (grad_comb - jnp.sum(grad_comb * combine, axis=1, keepdims=True)) / weight_sum
    grad_prob = jnp.sum(jnp.where(route_hot, grad_chosen[:, :, None], 0.0), axis=1)
    grad_logit = router_prob * (
        grad_prob - jnp.sum(router_prob * grad_prob, axis=-1, keepdims=True)
    )
    router_f = router_w.astype(jnp.float32)
    grad_hidden_two = grad_hidden_two + jnp.einsum(
        "re,de->rd", grad_logit, router_f, precision=HIGH
    )
    grad_router = jnp.einsum(
        "rd,re->de", hidden_two.astype(jnp.float32), grad_logit, precision=HIGH
    )
    grad_gain_two = jnp.sum(grad_hidden_two * normed_two, axis=0)
    grad_norm_two = grad_hidden_two * gain_two_f
    grad_mid = grad_out + inv_two * (
        grad_norm_two - normed_two * jnp.mean(grad_norm_two * normed_two, axis=-1, keepdims=True)
    )
    grad_proj_b = grad_mid.astype(jnp.bfloat16)
    grad_out_w = jnp.einsum("rh,rd->hd", attn_vals, grad_proj_b, preferred_element_type=jnp.float32)
    grad_vals_b = jnp.einsum(
        "rd,hd->rh", grad_proj_b, out_w, preferred_element_type=jnp.float32
    ).astype(jnp.bfloat16)
    grad_vals_b = grad_vals_b.reshape(num_rows, kv_heads, group_size, HD)
    logit_att = attention_scores(query_b, key_b, allowed)
    probs = jnp.exp(logit_att - log_total)
    probs_b = probs.astype(jnp.bfloat16)
    grad_value = jnp.einsum(
        "kgqp,qkgd->pkd", probs_b, grad_vals_b, preferred_element_type=jnp.float32
    )
    grad_prob_att = jnp.einsum(
        "qkgd,pkd->kgqp", grad_vals_b, value_h, preferred_element_type=jnp.float32
    )
    delta_row = jnp.sum(probs * grad_prob_att, axis=-1, keepdims=True)
    grad_score_b = (probs * (grad_prob_att - delta_row)).astype(jnp.bfloat16)
    grad_query = jnp.einsum(
        "kgqp,pkd->qkgd", grad_score_b, key_b, preferred_element_type=jnp.float32
    ) * HD ** (-0.5)
    grad_key = jnp.einsum(
        "kgqp,qkgd->pkd", grad_score_b, query_b, preferred_element_type=jnp.float32
    ) * HD ** (-0.5)
    grad_query_b = rotate(grad_query.reshape(num_rows, num_heads, HD), tok_pos, -1.0).astype(
        jnp.bfloat16
    )
    grad_query_b = grad_query_b.reshape(num_rows, num_heads * HD)
    grad_key_b = (
        rotate(grad_key, tok_pos, -1.0).astype(jnp.bfloat16).reshape(num_rows, kv_heads * HD)
    )
    grad_value_b = grad_value.astype(jnp.bfloat16).reshape(num_rows, kv_heads * HD)
    grad_query_w = jnp.einsum(
        "rd,rh->dh", hidden_one, grad_query_b, preferred_element_type=jnp.float32
    )
    grad_key_w = jnp.einsum("rd,rh->dh", hidden_one, grad_key_b, preferred_element_type=jnp.float32)
    grad_value_w = jnp.einsum(
        "rd,rh->dh", hidden_one, grad_value_b, preferred_element_type=jnp.float32
    )
    grad_hidden_one = (
        jnp.einsum("rh,dh->rd", grad_query_b, query_w, preferred_element_type=jnp.float32)
        + jnp.einsum("rh,dh->rd", grad_key_b, key_w, preferred_element_type=jnp.float32)
        + jnp.einsum("rh,dh->rd", grad_value_b, value_w, preferred_element_type=jnp.float32)
    )
    grad_gain_one = jnp.sum(grad_hidden_one * normed_one, axis=0)
    grad_norm_one = grad_hidden_one * gain_one.astype(jnp.float32)
    grad_in = grad_mid + inv_one * (
        grad_norm_one - normed_one * jnp.mean(grad_norm_one * normed_one, axis=-1, keepdims=True)
    )
    dense_sums = (
        lax.psum_scatter(grad_gain_one, ("dp", "exp"), scatter_dimension=0, tiled=True),
        lax.psum_scatter(grad_query_w, ("dp", "exp"), scatter_dimension=0, tiled=True),
        lax.psum_scatter(grad_key_w, ("dp", "exp"), scatter_dimension=0, tiled=True),
        lax.psum_scatter(grad_value_w, ("dp", "exp"), scatter_dimension=0, tiled=True),
        lax.psum_scatter(grad_out_w, ("dp", "exp"), scatter_dimension=0, tiled=True),
        lax.psum_scatter(grad_gain_two, ("dp", "exp"), scatter_dimension=0, tiled=True),
        lax.psum_scatter(grad_router, ("dp", "exp"), scatter_dimension=0, tiled=True),
    )
    expert_sums = (
        lax.psum_scatter(
            grad_gate_w.astype(jnp.bfloat16), "dp", scatter_dimension=1, tiled=True
        ).astype(jnp.float32),
        lax.psum_scatter(
            grad_up_w.astype(jnp.bfloat16), "dp", scatter_dimension=1, tiled=True
        ).astype(jnp.float32),
        lax.psum_scatter(
            grad_down_w.astype(jnp.bfloat16), "dp", scatter_dimension=1, tiled=True
        ).astype(jnp.float32),
    )
    return (
        layer_out,
        grad_in,
        dense_sums[0],
        dense_sums[1],
        dense_sums[2],
        dense_sums[3],
        dense_sums[4],
        dense_sums[5],
        dense_sums[6],
        expert_sums[0],
        expert_sums[1],
        expert_sums[2],
    )


MESH = pl.DeviceIdType.MESH
ANY = pl.BlockSpec(memory_space=pl.ANY)
VMEM = pl.BlockSpec(memory_space=pltpu.VMEM)
VMEM_BYTES = 62 * 2**20


def nn_dot(left, right):
    return jnp.dot(left, right, preferred_element_type=jnp.float32)


def nt_dot(left, right):
    return lax.dot_general(
        left, right, (((1,), (1,)), ((), ())), preferred_element_type=jnp.float32
    )


def tn_dot(left, right):
    return lax.dot_general(
        left, right, (((0,), (0,)), ((), ())), preferred_element_type=jnp.float32
    )


def plane_peers():
    me = lax.axis_index("exp")
    core = lax.rem(me, 2)
    x_pos = lax.rem(lax.div(me, 2), 2)
    y_pos = lax.div(me, 4)
    return me, me + 1 - 2 * core, me + 2 - 4 * x_pos, me + 4 - 8 * y_pos


def remote(src, dst, send_sem, recv_sem, peer):
    return pltpu.make_async_remote_copy(
        src_ref=src,
        dst_ref=dst,
        send_sem=send_sem,
        recv_sem=recv_sem,
        device_id={"exp": peer},
        device_id_type=MESH,
    )


def plane_barrier(peers):
    barrier = pltpu.get_barrier_semaphore()
    for peer in peers:
        pl.semaphore_signal(barrier, inc=1, device_id={"exp": peer}, device_id_type=MESH)
    pl.semaphore_wait(barrier, len(peers))


def step_place(step, quad):
    odd = lax.rem(step, 2)
    last = lax.div(quad, 3)
    mid = lax.rem(lax.div(quad + 1, 2), 2)
    return mid * (1 - odd) + last, mid * odd + last


class Gather:
    def __init__(self, own, buf, send, recv):
        self.own, self.buf, self.send, self.recv = own, buf, send, recv
        self.me, self.sib, self.xn, self.yn = plane_peers()
        self.diag = self.xn + self.yn - self.me

    def own_copy(self, half, peer, sem):
        return remote(
            self.own.at[half],
            self.buf.at[self.me, half],
            self.send.at[sem],
            self.recv.at[self.me, half],
            peer,
        )

    def pass_copy(self, slot, half, peer, sem):
        return remote(
            self.buf.at[slot, half],
            self.buf.at[slot, half],
            self.send.at[sem],
            self.recv.at[slot, half],
            peer,
        )

    def own_copies(self):
        return (
            self.own_copy(0, self.xn, 0),
            self.own_copy(1, self.yn, 1),
            self.own_copy(0, self.sib, 2),
            self.own_copy(1, self.sib, 3),
            self.own_copy(1, self.xn, 4),
            self.own_copy(0, self.yn, 5),
        )

    def near_copies(self):
        return (
            self.pass_copy(self.xn, 0, self.yn, 6),
            self.pass_copy(self.yn, 1, self.xn, 7),
            self.pass_copy(self.xn, 0, self.sib, 8),
            self.pass_copy(self.yn, 1, self.sib, 9),
        )

    def late_copies(self):
        return (
            self.pass_copy(self.xn, 1, self.sib, 10),
            self.pass_copy(self.yn, 0, self.sib, 11),
        )

    def far_copies(self):
        return (
            self.pass_copy(self.diag, 0, self.sib, 12),
            self.pass_copy(self.diag, 1, self.sib, 13),
        )

    def wait_block(self, slot, half):
        self.pass_copy(slot, half, self.sib, 0).wait_recv()

    def begin(self):
        plane_barrier((self.sib, self.xn, self.yn))
        for copy in self.own_copies():
            copy.start()

    def place(self, step):
        quad = lax.div(step, 4)
        far_x, far_y = step_place(step, quad)
        odd = lax.rem(step, 2)
        third = lax.div(quad, 2) * (1 - lax.div(quad, 3))
        other = lax.div(lax.rem(step, 4), 2)
        slot = (
            self.me
            + far_x * (self.xn - self.me)
            + far_y * (self.yn - self.me)
            + other * (self.sib - self.me)
        )
        return slot, odd + third * (1 - 2 * odd), other

    def arrive(self, step):
        @pl.when(step == 4)
        def _():
            self.wait_block(self.xn, 0)
            self.wait_block(self.yn, 1)
            for copy in self.near_copies():
                copy.start()

        @pl.when(step == 8)
        def _():
            self.wait_block(self.xn, 1)
            self.wait_block(self.yn, 0)
            for copy in self.late_copies():
                copy.start()

        @pl.when(step == 12)
        def _():
            self.wait_block(self.diag, 0)
            self.wait_block(self.diag, 1)
            for copy in self.far_copies():
                copy.start()

        slot, half, other = self.place(step)

        @pl.when(other == 1)
        def _():
            self.wait_block(slot, half)

        return slot, half

    def finish(self):
        for copies in (self.own_copies(), self.near_copies(), self.late_copies(), self.far_copies()):
            for copy in copies:
                copy.wait_send()


def expert_in_kernel(own, gate_hbm, up_hbm, rows_out, gua_out, buf, gua, gate_w, up_w, send, recv, load, store_a, store_b):
    width, hidden = gate_w.shape
    gather = Gather(own, buf, send, recv)
    loads = (
        pltpu.make_async_copy(gate_hbm, gate_w, load.at[0]),
        pltpu.make_async_copy(up_hbm, up_w, load.at[1]),
        pltpu.make_async_copy(own.at[0], buf.at[gather.me, 0], load.at[2]),
        pltpu.make_async_copy(own.at[1], buf.at[gather.me, 1], load.at[3]),
    )
    for copy in loads:
        copy.start()
    gather.begin()
    for copy in loads:
        copy.wait()

    def row_store(slot, half, step):
        return pltpu.make_async_copy(buf.at[slot, half], rows_out.at[slot, half], store_a.at[step])

    def gua_store(slot, half, step):
        return pltpu.make_async_copy(gua.at[slot, half], gua_out.at[slot, half], store_b.at[step])

    def one(step, carry):
        slot, half = gather.arrive(step)
        row_store(slot, half, step).start()
        rows = buf[slot, half, :, :width]
        lanes = lax.broadcasted_iota(jnp.int32, (buf.shape[2], 128), 1)
        tail = buf[slot, half, :, width:].astype(jnp.float32)
        weight = jnp.sum(jnp.where(lanes == gather.me, tail, 0.0), axis=1, keepdims=True)
        gate_val = nn_dot(rows, gate_w[...])
        up_val = nn_dot(rows, up_w[...])
        gua[slot, half, :, :hidden] = gate_val.astype(jnp.bfloat16)
        gua[slot, half, :, hidden : 2 * hidden] = up_val.astype(jnp.bfloat16)
        act_val = jnp.maximum(gate_val, 0.0) * up_val * weight
        gua[slot, half, :, 2 * hidden :] = act_val.astype(jnp.bfloat16)
        gua_store(slot, half, step).start()
        return carry

    lax.fori_loop(0, 16, one, 0)
    gather.finish()

    def drain(step, carry):
        slot, half, _ = gather.place(step)
        row_store(slot, half, step).wait()
        gua_store(slot, half, step).wait()
        return carry

    lax.fori_loop(0, 16, drain, 0)


def expert_in(own, gate_w, up_w):
    _, half, columns = own.shape
    width, hidden = gate_w.shape
    bf = jnp.bfloat16
    return pl.pallas_call(
        expert_in_kernel,
        out_shape=(
            jax.ShapeDtypeStruct((8, 2, half, columns), bf),
            jax.ShapeDtypeStruct((8, 2, half, 3 * hidden), bf),
        ),
        in_specs=[ANY] * 3,
        out_specs=(ANY, ANY),
        scratch_shapes=[
            pltpu.VMEM((8, 2, half, columns), bf),
            pltpu.VMEM((8, 2, half, 3 * hidden), bf),
            pltpu.VMEM((width, hidden), bf),
            pltpu.VMEM((width, hidden), bf),
            pltpu.SemaphoreType.DMA((14,)),
            pltpu.SemaphoreType.DMA((8, 2)),
            pltpu.SemaphoreType.DMA((4,)),
            pltpu.SemaphoreType.DMA((16,)),
            pltpu.SemaphoreType.DMA((16,)),
        ],
        compiler_params=pltpu.CompilerParams(
            collective_id=1, has_side_effects=True, vmem_limit_bytes=VMEM_BYTES
        ),
        name="expert_in",
    )(own, gate_w, up_w)


def row_chunk(rows):
    return 64 if rows % 64 == 0 else 16


def add_rows(target, others):
    parts, rows_all, _ = target.shape
    chunk = row_chunk(rows_all)
    for part in range(parts):

        def one(index, carry):
            rows = pl.ds(pl.multiple_of(index * chunk, chunk), chunk)
            total = target[part, rows, :].astype(jnp.float32)
            for other in others:
                total = total + other[part, rows, :].astype(jnp.float32)
            target[part, rows, :] = total.astype(target.dtype)
            return carry

        lax.fori_loop(0, rows_all // chunk, one, 0)


class Scatter:
    def __init__(self, mine, theirs, scratch):
        self.mine_of, self.theirs = mine, theirs
        self.side, self.relay, self.final = scratch[:3]
        self.send, self.side_sem, self.relay_sem, self.final_sem = scratch[3:]
        self.me, self.sib, self.xn, self.yn = plane_peers()

    def mine(self, place, half):
        slot = (self.me, self.xn, self.yn, self.xn + self.yn - self.me)[place]
        return self.mine_of(place, slot, half)

    def peers(self):
        return self.sib, self.xn, self.yn

    def place(self, step):
        quad = lax.div(step, 4)
        far_x, far_y = step_place(step, 3 - quad)
        odd = lax.rem(step, 2)
        third = lax.div(quad, 2) * (1 - lax.div(quad, 3))
        other = 1 - lax.div(lax.rem(step, 4), 2)
        slot = (
            self.me
            + far_x * (self.xn - self.me)
            + far_y * (self.yn - self.me)
            + other * (self.sib - self.me)
        )
        return slot, odd + third * (1 - 2 * odd), other, far_x + 2 * far_y

    def side_copy(self, step):
        slot, half, _, place = self.place(step)
        return remote(
            self.theirs(place, slot, half),
            self.side.at[place, half],
            self.send.at[step],
            self.side_sem.at[place, half],
            self.sib,
        )

    def side_wait(self, place, half):
        remote(
            self.side.at[place, half],
            self.side.at[place, half],
            self.send.at[0],
            self.side_sem.at[place, half],
            self.sib,
        ).wait_recv()

    def relay_copy(self, step, way):
        return remote(
            self.mine(3, way),
            self.relay.at[way],
            self.send.at[step],
            self.relay_sem.at[way],
            (self.xn, self.yn)[way],
        )

    def final_copy(self, step, way, half):
        return remote(
            self.mine(1 + way, half),
            self.final.at[way, half],
            self.send.at[step],
            self.final_sem.at[way, half],
            (self.xn, self.yn)[way],
        )

    def depart(self, step):
        @pl.when(self.place(step)[2] == 1)
        def _():
            self.side_copy(step).start()

        for way in (0, 1):

            @pl.when(step == 2 + way)
            def _():
                self.side_wait(3, way)
                add_rows(self.mine(3, way), (self.side.at[3, way],))
                self.relay_copy(2 + way, way).start()

            @pl.when(step == 6 + way)
            def _():
                self.side_wait(1 + way, way)
                add_rows(self.mine(1 + way, way), (self.side.at[1 + way, way],))
                self.final_copy(6 + way, way, way).start()

    def forward(self):
        for way in (0, 1):
            self.side_wait(1 + way, 1 - way)
            self.relay_copy(3 - way, 1 - way).wait_recv()
            add_rows(
                self.mine(1 + way, 1 - way),
                (self.side.at[1 + way, 1 - way], self.relay.at[1 - way]),
            )
            self.final_copy(10 + way, way, 1 - way).start()

    def finish(self, write):
        parts, rows_all = self.relay.shape[1:3]
        chunk = row_chunk(rows_all)
        for half in (0, 1):
            home = self.mine(0, half)
            self.side_wait(0, half)
            self.final_copy(0, 0, half).wait_recv()
            self.final_copy(0, 1, half).wait_recv()
            for part in range(parts):

                def one(index, carry, half=half, home=home, part=part):
                    rows = pl.ds(pl.multiple_of(index * chunk, chunk), chunk)
                    total = home[part, rows, :].astype(jnp.float32)
                    total = total + self.side[0, half, part, rows, :].astype(jnp.float32)
                    total = total + self.final[0, half, part, rows, :].astype(jnp.float32)
                    total = total + self.final[1, half, part, rows, :].astype(jnp.float32)
                    write(half, part, rows, total)
                    return carry

                lax.fori_loop(0, rows_all // chunk, one, 0)

    def drain(self):
        for way in (0, 1):
            self.relay_copy(2 + way, way).wait_send()
            self.final_copy(6 + way, way, way).wait_send()
            self.final_copy(10 + way, way, 1 - way).wait_send()

        def one(step, carry):
            @pl.when(self.place(step)[2] == 1)
            def _():
                self.side_copy(step).wait_send()

            return carry

        lax.fori_loop(0, 16, one, 0)


SCATTER_REFS = 7


def scatter_scratch(parts, rows, columns):
    bf = jnp.bfloat16
    return [
        pltpu.VMEM((4, 2, parts, rows, columns), bf),
        pltpu.VMEM((2, parts, rows, columns), bf),
        pltpu.VMEM((2, 2, parts, rows, columns), bf),
        pltpu.SemaphoreType.DMA((16,)),
        pltpu.SemaphoreType.DMA((4, 2)),
        pltpu.SemaphoreType.DMA((2,)),
        pltpu.SemaphoreType.DMA((2, 2)),
    ]


def expert_out_kernel(gua_hbm, down_hbm, resid, targets, scales, layer, grad, grad_b, act, down_w, mine, away, load, *scratch):
    hidden = down_w.shape[0]
    scatter = Scatter(
        lambda place, slot, half: mine.at[place, half],
        lambda place, slot, half: away.at[place, half],
        scratch,
    )
    down_load = pltpu.make_async_copy(down_hbm, down_w, load.at[16])
    down_load.start()

    def act_load(step):
        slot, half, _, _ = scatter.place(step)
        return pltpu.make_async_copy(
            gua_hbm.at[slot, half, :, pl.ds(2 * hidden, hidden)], act.at[slot, half], load.at[step]
        )

    def fetch(step, carry):
        act_load(step).start()
        return carry

    lax.fori_loop(0, 16, fetch, 0)
    plane_barrier(scatter.peers())
    down_load.wait()

    def one(step, carry):
        slot, half, other, place = scatter.place(step)
        act_load(step).wait()
        partial = nn_dot(act[slot, half], down_w[...]).astype(jnp.bfloat16)

        @pl.when(other == 1)
        def _():
            away[place, half, 0] = partial

        @pl.when(other == 0)
        def _():
            mine[place, half, 0] = partial

        scatter.depart(step)
        return carry

    lax.fori_loop(0, 16, one, 0)
    scatter.forward()

    def write(half, part, rows, total):
        value = resid[half, rows, :] + total
        layer[half, rows, :] = value.astype(layer.dtype)
        error = (value - targets[half, rows, :].astype(jnp.float32)) * scales[half, rows, 0:1]
        grad[half, rows, :] = error
        grad_b[half, rows, :] = error.astype(grad_b.dtype)

    scatter.finish(write)
    scatter.drain()


def expert_out(gua, down_w, resid, targets, scales):
    half = gua.shape[2]
    hidden, width = down_w.shape
    return pl.pallas_call(
        expert_out_kernel,
        out_shape=(
            jax.ShapeDtypeStruct((2, half, width), jnp.bfloat16),
            jax.ShapeDtypeStruct((2, half, width), jnp.float32),
            jax.ShapeDtypeStruct((2, half, width), jnp.bfloat16),
        ),
        in_specs=[ANY] * 2 + [VMEM] * 3,
        out_specs=(VMEM,) * 3,
        scratch_shapes=[
            pltpu.VMEM((8, 2, half, hidden), jnp.bfloat16),
            pltpu.VMEM((hidden, width), jnp.bfloat16),
            pltpu.VMEM((4, 2, 1, half, width), jnp.bfloat16),
            pltpu.VMEM((4, 2, 1, half, width), jnp.bfloat16),
            pltpu.SemaphoreType.DMA((17,)),
        ]
        + scatter_scratch(1, half, width),
        compiler_params=pltpu.CompilerParams(
            collective_id=2, has_side_effects=True, vmem_limit_bytes=VMEM_BYTES
        ),
        name="expert_out",
    )(
        gua,
        down_w,
        resid.reshape(2, half, width),
        targets.reshape(2, half, width),
        scales.reshape(2, half, 128),
    )


def expert_back_kernel(own, rows_hbm, gua_hbm, gate_hbm, up_hbm, down_hbm, dgu_out, part_out, down_out, buf, gua, tails, part, gate_w, up_w, down_w, down_acc, send, recv, load, load_gua, load_tail, store_b, store_c):
    width, hidden = gate_w.shape
    gather = Gather(own, buf, send, recv)
    loads = (
        pltpu.make_async_copy(down_hbm, down_w, load.at[0]),
        pltpu.make_async_copy(own.at[0], buf.at[gather.me, 0], load.at[1]),
        pltpu.make_async_copy(own.at[1], buf.at[gather.me, 1], load.at[2]),
        pltpu.make_async_copy(gate_hbm, gate_w, load.at[3]),
        pltpu.make_async_copy(up_hbm, up_w, load.at[4]),
    )
    for copy in loads:
        copy.start()

    def block_loads(step):
        slot, half, _ = gather.place(step)
        return (
            pltpu.make_async_copy(
                gua_hbm.at[slot, half], gua.at[slot, half], load_gua.at[step]
            ),
            pltpu.make_async_copy(
                rows_hbm.at[slot, half, :, pl.ds(width, 128)], tails.at[slot, half], load_tail.at[step]
            ),
        )

    def fetch(step, carry):
        for copy in block_loads(step):
            copy.start()
        return carry

    lax.fori_loop(0, 16, fetch, 0)
    gather.begin()
    for copy in loads:
        copy.wait()

    def dgu_store(step):
        slot, half, _ = gather.place(step)
        return pltpu.make_async_copy(
            gua.at[slot, half, :, pl.ds(0, 2 * hidden)], dgu_out.at[slot, half], store_b.at[step]
        )

    def part_store(step):
        slot, half, _ = gather.place(step)
        return pltpu.make_async_copy(
            part.at[lax.rem(step, PART_SLOTS)], part_out.at[slot, half], store_c.at[step]
        )

    def grad_down(step):
        slot_a, half_a, _ = gather.place(step - 1)
        slot_b, half_b, _ = gather.place(step)

        def tile(index, carry):
            rows = pl.ds(pl.multiple_of(index * 256, 256), 256)
            cols = pl.ds(pl.multiple_of(2 * hidden + index * 256, 256), 256)
            total = tn_dot(gua[slot_a, half_a, :, cols], buf[slot_a, half_a]) + tn_dot(
                gua[slot_b, half_b, :, cols], buf[slot_b, half_b]
            )

            @pl.when(step == 1)
            def _():
                down_acc[rows, :] = total

            @pl.when(step > 1)
            def _():
                down_acc[rows, :] = down_acc[rows, :] + total

            return carry

        lax.fori_loop(0, hidden // 256, tile, 0)

    def one(step, carry):
        slot, half = gather.arrive(step)

        @pl.when(step >= PART_SLOTS)
        def _():
            part_store(step - PART_SLOTS).wait()

        part_now = part.at[lax.rem(step, PART_SLOTS)]
        for copy in block_loads(step):
            copy.wait()
        lanes = lax.broadcasted_iota(jnp.int32, (buf.shape[2], 128), 1)
        tail = tails[slot, half].astype(jnp.float32)
        weight = jnp.sum(jnp.where(lanes == gather.me, tail, 0.0), axis=1, keepdims=True)
        grad_act = nt_dot(buf[slot, half], down_w[...])
        gate_val = gua[slot, half, :, :hidden].astype(jnp.float32)
        up_val = gua[slot, half, :, hidden : 2 * hidden].astype(jnp.float32)
        gate_relu = jnp.maximum(gate_val, 0.0)
        grad_comb = jnp.sum(gate_relu * up_val * grad_act, axis=1, keepdims=True)
        grad_act = grad_act * weight
        grad_gate = jnp.where(gate_val > 0, grad_act * up_val, 0.0).astype(jnp.bfloat16)
        grad_up = (grad_act * gate_relu).astype(jnp.bfloat16)
        gua[slot, half, :, :hidden] = grad_gate
        gua[slot, half, :, hidden : 2 * hidden] = grad_up
        dgu_store(step).start()
        part_now[:, :width] = (
            nt_dot(grad_gate, gate_w[...]) + nt_dot(grad_up, up_w[...])
        ).astype(jnp.bfloat16)
        part_now[:, width:] = jnp.where(lanes == gather.me, grad_comb, 0.0).astype(
            jnp.bfloat16
        )
        part_store(step).start()

        @pl.when(lax.rem(step, 2) == 1)
        def _():
            grad_down(step)

        return carry

    lax.fori_loop(0, 16, one, 0)
    gather.finish()

    def round_down(rows):
        down_out[rows, :] = down_acc[rows, :].astype(jnp.bfloat16)

    row_loop(hidden, 64, round_down)

    def drain(step, carry):
        dgu_store(step).wait()

        @pl.when(step >= 16 - PART_SLOTS)
        def _():
            part_store(step).wait()

        return carry

    lax.fori_loop(0, 16, drain, 0)


PART_SLOTS = 4


def expert_back(own, rows_all, gua, gate_w, up_w, down_w):
    _, half, columns = rows_all.shape[1:]
    width, hidden = gate_w.shape
    bf = jnp.bfloat16
    return pl.pallas_call(
        expert_back_kernel,
        out_shape=(
            jax.ShapeDtypeStruct((8, 2, half, 2 * hidden), bf),
            jax.ShapeDtypeStruct((8, 2, half, columns), bf),
            jax.ShapeDtypeStruct((hidden, width), bf),
        ),
        in_specs=[ANY] * 6,
        out_specs=(ANY, ANY, VMEM),
        scratch_shapes=[
            pltpu.VMEM((8, 2, half, width), bf),
            pltpu.VMEM((8, 2, half, 3 * hidden), bf),
            pltpu.VMEM((8, 2, half, 128), bf),
            pltpu.VMEM((PART_SLOTS, half, columns), bf),
            pltpu.VMEM((width, hidden), bf),
            pltpu.VMEM((width, hidden), bf),
            pltpu.VMEM((hidden, width), bf),
            pltpu.VMEM((hidden, width), jnp.float32),
            pltpu.SemaphoreType.DMA((14,)),
            pltpu.SemaphoreType.DMA((8, 2)),
            pltpu.SemaphoreType.DMA((5,)),
        ]
        + [pltpu.SemaphoreType.DMA((16,))] * 4,
        compiler_params=pltpu.CompilerParams(
            collective_id=3, has_side_effects=True, vmem_limit_bytes=VMEM_BYTES
        ),
        name="expert_back",
    )(own, rows_all, gua, gate_w, up_w, down_w)


def expert_grads_kernel(part_hbm, rows_hbm, dgu_hbm, out, gate_out, up_out, rows, dgu, acc, mine, load, block_load, *scratch):
    width = acc.shape[0]
    hidden = acc.shape[1] // 2
    scatter = Scatter(
        lambda place, slot, half: mine.at[place, half],
        lambda place, slot, half: part_hbm.at[slot, half],
        scratch,
    )

    def part_load(step):
        slot, half, _, place = scatter.place(step)
        return pltpu.make_async_copy(
            part_hbm.at[slot, half], mine.at[place, half], load.at[step]
        )

    def fetch(step, carry):
        @pl.when(scatter.place(step)[2] == 0)
        def _():
            part_load(step).start()

        return carry

    def block_copies(block):
        slot = lax.rem(block, 2)
        return (
            pltpu.make_async_copy(
                rows_hbm.at[block, :, :, pl.ds(0, width)], rows.at[slot], block_load.at[slot, 0]
            ),
            pltpu.make_async_copy(dgu_hbm.at[block], dgu.at[slot], block_load.at[slot, 1]),
        )

    lax.fori_loop(0, 16, fetch, 0)
    plane_barrier(scatter.peers())

    def one(step, carry):
        @pl.when(scatter.place(step)[2] == 0)
        def _():
            part_load(step).wait()

        scatter.depart(step)
        return carry

    lax.fori_loop(0, 16, one, 0)
    for copy in block_copies(0):
        copy.start()
    tile = 256

    def accumulate(block, carry):
        for copy in block_copies(block):
            copy.wait()

        @pl.when(block < 7)
        def _():
            for copy in block_copies(block + 1):
                copy.start()

        slot = lax.rem(block, 2)

        def add_tile(index, carry):
            cols = pl.ds(pl.multiple_of(index * tile, tile), tile)
            total = tn_dot(
                rows[slot, :, :, cols].reshape(-1, tile), dgu[slot].reshape(-1, 2 * hidden)
            )

            @pl.when(block == 0)
            def _():
                acc[cols, :] = total

            @pl.when(block > 0)
            def _():
                acc[cols, :] = acc[cols, :] + total

            return carry

        lax.fori_loop(0, width // tile, add_tile, 0)
        return carry

    def blocks(index, carry):
        @pl.when(index == 3)
        def _():
            scatter.forward()

        return accumulate(index, carry)

    lax.fori_loop(0, 8, blocks, 0)

    def round_tile(index, carry):
        cols = pl.ds(pl.multiple_of(index * 64, 64), 64)
        gate_out[cols, :] = acc[cols, :hidden].astype(jnp.bfloat16)
        up_out[cols, :] = acc[cols, hidden:].astype(jnp.bfloat16)
        return carry

    lax.fori_loop(0, width // 64, round_tile, 0)

    def write(half, part, rows, total):
        out[half, rows, :] = total

    scatter.finish(write)
    scatter.drain()


def expert_grads(part, rows_all, dgu):
    _, _, half, columns = part.shape
    width = columns - 128
    hidden = dgu.shape[3] // 2
    bf = jnp.bfloat16
    return pl.pallas_call(
        expert_grads_kernel,
        out_shape=(
            jax.ShapeDtypeStruct((2, half, columns), jnp.float32),
            jax.ShapeDtypeStruct((width, hidden), bf),
            jax.ShapeDtypeStruct((width, hidden), bf),
        ),
        in_specs=[ANY] * 3,
        out_specs=(VMEM,) * 3,
        scratch_shapes=[
            pltpu.VMEM((2, 2, half, width), bf),
            pltpu.VMEM((2, 2, half, 2 * hidden), bf),
            pltpu.VMEM((width, 2 * hidden), jnp.float32),
            pltpu.VMEM((4, 2, 1, half, columns), bf),
            pltpu.SemaphoreType.DMA((16,)),
            pltpu.SemaphoreType.DMA((2, 2)),
        ]
        + scatter_scratch(1, half, columns),
        compiler_params=pltpu.CompilerParams(
            collective_id=4, has_side_effects=True, vmem_limit_bytes=VMEM_BYTES
        ),
        name="expert_grads",
    )(part.reshape(8, 2, 1, half, columns), rows_all, dgu)


def line_peers():
    line = lax.axis_index("dp")
    return (
        line,
        line + 1 - 2 * lax.rem(line, 2),
        line + 2 - 4 * lax.div(line, 2),
        3 - line,
    )


def line_remote(src, dst, send_sem, recv_sem, peer):
    return pltpu.make_async_remote_copy(
        src_ref=src,
        dst_ref=dst,
        send_sem=send_sem,
        recv_sem=recv_sem,
        device_id={"dp": peer},
        device_id_type=MESH,
    )


def full_barrier(plane, line):
    barrier = pltpu.get_barrier_semaphore()
    for peer in plane:
        pl.semaphore_signal(barrier, inc=1, device_id={"exp": peer}, device_id_type=MESH)
    for peer in line:
        pl.semaphore_signal(barrier, inc=1, device_id={"dp": peer}, device_id_type=MESH)
    pl.semaphore_wait(barrier, len(plane) + len(line))


def dense_gather_kernel(own, everything, stage, send, recv, local):
    me, sib, xn, yn = plane_peers()
    diag = xn + yn - me
    line = line_peers()
    into = pltpu.make_async_copy(own, stage, local.at[0])
    into.start()
    full_barrier((sib, xn, yn), line[1:])
    started = []

    def put(src, slot, turn, peer):
        copy = remote(
            src, everything.at[line[turn], slot], send.at[len(started)], recv.at[line[turn], slot], peer
        )
        copy.start()
        started.append(copy)

    def pass_on(slot, turn, peer):
        put(everything.at[line[turn], slot], slot, turn, peer)

    def wait(slot, turn):
        ref = everything.at[line[turn], slot]
        remote(ref, ref, send.at[0], recv.at[line[turn], slot], sib).wait_recv()

    put(own, me, 0, xn)
    put(own, me, 0, yn)
    for turn in (1, 2, 3):
        copy = line_remote(
            own, everything.at[line[0], me], send.at[len(started)], recv.at[line[0], me], line[turn]
        )
        copy.start()
        started.append(copy)
    put(own, me, 0, sib)
    into.wait()
    out = pltpu.make_async_copy(stage, everything.at[line[0], me], local.at[1])
    out.start()
    for turn in (0, 1, 2, 3):
        if turn > 0:
            wait(me, turn)
            for peer in (xn, yn, sib):
                pass_on(me, turn, peer)
        wait(xn, turn)
        if turn % 2 == 0:
            pass_on(xn, turn, yn)
        pass_on(xn, turn, sib)
        wait(yn, turn)
        if turn % 2 == 1:
            pass_on(yn, turn, xn)
        pass_on(yn, turn, sib)
        if turn > 0:
            wait(diag, turn - 1)
            pass_on(diag, turn - 1, sib)
    wait(diag, 3)
    pass_on(diag, 3, sib)
    for turn in (0, 1, 2, 3):
        for slot in (sib, xn + sib - me, yn + sib - me, diag + sib - me):
            wait(slot, turn)
    out.wait()
    for copy in started:
        copy.wait_send()


def dense_gather(own):
    rows, columns = own.shape
    return pl.pallas_call(
        dense_gather_kernel,
        out_shape=jax.ShapeDtypeStruct((4, 8, rows, columns), own.dtype),
        in_specs=[ANY],
        out_specs=ANY,
        scratch_shapes=[
            pltpu.VMEM((rows, columns), own.dtype),
            pltpu.SemaphoreType.DMA((32,)),
            pltpu.SemaphoreType.DMA((4, 8)),
            pltpu.SemaphoreType.DMA((2,)),
        ],
        compiler_params=pltpu.CompilerParams(
            collective_id=5, has_side_effects=True, vmem_limit_bytes=48 * 2**20
        ),
        name="dense_gather",
    )(own).reshape(32 * rows, columns)


class LineScatter:
    def __init__(self, sums, scratch):
        self.sums = sums
        self.other, self.send, self.recv = scratch
        self.line = line_peers()

    def copy(self, turn):
        target = self.line[turn]
        return line_remote(
            self.sums(target),
            self.other.at[turn - 1],
            self.send.at[turn - 1],
            self.recv.at[turn - 1],
            target,
        )

    def begin(self):
        for turn in (1, 2, 3):
            self.copy(turn).start()

    def finish(self, outs):
        rows_all = self.other.shape[1]
        for turn in (1, 2, 3):
            self.copy(turn).wait_recv()
        own = self.sums(self.line[0])

        def one(index, carry):
            rows = pl.ds(pl.multiple_of(index * 16, 16), 16)
            total = own[rows, :].astype(jnp.float32)
            for turn in (0, 1, 2):
                total = total + self.other[turn, rows, :].astype(jnp.float32)
            first = 0
            for out, place, columns in outs:
                out[rows, place : place + columns] = total[:, first : first + columns]
                first += columns
            return carry

        lax.fori_loop(0, rows_all // 16, one, 0)
        for turn in (1, 2, 3):
            self.copy(turn).wait_send()


class DenseScatter:
    def __init__(self, total, scratch):
        def block(place, slot, half):
            return total.at[half, :, slot]

        self.plane = Scatter(block, block, scratch[:SCATTER_REFS])
        me = self.plane.me
        self.line = LineScatter(
            lambda line: total.at[lax.div(line, 2), lax.rem(line, 2), me], scratch[SCATTER_REFS:]
        )

    def begin(self):
        def one(step, carry):
            self.plane.depart(step)
            return carry

        lax.fori_loop(0, 16, one, 0)

    def forward(self):
        self.plane.forward()

    def turn(self):
        def write(half, part, rows, total):
            home = self.plane.mine(0, half)
            home[part, rows, :] = total.astype(home.dtype)

        self.plane.finish(write)
        self.line.begin()

    def finish(self, outs):
        self.line.finish(outs)
        self.plane.drain()


DENSE_REFS = SCATTER_REFS + 3


def dense_scratch(rows, columns):
    return scatter_scratch(2, rows, columns) + [
        pltpu.VMEM((3, rows, columns), jnp.bfloat16),
        pltpu.SemaphoreType.DMA((3,)),
        pltpu.SemaphoreType.DMA((3,)),
    ]


def rope(values, cosine, sine):
    return values * cosine + pltpu.roll(values, HD // 2, 1) * sine


def gain_rows(misc, out):
    for index in range(misc.shape[0] // 128):
        rows = pl.ds(index * 128, 128)
        out[:, rows] = jnp.transpose(misc[rows, :].astype(jnp.float32))


def inverse_rms(values):
    return lax.rsqrt(jnp.mean(values * values, axis=1, keepdims=True) + EPS)


def row_loop(count, chunk, body):
    def one(index, carry):
        body(pl.ds(pl.multiple_of(index * chunk, chunk), chunk))
        return carry

    lax.fori_loop(0, count // chunk, one, 0)


def tile_loop(count, tile, body):
    row_loop(count, tile, body)


ROW_CHUNK = 16
TILE = 256


def attend_kernel(q_heads, kv_heads, experts, tokens, dense_hbm, cosine, sine, bias, picked, rows_out, resid, heads, mixed, lse, prob, qkv_w, rest_w, gains, hidden, load):
    num_rows, width = tokens.shape
    group = q_heads // kv_heads
    q_cols = q_heads * HD
    loads = (
        pltpu.make_async_copy(dense_hbm.at[:, pl.ds(0, qkv_w.shape[1])], qkv_w, load.at[0]),
        pltpu.make_async_copy(
            dense_hbm.at[:, pl.ds(qkv_w.shape[1], rest_w.shape[1])], rest_w, load.at[1]
        ),
    )
    for copy in loads:
        copy.start()
    loads[1].wait()
    misc = rest_w.at[:, pl.ds(width, 128)]
    gain_rows(misc, gains)

    def norm_one(rows):
        value = tokens[rows, :].astype(jnp.float32)
        normed = value * inverse_rms(value)
        hidden[rows, :] = (normed * gains[experts : experts + 1, :]).astype(jnp.bfloat16)

    row_loop(num_rows, ROW_CHUNK, norm_one)
    loads[0].wait()

    def project(index, carry):
        cols = pl.ds(pl.multiple_of(index * TILE, TILE), TILE)
        raw = nn_dot(hidden[...], qkv_w[:, cols])
        turned = index < (q_heads + kv_heads) // 2
        cos_now = jnp.where(turned, cosine[...], 1.0)
        sin_now = jnp.where(turned, sine[...], 0.0)
        for part in (0, 1):
            value = rope(raw[:, part * HD : (part + 1) * HD], cos_now, sin_now)
            heads[2 * index + part] = value.astype(jnp.bfloat16)
        return carry

    lax.fori_loop(0, (q_heads + 2 * kv_heads) // 2, project, 0)
    lse[...] = jnp.zeros_like(lse)

    def head_step(head, carry):
        kv_head = q_heads + lax.div(head, group)
        cols = pl.ds(pl.multiple_of(head * HD, HD), HD)
        for first, keys in ((0, PROMPT), (PROMPT, num_rows)):
            rows = pl.ds(first, keys - first)
            query = heads[head, rows, :]
            score = nt_dot(query, heads[kv_head, :keys, :]) * HD ** (-0.5) + bias[rows, :keys]
            top = jnp.max(score, axis=1, keepdims=True)
            weight = jnp.exp(score - top)
            total = jnp.sum(weight, axis=1, keepdims=True)
            value = nn_dot(weight.astype(jnp.bfloat16), heads[kv_head + kv_heads, :keys, :])
            mixed[rows, cols] = (value / total).astype(jnp.bfloat16)
            lanes = lax.broadcasted_iota(jnp.int32, (keys - first, 128), 1)
            lse[rows, :] = jnp.where(lanes == head, top + jnp.log(total), lse[rows, :])
        return carry

    lax.fori_loop(0, q_heads, head_step, 0)

    def out_tile(cols):
        resid[:, cols] = tokens[:, cols].astype(jnp.float32) + nn_dot(mixed[...], rest_w[:, cols])

    tile_loop(width, TILE, out_tile)

    def norm_two(rows):
        value = resid[rows, :]
        normed = value * inverse_rms(value)
        rows_out[rows, :width] = (normed * gains[experts + 1 : experts + 2, :]).astype(jnp.bfloat16)

    row_loop(num_rows, ROW_CHUNK, norm_two)
    logits = nn_dot(rows_out[:, :width], misc[...])
    lanes = lax.broadcasted_iota(jnp.int32, logits.shape, 1)
    logits = jnp.where(lanes < experts, logits, NEG_BIG)
    weight = jnp.exp(logits - jnp.max(logits, axis=1, keepdims=True))
    value = weight / jnp.sum(weight, axis=1, keepdims=True)
    prob[...] = value
    chosen = value * picked[...]
    rows_out[:, width:] = (chosen / jnp.sum(chosen, axis=1, keepdims=True)).astype(jnp.bfloat16)


def attend(tokens, dense_w, cosine, sine, bias, picked, q_heads, kv_heads, experts):
    num_rows, width = tokens.shape
    bf = jnp.bfloat16
    all_heads = q_heads + 2 * kv_heads
    return pl.pallas_call(
        functools.partial(attend_kernel, q_heads, kv_heads, experts),
        out_shape=(
            jax.ShapeDtypeStruct((num_rows, width + 128), bf),
            jax.ShapeDtypeStruct((num_rows, width), jnp.float32),
            jax.ShapeDtypeStruct((all_heads, num_rows, HD), bf),
            jax.ShapeDtypeStruct((num_rows, q_heads * HD), bf),
            jax.ShapeDtypeStruct((num_rows, 128), jnp.float32),
            jax.ShapeDtypeStruct((num_rows, 128), jnp.float32),
        ),
        in_specs=[VMEM, ANY] + [VMEM] * 4,
        out_specs=(VMEM,) * 6,
        scratch_shapes=[
            pltpu.VMEM((width, all_heads * HD), bf),
            pltpu.VMEM((q_heads * HD, width + 128), bf),
            pltpu.VMEM((128, width), jnp.float32),
            pltpu.VMEM((num_rows, width), bf),
            pltpu.SemaphoreType.DMA((2,)),
        ],
        compiler_params=pltpu.CompilerParams(vmem_limit_bytes=VMEM_BYTES),
        name="attend",
    )(tokens, dense_w, cosine, sine, bias, picked)


def attend_back_kernel(q_heads, kv_heads, experts, back_hbm, grad_hbm, resid_hbm, rows_hbm, prob_hbm, picked_hbm, dense_hbm, mixed_hbm, heads_hbm, lse_hbm, bias_hbm, cos_hbm, sin_hbm, tokens_hbm, grad_in, out_sum, q_sum, k_sum, v_sum, misc_sum, back, grad, resid, hidden_two, prob, picked, dense, mixed, heads, lse, bias, cosine, sine, tokens, gains, gain_sums, grad_logit, grad_proj, grad_mixed, grad_qkv, grad_kv, hidden, load, *scratch):
    num_rows, width = tokens.shape
    group = q_heads // kv_heads
    q_cols = q_heads * HD
    k_cols = kv_heads * HD
    qkv_cols = q_cols + 2 * k_cols
    near_cols = group * HD
    bf = jnp.bfloat16
    parts, scatters = [], []
    for index in range(4):
        some = scratch[index * (1 + DENSE_REFS) : (index + 1) * (1 + DENSE_REFS)]
        parts.append(some[0])
        scatters.append(DenseScatter(some[0], some[1:]))
    out_part, near_part, rest_part, misc_part = parts
    out_scatter, near_scatter, rest_scatter, misc_scatter = scatters
    pairs = (
        (prob_hbm, prob),
        (picked_hbm, picked),
        (back_hbm, back),
        (dense_hbm, dense),
        (resid_hbm, resid),
        (grad_hbm, grad),
        (rows_hbm, hidden_two),
        (mixed_hbm, mixed),
        (heads_hbm, heads),
        (lse_hbm, lse),
        (bias_hbm, bias),
        (cos_hbm, cosine),
        (sin_hbm, sine),
        (tokens_hbm, tokens),
    )
    loads = [pltpu.make_async_copy(src, dst, load.at[i]) for i, (src, dst) in enumerate(pairs)]
    for copy in loads:
        copy.start()
    full_barrier(out_scatter.plane.peers(), out_scatter.line.line[1:])
    for copy in loads[:3]:
        copy.wait()
    gain_sums[...] = jnp.zeros_like(gain_sums)

    def router_rows(rows):
        value = prob[rows, :]
        chosen = value * picked[rows, :]
        total = jnp.sum(chosen, axis=1, keepdims=True)
        comb = chosen / total
        grad_comb = back[rows, width:]
        grad_chosen = (
            picked[rows, :] * (grad_comb - jnp.sum(grad_comb * comb, axis=1, keepdims=True)) / total
        )
        logit = value * (grad_chosen - jnp.sum(value * grad_chosen, axis=1, keepdims=True))
        grad_logit[rows, :] = logit.astype(bf)

    row_loop(num_rows, 64, router_rows)
    loads[3].wait()
    misc = dense.at[:, pl.ds(qkv_cols + width, 128)]
    gain_rows(misc, gains)
    lanes = lax.broadcasted_iota(jnp.int32, (TILE, 128), 1)

    def hidden_tile(cols):
        router = jnp.where(lanes < experts, misc[cols, :], jnp.zeros((), bf))
        back[:, cols] = back[:, cols] + nt_dot(grad_logit[...], router)

    tile_loop(width, TILE, hidden_tile)
    for copy in loads[4:]:
        copy.wait()

    def fold(values):
        return jnp.sum(values.reshape(-1, 8, width), axis=0)

    def norm_two(rows):
        value = resid[rows, :]
        inverse = inverse_rms(value)
        normed = value * inverse
        grad_hidden = back[rows, :width]
        gain_sums[8:16, :] = gain_sums[8:16, :] + fold(grad_hidden * normed)
        grad_norm = grad_hidden * gains[experts + 1 : experts + 2, :]
        mean = jnp.mean(grad_norm * normed, axis=1, keepdims=True)
        total = grad[rows, :] + inverse * (grad_norm - normed * mean)
        grad[rows, :] = total
        grad_proj[rows, :] = total.astype(bf)

    row_loop(num_rows, ROW_CHUNK, norm_two)

    def weight_loop(part, left, right):
        _, _, blocks, rows_each, columns = part.shape
        span = blocks * rows_each

        def one(line, carry):
            cols = pl.ds(pl.multiple_of(line * span, 128), span)
            total = tn_dot(left[:, cols], right[...]).astype(bf)
            part[lax.div(line, 2), lax.rem(line, 2)] = total.reshape(blocks, rows_each, columns)
            return carry

        lax.fori_loop(0, 4, one, 0)

    weight_loop(out_part, mixed, grad_proj)
    out_scatter.begin()

    def mixed_tile(cols):
        grad_mixed[:, cols] = nt_dot(
            grad_proj[...], dense[cols, pl.ds(qkv_cols, width)]
        ).astype(bf)

    tile_loop(q_cols, TILE, mixed_tile)

    def norm_one(rows):
        value = tokens[rows, :].astype(jnp.float32)
        normed = value * inverse_rms(value)
        hidden[rows, :] = (normed * gains[experts : experts + 1, :]).astype(bf)

    row_loop(num_rows, ROW_CHUNK, norm_one)
    scale = HD ** (-0.5)

    def head_step(head, carry):
        kv_head = lax.div(head, group)
        cols = pl.ds(pl.multiple_of(head * HD, HD), HD)

        @pl.when(lax.rem(head, group) == 0)
        def _():
            grad_kv[...] = jnp.zeros_like(grad_kv)

        for first, keys in ((0, PROMPT), (PROMPT, num_rows)):
            rows = pl.ds(first, keys - first)
            key = heads[q_heads + kv_head, :keys, :]
            query = heads[head, rows, :]
            up = grad_mixed[rows, cols]
            lane = lax.broadcasted_iota(jnp.int32, (keys - first, 128), 1)
            total = jnp.sum(jnp.where(lane == head, lse[rows, :], 0.0), axis=1, keepdims=True)
            weight = jnp.exp(nt_dot(query, key) * scale + bias[rows, :keys] - total)
            grad_weight = nt_dot(up, heads[q_heads + kv_heads + kv_head, :keys, :])
            delta = jnp.sum(weight * grad_weight, axis=1, keepdims=True)
            score = (weight * (grad_weight - delta)).astype(bf)
            grad_kv[1, :keys, :] = grad_kv[1, :keys, :] + tn_dot(weight.astype(bf), up)
            grad_kv[0, :keys, :] = grad_kv[0, :keys, :] + tn_dot(score, query) * scale
            value = rope(nn_dot(score, key) * scale, cosine[rows, :], -sine[rows, :])
            grad_qkv[rows, cols] = value.astype(bf)

        @pl.when(lax.rem(head, group) == group - 1)
        def _():
            key_cols = pl.ds(pl.multiple_of(q_cols + kv_head * HD, HD), HD)
            value_cols = pl.ds(pl.multiple_of(q_cols + (kv_heads + kv_head) * HD, HD), HD)
            grad_qkv[:, key_cols] = rope(grad_kv[0], cosine[...], -sine[...]).astype(bf)
            grad_qkv[:, value_cols] = grad_kv[1].astype(bf)

        @pl.when(head == 2)
        def _():
            out_scatter.forward()

        @pl.when(head == group - 1)
        def _():
            weight_loop(near_part, hidden, grad_qkv.at[:, pl.ds(0, near_cols)])
            near_scatter.begin()

        @pl.when(head == group + 1)
        def _():
            out_scatter.turn()

        @pl.when(head == group + 3)
        def _():
            near_scatter.forward()

        return carry

    lax.fori_loop(0, q_heads, head_step, 0)
    weight_loop(rest_part, hidden, grad_qkv.at[:, pl.ds(near_cols, qkv_cols - near_cols)])
    rest_scatter.begin()
    near_scatter.turn()

    def hidden_back_tile(cols):
        back[:, cols] = nt_dot(grad_qkv[...], dense[cols, pl.ds(0, qkv_cols)])

    tile_loop(width, TILE, hidden_back_tile)
    rest_scatter.forward()

    def last_rows(rows):
        value = tokens[rows, :].astype(jnp.float32)
        inverse = inverse_rms(value)
        normed = value * inverse
        grad_hidden = back[rows, :width]
        gain_sums[0:8, :] = gain_sums[0:8, :] + fold(grad_hidden * normed)
        grad_norm = grad_hidden * gains[experts : experts + 1, :]
        mean = jnp.mean(grad_norm * normed, axis=1, keepdims=True)
        grad[rows, :] = grad[rows, :] + inverse * (grad_norm - normed * mean)

    row_loop(num_rows, ROW_CHUNK, last_rows)
    store = pltpu.make_async_copy(grad, grad_in, load.at[0])
    store.start()
    gains[0:16, :] = gain_sums[...]
    _, _, blocks, rows_each, _ = misc_part.shape
    span = blocks * rows_each

    def misc_line(line, carry):
        cols = pl.ds(pl.multiple_of(line * span, 128), span)
        router = tn_dot(hidden_two[:, cols], grad_logit[...])
        one = jnp.sum(gains[0:8, cols], axis=0, keepdims=True)
        two = jnp.sum(gains[8:16, cols], axis=0, keepdims=True)
        place = lax.broadcasted_iota(jnp.int32, (128, span), 0)
        block = jnp.where(place == experts, one, jnp.where(place == experts + 1, two, 0.0))
        total = (router + jnp.transpose(block)).astype(bf)
        misc_part[lax.div(line, 2), lax.rem(line, 2)] = total.reshape(blocks, rows_each, 128)
        return carry

    lax.fori_loop(0, 4, misc_line, 0)
    misc_scatter.begin()
    misc_scatter.forward()
    rest_scatter.turn()
    misc_scatter.turn()
    out_scatter.finish(((out_sum, 0, width),))
    near_scatter.finish(((q_sum, 0, near_cols),))
    rest_scatter.finish(
        ((q_sum, near_cols, q_cols - near_cols), (k_sum, 0, k_cols), (v_sum, 0, k_cols))
    )
    misc_scatter.finish(((misc_sum, 0, 128),))
    store.wait()


def attend_back(back, grad, resid, rows_own, prob, picked, dense_w, mixed, heads, lse, bias, cosine, sine, tokens, q_heads, kv_heads, experts):
    num_rows, width = tokens.shape
    bf = jnp.bfloat16
    arrays = (back, grad, resid, rows_own, prob, picked, dense_w, mixed, heads, lse, bias, cosine, sine, tokens)
    k_cols = kv_heads * HD
    q_cols = q_heads * HD
    qkv_cols = q_cols + 2 * k_cols
    near_cols = q_cols // kv_heads
    block_rows = width // 32
    scratch = []
    for columns in (width, near_cols, qkv_cols - near_cols, 128):
        scratch += [pltpu.VMEM((2, 2, 8, block_rows, columns), bf)]
        scratch += dense_scratch(block_rows, columns)
    return pl.pallas_call(
        functools.partial(attend_back_kernel, q_heads, kv_heads, experts),
        out_shape=(jax.ShapeDtypeStruct((num_rows, width), jnp.float32),)
        + tuple(
            jax.ShapeDtypeStruct((block_rows, columns), jnp.float32)
            for columns in (width, q_cols, k_cols, k_cols, 128)
        ),
        in_specs=[ANY] * len(arrays),
        out_specs=(ANY,) + (VMEM,) * 5,
        scratch_shapes=[pltpu.VMEM(array.shape, array.dtype) for array in arrays]
        + [
            pltpu.VMEM((128, width), jnp.float32),
            pltpu.VMEM((16, width), jnp.float32),
            pltpu.VMEM((num_rows, 128), bf),
            pltpu.VMEM((num_rows, width), bf),
            pltpu.VMEM((num_rows, q_cols), bf),
            pltpu.VMEM((num_rows, qkv_cols), bf),
            pltpu.VMEM((2, num_rows, HD), jnp.float32),
            pltpu.VMEM((num_rows, width), bf),
            pltpu.SemaphoreType.DMA((len(arrays),)),
        ]
        + scratch,
        compiler_params=pltpu.CompilerParams(
            collective_id=6, has_side_effects=True, vmem_limit_bytes=67043328
        ),
        name="attend_back",
    )(*arrays)


def body_plane(
    tokens,
    targets,
    valid_count,
    segments,
    routes,
    gain_attn,
    w_query,
    w_key,
    w_value,
    w_out,
    gain_moe,
    w_router,
    w_gate,
    w_up,
    w_down,
):
    bf = jnp.bfloat16
    num_rows, width = tokens.shape
    half = num_rows // 2
    q_cols, k_cols = w_query.shape[1], w_key.shape[1]
    num_experts = w_router.shape[1]
    num_heads = q_cols // HD
    kv_heads = k_cols // HD
    pad_cols = 128 - 2 - num_experts
    dense_own = jnp.concatenate(
        [
            w_query,
            w_key,
            w_value,
            w_out,
            w_router,
            gain_attn[:, None],
            gain_moe[:, None],
            jnp.zeros((gain_attn.shape[0], pad_cols), bf),
        ],
        axis=1,
    )
    dense_w = dense_gather(dense_own)
    gate_w = lax.all_gather(w_gate, "dp", axis=1, tiled=True)[0]
    up_w = lax.all_gather(w_up, "dp", axis=1, tiled=True)[0]
    down_w = lax.all_gather(w_down, "dp", axis=1, tiled=True)[0]
    tok_pos = positions(segments)
    bias = jnp.where(key_mask(segments), 0.0, NEG_BIG)
    freq = THETA ** (-2.0 * jnp.arange(HD // 2, dtype=jnp.float32) / HD)
    angle = tok_pos.astype(jnp.float32)[:, None] * freq[None, :]
    cosine, sine_part = jnp.cos(angle), jnp.sin(angle)
    cosine = jnp.concatenate([cosine, cosine], axis=1)
    sine = jnp.concatenate([-sine_part, sine_part], axis=1)
    lane_ids = jnp.arange(128, dtype=jnp.int32)
    picked = jnp.sum((routes[:, :, None] == lane_ids[None, None, :]).astype(jnp.float32), axis=1)
    rows_own, resid_mid, heads, mixed, lse, prob = attend(
        tokens, dense_w, cosine, sine, bias, picked, num_heads, kv_heads, num_experts
    )
    rows_all, gua = expert_in(rows_own.reshape(2, half, width + 128), gate_w, up_w)
    total_rows = num_rows * lax.axis_size(("dp", "exp"))
    global_row = lax.axis_index(("dp", "exp")) * num_rows + jnp.arange(num_rows, dtype=jnp.int32)
    loss_scale = total_rows / valid_count[0].astype(jnp.float32)
    scales = jnp.broadcast_to(
        jnp.where(global_row < valid_count[0], loss_scale, 0.0)[:, None], (num_rows, 128)
    )
    layer_out, grad_out, grad_out_b = expert_out(gua, down_w, resid_mid, targets, scales)
    layer_out = layer_out.reshape(num_rows, width)
    dgu, part, down_part = expert_back(grad_out_b, rows_all, gua, gate_w, up_w, down_w)
    back, gate_part, up_part = expert_grads(part, rows_all, dgu)
    expert_sums = tuple(
        lax.psum_scatter(grad[None], "dp", scatter_dimension=1, tiled=True).astype(jnp.float32)
        for grad in (gate_part, up_part, down_part)
    )
    grad_in, out_sum, q_sum, k_sum, v_sum, misc_sum = attend_back(
        back.reshape(num_rows, width + 128),
        grad_out.reshape(num_rows, width),
        resid_mid,
        rows_own,
        prob,
        picked,
        dense_w,
        mixed,
        heads,
        lse,
        bias,
        cosine,
        sine,
        tokens,
        num_heads,
        kv_heads,
        num_experts,
    )
    return (
        layer_out,
        grad_in,
        misc_sum[:, num_experts],
        q_sum,
        k_sum,
        v_sum,
        out_sum,
        misc_sum[:, num_experts + 1],
        misc_sum[:, :num_experts],
        *expert_sums,
    )


def solution(mesh):
    in_specs = (
        P(("dp", "exp"), None),
        P(("dp", "exp"), None),
        P(),
        P(("dp", "exp")),
        P(("dp", "exp"), None),
        P(("dp", "exp")),
        P(("dp", "exp"), None),
        P(("dp", "exp"), None),
        P(("dp", "exp"), None),
        P(("dp", "exp"), None),
        P(("dp", "exp")),
        P(("dp", "exp"), None),
        P("exp", "dp", None),
        P("exp", "dp", None),
        P("exp", "dp", None),
    )
    out_specs = (
        P(("dp", "exp"), None),
        P(("dp", "exp"), None),
        P(("dp", "exp")),
        P(("dp", "exp"), None),
        P(("dp", "exp"), None),
        P(("dp", "exp"), None),
        P(("dp", "exp"), None),
        P(("dp", "exp")),
        P(("dp", "exp"), None),
        P("exp", "dp", None),
        P("exp", "dp", None),
        P("exp", "dp", None),
    )
    body = body_plane if (mesh.shape["dp"], mesh.shape["exp"]) == (4, 8) else body_general
    return jax.shard_map(body, mesh=mesh, in_specs=in_specs, out_specs=out_specs, check_vma=False)
```

```python
import functools

import jax
import jax.numpy as jnp
from jax import lax
from jax.experimental import pallas as pl
from jax.experimental.pallas import tpu as pltpu
from jax.sharding import PartitionSpec as P

HD = 128
PROMPT = 256
NCONT = 2


EPS = 1e-06
THETA = 10000.0
HIGH = lax.Precision.HIGHEST
NEG_BIG = -1e30


def positions(segments):
    count_rows = segments.shape[0]
    row_ids = jnp.arange(count_rows, dtype=jnp.int32)
    labels = jnp.arange(NCONT + 1, dtype=jnp.int32)
    member = segments[:, None] == labels[None, :]
    first_row = jnp.min(jnp.where(member, row_ids[:, None], count_rows), axis=0)
    start_row = jnp.sum(jnp.where(member, first_row[None, :], 0), axis=1)
    return jnp.where(segments == 0, row_ids, PROMPT + row_ids - start_row)


def key_mask(segments):
    row_ids = jnp.arange(segments.shape[0], dtype=jnp.int32)
    causal = row_ids[None, :] <= row_ids[:, None]
    visible = (segments[None, :] == 0) | (segments[None, :] == segments[:, None])
    return causal & visible


def rotate(values, pos_rows, sign_value):
    half_size = HD // 2
    freq = THETA ** (-2.0 * jnp.arange(half_size, dtype=jnp.float32) / HD)
    angle = pos_rows.astype(jnp.float32)[:, None] * freq[None, :]
    cosine = jnp.cos(angle)[:, None, :]
    sine_part = sign_value * jnp.sin(angle)[:, None, :]
    first_half = values[..., :half_size]
    second = values[..., half_size:]
    return jnp.concatenate(
        [first_half * cosine - second * sine_part, second * cosine + first_half * sine_part],
        axis=-1,
    )


def attention_scores(query_b, key_b, allowed):
    logits = jnp.einsum(
        "qkgd,pkd->kgqp", query_b, key_b, preferred_element_type=jnp.float32
    ) * HD ** (-0.5)
    return jnp.where(allowed[None, None], logits, NEG_BIG)


def expert_gates(rows_in, gate_w, up_w):
    gate_val = jnp.einsum("sacd,adf->sacf", rows_in, gate_w, preferred_element_type=jnp.float32)
    up_val = jnp.einsum("sacd,adf->sacf", rows_in, up_w, preferred_element_type=jnp.float32)
    return (gate_val, up_val)


def body_general(
    tokens,
    targets,
    valid_count,
    segments,
    routes,
    gain_attn,
    w_query,
    w_key,
    w_value,
    w_out,
    gain_moe,
    w_router,
    w_gate,
    w_up,
    w_down,
):
    gain_one, query_w, key_w, value_w, out_w, gain_two, router_w = (
        lax.all_gather(gain_attn, ("dp", "exp"), axis=0, tiled=True),
        lax.all_gather(w_query, ("dp", "exp"), axis=0, tiled=True),
        lax.all_gather(w_key, ("dp", "exp"), axis=0, tiled=True),
        lax.all_gather(w_value, ("dp", "exp"), axis=0, tiled=True),
        lax.all_gather(w_out, ("dp", "exp"), axis=0, tiled=True),
        lax.all_gather(gain_moe, ("dp", "exp"), axis=0, tiled=True),
        lax.all_gather(w_router, ("dp", "exp"), axis=0, tiled=True),
    )
    gate_w, up_w, down_w = (
        lax.all_gather(w_gate, "dp", axis=1, tiled=True),
        lax.all_gather(w_up, "dp", axis=1, tiled=True),
        lax.all_gather(w_down, "dp", axis=1, tiled=True),
    )
    num_rows = tokens.shape[0]
    width = tokens.shape[1]
    num_heads = query_w.shape[1] // HD
    kv_heads = key_w.shape[1] // HD
    group_size = num_heads // kv_heads
    num_experts = router_w.shape[1]
    top_count = routes.shape[1]
    exp_local = gate_w.shape[0]
    exp_ranks = lax.axis_size("exp")
    capacity = 5 * num_rows * top_count // (4 * num_experts)
    tok_pos = positions(segments)
    allowed = key_mask(segments)
    resid_in = tokens.astype(jnp.float32)
    inv_one = lax.rsqrt(jnp.mean(resid_in * resid_in, axis=-1, keepdims=True) + EPS)
    normed_one = resid_in * inv_one
    hidden_one = (normed_one * gain_one.astype(jnp.float32)).astype(jnp.bfloat16)
    query_raw = jnp.dot(hidden_one, query_w, preferred_element_type=jnp.float32)
    key_raw = jnp.dot(hidden_one, key_w, preferred_element_type=jnp.float32)
    value_b = jnp.dot(hidden_one, value_w, preferred_element_type=jnp.float32).astype(jnp.bfloat16)
    query_b = rotate(query_raw.reshape(num_rows, num_heads, HD), tok_pos, 1.0).astype(jnp.bfloat16)
    query_b = query_b.reshape(num_rows, kv_heads, group_size, HD)
    key_b = rotate(key_raw.reshape(num_rows, kv_heads, HD), tok_pos, 1.0).astype(jnp.bfloat16)
    value_h = value_b.reshape(num_rows, kv_heads, HD)
    logit_att = attention_scores(query_b, key_b, allowed)
    row_max = jnp.max(logit_att, axis=-1, keepdims=True)
    log_total = row_max + jnp.log(jnp.sum(jnp.exp(logit_att - row_max), axis=-1, keepdims=True))
    probs_b = jnp.exp(logit_att - log_total).astype(jnp.bfloat16)
    attn_vals = jnp.einsum("kgqp,pkd->qkgd", probs_b, value_h, preferred_element_type=jnp.float32)
    attn_vals = attn_vals.reshape(num_rows, num_heads * HD).astype(jnp.bfloat16)
    resid_mid = resid_in + jnp.dot(attn_vals, out_w, preferred_element_type=jnp.float32)
    inv_two = lax.rsqrt(jnp.mean(resid_mid * resid_mid, axis=-1, keepdims=True) + EPS)
    normed_two = resid_mid * inv_two
    gain_two_f = gain_two.astype(jnp.float32)
    hidden_two = (normed_two * gain_two_f).astype(jnp.bfloat16)
    router_prob = jax.nn.softmax(
        jnp.dot(hidden_two, router_w, preferred_element_type=jnp.float32), axis=-1
    )
    expert_ids = jnp.arange(num_experts, dtype=jnp.int32)
    route_hot = routes[:, :, None] == expert_ids[None, None, :]
    chosen = jnp.sum(jnp.where(route_hot, router_prob[:, None, :], 0.0), axis=-1)
    weight_sum = jnp.sum(chosen, axis=1, keepdims=True)
    combine = chosen / weight_sum
    flat_hot = route_hot.reshape(num_rows * top_count, num_experts).astype(jnp.int32)
    slot_index = jnp.sum((jnp.cumsum(flat_hot, axis=0) - flat_hot) * flat_hot, axis=1)
    dest_index = routes.reshape(-1) * capacity + slot_index
    send_shape = (exp_ranks, exp_local, capacity, width)
    send_rows = jnp.zeros((num_experts * capacity, width), jnp.bfloat16)
    send_rows = (
        send_rows.at[dest_index].set(jnp.repeat(hidden_two, top_count, axis=0)).reshape(send_shape)
    )
    gate_val, up_val = expert_gates(
        lax.all_to_all(send_rows, "exp", split_axis=0, concat_axis=0, tiled=True), gate_w, up_w
    )
    act_b = (jax.nn.relu(gate_val) * up_val).astype(jnp.bfloat16)
    out_b = jnp.einsum("sacf,afd->sacd", act_b, down_w, preferred_element_type=jnp.float32).astype(
        jnp.bfloat16
    )
    returned = lax.all_to_all(out_b, "exp", split_axis=0, concat_axis=0, tiled=True)
    route_out = returned.reshape(num_experts * capacity, width)[dest_index].reshape(
        num_rows, top_count, width
    )
    route_out_f = route_out.astype(jnp.float32)
    resid_out = resid_mid + jnp.sum(combine[:, :, None] * route_out_f, axis=1)
    layer_out = resid_out.astype(jnp.bfloat16)
    total_rows = num_rows * lax.axis_size(("dp", "exp"))
    global_row = lax.axis_index(("dp", "exp")) * num_rows + jnp.arange(num_rows, dtype=jnp.int32)
    loss_scale = total_rows / valid_count[0].astype(jnp.float32)
    grad_out = jnp.where(
        (global_row < valid_count[0])[:, None],
        (resid_out - targets.astype(jnp.float32)) * loss_scale,
        0.0,
    )
    gain_one, query_w, key_w, value_w, out_w, gain_two, router_w = (
        lax.all_gather(gain_attn, ("dp", "exp"), axis=0, tiled=True),
        lax.all_gather(w_query, ("dp", "exp"), axis=0, tiled=True),
        lax.all_gather(w_key, ("dp", "exp"), axis=0, tiled=True),
        lax.all_gather(w_value, ("dp", "exp"), axis=0, tiled=True),
        lax.all_gather(w_out, ("dp", "exp"), axis=0, tiled=True),
        lax.all_gather(gain_moe, ("dp", "exp"), axis=0, tiled=True),
        lax.all_gather(w_router, ("dp", "exp"), axis=0, tiled=True),
    )
    gain_two_f = gain_two.astype(jnp.float32)
    grad_route = (combine[:, :, None] * grad_out[:, None, :]).astype(jnp.bfloat16)
    grad_comb = jnp.sum(grad_out[:, None, :] * route_out_f, axis=-1)
    grad_send = jnp.zeros((num_experts * capacity, width), jnp.bfloat16)
    grad_send = (
        grad_send.at[dest_index]
        .set(grad_route.reshape(num_rows * top_count, width))
        .reshape(send_shape)
    )
    expert_rows, grad_recv = (
        lax.all_to_all(send_rows, "exp", split_axis=0, concat_axis=0, tiled=True),
        lax.all_to_all(grad_send, "exp", split_axis=0, concat_axis=0, tiled=True),
    )
    gate_val, up_val = expert_gates(expert_rows, gate_w, up_w)
    gate_relu = jax.nn.relu(gate_val)
    act_b = (gate_relu * up_val).astype(jnp.bfloat16)
    grad_act = jnp.einsum("sacd,afd->sacf", grad_recv, down_w, preferred_element_type=jnp.float32)
    grad_down_w = jnp.einsum("sacf,sacd->afd", act_b, grad_recv, preferred_element_type=jnp.float32)
    grad_gate_b = jnp.where(gate_val > 0, grad_act * up_val, 0.0).astype(jnp.bfloat16)
    grad_up_b = (grad_act * gate_relu).astype(jnp.bfloat16)
    grad_gate_w = jnp.einsum(
        "sacd,sacf->adf", expert_rows, grad_gate_b, preferred_element_type=jnp.float32
    )
    grad_up_w = jnp.einsum(
        "sacd,sacf->adf", expert_rows, grad_up_b, preferred_element_type=jnp.float32
    )
    grad_rows = (
        jnp.einsum("sacf,adf->sacd", grad_gate_b, gate_w, preferred_element_type=jnp.float32)
        + jnp.einsum("sacf,adf->sacd", grad_up_b, up_w, preferred_element_type=jnp.float32)
    ).astype(jnp.bfloat16)
    grad_back = lax.all_to_all(grad_rows, "exp", split_axis=0, concat_axis=0, tiled=True)
    grad_copies = grad_back.reshape(num_experts * capacity, width)[dest_index].reshape(
        num_rows, top_count, width
    )
    grad_hidden_two = jnp.sum(grad_copies.astype(jnp.float32), axis=1)
    grad_chosen = (grad_comb - jnp.sum(grad_comb * combine, axis=1, keepdims=True)) / weight_sum
    grad_prob = jnp.sum(jnp.where(route_hot, grad_chosen[:, :, None], 0.0), axis=1)
    grad_logit = router_prob * (
        grad_prob - jnp.sum(router_prob * grad_prob, axis=-1, keepdims=True)
    )
    router_f = router_w.astype(jnp.float32)
    grad_hidden_two = grad_hidden_two + jnp.einsum(
        "re,de->rd", grad_logit, router_f, precision=HIGH
    )
    grad_router = jnp.einsum(
        "rd,re->de", hidden_two.astype(jnp.float32), grad_logit, precision=HIGH
    )
    grad_gain_two = jnp.sum(grad_hidden_two * normed_two, axis=0)
    grad_norm_two = grad_hidden_two * gain_two_f
    grad_mid = grad_out + inv_two * (
        grad_norm_two - normed_two * jnp.mean(grad_norm_two * normed_two, axis=-1, keepdims=True)
    )
    grad_proj_b = grad_mid.astype(jnp.bfloat16)
    grad_out_w = jnp.einsum("rh,rd->hd", attn_vals, grad_proj_b, preferred_element_type=jnp.float32)
    grad_vals_b = jnp.einsum(
        "rd,hd->rh", grad_proj_b, out_w, preferred_element_type=jnp.float32
    ).astype(jnp.bfloat16)
    grad_vals_b = grad_vals_b.reshape(num_rows, kv_heads, group_size, HD)
    logit_att = attention_scores(query_b, key_b, allowed)
    probs = jnp.exp(logit_att - log_total)
    probs_b = probs.astype(jnp.bfloat16)
    grad_value = jnp.einsum(
        "kgqp,qkgd->pkd", probs_b, grad_vals_b, preferred_element_type=jnp.float32
    )
    grad_prob_att = jnp.einsum(
        "qkgd,pkd->kgqp", grad_vals_b, value_h, preferred_element_type=jnp.float32
    )
    delta_row = jnp.sum(probs * grad_prob_att, axis=-1, keepdims=True)
    grad_score_b = (probs * (grad_prob_att - delta_row)).astype(jnp.bfloat16)
    grad_query = jnp.einsum(
        "kgqp,pkd->qkgd", grad_score_b, key_b, preferred_element_type=jnp.float32
    ) * HD ** (-0.5)
    grad_key = jnp.einsum(
        "kgqp,qkgd->pkd", grad_score_b, query_b, preferred_element_type=jnp.float32
    ) * HD ** (-0.5)
    grad_query_b = rotate(grad_query.reshape(num_rows, num_heads, HD), tok_pos, -1.0).astype(
        jnp.bfloat16
    )
    grad_query_b = grad_query_b.reshape(num_rows, num_heads * HD)
    grad_key_b = (
        rotate(grad_key, tok_pos, -1.0).astype(jnp.bfloat16).reshape(num_rows, kv_heads * HD)
    )
    grad_value_b = grad_value.astype(jnp.bfloat16).reshape(num_rows, kv_heads * HD)
    grad_query_w = jnp.einsum(
        "rd,rh->dh", hidden_one, grad_query_b, preferred_element_type=jnp.float32
    )
    grad_key_w = jnp.einsum("rd,rh->dh", hidden_one, grad_key_b, preferred_element_type=jnp.float32)
    grad_value_w = jnp.einsum(
        "rd,rh->dh", hidden_one, grad_value_b, preferred_element_type=jnp.float32
    )
    grad_hidden_one = (
        jnp.einsum("rh,dh->rd", grad_query_b, query_w, preferred_element_type=jnp.float32)
        + jnp.einsum("rh,dh->rd", grad_key_b, key_w, preferred_element_type=jnp.float32)
        + jnp.einsum("rh,dh->rd", grad_value_b, value_w, preferred_element_type=jnp.float32)
    )
    grad_gain_one = jnp.sum(grad_hidden_one * normed_one, axis=0)
    grad_norm_one = grad_hidden_one * gain_one.astype(jnp.float32)
    grad_in = grad_mid + inv_one * (
        grad_norm_one - normed_one * jnp.mean(grad_norm_one * normed_one, axis=-1, keepdims=True)
    )
    dense_sums = (
        lax.psum_scatter(grad_gain_one, ("dp", "exp"), scatter_dimension=0, tiled=True),
        lax.psum_scatter(grad_query_w, ("dp", "exp"), scatter_dimension=0, tiled=True),
        lax.psum_scatter(grad_key_w, ("dp", "exp"), scatter_dimension=0, tiled=True),
        lax.psum_scatter(grad_value_w, ("dp", "exp"), scatter_dimension=0, tiled=True),
        lax.psum_scatter(grad_out_w, ("dp", "exp"), scatter_dimension=0, tiled=True),
        lax.psum_scatter(grad_gain_two, ("dp", "exp"), scatter_dimension=0, tiled=True),
        lax.psum_scatter(grad_router, ("dp", "exp"), scatter_dimension=0, tiled=True),
    )
    expert_sums = (
        lax.psum_scatter(
            grad_gate_w.astype(jnp.bfloat16), "dp", scatter_dimension=1, tiled=True
        ).astype(jnp.float32),
        lax.psum_scatter(
            grad_up_w.astype(jnp.bfloat16), "dp", scatter_dimension=1, tiled=True
        ).astype(jnp.float32),
        lax.psum_scatter(
            grad_down_w.astype(jnp.bfloat16), "dp", scatter_dimension=1, tiled=True
        ).astype(jnp.float32),
    )
    return (
        layer_out,
        grad_in,
        dense_sums[0],
        dense_sums[1],
        dense_sums[2],
        dense_sums[3],
        dense_sums[4],
        dense_sums[5],
        dense_sums[6],
        expert_sums[0],
        expert_sums[1],
        expert_sums[2],
    )


MESH = pl.DeviceIdType.MESH
ANY = pl.BlockSpec(memory_space=pl.ANY)
VMEM = pl.BlockSpec(memory_space=pltpu.VMEM)
VMEM_BYTES = 62 * 2**20


def nn_dot(left, right):
    return jnp.dot(left, right, preferred_element_type=jnp.float32)


def nt_dot(left, right):
    return lax.dot_general(
        left, right, (((1,), (1,)), ((), ())), preferred_element_type=jnp.float32
    )


def tn_dot(left, right):
    return lax.dot_general(
        left, right, (((0,), (0,)), ((), ())), preferred_element_type=jnp.float32
    )


def plane_peers():
    me = lax.axis_index("exp")
    core = lax.rem(me, 2)
    x_pos = lax.rem(lax.div(me, 2), 2)
    y_pos = lax.div(me, 4)
    return me, me + 1 - 2 * core, me + 2 - 4 * x_pos, me + 4 - 8 * y_pos


def remote(src, dst, send_sem, recv_sem, peer):
    return pltpu.make_async_remote_copy(
        src_ref=src,
        dst_ref=dst,
        send_sem=send_sem,
        recv_sem=recv_sem,
        device_id={"exp": peer},
        device_id_type=MESH,
    )


def plane_barrier(peers):
    barrier = pltpu.get_barrier_semaphore()
    for peer in peers:
        pl.semaphore_signal(barrier, inc=1, device_id={"exp": peer}, device_id_type=MESH)
    pl.semaphore_wait(barrier, len(peers))


def step_place(step, quad):
    odd = lax.rem(step, 2)
    last = lax.div(quad, 3)
    mid = lax.rem(lax.div(quad + 1, 2), 2)
    return mid * (1 - odd) + last, mid * odd + last


class Gather:
    def __init__(self, own, buf, send, recv):
        self.own, self.buf, self.send, self.recv = own, buf, send, recv
        self.me, self.sib, self.xn, self.yn = plane_peers()
        self.diag = self.xn + self.yn - self.me

    def own_copy(self, half, peer, sem):
        return remote(
            self.own.at[half],
            self.buf.at[self.me, half],
            self.send.at[sem],
            self.recv.at[self.me, half],
            peer,
        )

    def pass_copy(self, slot, half, peer, sem):
        return remote(
            self.buf.at[slot, half],
            self.buf.at[slot, half],
            self.send.at[sem],
            self.recv.at[slot, half],
            peer,
        )

    def own_copies(self):
        return (
            self.own_copy(0, self.xn, 0),
            self.own_copy(1, self.yn, 1),
            self.own_copy(0, self.sib, 2),
            self.own_copy(1, self.sib, 3),
            self.own_copy(1, self.xn, 4),
            self.own_copy(0, self.yn, 5),
        )

    def near_copies(self):
        return (
            self.pass_copy(self.xn, 0, self.yn, 6),
            self.pass_copy(self.yn, 1, self.xn, 7),
            self.pass_copy(self.xn, 0, self.sib, 8),
            self.pass_copy(self.yn, 1, self.sib, 9),
        )

    def late_copies(self):
        return (
            self.pass_copy(self.xn, 1, self.sib, 10),
            self.pass_copy(self.yn, 0, self.sib, 11),
        )

    def far_copies(self):
        return (
            self.pass_copy(self.diag, 0, self.sib, 12),
            self.pass_copy(self.diag, 1, self.sib, 13),
        )

    def wait_block(self, slot, half):
        self.pass_copy(slot, half, self.sib, 0).wait_recv()

    def begin(self):
        plane_barrier((self.sib, self.xn, self.yn))
        for copy in self.own_copies():
            copy.start()

    def place(self, step):
        quad = lax.div(step, 4)
        far_x, far_y = step_place(step, quad)
        odd = lax.rem(step, 2)
        third = lax.div(quad, 2) * (1 - lax.div(quad, 3))
        other = lax.div(lax.rem(step, 4), 2)
        slot = (
            self.me
            + far_x * (self.xn - self.me)
            + far_y * (self.yn - self.me)
            + other * (self.sib - self.me)
        )
        return slot, odd + third * (1 - 2 * odd), other

    def arrive(self, step):
        @pl.when(step == 4)
        def _():
            self.wait_block(self.xn, 0)
            self.wait_block(self.yn, 1)
            for copy in self.near_copies():
                copy.start()

        @pl.when(step == 8)
        def _():
            self.wait_block(self.xn, 1)
            self.wait_block(self.yn, 0)
            for copy in self.late_copies():
                copy.start()

        @pl.when(step == 12)
        def _():
            self.wait_block(self.diag, 0)
            self.wait_block(self.diag, 1)
            for copy in self.far_copies():
                copy.start()

        slot, half, other = self.place(step)

        @pl.when(other == 1)
        def _():
            self.wait_block(slot, half)

        return slot, half

    def finish(self):
        for copies in (self.own_copies(), self.near_copies(), self.late_copies(), self.far_copies()):
            for copy in copies:
                copy.wait_send()


def line_peers():
    line = lax.axis_index("dp")
    return (
        line,
        line + 1 - 2 * lax.rem(line, 2),
        line + 2 - 4 * lax.div(line, 2),
        3 - line,
    )


def line_remote(src, dst, send_sem, recv_sem, peer):
    return pltpu.make_async_remote_copy(
        src_ref=src,
        dst_ref=dst,
        send_sem=send_sem,
        recv_sem=recv_sem,
        device_id={"dp": peer},
        device_id_type=MESH,
    )


def full_barrier(plane, line):
    barrier = pltpu.get_barrier_semaphore()
    for peer in plane:
        pl.semaphore_signal(barrier, inc=1, device_id={"exp": peer}, device_id_type=MESH)
    for peer in line:
        pl.semaphore_signal(barrier, inc=1, device_id={"dp": peer}, device_id_type=MESH)
    pl.semaphore_wait(barrier, len(plane) + len(line))


def expert_in_kernel(own, gate_hbm, down_own, rows_out, gate_out, down_out, buf, gate, gate_w, down_stage, send, recv, load, store_a, store_b, line_send, line_recv):
    width = gate_w.shape[0]
    gather = Gather(own, buf, send, recv)
    line = line_peers()
    loads = (
        pltpu.make_async_copy(own.at[0], buf.at[gather.me, 0], load.at[0]),
        pltpu.make_async_copy(own.at[1], buf.at[gather.me, 1], load.at[1]),
        pltpu.make_async_copy(gate_hbm, gate_w, load.at[2]),
        pltpu.make_async_copy(down_own, down_stage, load.at[3]),
    )
    for copy in loads:
        copy.start()
    full_barrier((gather.sib, gather.xn, gather.yn), line[1:])
    for copy in gather.own_copies():
        copy.start()

    def down_copy(turn):
        return line_remote(
            down_own,
            down_out.at[line[0]],
            line_send.at[turn - 1],
            line_recv.at[turn - 1],
            line[turn],
        )

    for turn in (1, 2, 3):
        down_copy(turn).start()
    for copy in loads:
        copy.wait()
    down_store = pltpu.make_async_copy(down_stage, down_out.at[line[0]], load.at[4])
    down_store.start()

    def row_store(slot, half, step):
        return pltpu.make_async_copy(buf.at[slot, half], rows_out.at[slot, half], store_a.at[step])

    def gate_store(slot, half, step):
        return pltpu.make_async_copy(gate.at[slot, half], gate_out.at[slot, half], store_b.at[step])

    def one(step, carry):
        slot, half = gather.arrive(step)
        row_store(slot, half, step).start()
        gate[slot, half] = nn_dot(buf[slot, half, :, :width], gate_w[...]).astype(jnp.bfloat16)
        gate_store(slot, half, step).start()
        return carry

    lax.fori_loop(0, 16, one, 0)
    gather.finish()

    def drain(step, carry):
        slot, half, _ = gather.place(step)
        row_store(slot, half, step).wait()
        gate_store(slot, half, step).wait()
        return carry

    lax.fori_loop(0, 16, drain, 0)
    down_store.wait()
    for turn in (1, 2, 3):
        line_remote(
            down_own,
            down_out.at[line[turn]],
            line_send.at[turn - 1],
            line_recv.at[turn - 1],
            line[turn],
        ).wait()


def expert_in(own, gate_w, down_own):
    _, half, columns = own.shape
    width, hidden = gate_w.shape
    bf = jnp.bfloat16
    return pl.pallas_call(
        expert_in_kernel,
        out_shape=(
            jax.ShapeDtypeStruct((8, 2, half, columns), bf),
            jax.ShapeDtypeStruct((8, 2, half, hidden), bf),
            jax.ShapeDtypeStruct((4, *down_own.shape), bf),
        ),
        in_specs=[ANY] * 3,
        out_specs=(ANY, ANY, ANY),
        scratch_shapes=[
            pltpu.VMEM((8, 2, half, columns), bf),
            pltpu.VMEM((8, 2, half, hidden), bf),
            pltpu.VMEM((width, hidden), bf),
            pltpu.VMEM(down_own.shape, bf),
            pltpu.SemaphoreType.DMA((14,)),
            pltpu.SemaphoreType.DMA((8, 2)),
            pltpu.SemaphoreType.DMA((5,)),
            pltpu.SemaphoreType.DMA((16,)),
            pltpu.SemaphoreType.DMA((16,)),
            pltpu.SemaphoreType.DMA((3,)),
            pltpu.SemaphoreType.DMA((3,)),
        ],
        compiler_params=pltpu.CompilerParams(
            collective_id=1, has_side_effects=True, vmem_limit_bytes=VMEM_BYTES
        ),
        name="expert_in",
    )(own, gate_w, down_own)


def row_chunk(rows):
    return 64 if rows % 64 == 0 else 16


def add_rows(target, others):
    parts, rows_all, _ = target.shape
    chunk = row_chunk(rows_all)
    for part in range(parts):

        def one(index, carry):
            rows = pl.ds(pl.multiple_of(index * chunk, chunk), chunk)
            total = target[part, rows, :].astype(jnp.float32)
            for other in others:
                total = total + other[part, rows, :].astype(jnp.float32)
            target[part, rows, :] = total.astype(target.dtype)
            return carry

        lax.fori_loop(0, rows_all // chunk, one, 0)


class Scatter:
    def __init__(self, mine, theirs, scratch):
        self.mine_of, self.theirs = mine, theirs
        self.side, self.relay, self.final = scratch[:3]
        self.send, self.side_sem, self.relay_sem, self.final_sem = scratch[3:]
        self.me, self.sib, self.xn, self.yn = plane_peers()

    def mine(self, place, half):
        slot = (self.me, self.xn, self.yn, self.xn + self.yn - self.me)[place]
        return self.mine_of(place, slot, half)

    def peers(self):
        return self.sib, self.xn, self.yn

    def place(self, step):
        quad = lax.div(step, 4)
        odd = lax.div(lax.rem(step, 4), 2)
        far_x, far_y = step_place(odd, 3 - quad)
        third = lax.div(quad, 2) * (1 - lax.div(quad, 3))
        other = 1 - lax.rem(step, 2)
        slot = (
            self.me
            + far_x * (self.xn - self.me)
            + far_y * (self.yn - self.me)
            + other * (self.sib - self.me)
        )
        return slot, odd + third * (1 - 2 * odd), other, far_x + 2 * far_y

    def side_copy(self, step):
        slot, half, _, place = self.place(step)
        return remote(
            self.theirs(place, slot, half),
            self.side.at[place, half],
            self.send.at[step],
            self.side_sem.at[place, half],
            self.sib,
        )

    def side_wait(self, place, half):
        remote(
            self.side.at[place, half],
            self.side.at[place, half],
            self.send.at[0],
            self.side_sem.at[place, half],
            self.sib,
        ).wait_recv()

    def relay_copy(self, step, way):
        return remote(
            self.mine(3, way),
            self.relay.at[way],
            self.send.at[step],
            self.relay_sem.at[way],
            (self.xn, self.yn)[way],
        )

    def final_copy(self, step, way, half):
        return remote(
            self.mine(1 + way, half),
            self.final.at[way, half],
            self.send.at[step],
            self.final_sem.at[way, half],
            (self.xn, self.yn)[way],
        )

    def depart(self, step):
        @pl.when(self.place(step)[2] == 1)
        def _():
            self.side_copy(step).start()

        for way in (0, 1):

            @pl.when(step == 1 + 2 * way)
            def _():
                self.side_wait(3, way)
                add_rows(self.mine(3, way), (self.side.at[3, way],))
                self.relay_copy(1 + 2 * way, way).start()

            @pl.when(step == 5 + 2 * way)
            def _():
                self.side_wait(1 + way, way)
                add_rows(self.mine(1 + way, way), (self.side.at[1 + way, way],))
                self.final_copy(5 + 2 * way, way, way).start()

    def forward(self):
        for way in (0, 1):
            self.side_wait(1 + way, 1 - way)
            self.relay_copy(0, 1 - way).wait_recv()
            add_rows(
                self.mine(1 + way, 1 - way),
                (self.side.at[1 + way, 1 - way], self.relay.at[1 - way]),
            )
            self.final_copy(9 + 2 * way, way, 1 - way).start()

    def finish(self, write):
        parts, rows_all = self.relay.shape[1:3]
        chunk = row_chunk(rows_all)
        for half in (0, 1):
            home = self.mine(0, half)
            self.side_wait(0, half)
            self.final_copy(0, 0, half).wait_recv()
            self.final_copy(0, 1, half).wait_recv()
            for part in range(parts):

                def one(index, carry, half=half, home=home, part=part):
                    rows = pl.ds(pl.multiple_of(index * chunk, chunk), chunk)
                    total = home[part, rows, :].astype(jnp.float32)
                    total = total + self.side[0, half, part, rows, :].astype(jnp.float32)
                    total = total + self.final[0, half, part, rows, :].astype(jnp.float32)
                    total = total + self.final[1, half, part, rows, :].astype(jnp.float32)
                    write(half, part, rows, total)
                    return carry

                lax.fori_loop(0, rows_all // chunk, one, 0)

    def drain(self):
        for way in (0, 1):
            self.relay_copy(1 + 2 * way, way).wait_send()
            self.final_copy(5 + 2 * way, way, way).wait_send()
            self.final_copy(9 + 2 * way, way, 1 - way).wait_send()

        def one(step, carry):
            @pl.when(self.place(step)[2] == 1)
            def _():
                self.side_copy(step).wait_send()

            return carry

        lax.fori_loop(0, 16, one, 0)


SCATTER_REFS = 7


def scatter_scratch(parts, rows, columns):
    bf = jnp.bfloat16
    return [
        pltpu.VMEM((4, 2, parts, rows, columns), bf),
        pltpu.VMEM((2, parts, rows, columns), bf),
        pltpu.VMEM((2, 2, parts, rows, columns), bf),
        pltpu.SemaphoreType.DMA((16,)),
        pltpu.SemaphoreType.DMA((4, 2)),
        pltpu.SemaphoreType.DMA((2,)),
        pltpu.SemaphoreType.DMA((2, 2)),
    ]


OUT_SLOTS = 4


def expert_out_kernel(rows_hbm, gate_hbm, up_hbm, down_hbm, resid, targets, scales, layer, grad, grad_b, ua_out, rows, gate, ua, up_w, down_w, mine, away, load_w, load_rows, load_gate, store_ua, *scratch):
    hidden, width = down_w.shape
    scatter = Scatter(
        lambda place, slot, half: mine.at[place, half],
        lambda place, slot, half: away.at[place, half],
        scratch,
    )
    weights = (
        pltpu.make_async_copy(up_hbm, up_w, load_w.at[0]),
        pltpu.make_async_copy(down_hbm, down_w, load_w.at[1]),
    )

    def loads(step):
        slot, half, _, _ = scatter.place(step)
        spot = lax.rem(step, OUT_SLOTS)
        return (
            pltpu.make_async_copy(rows_hbm.at[slot, half], rows.at[spot], load_rows.at[step]),
            pltpu.make_async_copy(gate_hbm.at[slot, half], gate.at[spot], load_gate.at[step]),
        )

    def ua_store(step):
        slot, half, _, _ = scatter.place(step)
        return pltpu.make_async_copy(
            ua.at[lax.rem(step, OUT_SLOTS)], ua_out.at[slot, half], store_ua.at[step]
        )

    weights[0].start()
    for step in (0, 1):
        for copy in loads(step):
            copy.start()
    weights[1].start()
    plane_barrier(scatter.peers())
    for copy in weights:
        copy.wait()

    def one(step, carry):
        _, _, other, place = scatter.place(step)
        spot = lax.rem(step, OUT_SLOTS)
        for copy in loads(step):
            copy.wait()

        @pl.when(step < 14)
        def _():
            for copy in loads(step + 2):
                copy.start()

        @pl.when(step >= OUT_SLOTS)
        def _():
            ua_store(step - OUT_SLOTS).wait()

        lanes = lax.broadcasted_iota(jnp.int32, (rows.shape[1], 128), 1)
        tail = rows[spot, :, width:].astype(jnp.float32)
        weight = jnp.sum(jnp.where(lanes == scatter.me, tail, 0.0), axis=1, keepdims=True)
        up_val = nn_dot(rows[spot, :, :width], up_w[...])
        act_val = jnp.maximum(gate[spot].astype(jnp.float32), 0.0) * up_val * weight
        ua[spot, :, :hidden] = up_val.astype(jnp.bfloat16)
        ua[spot, :, hidden:] = act_val.astype(jnp.bfloat16)
        ua_store(step).start()
        partial = nn_dot(ua[spot, :, hidden:], down_w[...]).astype(jnp.bfloat16)

        @pl.when(other == 1)
        def _():
            away[place, half_of(scatter, step), 0] = partial

        @pl.when(other == 0)
        def _():
            mine[place, half_of(scatter, step), 0] = partial

        scatter.depart(step)
        return carry

    lax.fori_loop(0, 16, one, 0)
    scatter.forward()

    def write(half, part, rows, total):
        value = resid[half, rows, :] + total
        layer[half, rows, :] = value.astype(layer.dtype)
        error = (value - targets[half, rows, :].astype(jnp.float32)) * scales[half, rows, 0:1]
        grad[half, rows, :] = error
        grad_b[half, rows, :] = error.astype(grad_b.dtype)

    scatter.finish(write)
    scatter.drain()

    def drain(step, carry):
        ua_store(step).wait()
        return carry

    lax.fori_loop(16 - OUT_SLOTS, 16, drain, 0)


def half_of(scatter, step):
    return scatter.place(step)[1]


def expert_out(rows_all, gate_val, up_w, down_w, resid, targets, scales):
    half, columns = rows_all.shape[2:]
    hidden, width = down_w.shape
    bf = jnp.bfloat16
    return pl.pallas_call(
        expert_out_kernel,
        out_shape=(
            jax.ShapeDtypeStruct((2, half, width), bf),
            jax.ShapeDtypeStruct((2, half, width), jnp.float32),
            jax.ShapeDtypeStruct((2, half, width), bf),
            jax.ShapeDtypeStruct((8, 2, half, 2 * hidden), bf),
        ),
        in_specs=[ANY] * 4 + [VMEM] * 3,
        out_specs=(VMEM, VMEM, VMEM, ANY),
        scratch_shapes=[
            pltpu.VMEM((OUT_SLOTS, half, columns), bf),
            pltpu.VMEM((OUT_SLOTS, half, hidden), bf),
            pltpu.VMEM((OUT_SLOTS, half, 2 * hidden), bf),
            pltpu.VMEM((width, hidden), bf),
            pltpu.VMEM((hidden, width), bf),
            pltpu.VMEM((4, 2, 1, half, width), bf),
            pltpu.VMEM((4, 2, 1, half, width), bf),
            pltpu.SemaphoreType.DMA((2,)),
            pltpu.SemaphoreType.DMA((16,)),
            pltpu.SemaphoreType.DMA((16,)),
            pltpu.SemaphoreType.DMA((16,)),
        ]
        + scatter_scratch(1, half, width),
        compiler_params=pltpu.CompilerParams(
            collective_id=2, has_side_effects=True, vmem_limit_bytes=VMEM_BYTES
        ),
        name="expert_out",
    )(
        rows_all,
        gate_val,
        up_w,
        down_w,
        resid.reshape(2, half, width),
        targets.reshape(2, half, width),
        scales.reshape(2, half, 128),
    )


def expert_back_kernel(own, rows_hbm, g_hbm, ua_hbm, gate_hbm, up_hbm, down_hbm, dgu_out, part_out, down_out, buf, gua, tails, part, gate_w, up_w, down_w, down_acc, send, recv, load, load_g, load_ua, load_tail, store_b, store_c):
    width, hidden = gate_w.shape
    gather = Gather(own, buf, send, recv)
    loads = (
        pltpu.make_async_copy(down_hbm, down_w, load.at[0]),
        pltpu.make_async_copy(own.at[0], buf.at[gather.me, 0], load.at[1]),
        pltpu.make_async_copy(own.at[1], buf.at[gather.me, 1], load.at[2]),
        pltpu.make_async_copy(gate_hbm, gate_w, load.at[3]),
        pltpu.make_async_copy(up_hbm, up_w, load.at[4]),
    )
    for copy in loads:
        copy.start()

    def block_loads(step):
        slot, half, _ = gather.place(step)
        return (
            pltpu.make_async_copy(
                g_hbm.at[slot, half], gua.at[slot, half, :, pl.ds(0, hidden)], load_g.at[step]
            ),
            pltpu.make_async_copy(
                ua_hbm.at[slot, half],
                gua.at[slot, half, :, pl.ds(hidden, 2 * hidden)],
                load_ua.at[step],
            ),
            pltpu.make_async_copy(
                rows_hbm.at[slot, half, :, pl.ds(width, 128)], tails.at[slot, half], load_tail.at[step]
            ),
        )

    def fetch(step, carry):
        for copy in block_loads(step):
            copy.start()
        return carry

    lax.fori_loop(0, 16, fetch, 0)
    gather.begin()
    for copy in loads:
        copy.wait()

    def dgu_store(step):
        slot, half, _ = gather.place(step)
        return pltpu.make_async_copy(
            gua.at[slot, half, :, pl.ds(0, 2 * hidden)], dgu_out.at[slot, half], store_b.at[step]
        )

    def part_store(step):
        slot, half, _ = gather.place(step)
        return pltpu.make_async_copy(
            part.at[lax.rem(step, PART_SLOTS)], part_out.at[slot, half], store_c.at[step]
        )

    def grad_down(step):
        slot_a, half_a, _ = gather.place(step - 1)
        slot_b, half_b, _ = gather.place(step)

        def tile(index, carry):
            rows = pl.ds(pl.multiple_of(index * 256, 256), 256)
            cols = pl.ds(pl.multiple_of(2 * hidden + index * 256, 256), 256)
            total = tn_dot(gua[slot_a, half_a, :, cols], buf[slot_a, half_a]) + tn_dot(
                gua[slot_b, half_b, :, cols], buf[slot_b, half_b]
            )

            @pl.when(step == 1)
            def _():
                down_acc[rows, :] = total

            @pl.when(step > 1)
            def _():
                down_acc[rows, :] = down_acc[rows, :] + total

            return carry

        lax.fori_loop(0, hidden // 256, tile, 0)

    def one(step, carry):
        slot, half = gather.arrive(step)

        @pl.when(step >= PART_SLOTS)
        def _():
            part_store(step - PART_SLOTS).wait()

        part_now = part.at[lax.rem(step, PART_SLOTS)]
        for copy in block_loads(step):
            copy.wait()
        lanes = lax.broadcasted_iota(jnp.int32, (buf.shape[2], 128), 1)
        tail = tails[slot, half].astype(jnp.float32)
        weight = jnp.sum(jnp.where(lanes == gather.me, tail, 0.0), axis=1, keepdims=True)
        grad_act = nt_dot(buf[slot, half], down_w[...])
        gate_val = gua[slot, half, :, :hidden].astype(jnp.float32)
        up_val = gua[slot, half, :, hidden : 2 * hidden].astype(jnp.float32)
        gate_relu = jnp.maximum(gate_val, 0.0)
        grad_comb = jnp.sum(gate_relu * up_val * grad_act, axis=1, keepdims=True)
        grad_act = grad_act * weight
        grad_gate = jnp.where(gate_val > 0, grad_act * up_val, 0.0).astype(jnp.bfloat16)
        grad_up = (grad_act * gate_relu).astype(jnp.bfloat16)
        gua[slot, half, :, :hidden] = grad_gate
        gua[slot, half, :, hidden : 2 * hidden] = grad_up
        dgu_store(step).start()
        part_now[:, :width] = (
            nt_dot(grad_gate, gate_w[...]) + nt_dot(grad_up, up_w[...])
        ).astype(jnp.bfloat16)
        part_now[:, width:] = jnp.where(lanes == gather.me, grad_comb, 0.0).astype(
            jnp.bfloat16
        )
        part_store(step).start()

        @pl.when(lax.rem(step, 2) == 1)
        def _():
            grad_down(step)

        return carry

    lax.fori_loop(0, 16, one, 0)
    gather.finish()

    def round_down(rows):
        down_out[rows, :] = down_acc[rows, :].astype(jnp.bfloat16)

    row_loop(hidden, 64, round_down)

    def drain(step, carry):
        dgu_store(step).wait()

        @pl.when(step >= 16 - PART_SLOTS)
        def _():
            part_store(step).wait()

        return carry

    lax.fori_loop(0, 16, drain, 0)


PART_SLOTS = 4


def expert_back(own, rows_all, gate_val, ua, gate_w, up_w, down_w):
    _, half, columns = rows_all.shape[1:]
    width, hidden = gate_w.shape
    bf = jnp.bfloat16
    return pl.pallas_call(
        expert_back_kernel,
        out_shape=(
            jax.ShapeDtypeStruct((8, 2, half, 2 * hidden), bf),
            jax.ShapeDtypeStruct((8, 2, half, columns), bf),
            jax.ShapeDtypeStruct((hidden, width), bf),
        ),
        in_specs=[ANY] * 7,
        out_specs=(ANY, ANY, VMEM),
        scratch_shapes=[
            pltpu.VMEM((8, 2, half, width), bf),
            pltpu.VMEM((8, 2, half, 3 * hidden), bf),
            pltpu.VMEM((8, 2, half, 128), bf),
            pltpu.VMEM((PART_SLOTS, half, columns), bf),
            pltpu.VMEM((width, hidden), bf),
            pltpu.VMEM((width, hidden), bf),
            pltpu.VMEM((hidden, width), bf),
            pltpu.VMEM((hidden, width), jnp.float32),
            pltpu.SemaphoreType.DMA((14,)),
            pltpu.SemaphoreType.DMA((8, 2)),
            pltpu.SemaphoreType.DMA((5,)),
        ]
        + [pltpu.SemaphoreType.DMA((16,))] * 5,
        compiler_params=pltpu.CompilerParams(
            collective_id=3, has_side_effects=True, vmem_limit_bytes=VMEM_BYTES
        ),
        name="expert_back",
    )(own, rows_all, gate_val, ua, gate_w, up_w, down_w)


def expert_grads_kernel(part_hbm, rows_hbm, dgu_hbm, out, gate_out, up_out, rows, dgu, acc, mine, load, block_load, *scratch):
    width = acc.shape[0]
    hidden = acc.shape[1] // 2
    scatter = Scatter(
        lambda place, slot, half: mine.at[place, half],
        lambda place, slot, half: part_hbm.at[slot, half],
        scratch,
    )

    def part_load(step):
        slot, half, _, place = scatter.place(step)
        return pltpu.make_async_copy(
            part_hbm.at[slot, half], mine.at[place, half], load.at[step]
        )

    def fetch(step, carry):
        @pl.when(scatter.place(step)[2] == 0)
        def _():
            part_load(step).start()

        return carry

    def block_copies(block):
        slot = lax.rem(block, 2)
        return (
            pltpu.make_async_copy(
                rows_hbm.at[block, :, :, pl.ds(0, width)], rows.at[slot], block_load.at[slot, 0]
            ),
            pltpu.make_async_copy(dgu_hbm.at[block], dgu.at[slot], block_load.at[slot, 1]),
        )

    lax.fori_loop(0, 16, fetch, 0)
    plane_barrier(scatter.peers())

    def one(step, carry):
        @pl.when(scatter.place(step)[2] == 0)
        def _():
            part_load(step).wait()

        scatter.depart(step)
        return carry

    lax.fori_loop(0, 16, one, 0)
    for copy in block_copies(0):
        copy.start()
    tile = 256

    def accumulate(block, carry):
        for copy in block_copies(block):
            copy.wait()

        @pl.when(block < 7)
        def _():
            for copy in block_copies(block + 1):
                copy.start()

        slot = lax.rem(block, 2)

        def add_tile(index, carry):
            cols = pl.ds(pl.multiple_of(index * tile, tile), tile)
            total = tn_dot(
                rows[slot, :, :, cols].reshape(-1, tile), dgu[slot].reshape(-1, 2 * hidden)
            )

            @pl.when(block == 0)
            def _():
                acc[cols, :] = total

            @pl.when(block > 0)
            def _():
                acc[cols, :] = acc[cols, :] + total

            return carry

        lax.fori_loop(0, width // tile, add_tile, 0)
        return carry

    def blocks(index, carry):
        @pl.when(index == 3)
        def _():
            scatter.forward()

        return accumulate(index, carry)

    lax.fori_loop(0, 8, blocks, 0)

    def round_tile(index, carry):
        cols = pl.ds(pl.multiple_of(index * 64, 64), 64)
        gate_out[cols, :] = acc[cols, :hidden].astype(jnp.bfloat16)
        up_out[cols, :] = acc[cols, hidden:].astype(jnp.bfloat16)
        return carry

    lax.fori_loop(0, width // 64, round_tile, 0)

    def write(half, part, rows, total):
        out[half, rows, :] = total

    scatter.finish(write)
    scatter.drain()


def expert_grads(part, rows_all, dgu):
    _, _, half, columns = part.shape
    width = columns - 128
    hidden = dgu.shape[3] // 2
    bf = jnp.bfloat16
    return pl.pallas_call(
        expert_grads_kernel,
        out_shape=(
            jax.ShapeDtypeStruct((2, half, columns), jnp.float32),
            jax.ShapeDtypeStruct((width, hidden), bf),
            jax.ShapeDtypeStruct((width, hidden), bf),
        ),
        in_specs=[ANY] * 3,
        out_specs=(VMEM,) * 3,
        scratch_shapes=[
            pltpu.VMEM((2, 2, half, width), bf),
            pltpu.VMEM((2, 2, half, 2 * hidden), bf),
            pltpu.VMEM((width, 2 * hidden), jnp.float32),
            pltpu.VMEM((4, 2, 1, half, columns), bf),
            pltpu.SemaphoreType.DMA((16,)),
            pltpu.SemaphoreType.DMA((2, 2)),
        ]
        + scatter_scratch(1, half, columns),
        compiler_params=pltpu.CompilerParams(
            collective_id=4, has_side_effects=True, vmem_limit_bytes=VMEM_BYTES
        ),
        name="expert_grads",
    )(part.reshape(8, 2, 1, half, columns), rows_all, dgu)


class DenseGather:
    def __init__(self, own, everything, send, recv, local):
        self.own, self.everything, self.send, self.recv = own, everything, send, recv
        self.me, self.sib, self.xn, self.yn = plane_peers()
        self.diag = self.xn + self.yn - self.me
        self.line = line_peers()
        self.home = pltpu.make_async_copy(own, everything.at[self.line[0], self.me], local)
        self.started = []

    def copy(self, index, own, slot, turn, peer, make):
        target = self.everything.at[self.line[turn], slot]
        return make(
            self.own if own else target,
            target,
            self.send.at[index],
            self.recv.at[self.line[turn], slot],
            peer,
        )

    def put(self, own, slot, turn, peer, make=remote):
        what = (len(self.started), own, slot, turn, peer, make)
        self.started.append(what)
        self.copy(*what).start()

    def pass_on(self, slot, turn, peer):
        self.put(False, slot, turn, peer)

    def wait(self, slot, turn):
        ref = self.everything.at[self.line[turn], slot]
        remote(ref, ref, self.send.at[0], self.recv.at[self.line[turn], slot], self.sib).wait_recv()

    def start_line(self):
        for turn in (1, 2, 3):
            self.put(True, self.me, 0, self.line[turn], line_remote)

    def start_plane(self):
        for peer in (self.xn, self.yn, self.sib):
            self.put(True, self.me, 0, peer)

    def turn(self, turn):
        if turn > 0:
            self.wait(self.me, turn)
            for peer in (self.xn, self.yn, self.sib):
                self.pass_on(self.me, turn, peer)
        self.wait(self.xn, turn)
        if turn % 2 == 0:
            self.pass_on(self.xn, turn, self.yn)
        self.pass_on(self.xn, turn, self.sib)
        self.wait(self.yn, turn)
        if turn % 2 == 1:
            self.pass_on(self.yn, turn, self.xn)
        self.pass_on(self.yn, turn, self.sib)
        if turn > 0:
            self.far(turn - 1)

    def far(self, turn):
        self.wait(self.diag, turn)
        self.pass_on(self.diag, turn, self.sib)

    def arrived(self):
        for turn in (0, 1, 2, 3):
            for slot in (self.me, self.xn, self.yn, self.diag):
                self.wait(slot + self.sib - self.me, turn)
        self.home.wait()

    def finish(self):
        for what in self.started:
            self.copy(*what).wait_send()


def gather_scratch(rows, columns):
    return [
        pltpu.VMEM((4, 8, rows, columns), jnp.bfloat16),
        pltpu.SemaphoreType.DMA((32,)),
        pltpu.SemaphoreType.DMA((4, 8)),
        pltpu.SemaphoreType.DMA((2,)),
    ]


class LineScatter:
    def __init__(self, sums, scratch):
        self.sums = sums
        self.other, self.send, self.recv = scratch
        self.line = line_peers()

    def copy(self, turn):
        target = self.line[turn]
        return line_remote(
            self.sums(target),
            self.other.at[turn - 1],
            self.send.at[turn - 1],
            self.recv.at[turn - 1],
            target,
        )

    def begin(self):
        for turn in (1, 2, 3):
            self.copy(turn).start()

    def finish(self, outs):
        rows_all = self.other.shape[1]
        for turn in (1, 2, 3):
            self.copy(turn).wait_recv()
        own = self.sums(self.line[0])

        def one(index, carry):
            rows = pl.ds(pl.multiple_of(index * 16, 16), 16)
            total = own[rows, :].astype(jnp.float32)
            for turn in (0, 1, 2):
                total = total + self.other[turn, rows, :].astype(jnp.float32)
            first = 0
            for out, place, columns in outs:
                out[rows, place : place + columns] = total[:, first : first + columns]
                first += columns
            return carry

        lax.fori_loop(0, rows_all // 16, one, 0)
        for turn in (1, 2, 3):
            self.copy(turn).wait_send()


class DenseScatter:
    def __init__(self, total, scratch):
        def block(place, slot, half):
            return total.at[half, :, slot]

        self.plane = Scatter(block, block, scratch[:SCATTER_REFS])
        me = self.plane.me
        self.line = LineScatter(
            lambda line: total.at[lax.div(line, 2), lax.rem(line, 2), me], scratch[SCATTER_REFS:]
        )

    def begin(self):
        def one(step, carry):
            self.plane.depart(step)
            return carry

        lax.fori_loop(0, 16, one, 0)

    def forward(self):
        self.plane.forward()

    def turn(self):
        def write(half, part, rows, total):
            home = self.plane.mine(0, half)
            home[part, rows, :] = total.astype(home.dtype)

        self.plane.finish(write)
        self.line.begin()

    def finish(self, outs):
        self.line.finish(outs)
        self.plane.drain()


DENSE_REFS = SCATTER_REFS + 3


def dense_scratch(rows, columns):
    return scatter_scratch(2, rows, columns) + [
        pltpu.VMEM((3, rows, columns), jnp.bfloat16),
        pltpu.SemaphoreType.DMA((3,)),
        pltpu.SemaphoreType.DMA((3,)),
    ]


def rope(values, cosine, sine):
    return values * cosine + pltpu.roll(values, HD // 2, 1) * sine


def gain_rows(misc, out):
    for index in range(out.shape[1] // 128):
        rows = pl.ds(index * 128, 128)
        out[:, rows] = jnp.transpose(misc(rows).astype(jnp.float32))


def inverse_rms(values):
    return lax.rsqrt(jnp.mean(values * values, axis=1, keepdims=True) + EPS)


def row_loop(count, chunk, body):
    def one(index, carry):
        body(pl.ds(pl.multiple_of(index * chunk, chunk), chunk))
        return carry

    lax.fori_loop(0, count // chunk, one, 0)


def tile_loop(count, tile, body):
    row_loop(count, tile, body)


ROW_CHUNK = 16
TILE = 256


def attend_kernel(q_heads, kv_heads, experts, tokens, qkv_own, out_own, cosine, sine, bias, picked, rows_out, resid, heads, mixed, lse, prob, qkv_hbm, out_hbm, gains, hidden, *scratch):
    num_rows, width = tokens.shape
    group = q_heads // kv_heads
    qkv_cols = (q_heads + 2 * kv_heads) * HD
    qkv_w, out_w = scratch[0], scratch[4]
    first = DenseGather(qkv_own, qkv_w, scratch[1], scratch[2], scratch[3].at[0])
    second = DenseGather(out_own, out_w, scratch[5], scratch[6], scratch[7].at[0])
    stores = (
        pltpu.make_async_copy(qkv_w, qkv_hbm, scratch[3].at[1]),
        pltpu.make_async_copy(out_w, out_hbm, scratch[7].at[1]),
    )
    for gather in (first, second):
        gather.home.start()
    full_barrier((first.sib, first.xn, first.yn), first.line[1:])
    first.start_line()
    first.start_plane()
    second.start_line()
    for turn in (0, 1, 2, 3):
        first.turn(turn)
    first.far(3)
    second.start_plane()
    first.arrived()
    stores[0].start()
    second.turn(0)

    def flat(ref, cols):
        return ref[:, :, :, cols].reshape(-1, cols.size)

    misc = flat(qkv_w, pl.ds(qkv_cols, 128))
    for index in range(width // 128):
        rows = slice(index * 128, (index + 1) * 128)
        gains[:, rows] = jnp.transpose(misc[rows, :].astype(jnp.float32))

    def norm_one(rows):
        value = tokens[rows, :].astype(jnp.float32)
        normed = value * inverse_rms(value)
        hidden[rows, :] = (normed * gains[experts : experts + 1, :]).astype(jnp.bfloat16)

    row_loop(num_rows, ROW_CHUNK, norm_one)

    def project(index, carry):
        cols = pl.ds(pl.multiple_of(index * TILE, TILE), TILE)
        raw = nn_dot(hidden[...], flat(qkv_w, cols))
        turned = index < (q_heads + kv_heads) // 2
        cos_now = jnp.where(turned, cosine[...], 1.0)
        sin_now = jnp.where(turned, sine[...], 0.0)
        for part in (0, 1):
            value = rope(raw[:, part * HD : (part + 1) * HD], cos_now, sin_now)
            heads[2 * index + part] = value.astype(jnp.bfloat16)
        return carry

    lax.fori_loop(0, (q_heads + 2 * kv_heads) // 2, project, 0)
    second.turn(1)
    lse[...] = jnp.zeros_like(lse)

    def head_step(head, carry):
        kv_head = q_heads + lax.div(head, group)
        cols = pl.ds(pl.multiple_of(head * HD, HD), HD)
        for first, keys in ((0, PROMPT), (PROMPT, num_rows)):
            rows = pl.ds(first, keys - first)
            query = heads[head, rows, :]
            score = nt_dot(query, heads[kv_head, :keys, :]) * HD ** (-0.5) + bias[rows, :keys]
            top = jnp.max(score, axis=1, keepdims=True)
            weight = jnp.exp(score - top)
            total = jnp.sum(weight, axis=1, keepdims=True)
            value = nn_dot(weight.astype(jnp.bfloat16), heads[kv_head + kv_heads, :keys, :])
            mixed[rows, cols] = (value / total).astype(jnp.bfloat16)
            lanes = lax.broadcasted_iota(jnp.int32, (keys - first, 128), 1)
            lse[rows, :] = jnp.where(lanes == head, top + jnp.log(total), lse[rows, :])

        @pl.when(head == q_heads // 3)
        def _():
            second.turn(2)

        @pl.when(head == 2 * q_heads // 3)
        def _():
            second.turn(3)

        return carry

    lax.fori_loop(0, q_heads, head_step, 0)

    second.far(3)
    second.arrived()
    stores[1].start()

    def out_tile(cols):
        resid[:, cols] = tokens[:, cols].astype(jnp.float32) + nn_dot(mixed[...], flat(out_w, cols))

    tile_loop(width, TILE, out_tile)

    def norm_two(rows):
        value = resid[rows, :]
        normed = value * inverse_rms(value)
        rows_out[rows, :width] = (normed * gains[experts + 1 : experts + 2, :]).astype(jnp.bfloat16)

    row_loop(num_rows, ROW_CHUNK, norm_two)
    logits = nn_dot(rows_out[:, :width], flat(qkv_w, pl.ds(qkv_cols, 128)))
    lanes = lax.broadcasted_iota(jnp.int32, logits.shape, 1)
    logits = jnp.where(lanes < experts, logits, NEG_BIG)
    weight = jnp.exp(logits - jnp.max(logits, axis=1, keepdims=True))
    value = weight / jnp.sum(weight, axis=1, keepdims=True)
    prob[...] = value
    chosen = value * picked[...]
    rows_out[:, width:] = (chosen / jnp.sum(chosen, axis=1, keepdims=True)).astype(jnp.bfloat16)
    for gather, store in zip((first, second), stores):
        store.wait()
        gather.finish()


def attend(tokens, qkv_own, out_own, cosine, sine, bias, picked, q_heads, kv_heads, experts):
    num_rows, width = tokens.shape
    bf = jnp.bfloat16
    all_heads = q_heads + 2 * kv_heads
    return pl.pallas_call(
        functools.partial(attend_kernel, q_heads, kv_heads, experts),
        out_shape=(
            jax.ShapeDtypeStruct((num_rows, width + 128), bf),
            jax.ShapeDtypeStruct((num_rows, width), jnp.float32),
            jax.ShapeDtypeStruct((all_heads, num_rows, HD), bf),
            jax.ShapeDtypeStruct((num_rows, q_heads * HD), bf),
            jax.ShapeDtypeStruct((num_rows, 128), jnp.float32),
            jax.ShapeDtypeStruct((num_rows, 128), jnp.float32),
            jax.ShapeDtypeStruct((4, 8, *qkv_own.shape), bf),
            jax.ShapeDtypeStruct((4, 8, *out_own.shape), bf),
        ),
        in_specs=[VMEM, ANY, ANY] + [VMEM] * 4,
        out_specs=(VMEM,) * 6 + (ANY, ANY),
        scratch_shapes=[
            pltpu.VMEM((128, width), jnp.float32),
            pltpu.VMEM((num_rows, width), bf),
        ]
        + gather_scratch(*qkv_own.shape)
        + gather_scratch(*out_own.shape),
        compiler_params=pltpu.CompilerParams(
            collective_id=5, has_side_effects=True, vmem_limit_bytes=VMEM_BYTES
        ),
        name="attend",
    )(tokens, qkv_own, out_own, cosine, sine, bias, picked)


def attend_back_kernel(q_heads, kv_heads, experts, back_hbm, grad_hbm, resid_hbm, rows_hbm, prob_hbm, picked_hbm, qkv_hbm, out_hbm, mixed_hbm, heads_hbm, lse_hbm, bias_hbm, cos_hbm, sin_hbm, tokens_hbm, grad_in, out_sum, q_sum, k_sum, v_sum, misc_sum, back, grad, resid, hidden_two, prob, picked, qkv_w, out_w, mixed, heads, lse, bias, cosine, sine, tokens, gains, gain_sums, grad_logit, grad_proj, grad_mixed, grad_qkv, grad_kv, hidden, load, *scratch):
    num_rows, width = tokens.shape
    group = q_heads // kv_heads
    q_cols = q_heads * HD
    k_cols = kv_heads * HD
    qkv_cols = q_cols + 2 * k_cols
    near_cols = group * HD
    bf = jnp.bfloat16
    parts, scatters = [], []
    for index in range(4):
        some = scratch[index * (1 + DENSE_REFS) : (index + 1) * (1 + DENSE_REFS)]
        parts.append(some[0])
        scatters.append(DenseScatter(some[0], some[1:]))
    out_part, near_part, rest_part, misc_part = parts
    out_scatter, near_scatter, rest_scatter, misc_scatter = scatters
    pairs = (
        (prob_hbm, prob),
        (picked_hbm, picked),
        (back_hbm, back),
        (qkv_hbm, qkv_w),
        (resid_hbm, resid),
        (grad_hbm, grad),
        (rows_hbm, hidden_two),
        (out_hbm, out_w),
        (mixed_hbm, mixed),
        (heads_hbm, heads),
        (lse_hbm, lse),
        (bias_hbm, bias),
        (cos_hbm, cosine),
        (sin_hbm, sine),
        (tokens_hbm, tokens),
    )
    loads = [pltpu.make_async_copy(src, dst, load.at[i]) for i, (src, dst) in enumerate(pairs)]
    for copy in loads:
        copy.start()
    full_barrier(out_scatter.plane.peers(), out_scatter.line.line[1:])
    for copy in loads[:3]:
        copy.wait()
    gain_sums[...] = jnp.zeros_like(gain_sums)

    def router_rows(rows):
        value = prob[rows, :]
        chosen = value * picked[rows, :]
        total = jnp.sum(chosen, axis=1, keepdims=True)
        comb = chosen / total
        grad_comb = back[rows, width:]
        grad_chosen = (
            picked[rows, :] * (grad_comb - jnp.sum(grad_comb * comb, axis=1, keepdims=True)) / total
        )
        logit = value * (grad_chosen - jnp.sum(value * grad_chosen, axis=1, keepdims=True))
        grad_logit[rows, :] = logit.astype(bf)

    row_loop(num_rows, 64, router_rows)
    loads[3].wait()
    misc = qkv_w.at[:, pl.ds(qkv_cols, 128)]
    gain_rows(lambda rows: misc[rows, :], gains)
    lanes = lax.broadcasted_iota(jnp.int32, (TILE, 128), 1)

    def hidden_tile(cols):
        router = jnp.where(lanes < experts, misc[cols, :], jnp.zeros((), bf))
        back[:, cols] = back[:, cols] + nt_dot(grad_logit[...], router)

    tile_loop(width, TILE, hidden_tile)
    for copy in loads[4:]:
        copy.wait()

    def fold(values):
        return jnp.sum(values.reshape(-1, 8, width), axis=0)

    def norm_two(rows):
        value = resid[rows, :]
        inverse = inverse_rms(value)
        normed = value * inverse
        grad_hidden = back[rows, :width]
        gain_sums[8:16, :] = gain_sums[8:16, :] + fold(grad_hidden * normed)
        grad_norm = grad_hidden * gains[experts + 1 : experts + 2, :]
        mean = jnp.mean(grad_norm * normed, axis=1, keepdims=True)
        total = grad[rows, :] + inverse * (grad_norm - normed * mean)
        grad[rows, :] = total
        grad_proj[rows, :] = total.astype(bf)

    row_loop(num_rows, ROW_CHUNK, norm_two)

    def weight_loop(part, left, right):
        _, _, blocks, rows_each, columns = part.shape
        span = blocks * rows_each

        def one(line, carry):
            cols = pl.ds(pl.multiple_of(line * span, 128), span)
            total = tn_dot(left[:, cols], right[...]).astype(bf)
            part[lax.div(line, 2), lax.rem(line, 2)] = total.reshape(blocks, rows_each, columns)
            return carry

        lax.fori_loop(0, 4, one, 0)

    weight_loop(out_part, mixed, grad_proj)
    out_scatter.begin()

    def mixed_tile(cols):
        grad_mixed[:, cols] = nt_dot(
            grad_proj[...], out_w[cols, :]
        ).astype(bf)

    tile_loop(q_cols, TILE, mixed_tile)

    def norm_one(rows):
        value = tokens[rows, :].astype(jnp.float32)
        normed = value * inverse_rms(value)
        hidden[rows, :] = (normed * gains[experts : experts + 1, :]).astype(bf)

    row_loop(num_rows, ROW_CHUNK, norm_one)
    scale = HD ** (-0.5)

    def head_step(head, carry):
        kv_head = lax.div(head, group)
        cols = pl.ds(pl.multiple_of(head * HD, HD), HD)

        @pl.when(lax.rem(head, group) == 0)
        def _():
            grad_kv[...] = jnp.zeros_like(grad_kv)

        for first, keys in ((0, PROMPT), (PROMPT, num_rows)):
            rows = pl.ds(first, keys - first)
            key = heads[q_heads + kv_head, :keys, :]
            query = heads[head, rows, :]
            up = grad_mixed[rows, cols]
            lane = lax.broadcasted_iota(jnp.int32, (keys - first, 128), 1)
            total = jnp.sum(jnp.where(lane == head, lse[rows, :], 0.0), axis=1, keepdims=True)
            weight = jnp.exp(nt_dot(query, key) * scale + bias[rows, :keys] - total)
            grad_weight = nt_dot(up, heads[q_heads + kv_heads + kv_head, :keys, :])
            delta = jnp.sum(weight * grad_weight, axis=1, keepdims=True)
            score = (weight * (grad_weight - delta)).astype(bf)
            grad_kv[1, :keys, :] = grad_kv[1, :keys, :] + tn_dot(weight.astype(bf), up)
            grad_kv[0, :keys, :] = grad_kv[0, :keys, :] + tn_dot(score, query) * scale
            value = rope(nn_dot(score, key) * scale, cosine[rows, :], -sine[rows, :])
            grad_qkv[rows, cols] = value.astype(bf)

        @pl.when(lax.rem(head, group) == group - 1)
        def _():
            key_cols = pl.ds(pl.multiple_of(q_cols + kv_head * HD, HD), HD)
            value_cols = pl.ds(pl.multiple_of(q_cols + (kv_heads + kv_head) * HD, HD), HD)
            grad_qkv[:, key_cols] = rope(grad_kv[0], cosine[...], -sine[...]).astype(bf)
            grad_qkv[:, value_cols] = grad_kv[1].astype(bf)

        @pl.when(head == 2)
        def _():
            out_scatter.forward()

        @pl.when(head == group - 1)
        def _():
            weight_loop(near_part, hidden, grad_qkv.at[:, pl.ds(0, near_cols)])
            near_scatter.begin()

        @pl.when(head == group + 1)
        def _():
            out_scatter.turn()

        @pl.when(head == group + 3)
        def _():
            near_scatter.forward()

        return carry

    lax.fori_loop(0, q_heads, head_step, 0)
    weight_loop(rest_part, hidden, grad_qkv.at[:, pl.ds(near_cols, qkv_cols - near_cols)])
    rest_scatter.begin()
    near_scatter.turn()

    def hidden_back_tile(cols):
        back[:, cols] = nt_dot(grad_qkv[...], qkv_w[cols, pl.ds(0, qkv_cols)])

    tile_loop(width, TILE, hidden_back_tile)
    rest_scatter.forward()

    def last_rows(rows):
        value = tokens[rows, :].astype(jnp.float32)
        inverse = inverse_rms(value)
        normed = value * inverse
        grad_hidden = back[rows, :width]
        gain_sums[0:8, :] = gain_sums[0:8, :] + fold(grad_hidden * normed)
        grad_norm = grad_hidden * gains[experts : experts + 1, :]
        mean = jnp.mean(grad_norm * normed, axis=1, keepdims=True)
        grad[rows, :] = grad[rows, :] + inverse * (grad_norm - normed * mean)

    row_loop(num_rows, ROW_CHUNK, last_rows)
    store = pltpu.make_async_copy(grad, grad_in, load.at[0])
    store.start()
    gains[0:16, :] = gain_sums[...]
    _, _, blocks, rows_each, _ = misc_part.shape
    span = blocks * rows_each

    def misc_line(line, carry):
        cols = pl.ds(pl.multiple_of(line * span, 128), span)
        router = tn_dot(hidden_two[:, cols], grad_logit[...])
        one = jnp.sum(gains[0:8, cols], axis=0, keepdims=True)
        two = jnp.sum(gains[8:16, cols], axis=0, keepdims=True)
        place = lax.broadcasted_iota(jnp.int32, (128, span), 0)
        block = jnp.where(place == experts, one, jnp.where(place == experts + 1, two, 0.0))
        total = (router + jnp.transpose(block)).astype(bf)
        misc_part[lax.div(line, 2), lax.rem(line, 2)] = total.reshape(blocks, rows_each, 128)
        return carry

    lax.fori_loop(0, 4, misc_line, 0)
    misc_scatter.begin()
    misc_scatter.forward()
    rest_scatter.turn()
    misc_scatter.turn()
    out_scatter.finish(((out_sum, 0, width),))
    near_scatter.finish(((q_sum, 0, near_cols),))
    rest_scatter.finish(
        ((q_sum, near_cols, q_cols - near_cols), (k_sum, 0, k_cols), (v_sum, 0, k_cols))
    )
    misc_scatter.finish(((misc_sum, 0, 128),))
    store.wait()


def attend_back(back, grad, resid, rows_own, prob, picked, qkv_w, out_w, mixed, heads, lse, bias, cosine, sine, tokens, q_heads, kv_heads, experts):
    num_rows, width = tokens.shape
    bf = jnp.bfloat16
    arrays = (back, grad, resid, rows_own, prob, picked, qkv_w, out_w, mixed, heads, lse, bias, cosine, sine, tokens)
    k_cols = kv_heads * HD
    q_cols = q_heads * HD
    qkv_cols = q_cols + 2 * k_cols
    near_cols = q_cols // kv_heads
    block_rows = width // 32
    scratch = []
    for columns in (width, near_cols, qkv_cols - near_cols, 128):
        scratch += [pltpu.VMEM((2, 2, 8, block_rows, columns), bf)]
        scratch += dense_scratch(block_rows, columns)
    return pl.pallas_call(
        functools.partial(attend_back_kernel, q_heads, kv_heads, experts),
        out_shape=(jax.ShapeDtypeStruct((num_rows, width), jnp.float32),)
        + tuple(
            jax.ShapeDtypeStruct((block_rows, columns), jnp.float32)
            for columns in (width, q_cols, k_cols, k_cols, 128)
        ),
        in_specs=[ANY] * len(arrays),
        out_specs=(ANY,) + (VMEM,) * 5,
        scratch_shapes=[pltpu.VMEM(array.shape, array.dtype) for array in arrays]
        + [
            pltpu.VMEM((128, width), jnp.float32),
            pltpu.VMEM((16, width), jnp.float32),
            pltpu.VMEM((num_rows, 128), bf),
            pltpu.VMEM((num_rows, width), bf),
            pltpu.VMEM((num_rows, q_cols), bf),
            pltpu.VMEM((num_rows, qkv_cols), bf),
            pltpu.VMEM((2, num_rows, HD), jnp.float32),
            pltpu.VMEM((num_rows, width), bf),
            pltpu.SemaphoreType.DMA((len(arrays),)),
        ]
        + scratch,
        compiler_params=pltpu.CompilerParams(
            collective_id=6, has_side_effects=True, vmem_limit_bytes=67043328
        ),
        name="attend_back",
    )(*arrays)


def body_plane(
    tokens,
    targets,
    valid_count,
    segments,
    routes,
    gain_attn,
    w_query,
    w_key,
    w_value,
    w_out,
    gain_moe,
    w_router,
    w_gate,
    w_up,
    w_down,
):
    bf = jnp.bfloat16
    num_rows, width = tokens.shape
    half = num_rows // 2
    q_cols, k_cols = w_query.shape[1], w_key.shape[1]
    num_experts = w_router.shape[1]
    num_heads = q_cols // HD
    kv_heads = k_cols // HD
    pad_cols = 128 - 2 - num_experts
    qkv_own = jnp.concatenate(
        [
            w_query,
            w_key,
            w_value,
            w_router,
            gain_attn[:, None],
            gain_moe[:, None],
            jnp.zeros((gain_attn.shape[0], pad_cols), bf),
        ],
        axis=1,
    )
    gate_w = lax.all_gather(w_gate, "dp", axis=1, tiled=True)[0]
    up_w = lax.all_gather(w_up, "dp", axis=1, tiled=True)[0]
    tok_pos = positions(segments)
    bias = jnp.where(key_mask(segments), 0.0, NEG_BIG)
    freq = THETA ** (-2.0 * jnp.arange(HD // 2, dtype=jnp.float32) / HD)
    angle = tok_pos.astype(jnp.float32)[:, None] * freq[None, :]
    cosine, sine_part = jnp.cos(angle), jnp.sin(angle)
    cosine = jnp.concatenate([cosine, cosine], axis=1)
    sine = jnp.concatenate([-sine_part, sine_part], axis=1)
    lane_ids = jnp.arange(128, dtype=jnp.int32)
    picked = jnp.sum((routes[:, :, None] == lane_ids[None, None, :]).astype(jnp.float32), axis=1)
    rows_own, resid_mid, heads, mixed, lse, prob, qkv_w, out_w = attend(
        tokens, qkv_own, w_out, cosine, sine, bias, picked, num_heads, kv_heads, num_experts
    )
    rows_all, gate_val, down_w = expert_in(
        rows_own.reshape(2, half, width + 128), gate_w, w_down[0]
    )
    down_w = down_w.reshape(-1, width)
    total_rows = num_rows * lax.axis_size(("dp", "exp"))
    global_row = lax.axis_index(("dp", "exp")) * num_rows + jnp.arange(num_rows, dtype=jnp.int32)
    loss_scale = total_rows / valid_count[0].astype(jnp.float32)
    scales = jnp.broadcast_to(
        jnp.where(global_row < valid_count[0], loss_scale, 0.0)[:, None], (num_rows, 128)
    )
    layer_out, grad_out, grad_out_b, ua = expert_out(
        rows_all, gate_val, up_w, down_w, resid_mid, targets, scales
    )
    layer_out = layer_out.reshape(num_rows, width)
    dgu, part, down_part = expert_back(
        grad_out_b, rows_all, gate_val, ua, gate_w, up_w, down_w
    )
    back, gate_part, up_part = expert_grads(part, rows_all, dgu)
    expert_sums = tuple(
        lax.psum_scatter(grad[None], "dp", scatter_dimension=1, tiled=True).astype(jnp.float32)
        for grad in (gate_part, up_part, down_part)
    )
    grad_in, out_sum, q_sum, k_sum, v_sum, misc_sum = attend_back(
        back.reshape(num_rows, width + 128),
        grad_out.reshape(num_rows, width),
        resid_mid,
        rows_own,
        prob,
        picked,
        qkv_w.reshape(width, -1),
        out_w.reshape(q_cols, width),
        mixed,
        heads,
        lse,
        bias,
        cosine,
        sine,
        tokens,
        num_heads,
        kv_heads,
        num_experts,
    )
    return (
        layer_out,
        grad_in,
        misc_sum[:, num_experts],
        q_sum,
        k_sum,
        v_sum,
        out_sum,
        misc_sum[:, num_experts + 1],
        misc_sum[:, :num_experts],
        *expert_sums,
    )


def solution(mesh):
    in_specs = (
        P(("dp", "exp"), None),
        P(("dp", "exp"), None),
        P(),
        P(("dp", "exp")),
        P(("dp", "exp"), None),
        P(("dp", "exp")),
        P(("dp", "exp"), None),
        P(("dp", "exp"), None),
        P(("dp", "exp"), None),
        P(("dp", "exp"), None),
        P(("dp", "exp")),
        P(("dp", "exp"), None),
        P("exp", "dp", None),
        P("exp", "dp", None),
        P("exp", "dp", None),
    )
    out_specs = (
        P(("dp", "exp"), None),
        P(("dp", "exp"), None),
        P(("dp", "exp")),
        P(("dp", "exp"), None),
        P(("dp", "exp"), None),
        P(("dp", "exp"), None),
        P(("dp", "exp"), None),
        P(("dp", "exp")),
        P(("dp", "exp"), None),
        P("exp", "dp", None),
        P("exp", "dp", None),
        P("exp", "dp", None),
    )
    body = body_plane if (mesh.shape["dp"], mesh.shape["exp"]) == (4, 8) else body_general
    return jax.shard_map(body, mesh=mesh, in_specs=in_specs, out_specs=out_specs, check_vma=False)
```

```python
import functools

import jax
import jax.numpy as jnp
from jax import lax
from jax.experimental import pallas as pl
from jax.experimental.pallas import tpu as pltpu
from jax.sharding import PartitionSpec as P

HD = 128
PROMPT = 256
NCONT = 2


EPS = 1e-06
THETA = 10000.0
HIGH = lax.Precision.HIGHEST
NEG_BIG = -1e30


def positions(segments):
    count_rows = segments.shape[0]
    row_ids = jnp.arange(count_rows, dtype=jnp.int32)
    labels = jnp.arange(NCONT + 1, dtype=jnp.int32)
    member = segments[:, None] == labels[None, :]
    first_row = jnp.min(jnp.where(member, row_ids[:, None], count_rows), axis=0)
    start_row = jnp.sum(jnp.where(member, first_row[None, :], 0), axis=1)
    return jnp.where(segments == 0, row_ids, PROMPT + row_ids - start_row)


def key_mask(segments):
    row_ids = jnp.arange(segments.shape[0], dtype=jnp.int32)
    causal = row_ids[None, :] <= row_ids[:, None]
    visible = (segments[None, :] == 0) | (segments[None, :] == segments[:, None])
    return causal & visible


def rotate(values, pos_rows, sign_value):
    half_size = HD // 2
    freq = THETA ** (-2.0 * jnp.arange(half_size, dtype=jnp.float32) / HD)
    angle = pos_rows.astype(jnp.float32)[:, None] * freq[None, :]
    cosine = jnp.cos(angle)[:, None, :]
    sine_part = sign_value * jnp.sin(angle)[:, None, :]
    first_half = values[..., :half_size]
    second = values[..., half_size:]
    return jnp.concatenate(
        [first_half * cosine - second * sine_part, second * cosine + first_half * sine_part],
        axis=-1,
    )


def attention_scores(query_b, key_b, allowed):
    logits = jnp.einsum(
        "qkgd,pkd->kgqp", query_b, key_b, preferred_element_type=jnp.float32
    ) * HD ** (-0.5)
    return jnp.where(allowed[None, None], logits, NEG_BIG)


def expert_gates(rows_in, gate_w, up_w):
    gate_val = jnp.einsum("sacd,adf->sacf", rows_in, gate_w, preferred_element_type=jnp.float32)
    up_val = jnp.einsum("sacd,adf->sacf", rows_in, up_w, preferred_element_type=jnp.float32)
    return (gate_val, up_val)


def body_general(
    tokens,
    targets,
    valid_count,
    segments,
    routes,
    gain_attn,
    w_query,
    w_key,
    w_value,
    w_out,
    gain_moe,
    w_router,
    w_gate,
    w_up,
    w_down,
):
    gain_one, query_w, key_w, value_w, out_w, gain_two, router_w = (
        lax.all_gather(gain_attn, ("dp", "exp"), axis=0, tiled=True),
        lax.all_gather(w_query, ("dp", "exp"), axis=0, tiled=True),
        lax.all_gather(w_key, ("dp", "exp"), axis=0, tiled=True),
        lax.all_gather(w_value, ("dp", "exp"), axis=0, tiled=True),
        lax.all_gather(w_out, ("dp", "exp"), axis=0, tiled=True),
        lax.all_gather(gain_moe, ("dp", "exp"), axis=0, tiled=True),
        lax.all_gather(w_router, ("dp", "exp"), axis=0, tiled=True),
    )
    gate_w, up_w, down_w = (
        lax.all_gather(w_gate, "dp", axis=1, tiled=True),
        lax.all_gather(w_up, "dp", axis=1, tiled=True),
        lax.all_gather(w_down, "dp", axis=1, tiled=True),
    )
    num_rows = tokens.shape[0]
    width = tokens.shape[1]
    num_heads = query_w.shape[1] // HD
    kv_heads = key_w.shape[1] // HD
    group_size = num_heads // kv_heads
    num_experts = router_w.shape[1]
    top_count = routes.shape[1]
    exp_local = gate_w.shape[0]
    exp_ranks = lax.axis_size("exp")
    capacity = 5 * num_rows * top_count // (4 * num_experts)
    tok_pos = positions(segments)
    allowed = key_mask(segments)
    resid_in = tokens.astype(jnp.float32)
    inv_one = lax.rsqrt(jnp.mean(resid_in * resid_in, axis=-1, keepdims=True) + EPS)
    normed_one = resid_in * inv_one
    hidden_one = (normed_one * gain_one.astype(jnp.float32)).astype(jnp.bfloat16)
    query_raw = jnp.dot(hidden_one, query_w, preferred_element_type=jnp.float32)
    key_raw = jnp.dot(hidden_one, key_w, preferred_element_type=jnp.float32)
    value_b = jnp.dot(hidden_one, value_w, preferred_element_type=jnp.float32).astype(jnp.bfloat16)
    query_b = rotate(query_raw.reshape(num_rows, num_heads, HD), tok_pos, 1.0).astype(jnp.bfloat16)
    query_b = query_b.reshape(num_rows, kv_heads, group_size, HD)
    key_b = rotate(key_raw.reshape(num_rows, kv_heads, HD), tok_pos, 1.0).astype(jnp.bfloat16)
    value_h = value_b.reshape(num_rows, kv_heads, HD)
    logit_att = attention_scores(query_b, key_b, allowed)
    row_max = jnp.max(logit_att, axis=-1, keepdims=True)
    log_total = row_max + jnp.log(jnp.sum(jnp.exp(logit_att - row_max), axis=-1, keepdims=True))
    probs_b = jnp.exp(logit_att - log_total).astype(jnp.bfloat16)
    attn_vals = jnp.einsum("kgqp,pkd->qkgd", probs_b, value_h, preferred_element_type=jnp.float32)
    attn_vals = attn_vals.reshape(num_rows, num_heads * HD).astype(jnp.bfloat16)
    resid_mid = resid_in + jnp.dot(attn_vals, out_w, preferred_element_type=jnp.float32)
    inv_two = lax.rsqrt(jnp.mean(resid_mid * resid_mid, axis=-1, keepdims=True) + EPS)
    normed_two = resid_mid * inv_two
    gain_two_f = gain_two.astype(jnp.float32)
    hidden_two = (normed_two * gain_two_f).astype(jnp.bfloat16)
    router_prob = jax.nn.softmax(
        jnp.dot(hidden_two, router_w, preferred_element_type=jnp.float32), axis=-1
    )
    expert_ids = jnp.arange(num_experts, dtype=jnp.int32)
    route_hot = routes[:, :, None] == expert_ids[None, None, :]
    chosen = jnp.sum(jnp.where(route_hot, router_prob[:, None, :], 0.0), axis=-1)
    weight_sum = jnp.sum(chosen, axis=1, keepdims=True)
    combine = chosen / weight_sum
    flat_hot = route_hot.reshape(num_rows * top_count, num_experts).astype(jnp.int32)
    slot_index = jnp.sum((jnp.cumsum(flat_hot, axis=0) - flat_hot) * flat_hot, axis=1)
    dest_index = routes.reshape(-1) * capacity + slot_index
    send_shape = (exp_ranks, exp_local, capacity, width)
    send_rows = jnp.zeros((num_experts * capacity, width), jnp.bfloat16)
    send_rows = (
        send_rows.at[dest_index].set(jnp.repeat(hidden_two, top_count, axis=0)).reshape(send_shape)
    )
    gate_val, up_val = expert_gates(
        lax.all_to_all(send_rows, "exp", split_axis=0, concat_axis=0, tiled=True), gate_w, up_w
    )
    act_b = (jax.nn.relu(gate_val) * up_val).astype(jnp.bfloat16)
    out_b = jnp.einsum("sacf,afd->sacd", act_b, down_w, preferred_element_type=jnp.float32).astype(
        jnp.bfloat16
    )
    returned = lax.all_to_all(out_b, "exp", split_axis=0, concat_axis=0, tiled=True)
    route_out = returned.reshape(num_experts * capacity, width)[dest_index].reshape(
        num_rows, top_count, width
    )
    route_out_f = route_out.astype(jnp.float32)
    resid_out = resid_mid + jnp.sum(combine[:, :, None] * route_out_f, axis=1)
    layer_out = resid_out.astype(jnp.bfloat16)
    total_rows = num_rows * lax.axis_size(("dp", "exp"))
    global_row = lax.axis_index(("dp", "exp")) * num_rows + jnp.arange(num_rows, dtype=jnp.int32)
    loss_scale = total_rows / valid_count[0].astype(jnp.float32)
    grad_out = jnp.where(
        (global_row < valid_count[0])[:, None],
        (resid_out - targets.astype(jnp.float32)) * loss_scale,
        0.0,
    )
    gain_one, query_w, key_w, value_w, out_w, gain_two, router_w = (
        lax.all_gather(gain_attn, ("dp", "exp"), axis=0, tiled=True),
        lax.all_gather(w_query, ("dp", "exp"), axis=0, tiled=True),
        lax.all_gather(w_key, ("dp", "exp"), axis=0, tiled=True),
        lax.all_gather(w_value, ("dp", "exp"), axis=0, tiled=True),
        lax.all_gather(w_out, ("dp", "exp"), axis=0, tiled=True),
        lax.all_gather(gain_moe, ("dp", "exp"), axis=0, tiled=True),
        lax.all_gather(w_router, ("dp", "exp"), axis=0, tiled=True),
    )
    gain_two_f = gain_two.astype(jnp.float32)
    grad_route = (combine[:, :, None] * grad_out[:, None, :]).astype(jnp.bfloat16)
    grad_comb = jnp.sum(grad_out[:, None, :] * route_out_f, axis=-1)
    grad_send = jnp.zeros((num_experts * capacity, width), jnp.bfloat16)
    grad_send = (
        grad_send.at[dest_index]
        .set(grad_route.reshape(num_rows * top_count, width))
        .reshape(send_shape)
    )
    expert_rows, grad_recv = (
        lax.all_to_all(send_rows, "exp", split_axis=0, concat_axis=0, tiled=True),
        lax.all_to_all(grad_send, "exp", split_axis=0, concat_axis=0, tiled=True),
    )
    gate_val, up_val = expert_gates(expert_rows, gate_w, up_w)
    gate_relu = jax.nn.relu(gate_val)
    act_b = (gate_relu * up_val).astype(jnp.bfloat16)
    grad_act = jnp.einsum("sacd,afd->sacf", grad_recv, down_w, preferred_element_type=jnp.float32)
    grad_down_w = jnp.einsum("sacf,sacd->afd", act_b, grad_recv, preferred_element_type=jnp.float32)
    grad_gate_b = jnp.where(gate_val > 0, grad_act * up_val, 0.0).astype(jnp.bfloat16)
    grad_up_b = (grad_act * gate_relu).astype(jnp.bfloat16)
    grad_gate_w = jnp.einsum(
        "sacd,sacf->adf", expert_rows, grad_gate_b, preferred_element_type=jnp.float32
    )
    grad_up_w = jnp.einsum(
        "sacd,sacf->adf", expert_rows, grad_up_b, preferred_element_type=jnp.float32
    )
    grad_rows = (
        jnp.einsum("sacf,adf->sacd", grad_gate_b, gate_w, preferred_element_type=jnp.float32)
        + jnp.einsum("sacf,adf->sacd", grad_up_b, up_w, preferred_element_type=jnp.float32)
    ).astype(jnp.bfloat16)
    grad_back = lax.all_to_all(grad_rows, "exp", split_axis=0, concat_axis=0, tiled=True)
    grad_copies = grad_back.reshape(num_experts * capacity, width)[dest_index].reshape(
        num_rows, top_count, width
    )
    grad_hidden_two = jnp.sum(grad_copies.astype(jnp.float32), axis=1)
    grad_chosen = (grad_comb - jnp.sum(grad_comb * combine, axis=1, keepdims=True)) / weight_sum
    grad_prob = jnp.sum(jnp.where(route_hot, grad_chosen[:, :, None], 0.0), axis=1)
    grad_logit = router_prob * (
        grad_prob - jnp.sum(router_prob * grad_prob, axis=-1, keepdims=True)
    )
    router_f = router_w.astype(jnp.float32)
    grad_hidden_two = grad_hidden_two + jnp.einsum(
        "re,de->rd", grad_logit, router_f, precision=HIGH
    )
    grad_router = jnp.einsum(
        "rd,re->de", hidden_two.astype(jnp.float32), grad_logit, precision=HIGH
    )
    grad_gain_two = jnp.sum(grad_hidden_two * normed_two, axis=0)
    grad_norm_two = grad_hidden_two * gain_two_f
    grad_mid = grad_out + inv_two * (
        grad_norm_two - normed_two * jnp.mean(grad_norm_two * normed_two, axis=-1, keepdims=True)
    )
    grad_proj_b = grad_mid.astype(jnp.bfloat16)
    grad_out_w = jnp.einsum("rh,rd->hd", attn_vals, grad_proj_b, preferred_element_type=jnp.float32)
    grad_vals_b = jnp.einsum(
        "rd,hd->rh", grad_proj_b, out_w, preferred_element_type=jnp.float32
    ).astype(jnp.bfloat16)
    grad_vals_b = grad_vals_b.reshape(num_rows, kv_heads, group_size, HD)
    logit_att = attention_scores(query_b, key_b, allowed)
    probs = jnp.exp(logit_att - log_total)
    probs_b = probs.astype(jnp.bfloat16)
    grad_value = jnp.einsum(
        "kgqp,qkgd->pkd", probs_b, grad_vals_b, preferred_element_type=jnp.float32
    )
    grad_prob_att = jnp.einsum(
        "qkgd,pkd->kgqp", grad_vals_b, value_h, preferred_element_type=jnp.float32
    )
    delta_row = jnp.sum(probs * grad_prob_att, axis=-1, keepdims=True)
    grad_score_b = (probs * (grad_prob_att - delta_row)).astype(jnp.bfloat16)
    grad_query = jnp.einsum(
        "kgqp,pkd->qkgd", grad_score_b, key_b, preferred_element_type=jnp.float32
    ) * HD ** (-0.5)
    grad_key = jnp.einsum(
        "kgqp,qkgd->pkd", grad_score_b, query_b, preferred_element_type=jnp.float32
    ) * HD ** (-0.5)
    grad_query_b = rotate(grad_query.reshape(num_rows, num_heads, HD), tok_pos, -1.0).astype(
        jnp.bfloat16
    )
    grad_query_b = grad_query_b.reshape(num_rows, num_heads * HD)
    grad_key_b = (
        rotate(grad_key, tok_pos, -1.0).astype(jnp.bfloat16).reshape(num_rows, kv_heads * HD)
    )
    grad_value_b = grad_value.astype(jnp.bfloat16).reshape(num_rows, kv_heads * HD)
    grad_query_w = jnp.einsum(
        "rd,rh->dh", hidden_one, grad_query_b, preferred_element_type=jnp.float32
    )
    grad_key_w = jnp.einsum("rd,rh->dh", hidden_one, grad_key_b, preferred_element_type=jnp.float32)
    grad_value_w = jnp.einsum(
        "rd,rh->dh", hidden_one, grad_value_b, preferred_element_type=jnp.float32
    )
    grad_hidden_one = (
        jnp.einsum("rh,dh->rd", grad_query_b, query_w, preferred_element_type=jnp.float32)
        + jnp.einsum("rh,dh->rd", grad_key_b, key_w, preferred_element_type=jnp.float32)
        + jnp.einsum("rh,dh->rd", grad_value_b, value_w, preferred_element_type=jnp.float32)
    )
    grad_gain_one = jnp.sum(grad_hidden_one * normed_one, axis=0)
    grad_norm_one = grad_hidden_one * gain_one.astype(jnp.float32)
    grad_in = grad_mid + inv_one * (
        grad_norm_one - normed_one * jnp.mean(grad_norm_one * normed_one, axis=-1, keepdims=True)
    )
    dense_sums = (
        lax.psum_scatter(grad_gain_one, ("dp", "exp"), scatter_dimension=0, tiled=True),
        lax.psum_scatter(grad_query_w, ("dp", "exp"), scatter_dimension=0, tiled=True),
        lax.psum_scatter(grad_key_w, ("dp", "exp"), scatter_dimension=0, tiled=True),
        lax.psum_scatter(grad_value_w, ("dp", "exp"), scatter_dimension=0, tiled=True),
        lax.psum_scatter(grad_out_w, ("dp", "exp"), scatter_dimension=0, tiled=True),
        lax.psum_scatter(grad_gain_two, ("dp", "exp"), scatter_dimension=0, tiled=True),
        lax.psum_scatter(grad_router, ("dp", "exp"), scatter_dimension=0, tiled=True),
    )
    expert_sums = (
        lax.psum_scatter(
            grad_gate_w.astype(jnp.bfloat16), "dp", scatter_dimension=1, tiled=True
        ).astype(jnp.float32),
        lax.psum_scatter(
            grad_up_w.astype(jnp.bfloat16), "dp", scatter_dimension=1, tiled=True
        ).astype(jnp.float32),
        lax.psum_scatter(
            grad_down_w.astype(jnp.bfloat16), "dp", scatter_dimension=1, tiled=True
        ).astype(jnp.float32),
    )
    return (
        layer_out,
        grad_in,
        dense_sums[0],
        dense_sums[1],
        dense_sums[2],
        dense_sums[3],
        dense_sums[4],
        dense_sums[5],
        dense_sums[6],
        expert_sums[0],
        expert_sums[1],
        expert_sums[2],
    )


MESH = pl.DeviceIdType.MESH
ANY = pl.BlockSpec(memory_space=pl.ANY)
VMEM = pl.BlockSpec(memory_space=pltpu.VMEM)
VMEM_BYTES = 62 * 2**20


def nn_dot(left, right):
    return jnp.dot(left, right, preferred_element_type=jnp.float32)


def nt_dot(left, right):
    return lax.dot_general(
        left, right, (((1,), (1,)), ((), ())), preferred_element_type=jnp.float32
    )


def tn_dot(left, right):
    return lax.dot_general(
        left, right, (((0,), (0,)), ((), ())), preferred_element_type=jnp.float32
    )


def plane_peers():
    me = lax.axis_index("exp")
    core = lax.rem(me, 2)
    x_pos = lax.rem(lax.div(me, 2), 2)
    y_pos = lax.div(me, 4)
    return me, me + 1 - 2 * core, me + 2 - 4 * x_pos, me + 4 - 8 * y_pos


def remote(src, dst, send_sem, recv_sem, peer):
    return pltpu.make_async_remote_copy(
        src_ref=src,
        dst_ref=dst,
        send_sem=send_sem,
        recv_sem=recv_sem,
        device_id={"exp": peer},
        device_id_type=MESH,
    )


def plane_barrier(peers):
    barrier = pltpu.get_barrier_semaphore()
    for peer in peers:
        pl.semaphore_signal(barrier, inc=1, device_id={"exp": peer}, device_id_type=MESH)
    pl.semaphore_wait(barrier, len(peers))


def step_place(step, quad):
    odd = lax.rem(step, 2)
    last = lax.div(quad, 3)
    mid = lax.rem(lax.div(quad + 1, 2), 2)
    return mid * (1 - odd) + last, mid * odd + last


class Gather:
    def __init__(self, own, buf, send, recv):
        self.own, self.buf, self.send, self.recv = own, buf, send, recv
        self.me, self.sib, self.xn, self.yn = plane_peers()
        self.diag = self.xn + self.yn - self.me

    def own_copy(self, half, peer, sem):
        return remote(
            self.own.at[half],
            self.buf.at[self.me, half],
            self.send.at[sem],
            self.recv.at[self.me, half],
            peer,
        )

    def pass_copy(self, slot, half, peer, sem):
        return remote(
            self.buf.at[slot, half],
            self.buf.at[slot, half],
            self.send.at[sem],
            self.recv.at[slot, half],
            peer,
        )

    def own_copies(self):
        return (
            self.own_copy(0, self.xn, 0),
            self.own_copy(1, self.yn, 1),
            self.own_copy(0, self.sib, 2),
            self.own_copy(1, self.sib, 3),
            self.own_copy(1, self.xn, 4),
            self.own_copy(0, self.yn, 5),
        )

    def near_copies(self):
        return (
            self.pass_copy(self.xn, 0, self.yn, 6),
            self.pass_copy(self.yn, 1, self.xn, 7),
            self.pass_copy(self.xn, 0, self.sib, 8),
            self.pass_copy(self.yn, 1, self.sib, 9),
        )

    def late_copies(self):
        return (
            self.pass_copy(self.xn, 1, self.sib, 10),
            self.pass_copy(self.yn, 0, self.sib, 11),
        )

    def far_copies(self):
        return (
            self.pass_copy(self.diag, 0, self.sib, 12),
            self.pass_copy(self.diag, 1, self.sib, 13),
        )

    def wait_block(self, slot, half):
        self.pass_copy(slot, half, self.sib, 0).wait_recv()

    def begin(self):
        plane_barrier((self.sib, self.xn, self.yn))
        for copy in self.own_copies():
            copy.start()

    def place(self, step):
        quad = lax.div(step, 4)
        far_x, far_y = step_place(step, quad)
        odd = lax.rem(step, 2)
        third = lax.div(quad, 2) * (1 - lax.div(quad, 3))
        other = lax.div(lax.rem(step, 4), 2)
        slot = (
            self.me
            + far_x * (self.xn - self.me)
            + far_y * (self.yn - self.me)
            + other * (self.sib - self.me)
        )
        return slot, odd + third * (1 - 2 * odd), other

    def arrive(self, step):
        @pl.when(step == 4)
        def _():
            self.wait_block(self.xn, 0)
            self.wait_block(self.yn, 1)
            for copy in self.near_copies():
                copy.start()

        @pl.when(step == 8)
        def _():
            self.wait_block(self.xn, 1)
            self.wait_block(self.yn, 0)
            for copy in self.late_copies():
                copy.start()

        @pl.when(step == 12)
        def _():
            self.wait_block(self.diag, 0)
            self.wait_block(self.diag, 1)
            for copy in self.far_copies():
                copy.start()

        slot, half, other = self.place(step)

        @pl.when(other == 1)
        def _():
            self.wait_block(slot, half)

        return slot, half

    def finish(self):
        for copies in (self.own_copies(), self.near_copies(), self.late_copies(), self.far_copies()):
            for copy in copies:
                copy.wait_send()


def line_peers():
    line = lax.axis_index("dp")
    return (
        line,
        line + 1 - 2 * lax.rem(line, 2),
        line + 2 - 4 * lax.div(line, 2),
        3 - line,
    )


def line_remote(src, dst, send_sem, recv_sem, peer):
    return pltpu.make_async_remote_copy(
        src_ref=src,
        dst_ref=dst,
        send_sem=send_sem,
        recv_sem=recv_sem,
        device_id={"dp": peer},
        device_id_type=MESH,
    )


def full_barrier(plane, line):
    barrier = pltpu.get_barrier_semaphore()
    for peer in plane:
        pl.semaphore_signal(barrier, inc=1, device_id={"exp": peer}, device_id_type=MESH)
    for peer in line:
        pl.semaphore_signal(barrier, inc=1, device_id={"dp": peer}, device_id_type=MESH)
    pl.semaphore_wait(barrier, len(plane) + len(line))


def expert_in_kernel(own, gate_hbm, down_own, rows_out, gate_out, down_out, buf, gate, gate_w, down_stage, send, recv, load, store_a, store_b, line_send, line_recv):
    width = gate_w.shape[0]
    gather = Gather(own, buf, send, recv)
    line = line_peers()
    loads = (
        pltpu.make_async_copy(own.at[0], buf.at[gather.me, 0], load.at[0]),
        pltpu.make_async_copy(own.at[1], buf.at[gather.me, 1], load.at[1]),
        pltpu.make_async_copy(gate_hbm, gate_w, load.at[2]),
        pltpu.make_async_copy(down_own, down_stage, load.at[3]),
    )
    for copy in loads:
        copy.start()
    full_barrier((gather.sib, gather.xn, gather.yn), line[1:])
    for copy in gather.own_copies():
        copy.start()

    def down_copy(turn):
        return line_remote(
            down_own,
            down_out.at[line[0]],
            line_send.at[turn - 1],
            line_recv.at[turn - 1],
            line[turn],
        )

    for turn in (1, 2, 3):
        down_copy(turn).start()
    for copy in loads:
        copy.wait()
    down_store = pltpu.make_async_copy(down_stage, down_out.at[line[0]], load.at[4])
    down_store.start()

    def row_store(slot, half, step):
        return pltpu.make_async_copy(buf.at[slot, half], rows_out.at[slot, half], store_a.at[step])

    def gate_store(slot, half, step):
        return pltpu.make_async_copy(gate.at[slot, half], gate_out.at[slot, half], store_b.at[step])

    def one(step, carry):
        slot, half = gather.arrive(step)
        row_store(slot, half, step).start()
        gate[slot, half] = nn_dot(buf[slot, half, :, :width], gate_w[...]).astype(jnp.bfloat16)
        gate_store(slot, half, step).start()
        return carry

    lax.fori_loop(0, 16, one, 0)
    gather.finish()

    def drain(step, carry):
        slot, half, _ = gather.place(step)
        row_store(slot, half, step).wait()
        gate_store(slot, half, step).wait()
        return carry

    lax.fori_loop(0, 16, drain, 0)
    down_store.wait()
    for turn in (1, 2, 3):
        line_remote(
            down_own,
            down_out.at[line[turn]],
            line_send.at[turn - 1],
            line_recv.at[turn - 1],
            line[turn],
        ).wait()


def expert_in(own, gate_w, down_own):
    _, half, columns = own.shape
    width, hidden = gate_w.shape
    bf = jnp.bfloat16
    return pl.pallas_call(
        expert_in_kernel,
        out_shape=(
            jax.ShapeDtypeStruct((8, 2, half, columns), bf),
            jax.ShapeDtypeStruct((8, 2, half, hidden), bf),
            jax.ShapeDtypeStruct((4, *down_own.shape), bf),
        ),
        in_specs=[ANY] * 3,
        out_specs=(ANY, ANY, ANY),
        scratch_shapes=[
            pltpu.VMEM((8, 2, half, columns), bf),
            pltpu.VMEM((8, 2, half, hidden), bf),
            pltpu.VMEM((width, hidden), bf),
            pltpu.VMEM(down_own.shape, bf),
            pltpu.SemaphoreType.DMA((14,)),
            pltpu.SemaphoreType.DMA((8, 2)),
            pltpu.SemaphoreType.DMA((5,)),
            pltpu.SemaphoreType.DMA((16,)),
            pltpu.SemaphoreType.DMA((16,)),
            pltpu.SemaphoreType.DMA((3,)),
            pltpu.SemaphoreType.DMA((3,)),
        ],
        compiler_params=pltpu.CompilerParams(
            collective_id=1, has_side_effects=True, vmem_limit_bytes=VMEM_BYTES
        ),
        name="expert_in",
    )(own, gate_w, down_own)


def row_chunk(rows):
    return 64 if rows % 64 == 0 else 16


def add_rows(target, others):
    parts, rows_all, _ = target.shape
    chunk = row_chunk(rows_all)
    for part in range(parts):

        def one(index, carry):
            rows = pl.ds(pl.multiple_of(index * chunk, chunk), chunk)
            total = target[part, rows, :].astype(jnp.float32)
            for other in others:
                total = total + other[part, rows, :].astype(jnp.float32)
            target[part, rows, :] = total.astype(target.dtype)
            return carry

        lax.fori_loop(0, rows_all // chunk, one, 0)


class Scatter:
    def __init__(self, mine, theirs, scratch):
        self.mine_of, self.theirs = mine, theirs
        self.side, self.relay, self.final = scratch[:3]
        self.send, self.side_sem, self.relay_sem, self.final_sem = scratch[3:]
        self.me, self.sib, self.xn, self.yn = plane_peers()

    def mine(self, place, half):
        slot = (self.me, self.xn, self.yn, self.xn + self.yn - self.me)[place]
        return self.mine_of(place, slot, half)

    def peers(self):
        return self.sib, self.xn, self.yn

    def place(self, step):
        quad = lax.div(step, 4)
        odd = lax.div(lax.rem(step, 4), 2)
        far_x, far_y = step_place(odd, 3 - quad)
        third = lax.div(quad, 2) * (1 - lax.div(quad, 3))
        other = 1 - lax.rem(step, 2)
        slot = (
            self.me
            + far_x * (self.xn - self.me)
            + far_y * (self.yn - self.me)
            + other * (self.sib - self.me)
        )
        return slot, odd + third * (1 - 2 * odd), other, far_x + 2 * far_y

    def side_copy(self, step):
        slot, half, _, place = self.place(step)
        return remote(
            self.theirs(place, slot, half),
            self.side.at[place, half],
            self.send.at[step],
            self.side_sem.at[place, half],
            self.sib,
        )

    def side_wait(self, place, half):
        remote(
            self.side.at[place, half],
            self.side.at[place, half],
            self.send.at[0],
            self.side_sem.at[place, half],
            self.sib,
        ).wait_recv()

    def relay_copy(self, step, way):
        return remote(
            self.mine(3, way),
            self.relay.at[way],
            self.send.at[step],
            self.relay_sem.at[way],
            (self.xn, self.yn)[way],
        )

    def final_copy(self, step, way, half):
        return remote(
            self.mine(1 + way, half),
            self.final.at[way, half],
            self.send.at[step],
            self.final_sem.at[way, half],
            (self.xn, self.yn)[way],
        )

    def depart(self, step):
        @pl.when(self.place(step)[2] == 1)
        def _():
            self.side_copy(step).start()

        for way in (0, 1):

            @pl.when(step == 1 + 2 * way)
            def _():
                self.side_wait(3, way)
                add_rows(self.mine(3, way), (self.side.at[3, way],))
                self.relay_copy(1 + 2 * way, way).start()

            @pl.when(step == 5 + 2 * way)
            def _():
                self.side_wait(1 + way, way)
                add_rows(self.mine(1 + way, way), (self.side.at[1 + way, way],))
                self.final_copy(5 + 2 * way, way, way).start()

    def forward(self):
        for way in (0, 1):
            self.side_wait(1 + way, 1 - way)
            self.relay_copy(0, 1 - way).wait_recv()
            add_rows(
                self.mine(1 + way, 1 - way),
                (self.side.at[1 + way, 1 - way], self.relay.at[1 - way]),
            )
            self.final_copy(9 + 2 * way, way, 1 - way).start()

    def finish(self, write):
        parts, rows_all = self.relay.shape[1:3]
        chunk = row_chunk(rows_all)
        for half in (0, 1):
            home = self.mine(0, half)
            self.side_wait(0, half)
            self.final_copy(0, 0, half).wait_recv()
            self.final_copy(0, 1, half).wait_recv()
            for part in range(parts):

                def one(index, carry, half=half, home=home, part=part):
                    rows = pl.ds(pl.multiple_of(index * chunk, chunk), chunk)
                    total = home[part, rows, :].astype(jnp.float32)
                    total = total + self.side[0, half, part, rows, :].astype(jnp.float32)
                    total = total + self.final[0, half, part, rows, :].astype(jnp.float32)
                    total = total + self.final[1, half, part, rows, :].astype(jnp.float32)
                    write(half, part, rows, total)
                    return carry

                lax.fori_loop(0, rows_all // chunk, one, 0)

    def drain(self):
        for way in (0, 1):
            self.relay_copy(1 + 2 * way, way).wait_send()
            self.final_copy(5 + 2 * way, way, way).wait_send()
            self.final_copy(9 + 2 * way, way, 1 - way).wait_send()

        def one(step, carry):
            @pl.when(self.place(step)[2] == 1)
            def _():
                self.side_copy(step).wait_send()

            return carry

        lax.fori_loop(0, 16, one, 0)


SCATTER_REFS = 7


def scatter_scratch(parts, rows, columns):
    bf = jnp.bfloat16
    return [
        pltpu.VMEM((4, 2, parts, rows, columns), bf),
        pltpu.VMEM((2, parts, rows, columns), bf),
        pltpu.VMEM((2, 2, parts, rows, columns), bf),
        pltpu.SemaphoreType.DMA((16,)),
        pltpu.SemaphoreType.DMA((4, 2)),
        pltpu.SemaphoreType.DMA((2,)),
        pltpu.SemaphoreType.DMA((2, 2)),
    ]


OUT_SLOTS = 4


def expert_out_kernel(rows_hbm, gate_hbm, up_hbm, down_hbm, resid, targets, scales, layer, grad, grad_b, ua_out, rows, gate, ua, up_w, down_w, mine, away, load_w, load_rows, load_gate, store_ua, *scratch):
    hidden, width = down_w.shape
    scatter = Scatter(
        lambda place, slot, half: mine.at[place, half],
        lambda place, slot, half: away.at[place, half],
        scratch,
    )
    weights = (
        pltpu.make_async_copy(up_hbm, up_w, load_w.at[0]),
        pltpu.make_async_copy(down_hbm, down_w, load_w.at[1]),
    )

    def loads(step):
        slot, half, _, _ = scatter.place(step)
        spot = lax.rem(step, OUT_SLOTS)
        return (
            pltpu.make_async_copy(rows_hbm.at[slot, half], rows.at[spot], load_rows.at[step]),
            pltpu.make_async_copy(gate_hbm.at[slot, half], gate.at[spot], load_gate.at[step]),
        )

    def ua_store(step):
        slot, half, _, _ = scatter.place(step)
        return pltpu.make_async_copy(
            ua.at[lax.rem(step, OUT_SLOTS)], ua_out.at[slot, half], store_ua.at[step]
        )

    weights[0].start()
    for step in (0, 1):
        for copy in loads(step):
            copy.start()
    weights[1].start()
    plane_barrier(scatter.peers())
    for copy in weights:
        copy.wait()

    def one(step, carry):
        _, _, other, place = scatter.place(step)
        spot = lax.rem(step, OUT_SLOTS)
        for copy in loads(step):
            copy.wait()

        @pl.when(step < 14)
        def _():
            for copy in loads(step + 2):
                copy.start()

        @pl.when(step >= OUT_SLOTS)
        def _():
            ua_store(step - OUT_SLOTS).wait()

        lanes = lax.broadcasted_iota(jnp.int32, (rows.shape[1], 128), 1)
        tail = rows[spot, :, width:].astype(jnp.float32)
        weight = jnp.sum(jnp.where(lanes == scatter.me, tail, 0.0), axis=1, keepdims=True)
        up_val = nn_dot(rows[spot, :, :width], up_w[...])
        act_val = jnp.maximum(gate[spot].astype(jnp.float32), 0.0) * up_val * weight
        ua[spot, :, :hidden] = up_val.astype(jnp.bfloat16)
        ua[spot, :, hidden:] = act_val.astype(jnp.bfloat16)
        ua_store(step).start()
        partial = nn_dot(ua[spot, :, hidden:], down_w[...]).astype(jnp.bfloat16)

        @pl.when(other == 1)
        def _():
            away[place, half_of(scatter, step), 0] = partial

        @pl.when(other == 0)
        def _():
            mine[place, half_of(scatter, step), 0] = partial

        scatter.depart(step)

        @pl.when(step == 12)
        def _():
            scatter.forward()

        return carry

    lax.fori_loop(0, 16, one, 0)

    def write(half, part, rows, total):
        value = resid[half, rows, :] + total
        layer[half, rows, :] = value.astype(layer.dtype)
        error = (value - targets[half, rows, :].astype(jnp.float32)) * scales[half, rows, 0:1]
        grad[half, rows, :] = error
        grad_b[half, rows, :] = error.astype(grad_b.dtype)

    scatter.finish(write)
    scatter.drain()

    def drain(step, carry):
        ua_store(step).wait()
        return carry

    lax.fori_loop(16 - OUT_SLOTS, 16, drain, 0)


def half_of(scatter, step):
    return scatter.place(step)[1]


def expert_out(rows_all, gate_val, up_w, down_w, resid, targets, scales):
    half, columns = rows_all.shape[2:]
    hidden, width = down_w.shape
    bf = jnp.bfloat16
    return pl.pallas_call(
        expert_out_kernel,
        out_shape=(
            jax.ShapeDtypeStruct((2, half, width), bf),
            jax.ShapeDtypeStruct((2, half, width), jnp.float32),
            jax.ShapeDtypeStruct((2, half, width), bf),
            jax.ShapeDtypeStruct((8, 2, half, 2 * hidden), bf),
        ),
        in_specs=[ANY] * 4 + [VMEM] * 3,
        out_specs=(VMEM, VMEM, VMEM, ANY),
        scratch_shapes=[
            pltpu.VMEM((OUT_SLOTS, half, columns), bf),
            pltpu.VMEM((OUT_SLOTS, half, hidden), bf),
            pltpu.VMEM((OUT_SLOTS, half, 2 * hidden), bf),
            pltpu.VMEM((width, hidden), bf),
            pltpu.VMEM((hidden, width), bf),
            pltpu.VMEM((4, 2, 1, half, width), bf),
            pltpu.VMEM((4, 2, 1, half, width), bf),
            pltpu.SemaphoreType.DMA((2,)),
            pltpu.SemaphoreType.DMA((16,)),
            pltpu.SemaphoreType.DMA((16,)),
            pltpu.SemaphoreType.DMA((16,)),
        ]
        + scatter_scratch(1, half, width),
        compiler_params=pltpu.CompilerParams(
            collective_id=2, has_side_effects=True, vmem_limit_bytes=VMEM_BYTES
        ),
        name="expert_out",
    )(
        rows_all,
        gate_val,
        up_w,
        down_w,
        resid.reshape(2, half, width),
        targets.reshape(2, half, width),
        scales.reshape(2, half, 128),
    )


BACK_SLOTS = 4


def expert_back_kernel(own, rows_hbm, g_hbm, ua_hbm, down_hbm, dgu_out, tail_out, gate_out, up_out, down_out, buf, gua, rows, tails, down_w, acc, down_acc, send, recv, load, load_g, load_ua, load_rows, store_dgu, store_tail):
    hidden, width = down_w.shape
    gather = Gather(own, buf, send, recv)
    loads = (
        pltpu.make_async_copy(own.at[0], buf.at[gather.me, 0], load.at[0]),
        pltpu.make_async_copy(own.at[1], buf.at[gather.me, 1], load.at[1]),
        pltpu.make_async_copy(down_hbm, down_w, load.at[2]),
    )
    for copy in loads:
        copy.start()

    def block_loads(step):
        slot, half, _ = gather.place(step)
        spot = lax.rem(step, BACK_SLOTS)
        return (
            pltpu.make_async_copy(
                g_hbm.at[slot, half], gua.at[spot, :, pl.ds(0, hidden)], load_g.at[step]
            ),
            pltpu.make_async_copy(
                ua_hbm.at[slot, half], gua.at[spot, :, pl.ds(hidden, 2 * hidden)], load_ua.at[step]
            ),
            pltpu.make_async_copy(rows_hbm.at[slot, half], rows.at[spot], load_rows.at[step]),
        )

    def block_stores(step):
        slot, half, _ = gather.place(step)
        spot = lax.rem(step, BACK_SLOTS)
        return (
            pltpu.make_async_copy(
                gua.at[spot, :, pl.ds(0, 2 * hidden)], dgu_out.at[slot, half], store_dgu.at[step]
            ),
            pltpu.make_async_copy(tails.at[spot], tail_out.at[slot, half], store_tail.at[step]),
        )

    def fetch(step, carry):
        for copy in block_loads(step):
            copy.start()
        return carry

    lax.fori_loop(0, BACK_SLOTS, fetch, 0)
    gather.begin()
    for copy in loads:
        copy.wait()

    def weight_grads(step):
        spot_a, spot_b = lax.rem(step - 1, BACK_SLOTS), lax.rem(step, BACK_SLOTS)
        slot_a, half_a, _ = gather.place(step - 1)
        slot_b, half_b, _ = gather.place(step)

        def add(ref, index, total):
            at = pl.ds(pl.multiple_of(index * 256, 256), 256)

            @pl.when(step == 1)
            def _():
                ref[at, :] = total

            @pl.when(step > 1)
            def _():
                ref[at, :] = ref[at, :] + total

        def gate_up_tile(index, carry):
            cols = pl.ds(pl.multiple_of(index * 256, 256), 256)
            total = tn_dot(rows[spot_a, :, cols], gua[spot_a, :, : 2 * hidden])
            total = total + tn_dot(rows[spot_b, :, cols], gua[spot_b, :, : 2 * hidden])
            add(acc, index, total)
            return carry

        def down_tile(index, carry):
            cols = pl.ds(pl.multiple_of(2 * hidden + index * 256, 256), 256)
            total = tn_dot(gua[spot_a, :, cols], buf[slot_a, half_a])
            total = total + tn_dot(gua[spot_b, :, cols], buf[slot_b, half_b])
            add(down_acc, index, total)
            return carry

        lax.fori_loop(0, width // 256, gate_up_tile, 0)
        lax.fori_loop(0, hidden // 256, down_tile, 0)

    def one(step, carry):
        slot, half = gather.arrive(step)
        spot = lax.rem(step, BACK_SLOTS)
        for copy in block_loads(step):
            copy.wait()

        @pl.when((step >= 2) & (step < 14))
        def _():
            for copy in block_stores(step - 2):
                copy.wait()
            for copy in block_loads(step + 2):
                copy.start()

        lanes = lax.broadcasted_iota(jnp.int32, (buf.shape[2], 128), 1)
        tail = rows[spot, :, width:].astype(jnp.float32)
        weight = jnp.sum(jnp.where(lanes == gather.me, tail, 0.0), axis=1, keepdims=True)
        grad_act = nt_dot(buf[slot, half], down_w[...])
        gate_val = gua[spot, :, :hidden].astype(jnp.float32)
        up_val = gua[spot, :, hidden : 2 * hidden].astype(jnp.float32)
        gate_relu = jnp.maximum(gate_val, 0.0)
        grad_comb = jnp.sum(gate_relu * up_val * grad_act, axis=1, keepdims=True)
        grad_act = grad_act * weight
        grad_gate = jnp.where(gate_val > 0, grad_act * up_val, 0.0).astype(jnp.bfloat16)
        grad_up = (grad_act * gate_relu).astype(jnp.bfloat16)
        gua[spot, :, :hidden] = grad_gate
        gua[spot, :, hidden : 2 * hidden] = grad_up
        tails[spot] = jnp.where(lanes == gather.me, grad_comb, 0.0).astype(jnp.bfloat16)
        for copy in block_stores(step):
            copy.start()

        @pl.when(lax.rem(step, 2) == 1)
        def _():
            weight_grads(step)

        return carry

    lax.fori_loop(0, 16, one, 0)
    gather.finish()

    def round_gate_up(at):
        gate_out[at, :] = acc[at, :hidden].astype(jnp.bfloat16)
        up_out[at, :] = acc[at, hidden:].astype(jnp.bfloat16)

    row_loop(width, 64, round_gate_up)

    def round_down(at):
        down_out[at, :] = down_acc[at, :].astype(jnp.bfloat16)

    row_loop(hidden, 64, round_down)

    def drain(step, carry):
        for copy in block_stores(step):
            copy.wait()
        return carry

    lax.fori_loop(12, 16, drain, 0)


def expert_back(own, rows_all, gate_val, ua, down_w):
    half, columns = rows_all.shape[2:]
    hidden, width = down_w.shape
    bf = jnp.bfloat16
    return pl.pallas_call(
        expert_back_kernel,
        out_shape=(
            jax.ShapeDtypeStruct((8, 2, half, 2 * hidden), bf),
            jax.ShapeDtypeStruct((8, 2, half, 128), bf),
            jax.ShapeDtypeStruct((width, hidden), bf),
            jax.ShapeDtypeStruct((width, hidden), bf),
            jax.ShapeDtypeStruct((hidden, width), bf),
        ),
        in_specs=[ANY] * 5,
        out_specs=(ANY, ANY, VMEM, VMEM, VMEM),
        scratch_shapes=[
            pltpu.VMEM((8, 2, half, width), bf),
            pltpu.VMEM((BACK_SLOTS, half, 3 * hidden), bf),
            pltpu.VMEM((BACK_SLOTS, half, columns), bf),
            pltpu.VMEM((BACK_SLOTS, half, 128), bf),
            pltpu.VMEM((hidden, width), bf),
            pltpu.VMEM((width, 2 * hidden), jnp.float32),
            pltpu.VMEM((hidden, width), jnp.float32),
            pltpu.SemaphoreType.DMA((14,)),
            pltpu.SemaphoreType.DMA((8, 2)),
            pltpu.SemaphoreType.DMA((3,)),
        ]
        + [pltpu.SemaphoreType.DMA((16,))] * 5,
        compiler_params=pltpu.CompilerParams(
            collective_id=3, has_side_effects=True, vmem_limit_bytes=VMEM_BYTES
        ),
        name="expert_back",
    )(own, rows_all, gate_val, ua, down_w)


def expert_rows_kernel(dgu_hbm, tail_hbm, gate_hbm, up_hbm, out, dgu, tails, gate_w, up_w, mine, away, load_w, load_dgu, load_tail, *scratch):
    width, hidden = gate_w.shape
    scatter = Scatter(
        lambda place, slot, half: mine.at[place, half],
        lambda place, slot, half: away.at[place, half],
        scratch,
    )
    weights = (
        pltpu.make_async_copy(gate_hbm, gate_w, load_w.at[0]),
        pltpu.make_async_copy(up_hbm, up_w, load_w.at[1]),
    )

    def loads(step):
        slot, half, _, _ = scatter.place(step)
        spot = lax.rem(step, OUT_SLOTS)
        return (
            pltpu.make_async_copy(dgu_hbm.at[slot, half], dgu.at[spot], load_dgu.at[step]),
            pltpu.make_async_copy(tail_hbm.at[slot, half], tails.at[spot], load_tail.at[step]),
        )

    for copy in weights:
        copy.start()
    for step in (0, 1):
        for copy in loads(step):
            copy.start()
    plane_barrier(scatter.peers())
    for copy in weights:
        copy.wait()

    def one(step, carry):
        _, half, other, place = scatter.place(step)
        spot = lax.rem(step, OUT_SLOTS)
        for copy in loads(step):
            copy.wait()

        @pl.when(step < 14)
        def _():
            for copy in loads(step + 2):
                copy.start()

        total = nt_dot(dgu[spot, :, :hidden], gate_w[...]) + nt_dot(dgu[spot, :, hidden:], up_w[...])
        partial = total.astype(jnp.bfloat16)

        @pl.when(other == 1)
        def _():
            away[place, half, 0, :, :width] = partial
            away[place, half, 0, :, width:] = tails[spot]

        @pl.when(other == 0)
        def _():
            mine[place, half, 0, :, :width] = partial
            mine[place, half, 0, :, width:] = tails[spot]

        scatter.depart(step)

        @pl.when(step == 12)
        def _():
            scatter.forward()

        return carry

    lax.fori_loop(0, 16, one, 0)

    def write(half, part, rows, total):
        out[half, rows, :] = total

    scatter.finish(write)
    scatter.drain()


def expert_rows(dgu, tails, gate_w, up_w):
    half = dgu.shape[2]
    width, hidden = gate_w.shape
    columns = width + 128
    bf = jnp.bfloat16
    return pl.pallas_call(
        expert_rows_kernel,
        out_shape=jax.ShapeDtypeStruct((2, half, columns), jnp.float32),
        in_specs=[ANY] * 4,
        out_specs=VMEM,
        scratch_shapes=[
            pltpu.VMEM((OUT_SLOTS, half, 2 * hidden), bf),
            pltpu.VMEM((OUT_SLOTS, half, 128), bf),
            pltpu.VMEM((width, hidden), bf),
            pltpu.VMEM((width, hidden), bf),
            pltpu.VMEM((4, 2, 1, half, columns), bf),
            pltpu.VMEM((4, 2, 1, half, columns), bf),
            pltpu.SemaphoreType.DMA((2,)),
            pltpu.SemaphoreType.DMA((16,)),
            pltpu.SemaphoreType.DMA((16,)),
        ]
        + scatter_scratch(1, half, columns),
        compiler_params=pltpu.CompilerParams(
            collective_id=4, has_side_effects=True, vmem_limit_bytes=VMEM_BYTES
        ),
        name="expert_rows",
    )(dgu, tails, gate_w, up_w)


def line_gather_kernel(own, everything, stage, send, recv, local):
    line = line_peers()
    into = pltpu.make_async_copy(own, stage, local.at[0])
    into.start()
    full_barrier((), line[1:])

    def copy(turn, block):
        return line_remote(
            own, everything.at[block], send.at[turn - 1], recv.at[turn - 1], line[turn]
        )

    for turn in (1, 2, 3):
        copy(turn, line[0]).start()
    into.wait()
    out = pltpu.make_async_copy(stage, everything.at[line[0]], local.at[1])
    out.start()
    out.wait()
    for turn in (1, 2, 3):
        copy(turn, line[turn]).wait()


def line_gather(own):
    return pl.pallas_call(
        line_gather_kernel,
        out_shape=jax.ShapeDtypeStruct((4, *own.shape), own.dtype),
        in_specs=[ANY],
        out_specs=ANY,
        scratch_shapes=[
            pltpu.VMEM(own.shape, own.dtype),
            pltpu.SemaphoreType.DMA((3,)),
            pltpu.SemaphoreType.DMA((3,)),
            pltpu.SemaphoreType.DMA((2,)),
        ],
        compiler_params=pltpu.CompilerParams(
            collective_id=7, has_side_effects=True, vmem_limit_bytes=VMEM_BYTES
        ),
        name="line_gather",
    )(own)


class DenseGather:
    def __init__(self, own, everything, send, recv, local, lined):
        self.own, self.everything, self.send, self.recv = own, everything, send, recv
        self.lined = lined
        self.me, self.sib, self.xn, self.yn = plane_peers()
        self.diag = self.xn + self.yn - self.me
        self.line = line_peers()
        if lined:
            self.home = pltpu.make_async_copy(own, everything.at[:, self.me], local)
        else:
            self.home = pltpu.make_async_copy(own, everything.at[self.line[0], self.me], local)
        self.started = []

    def copy(self, index, own, slot, turn, peer, make):
        target = self.everything.at[self.line[turn], slot]
        return make(
            (self.own.at[self.line[turn]] if self.lined else self.own) if own else target,
            target,
            self.send.at[index],
            self.recv.at[self.line[turn], slot],
            peer,
        )

    def put(self, own, slot, turn, peer, make=remote):
        what = (len(self.started), own, slot, turn, peer, make)
        self.started.append(what)
        self.copy(*what).start()

    def pass_on(self, slot, turn, peer):
        self.put(False, slot, turn, peer)

    def wait(self, slot, turn):
        ref = self.everything.at[self.line[turn], slot]
        remote(ref, ref, self.send.at[0], self.recv.at[self.line[turn], slot], self.sib).wait_recv()

    def start_line(self):
        for turn in (1, 2, 3):
            self.put(True, self.me, 0, self.line[turn], line_remote)

    def start_plane(self):
        for turn in (0, 1, 2, 3) if self.lined else (0,):
            for peer in (self.xn, self.yn, self.sib):
                self.put(True, self.me, turn, peer)

    def turn(self, turn):
        if turn > 0 and not self.lined:
            self.wait(self.me, turn)
            for peer in (self.xn, self.yn, self.sib):
                self.pass_on(self.me, turn, peer)
        self.wait(self.xn, turn)
        if turn % 2 == 0:
            self.pass_on(self.xn, turn, self.yn)
        self.pass_on(self.xn, turn, self.sib)
        self.wait(self.yn, turn)
        if turn % 2 == 1:
            self.pass_on(self.yn, turn, self.xn)
        self.pass_on(self.yn, turn, self.sib)
        if turn > 0:
            self.far(turn - 1)

    def far(self, turn):
        self.wait(self.diag, turn)
        self.pass_on(self.diag, turn, self.sib)

    def arrived(self):
        for turn in (0, 1, 2, 3):
            for slot in (self.me, self.xn, self.yn, self.diag):
                self.wait(slot + self.sib - self.me, turn)
        self.home.wait()

    def finish(self):
        for what in self.started:
            self.copy(*what).wait_send()


def gather_scratch(rows, columns):
    return [
        pltpu.VMEM((4, 8, rows, columns), jnp.bfloat16),
        pltpu.SemaphoreType.DMA((32,)),
        pltpu.SemaphoreType.DMA((4, 8)),
        pltpu.SemaphoreType.DMA((2,)),
    ]


class LineScatter:
    def __init__(self, sums, scratch):
        self.sums = sums
        self.other, self.send, self.recv = scratch
        self.line = line_peers()

    def copy(self, turn):
        target = self.line[turn]
        return line_remote(
            self.sums(target),
            self.other.at[turn - 1],
            self.send.at[turn - 1],
            self.recv.at[turn - 1],
            target,
        )

    def begin(self):
        for turn in (1, 2, 3):
            self.copy(turn).start()

    def finish(self, outs):
        rows_all = self.other.shape[1]
        for turn in (1, 2, 3):
            self.copy(turn).wait_recv()
        own = self.sums(self.line[0])

        def one(index, carry):
            rows = pl.ds(pl.multiple_of(index * 16, 16), 16)
            total = own[rows, :].astype(jnp.float32)
            for turn in (0, 1, 2):
                total = total + self.other[turn, rows, :].astype(jnp.float32)
            first = 0
            for out, place, columns in outs:
                out[rows, place : place + columns] = total[:, first : first + columns]
                first += columns
            return carry

        lax.fori_loop(0, rows_all // 16, one, 0)
        for turn in (1, 2, 3):
            self.copy(turn).wait_send()


class DenseScatter:
    def __init__(self, total, scratch):
        def block(place, slot, half):
            return total.at[half, :, slot]

        self.plane = Scatter(block, block, scratch[:SCATTER_REFS])
        me = self.plane.me
        self.line = LineScatter(
            lambda line: total.at[lax.div(line, 2), lax.rem(line, 2), me], scratch[SCATTER_REFS:]
        )

    def begin(self):
        def one(step, carry):
            self.plane.depart(step)
            return carry

        lax.fori_loop(0, 16, one, 0)

    def forward(self):
        self.plane.forward()

    def turn(self):
        def write(half, part, rows, total):
            home = self.plane.mine(0, half)
            home[part, rows, :] = total.astype(home.dtype)

        self.plane.finish(write)
        self.line.begin()

    def finish(self, outs):
        self.line.finish(outs)
        self.plane.drain()


DENSE_REFS = SCATTER_REFS + 3


def dense_scratch(rows, columns):
    return scatter_scratch(2, rows, columns) + [
        pltpu.VMEM((3, rows, columns), jnp.bfloat16),
        pltpu.SemaphoreType.DMA((3,)),
        pltpu.SemaphoreType.DMA((3,)),
    ]


def rope(values, cosine, sine):
    return values * cosine + pltpu.roll(values, HD // 2, 1) * sine


def gain_rows(misc, out):
    for index in range(out.shape[1] // 128):
        rows = pl.ds(index * 128, 128)
        out[:, rows] = jnp.transpose(misc(rows).astype(jnp.float32))


def inverse_rms(values):
    return lax.rsqrt(jnp.mean(values * values, axis=1, keepdims=True) + EPS)


def row_loop(count, chunk, body):
    def one(index, carry):
        body(pl.ds(pl.multiple_of(index * chunk, chunk), chunk))
        return carry

    lax.fori_loop(0, count // chunk, one, 0)


def tile_loop(count, tile, body):
    row_loop(count, tile, body)


ROW_CHUNK = 16
TILE = 256


def attend_kernel(q_heads, kv_heads, experts, tokens, qkv_own, out_own, cosine, sine, segments, routes, rows_out, resid, heads, mixed, lse, prob, bias, picked, qkv_hbm, out_hbm, gains, hidden, *scratch):
    num_rows, width = tokens.shape
    group = q_heads // kv_heads
    qkv_cols = (q_heads + 2 * kv_heads) * HD
    qkv_w, out_w = scratch[0], scratch[4]
    first = DenseGather(qkv_own, qkv_w, scratch[1], scratch[2], scratch[3].at[0], True)
    second = DenseGather(out_own, out_w, scratch[5], scratch[6], scratch[7].at[0], False)
    stores = (
        pltpu.make_async_copy(qkv_w, qkv_hbm, scratch[3].at[1]),
        pltpu.make_async_copy(out_w, out_hbm, scratch[7].at[1]),
    )
    for gather in (first, second):
        gather.home.start()
    full_barrier((first.sib, first.xn, first.yn), first.line[1:])
    first.start_plane()
    second.start_line()
    picked[...] = jnp.zeros_like(picked)
    lane_ids = lax.broadcasted_iota(jnp.int32, picked.shape, 1)
    for index in range(routes.shape[1]):
        picked[...] = picked[...] + jnp.where(lane_ids == routes[:, index : index + 1], 1.0, 0.0)
    seg_row = segments[0:1, :]
    for index in range(num_rows // 128):
        rows = slice(index * 128, (index + 1) * 128)
        wide = jnp.broadcast_to(seg_row[:, rows].astype(jnp.float32), (128, 128))
        seg_col = jnp.transpose(wide)[:, 0:1].astype(jnp.int32)
        keys = lax.broadcasted_iota(jnp.int32, (128, num_rows), 1)
        queries = lax.broadcasted_iota(jnp.int32, (128, num_rows), 0) + index * 128
        visible = (keys <= queries) & ((seg_row == 0) | (seg_row == seg_col))
        bias[rows, :] = jnp.where(visible, 0.0, NEG_BIG)
    for turn in (0, 1, 2, 3):
        first.turn(turn)
    first.far(3)
    second.start_plane()
    first.arrived()
    stores[0].start()
    second.turn(0)

    def flat(ref, cols):
        return ref[:, :, :, cols].reshape(-1, cols.size)

    misc = flat(qkv_w, pl.ds(qkv_cols, 128))
    for index in range(width // 128):
        rows = slice(index * 128, (index + 1) * 128)
        gains[:, rows] = jnp.transpose(misc[rows, :].astype(jnp.float32))

    def norm_one(rows):
        value = tokens[rows, :].astype(jnp.float32)
        normed = value * inverse_rms(value)
        hidden[rows, :] = (normed * gains[experts : experts + 1, :]).astype(jnp.bfloat16)

    row_loop(num_rows, ROW_CHUNK, norm_one)

    def project(index, carry):
        cols = pl.ds(pl.multiple_of(index * TILE, TILE), TILE)
        raw = nn_dot(hidden[...], flat(qkv_w, cols))
        turned = index < (q_heads + kv_heads) // 2
        cos_now = jnp.where(turned, cosine[...], 1.0)
        sin_now = jnp.where(turned, sine[...], 0.0)
        for part in (0, 1):
            value = rope(raw[:, part * HD : (part + 1) * HD], cos_now, sin_now)
            heads[2 * index + part] = value.astype(jnp.bfloat16)
        return carry

    lax.fori_loop(0, (q_heads + 2 * kv_heads) // 2, project, 0)
    second.turn(1)
    lse[...] = jnp.zeros_like(lse)

    def head_step(head, carry):
        kv_head = q_heads + lax.div(head, group)
        cols = pl.ds(pl.multiple_of(head * HD, HD), HD)
        for first, keys in ((0, PROMPT), (PROMPT, num_rows)):
            rows = pl.ds(first, keys - first)
            query = heads[head, rows, :]
            score = nt_dot(query, heads[kv_head, :keys, :]) * HD ** (-0.5) + bias[rows, :keys]
            top = jnp.max(score, axis=1, keepdims=True)
            weight = jnp.exp(score - top)
            total = jnp.sum(weight, axis=1, keepdims=True)
            value = nn_dot(weight.astype(jnp.bfloat16), heads[kv_head + kv_heads, :keys, :])
            mixed[rows, cols] = (value / total).astype(jnp.bfloat16)
            lanes = lax.broadcasted_iota(jnp.int32, (keys - first, 128), 1)
            lse[rows, :] = jnp.where(lanes == head, top + jnp.log(total), lse[rows, :])

        @pl.when(head == q_heads // 3)
        def _():
            second.turn(2)

        @pl.when(head == 2 * q_heads // 3)
        def _():
            second.turn(3)

        return carry

    lax.fori_loop(0, q_heads, head_step, 0)

    second.far(3)
    second.arrived()
    stores[1].start()

    def out_tile(cols):
        resid[:, cols] = tokens[:, cols].astype(jnp.float32) + nn_dot(mixed[...], flat(out_w, cols))

    tile_loop(width, TILE, out_tile)

    def norm_two(rows):
        value = resid[rows, :]
        normed = value * inverse_rms(value)
        rows_out[rows, :width] = (normed * gains[experts + 1 : experts + 2, :]).astype(jnp.bfloat16)

    row_loop(num_rows, ROW_CHUNK, norm_two)
    logits = nn_dot(rows_out[:, :width], flat(qkv_w, pl.ds(qkv_cols, 128)))
    lanes = lax.broadcasted_iota(jnp.int32, logits.shape, 1)
    logits = jnp.where(lanes < experts, logits, NEG_BIG)
    weight = jnp.exp(logits - jnp.max(logits, axis=1, keepdims=True))
    value = weight / jnp.sum(weight, axis=1, keepdims=True)
    prob[...] = value
    chosen = value * picked[...]
    rows_out[:, width:] = (chosen / jnp.sum(chosen, axis=1, keepdims=True)).astype(jnp.bfloat16)
    for gather, store in zip((first, second), stores):
        store.wait()
        gather.finish()


def attend(tokens, qkv_own, out_own, cosine, sine, segments, routes, q_heads, kv_heads, experts):
    num_rows, width = tokens.shape
    bf = jnp.bfloat16
    all_heads = q_heads + 2 * kv_heads
    return pl.pallas_call(
        functools.partial(attend_kernel, q_heads, kv_heads, experts),
        out_shape=(
            jax.ShapeDtypeStruct((num_rows, width + 128), bf),
            jax.ShapeDtypeStruct((num_rows, width), jnp.float32),
            jax.ShapeDtypeStruct((all_heads, num_rows, HD), bf),
            jax.ShapeDtypeStruct((num_rows, q_heads * HD), bf),
            jax.ShapeDtypeStruct((num_rows, 128), jnp.float32),
            jax.ShapeDtypeStruct((num_rows, 128), jnp.float32),
            jax.ShapeDtypeStruct((num_rows, num_rows), jnp.float32),
            jax.ShapeDtypeStruct((num_rows, 128), jnp.float32),
            jax.ShapeDtypeStruct((4, 8, *qkv_own.shape[1:]), bf),
            jax.ShapeDtypeStruct((4, 8, *out_own.shape), bf),
        ),
        in_specs=[VMEM, ANY, ANY] + [VMEM] * 4,
        out_specs=(VMEM,) * 8 + (ANY, ANY),
        scratch_shapes=[
            pltpu.VMEM((128, width), jnp.float32),
            pltpu.VMEM((num_rows, width), bf),
        ]
        + gather_scratch(*qkv_own.shape[1:])
        + gather_scratch(*out_own.shape),
        compiler_params=pltpu.CompilerParams(
            collective_id=5, has_side_effects=True, vmem_limit_bytes=VMEM_BYTES
        ),
        name="attend",
    )(tokens, qkv_own, out_own, cosine, sine, segments.reshape(1, num_rows), routes)


def attend_back_kernel(q_heads, kv_heads, experts, back_hbm, grad_hbm, resid_hbm, rows_hbm, prob_hbm, picked_hbm, qkv_hbm, out_hbm, mixed_hbm, heads_hbm, lse_hbm, bias_hbm, cos_hbm, sin_hbm, tokens_hbm, grad_in, out_sum, q_sum, k_sum, v_sum, misc_sum, back, grad, resid, hidden_two, prob, picked, qkv_w, out_w, mixed, heads, lse, bias, cosine, sine, tokens, gains, gain_sums, grad_logit, grad_proj, grad_mixed, grad_qkv, grad_kv, hidden, load, *scratch):
    num_rows, width = tokens.shape
    group = q_heads // kv_heads
    q_cols = q_heads * HD
    k_cols = kv_heads * HD
    qkv_cols = q_cols + 2 * k_cols
    near_cols = group * HD
    bf = jnp.bfloat16
    parts, scatters = [], []
    for index in range(4):
        some = scratch[index * (1 + DENSE_REFS) : (index + 1) * (1 + DENSE_REFS)]
        parts.append(some[0])
        scatters.append(DenseScatter(some[0], some[1:]))
    out_part, near_part, rest_part, misc_part = parts
    out_scatter, near_scatter, rest_scatter, misc_scatter = scatters
    pairs = (
        (prob_hbm, prob),
        (picked_hbm, picked),
        (back_hbm, back),
        (qkv_hbm, qkv_w),
        (resid_hbm, resid),
        (grad_hbm, grad),
        (rows_hbm, hidden_two),
        (out_hbm, out_w),
        (mixed_hbm, mixed),
        (heads_hbm, heads),
        (lse_hbm, lse),
        (bias_hbm, bias),
        (cos_hbm, cosine),
        (sin_hbm, sine),
        (tokens_hbm, tokens),
    )
    loads = [pltpu.make_async_copy(src, dst, load.at[i]) for i, (src, dst) in enumerate(pairs)]
    for copy in loads:
        copy.start()
    full_barrier(out_scatter.plane.peers(), out_scatter.line.line[1:])
    for copy in loads[:3]:
        copy.wait()
    gain_sums[...] = jnp.zeros_like(gain_sums)

    def router_rows(rows):
        value = prob[rows, :]
        chosen = value * picked[rows, :]
        total = jnp.sum(chosen, axis=1, keepdims=True)
        comb = chosen / total
        grad_comb = back[rows, width:]
        grad_chosen = (
            picked[rows, :] * (grad_comb - jnp.sum(grad_comb * comb, axis=1, keepdims=True)) / total
        )
        logit = value * (grad_chosen - jnp.sum(value * grad_chosen, axis=1, keepdims=True))
        grad_logit[rows, :] = logit.astype(bf)

    row_loop(num_rows, 64, router_rows)
    loads[3].wait()
    misc = qkv_w.at[:, pl.ds(qkv_cols, 128)]
    gain_rows(lambda rows: misc[rows, :], gains)
    lanes = lax.broadcasted_iota(jnp.int32, (TILE, 128), 1)

    def hidden_tile(cols):
        router = jnp.where(lanes < experts, misc[cols, :], jnp.zeros((), bf))
        back[:, cols] = back[:, cols] + nt_dot(grad_logit[...], router)

    tile_loop(width, TILE, hidden_tile)
    for copy in loads[4:]:
        copy.wait()

    def fold(values):
        return jnp.sum(values.reshape(-1, 8, width), axis=0)

    def norm_two(rows):
        value = resid[rows, :]
        inverse = inverse_rms(value)
        normed = value * inverse
        grad_hidden = back[rows, :width]
        gain_sums[8:16, :] = gain_sums[8:16, :] + fold(grad_hidden * normed)
        grad_norm = grad_hidden * gains[experts + 1 : experts + 2, :]
        mean = jnp.mean(grad_norm * normed, axis=1, keepdims=True)
        total = grad[rows, :] + inverse * (grad_norm - normed * mean)
        grad[rows, :] = total
        grad_proj[rows, :] = total.astype(bf)

    row_loop(num_rows, ROW_CHUNK, norm_two)

    def weight_loop(part, left, right):
        _, _, blocks, rows_each, columns = part.shape
        span = blocks * rows_each

        def one(line, carry):
            cols = pl.ds(pl.multiple_of(line * span, 128), span)
            total = tn_dot(left[:, cols], right[...]).astype(bf)
            part[lax.div(line, 2), lax.rem(line, 2)] = total.reshape(blocks, rows_each, columns)
            return carry

        lax.fori_loop(0, 4, one, 0)

    weight_loop(out_part, mixed, grad_proj)
    out_scatter.begin()

    def mixed_tile(cols):
        grad_mixed[:, cols] = nt_dot(
            grad_proj[...], out_w[cols, :]
        ).astype(bf)

    tile_loop(q_cols, TILE, mixed_tile)

    def norm_one(rows):
        value = tokens[rows, :].astype(jnp.float32)
        normed = value * inverse_rms(value)
        hidden[rows, :] = (normed * gains[experts : experts + 1, :]).astype(bf)

    row_loop(num_rows, ROW_CHUNK, norm_one)
    scale = HD ** (-0.5)

    def head_step(head, carry):
        kv_head = lax.div(head, group)
        cols = pl.ds(pl.multiple_of(head * HD, HD), HD)

        @pl.when(lax.rem(head, group) == 0)
        def _():
            grad_kv[...] = jnp.zeros_like(grad_kv)

        for first, keys in ((0, PROMPT), (PROMPT, num_rows)):
            rows = pl.ds(first, keys - first)
            key = heads[q_heads + kv_head, :keys, :]
            query = heads[head, rows, :]
            up = grad_mixed[rows, cols]
            lane = lax.broadcasted_iota(jnp.int32, (keys - first, 128), 1)
            total = jnp.sum(jnp.where(lane == head, lse[rows, :], 0.0), axis=1, keepdims=True)
            weight = jnp.exp(nt_dot(query, key) * scale + bias[rows, :keys] - total)
            grad_weight = nt_dot(up, heads[q_heads + kv_heads + kv_head, :keys, :])
            delta = jnp.sum(weight * grad_weight, axis=1, keepdims=True)
            score = (weight * (grad_weight - delta)).astype(bf)
            grad_kv[1, :keys, :] = grad_kv[1, :keys, :] + tn_dot(weight.astype(bf), up)
            grad_kv[0, :keys, :] = grad_kv[0, :keys, :] + tn_dot(score, query) * scale
            value = rope(nn_dot(score, key) * scale, cosine[rows, :], -sine[rows, :])
            grad_qkv[rows, cols] = value.astype(bf)

        @pl.when(lax.rem(head, group) == group - 1)
        def _():
            key_cols = pl.ds(pl.multiple_of(q_cols + kv_head * HD, HD), HD)
            value_cols = pl.ds(pl.multiple_of(q_cols + (kv_heads + kv_head) * HD, HD), HD)
            grad_qkv[:, key_cols] = rope(grad_kv[0], cosine[...], -sine[...]).astype(bf)
            grad_qkv[:, value_cols] = grad_kv[1].astype(bf)

        @pl.when(head == 2)
        def _():
            out_scatter.forward()

        @pl.when(head == group - 1)
        def _():
            weight_loop(near_part, hidden, grad_qkv.at[:, pl.ds(0, near_cols)])
            near_scatter.begin()

        @pl.when(head == group + 1)
        def _():
            out_scatter.turn()

        @pl.when(head == group + 3)
        def _():
            near_scatter.forward()

        return carry

    lax.fori_loop(0, q_heads, head_step, 0)
    weight_loop(rest_part, hidden, grad_qkv.at[:, pl.ds(near_cols, qkv_cols - near_cols)])
    rest_scatter.begin()
    near_scatter.turn()

    def hidden_back_tile(cols):
        back[:, cols] = nt_dot(grad_qkv[...], qkv_w[cols, pl.ds(0, qkv_cols)])

    tile_loop(width, TILE, hidden_back_tile)
    rest_scatter.forward()

    def last_rows(rows):
        value = tokens[rows, :].astype(jnp.float32)
        inverse = inverse_rms(value)
        normed = value * inverse
        grad_hidden = back[rows, :width]
        gain_sums[0:8, :] = gain_sums[0:8, :] + fold(grad_hidden * normed)
        grad_norm = grad_hidden * gains[experts : experts + 1, :]
        mean = jnp.mean(grad_norm * normed, axis=1, keepdims=True)
        grad[rows, :] = grad[rows, :] + inverse * (grad_norm - normed * mean)

    row_loop(num_rows, ROW_CHUNK, last_rows)
    store = pltpu.make_async_copy(grad, grad_in, load.at[0])
    store.start()
    gains[0:16, :] = gain_sums[...]
    _, _, blocks, rows_each, _ = misc_part.shape
    span = blocks * rows_each

    def misc_line(line, carry):
        cols = pl.ds(pl.multiple_of(line * span, 128), span)
        router = tn_dot(hidden_two[:, cols], grad_logit[...])
        one = jnp.sum(gains[0:8, cols], axis=0, keepdims=True)
        two = jnp.sum(gains[8:16, cols], axis=0, keepdims=True)
        place = lax.broadcasted_iota(jnp.int32, (128, span), 0)
        block = jnp.where(place == experts, one, jnp.where(place == experts + 1, two, 0.0))
        total = (router + jnp.transpose(block)).astype(bf)
        misc_part[lax.div(line, 2), lax.rem(line, 2)] = total.reshape(blocks, rows_each, 128)
        return carry

    lax.fori_loop(0, 4, misc_line, 0)
    misc_scatter.begin()
    misc_scatter.forward()
    rest_scatter.turn()
    misc_scatter.turn()
    out_scatter.finish(((out_sum, 0, width),))
    near_scatter.finish(((q_sum, 0, near_cols),))
    rest_scatter.finish(
        ((q_sum, near_cols, q_cols - near_cols), (k_sum, 0, k_cols), (v_sum, 0, k_cols))
    )
    misc_scatter.finish(((misc_sum, 0, 128),))
    store.wait()


def attend_back(back, grad, resid, rows_own, prob, picked, qkv_w, out_w, mixed, heads, lse, bias, cosine, sine, tokens, q_heads, kv_heads, experts):
    num_rows, width = tokens.shape
    bf = jnp.bfloat16
    arrays = (back, grad, resid, rows_own, prob, picked, qkv_w, out_w, mixed, heads, lse, bias, cosine, sine, tokens)
    k_cols = kv_heads * HD
    q_cols = q_heads * HD
    qkv_cols = q_cols + 2 * k_cols
    near_cols = q_cols // kv_heads
    block_rows = width // 32
    scratch = []
    for columns in (width, near_cols, qkv_cols - near_cols, 128):
        scratch += [pltpu.VMEM((2, 2, 8, block_rows, columns), bf)]
        scratch += dense_scratch(block_rows, columns)
    return pl.pallas_call(
        functools.partial(attend_back_kernel, q_heads, kv_heads, experts),
        out_shape=(jax.ShapeDtypeStruct((num_rows, width), jnp.float32),)
        + tuple(
            jax.ShapeDtypeStruct((block_rows, columns), jnp.float32)
            for columns in (width, q_cols, k_cols, k_cols, 128)
        ),
        in_specs=[ANY] * len(arrays),
        out_specs=(ANY,) + (VMEM,) * 5,
        scratch_shapes=[pltpu.VMEM(array.shape, array.dtype) for array in arrays]
        + [
            pltpu.VMEM((128, width), jnp.float32),
            pltpu.VMEM((16, width), jnp.float32),
            pltpu.VMEM((num_rows, 128), bf),
            pltpu.VMEM((num_rows, width), bf),
            pltpu.VMEM((num_rows, q_cols), bf),
            pltpu.VMEM((num_rows, qkv_cols), bf),
            pltpu.VMEM((2, num_rows, HD), jnp.float32),
            pltpu.VMEM((num_rows, width), bf),
            pltpu.SemaphoreType.DMA((len(arrays),)),
        ]
        + scratch,
        compiler_params=pltpu.CompilerParams(
            collective_id=6, has_side_effects=True, vmem_limit_bytes=67043328
        ),
        name="attend_back",
    )(*arrays)


def body_plane(
    tokens,
    targets,
    valid_count,
    segments,
    routes,
    gain_attn,
    w_query,
    w_key,
    w_value,
    w_out,
    gain_moe,
    w_router,
    w_gate,
    w_up,
    w_down,
):
    bf = jnp.bfloat16
    num_rows, width = tokens.shape
    half = num_rows // 2
    q_cols, k_cols = w_query.shape[1], w_key.shape[1]
    num_experts = w_router.shape[1]
    num_heads = q_cols // HD
    kv_heads = k_cols // HD
    pad_cols = 128 - 2 - num_experts
    qkv_own = jnp.concatenate(
        [
            w_query,
            w_key,
            w_value,
            w_router,
            gain_attn[:, None],
            gain_moe[:, None],
            jnp.zeros((gain_attn.shape[0], pad_cols), bf),
        ],
        axis=1,
    )
    qkv_line, w_gate, w_up = lax.optimization_barrier((line_gather(qkv_own), w_gate, w_up))
    gate_w = lax.all_gather(w_gate, "dp", axis=1, tiled=True)[0]
    up_w = lax.all_gather(w_up, "dp", axis=1, tiled=True)[0]
    tok_pos = positions(segments)
    freq = THETA ** (-2.0 * jnp.arange(HD // 2, dtype=jnp.float32) / HD)
    angle = tok_pos.astype(jnp.float32)[:, None] * freq[None, :]
    cosine, sine_part = jnp.cos(angle), jnp.sin(angle)
    cosine = jnp.concatenate([cosine, cosine], axis=1)
    sine = jnp.concatenate([-sine_part, sine_part], axis=1)
    rows_own, resid_mid, heads, mixed, lse, prob, bias, picked, qkv_w, out_w = attend(
        tokens, qkv_line, w_out, cosine, sine, segments, routes, num_heads, kv_heads, num_experts
    )
    rows_all, gate_val, down_w = expert_in(
        rows_own.reshape(2, half, width + 128), gate_w, w_down[0]
    )
    down_w = down_w.reshape(-1, width)
    total_rows = num_rows * lax.axis_size(("dp", "exp"))
    global_row = lax.axis_index(("dp", "exp")) * num_rows + jnp.arange(num_rows, dtype=jnp.int32)
    loss_scale = total_rows / valid_count[0].astype(jnp.float32)
    scales = jnp.broadcast_to(
        jnp.where(global_row < valid_count[0], loss_scale, 0.0)[:, None], (num_rows, 128)
    )
    layer_out, grad_out, grad_out_b, ua = expert_out(
        rows_all, gate_val, up_w, down_w, resid_mid, targets, scales
    )
    layer_out = layer_out.reshape(num_rows, width)
    dgu, tails, gate_part, up_part, down_part = expert_back(
        grad_out_b, rows_all, gate_val, ua, down_w
    )
    back = expert_rows(dgu, tails, gate_w, up_w)
    expert_sums = tuple(
        lax.psum_scatter(grad[None], "dp", scatter_dimension=1, tiled=True).astype(jnp.float32)
        for grad in (gate_part, up_part, down_part)
    )
    grad_in, out_sum, q_sum, k_sum, v_sum, misc_sum = attend_back(
        back.reshape(num_rows, width + 128),
        grad_out.reshape(num_rows, width),
        resid_mid,
        rows_own,
        prob,
        picked,
        qkv_w.reshape(width, -1),
        out_w.reshape(q_cols, width),
        mixed,
        heads,
        lse,
        bias,
        cosine,
        sine,
        tokens,
        num_heads,
        kv_heads,
        num_experts,
    )
    return (
        layer_out,
        grad_in,
        misc_sum[:, num_experts],
        q_sum,
        k_sum,
        v_sum,
        out_sum,
        misc_sum[:, num_experts + 1],
        misc_sum[:, :num_experts],
        *expert_sums,
    )


def solution(mesh):
    in_specs = (
        P(("dp", "exp"), None),
        P(("dp", "exp"), None),
        P(),
        P(("dp", "exp")),
        P(("dp", "exp"), None),
        P(("dp", "exp")),
        P(("dp", "exp"), None),
        P(("dp", "exp"), None),
        P(("dp", "exp"), None),
        P(("dp", "exp"), None),
        P(("dp", "exp")),
        P(("dp", "exp"), None),
        P("exp", "dp", None),
        P("exp", "dp", None),
        P("exp", "dp", None),
    )
    out_specs = (
        P(("dp", "exp"), None),
        P(("dp", "exp"), None),
        P(("dp", "exp")),
        P(("dp", "exp"), None),
        P(("dp", "exp"), None),
        P(("dp", "exp"), None),
        P(("dp", "exp"), None),
        P(("dp", "exp")),
        P(("dp", "exp"), None),
        P("exp", "dp", None),
        P("exp", "dp", None),
        P("exp", "dp", None),
    )
    body = body_plane if (mesh.shape["dp"], mesh.shape["exp"]) == (4, 8) else body_general
    return jax.shard_map(body, mesh=mesh, in_specs=in_specs, out_specs=out_specs, check_vma=False)
```

```python
import functools

import jax
import jax.numpy as jnp
from jax import lax
from jax.experimental import pallas as pl
from jax.experimental.pallas import tpu as pltpu
from jax.sharding import PartitionSpec as P

HD = 128
PROMPT = 256
NCONT = 2


EPS = 1e-06
THETA = 10000.0
HIGH = lax.Precision.HIGHEST
NEG_BIG = -1e30


def positions(segments):
    count_rows = segments.shape[0]
    row_ids = jnp.arange(count_rows, dtype=jnp.int32)
    labels = jnp.arange(NCONT + 1, dtype=jnp.int32)
    member = segments[:, None] == labels[None, :]
    first_row = jnp.min(jnp.where(member, row_ids[:, None], count_rows), axis=0)
    start_row = jnp.sum(jnp.where(member, first_row[None, :], 0), axis=1)
    return jnp.where(segments == 0, row_ids, PROMPT + row_ids - start_row)


def key_mask(segments):
    row_ids = jnp.arange(segments.shape[0], dtype=jnp.int32)
    causal = row_ids[None, :] <= row_ids[:, None]
    visible = (segments[None, :] == 0) | (segments[None, :] == segments[:, None])
    return causal & visible


def rotate(values, pos_rows, sign_value):
    half_size = HD // 2
    freq = THETA ** (-2.0 * jnp.arange(half_size, dtype=jnp.float32) / HD)
    angle = pos_rows.astype(jnp.float32)[:, None] * freq[None, :]
    cosine = jnp.cos(angle)[:, None, :]
    sine_part = sign_value * jnp.sin(angle)[:, None, :]
    first_half = values[..., :half_size]
    second = values[..., half_size:]
    return jnp.concatenate(
        [first_half * cosine - second * sine_part, second * cosine + first_half * sine_part],
        axis=-1,
    )


def attention_scores(query_b, key_b, allowed):
    logits = jnp.einsum(
        "qkgd,pkd->kgqp", query_b, key_b, preferred_element_type=jnp.float32
    ) * HD ** (-0.5)
    return jnp.where(allowed[None, None], logits, NEG_BIG)


def expert_gates(rows_in, gate_w, up_w):
    gate_val = jnp.einsum("sacd,adf->sacf", rows_in, gate_w, preferred_element_type=jnp.float32)
    up_val = jnp.einsum("sacd,adf->sacf", rows_in, up_w, preferred_element_type=jnp.float32)
    return (gate_val, up_val)


def body_general(
    tokens,
    targets,
    valid_count,
    segments,
    routes,
    gain_attn,
    w_query,
    w_key,
    w_value,
    w_out,
    gain_moe,
    w_router,
    w_gate,
    w_up,
    w_down,
):
    gain_one, query_w, key_w, value_w, out_w, gain_two, router_w = (
        lax.all_gather(gain_attn, ("dp", "exp"), axis=0, tiled=True),
        lax.all_gather(w_query, ("dp", "exp"), axis=0, tiled=True),
        lax.all_gather(w_key, ("dp", "exp"), axis=0, tiled=True),
        lax.all_gather(w_value, ("dp", "exp"), axis=0, tiled=True),
        lax.all_gather(w_out, ("dp", "exp"), axis=0, tiled=True),
        lax.all_gather(gain_moe, ("dp", "exp"), axis=0, tiled=True),
        lax.all_gather(w_router, ("dp", "exp"), axis=0, tiled=True),
    )
    gate_w, up_w, down_w = (
        lax.all_gather(w_gate, "dp", axis=1, tiled=True),
        lax.all_gather(w_up, "dp", axis=1, tiled=True),
        lax.all_gather(w_down, "dp", axis=1, tiled=True),
    )
    num_rows = tokens.shape[0]
    width = tokens.shape[1]
    num_heads = query_w.shape[1] // HD
    kv_heads = key_w.shape[1] // HD
    group_size = num_heads // kv_heads
    num_experts = router_w.shape[1]
    top_count = routes.shape[1]
    exp_local = gate_w.shape[0]
    exp_ranks = lax.axis_size("exp")
    capacity = 5 * num_rows * top_count // (4 * num_experts)
    tok_pos = positions(segments)
    allowed = key_mask(segments)
    resid_in = tokens.astype(jnp.float32)
    inv_one = lax.rsqrt(jnp.mean(resid_in * resid_in, axis=-1, keepdims=True) + EPS)
    normed_one = resid_in * inv_one
    hidden_one = (normed_one * gain_one.astype(jnp.float32)).astype(jnp.bfloat16)
    query_raw = jnp.dot(hidden_one, query_w, preferred_element_type=jnp.float32)
    key_raw = jnp.dot(hidden_one, key_w, preferred_element_type=jnp.float32)
    value_b = jnp.dot(hidden_one, value_w, preferred_element_type=jnp.float32).astype(jnp.bfloat16)
    query_b = rotate(query_raw.reshape(num_rows, num_heads, HD), tok_pos, 1.0).astype(jnp.bfloat16)
    query_b = query_b.reshape(num_rows, kv_heads, group_size, HD)
    key_b = rotate(key_raw.reshape(num_rows, kv_heads, HD), tok_pos, 1.0).astype(jnp.bfloat16)
    value_h = value_b.reshape(num_rows, kv_heads, HD)
    logit_att = attention_scores(query_b, key_b, allowed)
    row_max = jnp.max(logit_att, axis=-1, keepdims=True)
    log_total = row_max + jnp.log(jnp.sum(jnp.exp(logit_att - row_max), axis=-1, keepdims=True))
    probs_b = jnp.exp(logit_att - log_total).astype(jnp.bfloat16)
    attn_vals = jnp.einsum("kgqp,pkd->qkgd", probs_b, value_h, preferred_element_type=jnp.float32)
    attn_vals = attn_vals.reshape(num_rows, num_heads * HD).astype(jnp.bfloat16)
    resid_mid = resid_in + jnp.dot(attn_vals, out_w, preferred_element_type=jnp.float32)
    inv_two = lax.rsqrt(jnp.mean(resid_mid * resid_mid, axis=-1, keepdims=True) + EPS)
    normed_two = resid_mid * inv_two
    gain_two_f = gain_two.astype(jnp.float32)
    hidden_two = (normed_two * gain_two_f).astype(jnp.bfloat16)
    router_prob = jax.nn.softmax(
        jnp.dot(hidden_two, router_w, preferred_element_type=jnp.float32), axis=-1
    )
    expert_ids = jnp.arange(num_experts, dtype=jnp.int32)
    route_hot = routes[:, :, None] == expert_ids[None, None, :]
    chosen = jnp.sum(jnp.where(route_hot, router_prob[:, None, :], 0.0), axis=-1)
    weight_sum = jnp.sum(chosen, axis=1, keepdims=True)
    combine = chosen / weight_sum
    flat_hot = route_hot.reshape(num_rows * top_count, num_experts).astype(jnp.int32)
    slot_index = jnp.sum((jnp.cumsum(flat_hot, axis=0) - flat_hot) * flat_hot, axis=1)
    dest_index = routes.reshape(-1) * capacity + slot_index
    send_shape = (exp_ranks, exp_local, capacity, width)
    send_rows = jnp.zeros((num_experts * capacity, width), jnp.bfloat16)
    send_rows = (
        send_rows.at[dest_index].set(jnp.repeat(hidden_two, top_count, axis=0)).reshape(send_shape)
    )
    gate_val, up_val = expert_gates(
        lax.all_to_all(send_rows, "exp", split_axis=0, concat_axis=0, tiled=True), gate_w, up_w
    )
    act_b = (jax.nn.relu(gate_val) * up_val).astype(jnp.bfloat16)
    out_b = jnp.einsum("sacf,afd->sacd", act_b, down_w, preferred_element_type=jnp.float32).astype(
        jnp.bfloat16
    )
    returned = lax.all_to_all(out_b, "exp", split_axis=0, concat_axis=0, tiled=True)
    route_out = returned.reshape(num_experts * capacity, width)[dest_index].reshape(
        num_rows, top_count, width
    )
    route_out_f = route_out.astype(jnp.float32)
    resid_out = resid_mid + jnp.sum(combine[:, :, None] * route_out_f, axis=1)
    layer_out = resid_out.astype(jnp.bfloat16)
    total_rows = num_rows * lax.axis_size(("dp", "exp"))
    global_row = lax.axis_index(("dp", "exp")) * num_rows + jnp.arange(num_rows, dtype=jnp.int32)
    loss_scale = total_rows / valid_count[0].astype(jnp.float32)
    grad_out = jnp.where(
        (global_row < valid_count[0])[:, None],
        (resid_out - targets.astype(jnp.float32)) * loss_scale,
        0.0,
    )
    gain_one, query_w, key_w, value_w, out_w, gain_two, router_w = (
        lax.all_gather(gain_attn, ("dp", "exp"), axis=0, tiled=True),
        lax.all_gather(w_query, ("dp", "exp"), axis=0, tiled=True),
        lax.all_gather(w_key, ("dp", "exp"), axis=0, tiled=True),
        lax.all_gather(w_value, ("dp", "exp"), axis=0, tiled=True),
        lax.all_gather(w_out, ("dp", "exp"), axis=0, tiled=True),
        lax.all_gather(gain_moe, ("dp", "exp"), axis=0, tiled=True),
        lax.all_gather(w_router, ("dp", "exp"), axis=0, tiled=True),
    )
    gain_two_f = gain_two.astype(jnp.float32)
    grad_route = (combine[:, :, None] * grad_out[:, None, :]).astype(jnp.bfloat16)
    grad_comb = jnp.sum(grad_out[:, None, :] * route_out_f, axis=-1)
    grad_send = jnp.zeros((num_experts * capacity, width), jnp.bfloat16)
    grad_send = (
        grad_send.at[dest_index]
        .set(grad_route.reshape(num_rows * top_count, width))
        .reshape(send_shape)
    )
    expert_rows, grad_recv = (
        lax.all_to_all(send_rows, "exp", split_axis=0, concat_axis=0, tiled=True),
        lax.all_to_all(grad_send, "exp", split_axis=0, concat_axis=0, tiled=True),
    )
    gate_val, up_val = expert_gates(expert_rows, gate_w, up_w)
    gate_relu = jax.nn.relu(gate_val)
    act_b = (gate_relu * up_val).astype(jnp.bfloat16)
    grad_act = jnp.einsum("sacd,afd->sacf", grad_recv, down_w, preferred_element_type=jnp.float32)
    grad_down_w = jnp.einsum("sacf,sacd->afd", act_b, grad_recv, preferred_element_type=jnp.float32)
    grad_gate_b = jnp.where(gate_val > 0, grad_act * up_val, 0.0).astype(jnp.bfloat16)
    grad_up_b = (grad_act * gate_relu).astype(jnp.bfloat16)
    grad_gate_w = jnp.einsum(
        "sacd,sacf->adf", expert_rows, grad_gate_b, preferred_element_type=jnp.float32
    )
    grad_up_w = jnp.einsum(
        "sacd,sacf->adf", expert_rows, grad_up_b, preferred_element_type=jnp.float32
    )
    grad_rows = (
        jnp.einsum("sacf,adf->sacd", grad_gate_b, gate_w, preferred_element_type=jnp.float32)
        + jnp.einsum("sacf,adf->sacd", grad_up_b, up_w, preferred_element_type=jnp.float32)
    ).astype(jnp.bfloat16)
    grad_back = lax.all_to_all(grad_rows, "exp", split_axis=0, concat_axis=0, tiled=True)
    grad_copies = grad_back.reshape(num_experts * capacity, width)[dest_index].reshape(
        num_rows, top_count, width
    )
    grad_hidden_two = jnp.sum(grad_copies.astype(jnp.float32), axis=1)
    grad_chosen = (grad_comb - jnp.sum(grad_comb * combine, axis=1, keepdims=True)) / weight_sum
    grad_prob = jnp.sum(jnp.where(route_hot, grad_chosen[:, :, None], 0.0), axis=1)
    grad_logit = router_prob * (
        grad_prob - jnp.sum(router_prob * grad_prob, axis=-1, keepdims=True)
    )
    router_f = router_w.astype(jnp.float32)
    grad_hidden_two = grad_hidden_two + jnp.einsum(
        "re,de->rd", grad_logit, router_f, precision=HIGH
    )
    grad_router = jnp.einsum(
        "rd,re->de", hidden_two.astype(jnp.float32), grad_logit, precision=HIGH
    )
    grad_gain_two = jnp.sum(grad_hidden_two * normed_two, axis=0)
    grad_norm_two = grad_hidden_two * gain_two_f
    grad_mid = grad_out + inv_two * (
        grad_norm_two - normed_two * jnp.mean(grad_norm_two * normed_two, axis=-1, keepdims=True)
    )
    grad_proj_b = grad_mid.astype(jnp.bfloat16)
    grad_out_w = jnp.einsum("rh,rd->hd", attn_vals, grad_proj_b, preferred_element_type=jnp.float32)
    grad_vals_b = jnp.einsum(
        "rd,hd->rh", grad_proj_b, out_w, preferred_element_type=jnp.float32
    ).astype(jnp.bfloat16)
    grad_vals_b = grad_vals_b.reshape(num_rows, kv_heads, group_size, HD)
    logit_att = attention_scores(query_b, key_b, allowed)
    probs = jnp.exp(logit_att - log_total)
    probs_b = probs.astype(jnp.bfloat16)
    grad_value = jnp.einsum(
        "kgqp,qkgd->pkd", probs_b, grad_vals_b, preferred_element_type=jnp.float32
    )
    grad_prob_att = jnp.einsum(
        "qkgd,pkd->kgqp", grad_vals_b, value_h, preferred_element_type=jnp.float32
    )
    delta_row = jnp.sum(probs * grad_prob_att, axis=-1, keepdims=True)
    grad_score_b = (probs * (grad_prob_att - delta_row)).astype(jnp.bfloat16)
    grad_query = jnp.einsum(
        "kgqp,pkd->qkgd", grad_score_b, key_b, preferred_element_type=jnp.float32
    ) * HD ** (-0.5)
    grad_key = jnp.einsum(
        "kgqp,qkgd->pkd", grad_score_b, query_b, preferred_element_type=jnp.float32
    ) * HD ** (-0.5)
    grad_query_b = rotate(grad_query.reshape(num_rows, num_heads, HD), tok_pos, -1.0).astype(
        jnp.bfloat16
    )
    grad_query_b = grad_query_b.reshape(num_rows, num_heads * HD)
    grad_key_b = (
        rotate(grad_key, tok_pos, -1.0).astype(jnp.bfloat16).reshape(num_rows, kv_heads * HD)
    )
    grad_value_b = grad_value.astype(jnp.bfloat16).reshape(num_rows, kv_heads * HD)
    grad_query_w = jnp.einsum(
        "rd,rh->dh", hidden_one, grad_query_b, preferred_element_type=jnp.float32
    )
    grad_key_w = jnp.einsum("rd,rh->dh", hidden_one, grad_key_b, preferred_element_type=jnp.float32)
    grad_value_w = jnp.einsum(
        "rd,rh->dh", hidden_one, grad_value_b, preferred_element_type=jnp.float32
    )
    grad_hidden_one = (
        jnp.einsum("rh,dh->rd", grad_query_b, query_w, preferred_element_type=jnp.float32)
        + jnp.einsum("rh,dh->rd", grad_key_b, key_w, preferred_element_type=jnp.float32)
        + jnp.einsum("rh,dh->rd", grad_value_b, value_w, preferred_element_type=jnp.float32)
    )
    grad_gain_one = jnp.sum(grad_hidden_one * normed_one, axis=0)
    grad_norm_one = grad_hidden_one * gain_one.astype(jnp.float32)
    grad_in = grad_mid + inv_one * (
        grad_norm_one - normed_one * jnp.mean(grad_norm_one * normed_one, axis=-1, keepdims=True)
    )
    dense_sums = (
        lax.psum_scatter(grad_gain_one, ("dp", "exp"), scatter_dimension=0, tiled=True),
        lax.psum_scatter(grad_query_w, ("dp", "exp"), scatter_dimension=0, tiled=True),
        lax.psum_scatter(grad_key_w, ("dp", "exp"), scatter_dimension=0, tiled=True),
        lax.psum_scatter(grad_value_w, ("dp", "exp"), scatter_dimension=0, tiled=True),
        lax.psum_scatter(grad_out_w, ("dp", "exp"), scatter_dimension=0, tiled=True),
        lax.psum_scatter(grad_gain_two, ("dp", "exp"), scatter_dimension=0, tiled=True),
        lax.psum_scatter(grad_router, ("dp", "exp"), scatter_dimension=0, tiled=True),
    )
    expert_sums = (
        lax.psum_scatter(
            grad_gate_w.astype(jnp.bfloat16), "dp", scatter_dimension=1, tiled=True
        ).astype(jnp.float32),
        lax.psum_scatter(
            grad_up_w.astype(jnp.bfloat16), "dp", scatter_dimension=1, tiled=True
        ).astype(jnp.float32),
        lax.psum_scatter(
            grad_down_w.astype(jnp.bfloat16), "dp", scatter_dimension=1, tiled=True
        ).astype(jnp.float32),
    )
    return (
        layer_out,
        grad_in,
        dense_sums[0],
        dense_sums[1],
        dense_sums[2],
        dense_sums[3],
        dense_sums[4],
        dense_sums[5],
        dense_sums[6],
        expert_sums[0],
        expert_sums[1],
        expert_sums[2],
    )


MESH = pl.DeviceIdType.MESH
ANY = pl.BlockSpec(memory_space=pl.ANY)
VMEM = pl.BlockSpec(memory_space=pltpu.VMEM)
VMEM_BYTES = 62 * 2**20


def nn_dot(left, right):
    return jnp.dot(left, right, preferred_element_type=jnp.float32)


def nt_dot(left, right):
    return lax.dot_general(
        left, right, (((1,), (1,)), ((), ())), preferred_element_type=jnp.float32
    )


def tn_dot(left, right):
    return lax.dot_general(
        left, right, (((0,), (0,)), ((), ())), preferred_element_type=jnp.float32
    )


def plane_peers():
    me = lax.axis_index("exp")
    core = lax.rem(me, 2)
    x_pos = lax.rem(lax.div(me, 2), 2)
    y_pos = lax.div(me, 4)
    return me, me + 1 - 2 * core, me + 2 - 4 * x_pos, me + 4 - 8 * y_pos


def remote(src, dst, send_sem, recv_sem, peer):
    return pltpu.make_async_remote_copy(
        src_ref=src,
        dst_ref=dst,
        send_sem=send_sem,
        recv_sem=recv_sem,
        device_id={"exp": peer},
        device_id_type=MESH,
    )


def plane_barrier(peers):
    barrier = pltpu.get_barrier_semaphore()
    for peer in peers:
        pl.semaphore_signal(barrier, inc=1, device_id={"exp": peer}, device_id_type=MESH)
    pl.semaphore_wait(barrier, len(peers))


def step_place(step, quad):
    odd = lax.rem(step, 2)
    last = lax.div(quad, 3)
    mid = lax.rem(lax.div(quad + 1, 2), 2)
    return mid * (1 - odd) + last, mid * odd + last


class Gather:
    def __init__(self, own, buf, send, recv):
        self.own, self.buf, self.send, self.recv = own, buf, send, recv
        self.me, self.sib, self.xn, self.yn = plane_peers()
        self.diag = self.xn + self.yn - self.me

    def own_copy(self, half, peer, sem):
        return remote(
            self.own.at[half],
            self.buf.at[self.me, half],
            self.send.at[sem],
            self.recv.at[self.me, half],
            peer,
        )

    def pass_copy(self, slot, half, peer, sem):
        return remote(
            self.buf.at[slot, half],
            self.buf.at[slot, half],
            self.send.at[sem],
            self.recv.at[slot, half],
            peer,
        )

    def own_copies(self):
        return (
            self.own_copy(0, self.xn, 0),
            self.own_copy(1, self.yn, 1),
            self.own_copy(0, self.sib, 2),
            self.own_copy(1, self.sib, 3),
            self.own_copy(1, self.xn, 4),
            self.own_copy(0, self.yn, 5),
        )

    def near_copies(self):
        return (
            self.pass_copy(self.xn, 0, self.yn, 6),
            self.pass_copy(self.yn, 1, self.xn, 7),
            self.pass_copy(self.xn, 0, self.sib, 8),
            self.pass_copy(self.yn, 1, self.sib, 9),
        )

    def late_copies(self):
        return (
            self.pass_copy(self.xn, 1, self.sib, 10),
            self.pass_copy(self.yn, 0, self.sib, 11),
        )

    def far_copies(self):
        return (
            self.pass_copy(self.diag, 0, self.sib, 12),
            self.pass_copy(self.diag, 1, self.sib, 13),
        )

    def wait_block(self, slot, half):
        self.pass_copy(slot, half, self.sib, 0).wait_recv()

    def begin(self):
        plane_barrier((self.sib, self.xn, self.yn))
        for copy in self.own_copies():
            copy.start()

    def place(self, step):
        quad = lax.div(step, 4)
        far_x, far_y = step_place(step, quad)
        odd = lax.rem(step, 2)
        third = lax.div(quad, 2) * (1 - lax.div(quad, 3))
        other = lax.div(lax.rem(step, 4), 2)
        slot = (
            self.me
            + far_x * (self.xn - self.me)
            + far_y * (self.yn - self.me)
            + other * (self.sib - self.me)
        )
        return slot, odd + third * (1 - 2 * odd), other

    def arrive(self, step):
        @pl.when(step == 4)
        def _():
            self.wait_block(self.xn, 0)
            self.wait_block(self.yn, 1)
            for copy in self.near_copies():
                copy.start()

        @pl.when(step == 8)
        def _():
            self.wait_block(self.xn, 1)
            self.wait_block(self.yn, 0)
            for copy in self.late_copies():
                copy.start()

        @pl.when(step == 12)
        def _():
            self.wait_block(self.diag, 0)
            self.wait_block(self.diag, 1)
            for copy in self.far_copies():
                copy.start()

        slot, half, other = self.place(step)

        @pl.when(other == 1)
        def _():
            self.wait_block(slot, half)

        return slot, half

    def finish(self):
        for copies in (self.own_copies(), self.near_copies(), self.late_copies(), self.far_copies()):
            for copy in copies:
                copy.wait_send()


def line_peers():
    line = lax.axis_index("dp")
    return (
        line,
        line + 1 - 2 * lax.rem(line, 2),
        line + 2 - 4 * lax.div(line, 2),
        3 - line,
    )


def line_remote(src, dst, send_sem, recv_sem, peer):
    return pltpu.make_async_remote_copy(
        src_ref=src,
        dst_ref=dst,
        send_sem=send_sem,
        recv_sem=recv_sem,
        device_id={"dp": peer},
        device_id_type=MESH,
    )


def full_barrier(plane, line):
    barrier = pltpu.get_barrier_semaphore()
    for peer in plane:
        pl.semaphore_signal(barrier, inc=1, device_id={"exp": peer}, device_id_type=MESH)
    for peer in line:
        pl.semaphore_signal(barrier, inc=1, device_id={"dp": peer}, device_id_type=MESH)
    pl.semaphore_wait(barrier, len(plane) + len(line))


def expert_in_kernel(own, gate_hbm, down_own, rows_out, gate_out, down_out, buf, gate, gate_w, down_stage, send, recv, load, store_a, store_b, line_send, line_recv):
    width = gate_w.shape[0]
    gather = Gather(own, buf, send, recv)
    line = line_peers()
    loads = (
        pltpu.make_async_copy(own.at[0], buf.at[gather.me, 0], load.at[0]),
        pltpu.make_async_copy(own.at[1], buf.at[gather.me, 1], load.at[1]),
        pltpu.make_async_copy(gate_hbm, gate_w, load.at[2]),
        pltpu.make_async_copy(down_own, down_stage, load.at[3]),
    )
    for copy in loads:
        copy.start()
    full_barrier((gather.sib, gather.xn, gather.yn), line[1:])
    for copy in gather.own_copies():
        copy.start()

    def down_copy(turn):
        return line_remote(
            down_own,
            down_out.at[line[0]],
            line_send.at[turn - 1],
            line_recv.at[turn - 1],
            line[turn],
        )

    for turn in (1, 2, 3):
        down_copy(turn).start()
    for copy in loads:
        copy.wait()
    down_store = pltpu.make_async_copy(down_stage, down_out.at[line[0]], load.at[4])
    down_store.start()

    def row_store(slot, half, step):
        return pltpu.make_async_copy(buf.at[slot, half], rows_out.at[slot, half], store_a.at[step])

    def gate_store(slot, half, step):
        return pltpu.make_async_copy(gate.at[slot, half], gate_out.at[slot, half], store_b.at[step])

    def one(step, carry):
        slot, half = gather.arrive(step)
        row_store(slot, half, step).start()
        gate[slot, half] = nn_dot(buf[slot, half, :, :width], gate_w[...]).astype(jnp.bfloat16)
        gate_store(slot, half, step).start()
        return carry

    lax.fori_loop(0, 16, one, 0)
    gather.finish()

    def drain(step, carry):
        slot, half, _ = gather.place(step)
        row_store(slot, half, step).wait()
        gate_store(slot, half, step).wait()
        return carry

    lax.fori_loop(0, 16, drain, 0)
    down_store.wait()
    for turn in (1, 2, 3):
        line_remote(
            down_own,
            down_out.at[line[turn]],
            line_send.at[turn - 1],
            line_recv.at[turn - 1],
            line[turn],
        ).wait()


def expert_in(own, gate_w, down_own):
    _, half, columns = own.shape
    width, hidden = gate_w.shape
    bf = jnp.bfloat16
    return pl.pallas_call(
        expert_in_kernel,
        out_shape=(
            jax.ShapeDtypeStruct((8, 2, half, columns), bf),
            jax.ShapeDtypeStruct((8, 2, half, hidden), bf),
            jax.ShapeDtypeStruct((4, *down_own.shape), bf),
        ),
        in_specs=[ANY] * 3,
        out_specs=(ANY, ANY, ANY),
        scratch_shapes=[
            pltpu.VMEM((8, 2, half, columns), bf),
            pltpu.VMEM((8, 2, half, hidden), bf),
            pltpu.VMEM((width, hidden), bf),
            pltpu.VMEM(down_own.shape, bf),
            pltpu.SemaphoreType.DMA((14,)),
            pltpu.SemaphoreType.DMA((8, 2)),
            pltpu.SemaphoreType.DMA((5,)),
            pltpu.SemaphoreType.DMA((16,)),
            pltpu.SemaphoreType.DMA((16,)),
            pltpu.SemaphoreType.DMA((3,)),
            pltpu.SemaphoreType.DMA((3,)),
        ],
        compiler_params=pltpu.CompilerParams(
            collective_id=1, has_side_effects=True, vmem_limit_bytes=VMEM_BYTES
        ),
        name="expert_in",
    )(own, gate_w, down_own)


def row_chunk(rows):
    return 64 if rows % 64 == 0 else 16


def add_rows(target, others):
    parts, rows_all, _ = target.shape
    chunk = row_chunk(rows_all)
    for part in range(parts):

        def one(index, carry):
            rows = pl.ds(pl.multiple_of(index * chunk, chunk), chunk)
            total = target[part, rows, :].astype(jnp.float32)
            for other in others:
                total = total + other[part, rows, :].astype(jnp.float32)
            target[part, rows, :] = total.astype(target.dtype)
            return carry

        lax.fori_loop(0, rows_all // chunk, one, 0)


class Scatter:
    def __init__(self, mine, theirs, scratch):
        self.mine_of, self.theirs = mine, theirs
        self.side, self.relay, self.final = scratch[:3]
        self.send, self.side_sem, self.relay_sem, self.final_sem = scratch[3:]
        self.me, self.sib, self.xn, self.yn = plane_peers()

    def mine(self, place, half):
        slot = (self.me, self.xn, self.yn, self.xn + self.yn - self.me)[place]
        return self.mine_of(place, slot, half)

    def peers(self):
        return self.sib, self.xn, self.yn

    def place(self, step):
        quad = lax.div(step, 4)
        odd = lax.div(lax.rem(step, 4), 2)
        far_x, far_y = step_place(odd, 3 - quad)
        third = lax.div(quad, 2) * (1 - lax.div(quad, 3))
        other = 1 - lax.rem(step, 2)
        slot = (
            self.me
            + far_x * (self.xn - self.me)
            + far_y * (self.yn - self.me)
            + other * (self.sib - self.me)
        )
        return slot, odd + third * (1 - 2 * odd), other, far_x + 2 * far_y

    def side_copy(self, step):
        slot, half, _, place = self.place(step)
        return remote(
            self.theirs(place, slot, half),
            self.side.at[place, half],
            self.send.at[step],
            self.side_sem.at[place, half],
            self.sib,
        )

    def side_wait(self, place, half):
        remote(
            self.side.at[place, half],
            self.side.at[place, half],
            self.send.at[0],
            self.side_sem.at[place, half],
            self.sib,
        ).wait_recv()

    def relay_copy(self, step, way):
        return remote(
            self.mine(3, way),
            self.relay.at[way],
            self.send.at[step],
            self.relay_sem.at[way],
            (self.xn, self.yn)[way],
        )

    def final_copy(self, step, way, half):
        return remote(
            self.mine(1 + way, half),
            self.final.at[way, half],
            self.send.at[step],
            self.final_sem.at[way, half],
            (self.xn, self.yn)[way],
        )

    def depart(self, step):
        @pl.when(self.place(step)[2] == 1)
        def _():
            self.side_copy(step).start()

        for way in (0, 1):

            @pl.when(step == 1 + 2 * way)
            def _():
                self.side_wait(3, way)
                add_rows(self.mine(3, way), (self.side.at[3, way],))
                self.relay_copy(1 + 2 * way, way).start()

            @pl.when(step == 5 + 2 * way)
            def _():
                self.side_wait(1 + way, way)
                add_rows(self.mine(1 + way, way), (self.side.at[1 + way, way],))
                self.final_copy(5 + 2 * way, way, way).start()

    def send_theirs(self):
        def one(index, carry):
            self.side_copy(2 * index).start()
            return carry

        lax.fori_loop(0, 8, one, 0)

    def send_mine(self):
        for way in (0, 1):
            self.side_wait(3, way)
            add_rows(self.mine(3, way), (self.side.at[3, way],))
            self.relay_copy(1 + 2 * way, way).start()
        for way in (0, 1):
            self.side_wait(1 + way, way)
            add_rows(self.mine(1 + way, way), (self.side.at[1 + way, way],))
            self.final_copy(5 + 2 * way, way, way).start()

    def forward(self):
        for way in (0, 1):
            self.side_wait(1 + way, 1 - way)
            self.relay_copy(0, 1 - way).wait_recv()
            add_rows(
                self.mine(1 + way, 1 - way),
                (self.side.at[1 + way, 1 - way], self.relay.at[1 - way]),
            )
            self.final_copy(9 + 2 * way, way, 1 - way).start()

    def finish(self, write):
        parts, rows_all = self.relay.shape[1:3]
        chunk = row_chunk(rows_all)
        for half in (0, 1):
            home = self.mine(0, half)
            self.side_wait(0, half)
            self.final_copy(0, 0, half).wait_recv()
            self.final_copy(0, 1, half).wait_recv()
            for part in range(parts):

                def one(index, carry, half=half, home=home, part=part):
                    rows = pl.ds(pl.multiple_of(index * chunk, chunk), chunk)
                    total = home[part, rows, :].astype(jnp.float32)
                    total = total + self.side[0, half, part, rows, :].astype(jnp.float32)
                    total = total + self.final[0, half, part, rows, :].astype(jnp.float32)
                    total = total + self.final[1, half, part, rows, :].astype(jnp.float32)
                    write(half, part, rows, total)
                    return carry

                lax.fori_loop(0, rows_all // chunk, one, 0)

    def drain(self):
        for way in (0, 1):
            self.relay_copy(1 + 2 * way, way).wait_send()
            self.final_copy(5 + 2 * way, way, way).wait_send()
            self.final_copy(9 + 2 * way, way, 1 - way).wait_send()

        def one(step, carry):
            @pl.when(self.place(step)[2] == 1)
            def _():
                self.side_copy(step).wait_send()

            return carry

        lax.fori_loop(0, 16, one, 0)


SCATTER_REFS = 7


def scatter_scratch(parts, rows, columns):
    bf = jnp.bfloat16
    return [
        pltpu.VMEM((4, 2, parts, rows, columns), bf),
        pltpu.VMEM((2, parts, rows, columns), bf),
        pltpu.VMEM((2, 2, parts, rows, columns), bf),
        pltpu.SemaphoreType.DMA((16,)),
        pltpu.SemaphoreType.DMA((4, 2)),
        pltpu.SemaphoreType.DMA((2,)),
        pltpu.SemaphoreType.DMA((2, 2)),
    ]


OUT_SLOTS = 4


def expert_out_kernel(rows_hbm, gate_hbm, up_hbm, down_hbm, resid, targets, scales, layer, grad, grad_b, ua_out, rows, gate, ua, up_w, down_w, mine, away, load_w, load_rows, load_gate, store_ua, *scratch):
    hidden, width = down_w.shape
    scatter = Scatter(
        lambda place, slot, half: mine.at[place, half],
        lambda place, slot, half: away.at[place, half],
        scratch,
    )
    weights = (
        pltpu.make_async_copy(up_hbm, up_w, load_w.at[0]),
        pltpu.make_async_copy(down_hbm, down_w, load_w.at[1]),
    )

    def loads(step):
        slot, half, _, _ = scatter.place(step)
        spot = lax.rem(step, OUT_SLOTS)
        return (
            pltpu.make_async_copy(rows_hbm.at[slot, half], rows.at[spot], load_rows.at[step]),
            pltpu.make_async_copy(gate_hbm.at[slot, half], gate.at[spot], load_gate.at[step]),
        )

    def ua_store(step):
        slot, half, _, _ = scatter.place(step)
        return pltpu.make_async_copy(
            ua.at[lax.rem(step, OUT_SLOTS)], ua_out.at[slot, half], store_ua.at[step]
        )

    weights[0].start()
    for step in (0, 1):
        for copy in loads(step):
            copy.start()
    weights[1].start()
    plane_barrier(scatter.peers())
    for copy in weights:
        copy.wait()

    def one(step, carry):
        _, _, other, place = scatter.place(step)
        spot = lax.rem(step, OUT_SLOTS)
        for copy in loads(step):
            copy.wait()

        @pl.when(step < 14)
        def _():
            for copy in loads(step + 2):
                copy.start()

        @pl.when(step >= OUT_SLOTS)
        def _():
            ua_store(step - OUT_SLOTS).wait()

        lanes = lax.broadcasted_iota(jnp.int32, (rows.shape[1], 128), 1)
        tail = rows[spot, :, width:].astype(jnp.float32)
        weight = jnp.sum(jnp.where(lanes == scatter.me, tail, 0.0), axis=1, keepdims=True)
        up_val = nn_dot(rows[spot, :, :width], up_w[...])
        act_val = jnp.maximum(gate[spot].astype(jnp.float32), 0.0) * up_val * weight
        ua[spot, :, :hidden] = up_val.astype(jnp.bfloat16)
        ua[spot, :, hidden:] = act_val.astype(jnp.bfloat16)
        ua_store(step).start()
        partial = nn_dot(ua[spot, :, hidden:], down_w[...]).astype(jnp.bfloat16)

        @pl.when(other == 1)
        def _():
            away[place, half_of(scatter, step), 0] = partial

        @pl.when(other == 0)
        def _():
            mine[place, half_of(scatter, step), 0] = partial

        scatter.depart(step)

        @pl.when(step == 12)
        def _():
            scatter.forward()

        return carry

    lax.fori_loop(0, 16, one, 0)

    def write(half, part, rows, total):
        value = resid[half, rows, :] + total
        layer[half, rows, :] = value.astype(layer.dtype)
        error = (value - targets[half, rows, :].astype(jnp.float32)) * scales[half, rows, 0:1]
        grad[half, rows, :] = error
        grad_b[half, rows, :] = error.astype(grad_b.dtype)

    scatter.finish(write)
    scatter.drain()

    def drain(step, carry):
        ua_store(step).wait()
        return carry

    lax.fori_loop(16 - OUT_SLOTS, 16, drain, 0)


def half_of(scatter, step):
    return scatter.place(step)[1]


def expert_out(rows_all, gate_val, up_w, down_w, resid, targets, scales):
    half, columns = rows_all.shape[2:]
    hidden, width = down_w.shape
    bf = jnp.bfloat16
    return pl.pallas_call(
        expert_out_kernel,
        out_shape=(
            jax.ShapeDtypeStruct((2, half, width), bf),
            jax.ShapeDtypeStruct((2, half, width), jnp.float32),
            jax.ShapeDtypeStruct((2, half, width), bf),
            jax.ShapeDtypeStruct((8, 2, half, 2 * hidden), bf),
        ),
        in_specs=[ANY] * 4 + [VMEM] * 3,
        out_specs=(VMEM, VMEM, VMEM, ANY),
        scratch_shapes=[
            pltpu.VMEM((OUT_SLOTS, half, columns), bf),
            pltpu.VMEM((OUT_SLOTS, half, hidden), bf),
            pltpu.VMEM((OUT_SLOTS, half, 2 * hidden), bf),
            pltpu.VMEM((width, hidden), bf),
            pltpu.VMEM((hidden, width), bf),
            pltpu.VMEM((4, 2, 1, half, width), bf),
            pltpu.VMEM((4, 2, 1, half, width), bf),
            pltpu.SemaphoreType.DMA((2,)),
            pltpu.SemaphoreType.DMA((16,)),
            pltpu.SemaphoreType.DMA((16,)),
            pltpu.SemaphoreType.DMA((16,)),
        ]
        + scatter_scratch(1, half, width),
        compiler_params=pltpu.CompilerParams(
            collective_id=2, has_side_effects=True, vmem_limit_bytes=VMEM_BYTES
        ),
        name="expert_out",
    )(
        rows_all,
        gate_val,
        up_w,
        down_w,
        resid.reshape(2, half, width),
        targets.reshape(2, half, width),
        scales.reshape(2, half, 128),
    )


BACK_SLOTS = 8


def expert_back_kernel(own, rows_hbm, g_hbm, ua_hbm, down_hbm, dgu_out, tail_out, gate_out, up_out, down_out, buf, gua, rows, tails, down_w, acc, down_acc, send, recv, load, load_g, load_ua, load_rows, store_dgu, store_tail):
    hidden, width = down_w.shape
    gather = Gather(own, buf, send, recv)
    loads = (
        pltpu.make_async_copy(own.at[0], buf.at[gather.me, 0], load.at[0]),
        pltpu.make_async_copy(own.at[1], buf.at[gather.me, 1], load.at[1]),
        pltpu.make_async_copy(down_hbm, down_w, load.at[2]),
    )
    for copy in loads:
        copy.start()

    def block_loads(step):
        slot, half, _ = gather.place(step)
        spot = lax.rem(step, BACK_SLOTS)
        return (
            pltpu.make_async_copy(
                g_hbm.at[slot, half], gua.at[spot, :, pl.ds(0, hidden)], load_g.at[step]
            ),
            pltpu.make_async_copy(
                ua_hbm.at[slot, half], gua.at[spot, :, pl.ds(hidden, 2 * hidden)], load_ua.at[step]
            ),
            pltpu.make_async_copy(rows_hbm.at[slot, half], rows.at[spot], load_rows.at[step]),
        )

    def block_stores(step):
        slot, half, _ = gather.place(step)
        spot = lax.rem(step, BACK_SLOTS)
        return (
            pltpu.make_async_copy(
                gua.at[spot, :, pl.ds(0, 2 * hidden)], dgu_out.at[slot, half], store_dgu.at[step]
            ),
            pltpu.make_async_copy(tails.at[spot], tail_out.at[slot, half], store_tail.at[step]),
        )

    def fetch(step, carry):
        for copy in block_loads(step):
            copy.start()
        return carry

    lax.fori_loop(0, BACK_SLOTS, fetch, 0)
    gather.begin()
    for copy in loads:
        copy.wait()

    def weight_grads(step):
        first = 4 * lax.rem(lax.div(step, 4), 2)
        spots = pl.ds(first, 4)
        places = [gather.place(step - 3 + index)[:2] for index in range(4)]

        def add(ref, index, total):
            at = pl.ds(pl.multiple_of(index * 256, 256), 256)

            @pl.when(step == 3)
            def _():
                ref[at, :] = total

            @pl.when(step > 3)
            def _():
                ref[at, :] = ref[at, :] + total

        def gate_up_tile(index, carry):
            cols = pl.ds(pl.multiple_of(index * 256, 256), 256)
            left = rows[spots, :, cols].reshape(-1, 256)
            right = gua[spots, :, : 2 * hidden].reshape(-1, 2 * hidden)
            add(acc, index, tn_dot(left, right))
            return carry

        def down_tile(index, carry):
            cols = pl.ds(pl.multiple_of(2 * hidden + index * 256, 256), 256)
            total = jnp.zeros((256, width), jnp.float32)
            for place, (slot, half) in enumerate(places):
                total = total + tn_dot(gua[first + place, :, cols], buf[slot, half])
            add(down_acc, index, total)
            return carry

        lax.fori_loop(0, width // 256, gate_up_tile, 0)
        lax.fori_loop(0, hidden // 256, down_tile, 0)

    def one(step, carry):
        slot, half = gather.arrive(step)
        spot = lax.rem(step, BACK_SLOTS)
        for copy in block_loads(step):
            copy.wait()

        lanes = lax.broadcasted_iota(jnp.int32, (buf.shape[2], 128), 1)
        tail = rows[spot, :, width:].astype(jnp.float32)
        weight = jnp.sum(jnp.where(lanes == gather.me, tail, 0.0), axis=1, keepdims=True)
        grad_act = nt_dot(buf[slot, half], down_w[...])
        gate_val = gua[spot, :, :hidden].astype(jnp.float32)
        up_val = gua[spot, :, hidden : 2 * hidden].astype(jnp.float32)
        gate_relu = jnp.maximum(gate_val, 0.0)
        grad_comb = jnp.sum(gate_relu * up_val * grad_act, axis=1, keepdims=True)
        grad_act = grad_act * weight
        grad_gate = jnp.where(gate_val > 0, grad_act * up_val, 0.0).astype(jnp.bfloat16)
        grad_up = (grad_act * gate_relu).astype(jnp.bfloat16)
        gua[spot, :, :hidden] = grad_gate
        gua[spot, :, hidden : 2 * hidden] = grad_up
        tails[spot] = jnp.where(lanes == gather.me, grad_comb, 0.0).astype(jnp.bfloat16)
        for copy in block_stores(step):
            copy.start()

        @pl.when(lax.rem(step, 4) == 3)
        def _():
            weight_grads(step)

            @pl.when(step < 8)
            def _():
                for index in range(4):
                    for copy in block_stores(step - 3 + index):
                        copy.wait()
                    for copy in block_loads(step + 5 + index):
                        copy.start()

        return carry

    lax.fori_loop(0, 16, one, 0)
    gather.finish()

    def round_gate_up(at):
        gate_out[at, :] = acc[at, :hidden].astype(jnp.bfloat16)
        up_out[at, :] = acc[at, hidden:].astype(jnp.bfloat16)

    row_loop(width, 64, round_gate_up)

    def round_down(at):
        down_out[at, :] = down_acc[at, :].astype(jnp.bfloat16)

    row_loop(hidden, 64, round_down)

    def drain(step, carry):
        for copy in block_stores(step):
            copy.wait()
        return carry

    lax.fori_loop(8, 16, drain, 0)


def expert_back(own, rows_all, gate_val, ua, down_w):
    half, columns = rows_all.shape[2:]
    hidden, width = down_w.shape
    bf = jnp.bfloat16
    return pl.pallas_call(
        expert_back_kernel,
        out_shape=(
            jax.ShapeDtypeStruct((8, 2, half, 2 * hidden), bf),
            jax.ShapeDtypeStruct((8, 2, half, 128), bf),
            jax.ShapeDtypeStruct((width, hidden), bf),
            jax.ShapeDtypeStruct((width, hidden), bf),
            jax.ShapeDtypeStruct((hidden, width), bf),
        ),
        in_specs=[ANY] * 5,
        out_specs=(ANY, ANY, VMEM, VMEM, VMEM),
        scratch_shapes=[
            pltpu.VMEM((8, 2, half, width), bf),
            pltpu.VMEM((BACK_SLOTS, half, 3 * hidden), bf),
            pltpu.VMEM((BACK_SLOTS, half, columns), bf),
            pltpu.VMEM((BACK_SLOTS, half, 128), bf),
            pltpu.VMEM((hidden, width), bf),
            pltpu.VMEM((width, 2 * hidden), jnp.float32),
            pltpu.VMEM((hidden, width), jnp.float32),
            pltpu.SemaphoreType.DMA((14,)),
            pltpu.SemaphoreType.DMA((8, 2)),
            pltpu.SemaphoreType.DMA((3,)),
        ]
        + [pltpu.SemaphoreType.DMA((16,))] * 5,
        compiler_params=pltpu.CompilerParams(
            collective_id=3, has_side_effects=True, vmem_limit_bytes=VMEM_BYTES
        ),
        name="expert_back",
    )(own, rows_all, gate_val, ua, down_w)


def expert_rows_kernel(dgu_hbm, tail_hbm, gate_hbm, up_hbm, out, dgu, tails, gate_w, up_w, mine, away, load_w, load_dgu, load_tail, *scratch):
    width, hidden = gate_w.shape
    scatter = Scatter(
        lambda place, slot, half: mine.at[place, half],
        lambda place, slot, half: away.at[place, half],
        scratch,
    )
    weights = (
        pltpu.make_async_copy(gate_hbm, gate_w, load_w.at[0]),
        pltpu.make_async_copy(up_hbm, up_w, load_w.at[1]),
    )

    def loads(step):
        slot, half, _, _ = scatter.place(step)
        spot = lax.rem(step, OUT_SLOTS)
        return (
            pltpu.make_async_copy(dgu_hbm.at[slot, half], dgu.at[spot], load_dgu.at[step]),
            pltpu.make_async_copy(tail_hbm.at[slot, half], tails.at[spot], load_tail.at[step]),
        )

    for copy in weights:
        copy.start()
    for step in (0, 1):
        for copy in loads(step):
            copy.start()
    plane_barrier(scatter.peers())
    for copy in weights:
        copy.wait()

    def one(step, carry):
        _, half, other, place = scatter.place(step)
        spot = lax.rem(step, OUT_SLOTS)
        for copy in loads(step):
            copy.wait()

        @pl.when(step < 14)
        def _():
            for copy in loads(step + 2):
                copy.start()

        total = nt_dot(dgu[spot, :, :hidden], gate_w[...]) + nt_dot(dgu[spot, :, hidden:], up_w[...])
        partial = total.astype(jnp.bfloat16)

        @pl.when(other == 1)
        def _():
            away[place, half, 0, :, :width] = partial
            away[place, half, 0, :, width:] = tails[spot]

        @pl.when(other == 0)
        def _():
            mine[place, half, 0, :, :width] = partial
            mine[place, half, 0, :, width:] = tails[spot]

        scatter.depart(step)

        @pl.when(step == 12)
        def _():
            scatter.forward()

        return carry

    lax.fori_loop(0, 16, one, 0)

    def write(half, part, rows, total):
        out[half, rows, :] = total

    scatter.finish(write)
    scatter.drain()


def expert_rows(dgu, tails, gate_w, up_w):
    half = dgu.shape[2]
    width, hidden = gate_w.shape
    columns = width + 128
    bf = jnp.bfloat16
    return pl.pallas_call(
        expert_rows_kernel,
        out_shape=jax.ShapeDtypeStruct((2, half, columns), jnp.float32),
        in_specs=[ANY] * 4,
        out_specs=VMEM,
        scratch_shapes=[
            pltpu.VMEM((OUT_SLOTS, half, 2 * hidden), bf),
            pltpu.VMEM((OUT_SLOTS, half, 128), bf),
            pltpu.VMEM((width, hidden), bf),
            pltpu.VMEM((width, hidden), bf),
            pltpu.VMEM((4, 2, 1, half, columns), bf),
            pltpu.VMEM((4, 2, 1, half, columns), bf),
            pltpu.SemaphoreType.DMA((2,)),
            pltpu.SemaphoreType.DMA((16,)),
            pltpu.SemaphoreType.DMA((16,)),
        ]
        + scatter_scratch(1, half, columns),
        compiler_params=pltpu.CompilerParams(
            collective_id=4, has_side_effects=True, vmem_limit_bytes=VMEM_BYTES
        ),
        name="expert_rows",
    )(dgu, tails, gate_w, up_w)


def line_gather_kernel(own, everything, stage, send, recv, local):
    line = line_peers()
    into = pltpu.make_async_copy(own, stage, local.at[0])
    into.start()
    full_barrier((), line[1:])

    def copy(turn, block):
        return line_remote(
            own, everything.at[block], send.at[turn - 1], recv.at[turn - 1], line[turn]
        )

    for turn in (1, 2, 3):
        copy(turn, line[0]).start()
    into.wait()
    out = pltpu.make_async_copy(stage, everything.at[line[0]], local.at[1])
    out.start()
    out.wait()
    for turn in (1, 2, 3):
        copy(turn, line[turn]).wait()


def line_gather(own):
    return pl.pallas_call(
        line_gather_kernel,
        out_shape=jax.ShapeDtypeStruct((4, *own.shape), own.dtype),
        in_specs=[ANY],
        out_specs=ANY,
        scratch_shapes=[
            pltpu.VMEM(own.shape, own.dtype),
            pltpu.SemaphoreType.DMA((3,)),
            pltpu.SemaphoreType.DMA((3,)),
            pltpu.SemaphoreType.DMA((2,)),
        ],
        compiler_params=pltpu.CompilerParams(
            collective_id=7, has_side_effects=True, vmem_limit_bytes=VMEM_BYTES
        ),
        name="line_gather",
    )(own)


class DenseGather:
    def __init__(self, own, everything, send, recv, local, lined):
        self.own, self.everything, self.send, self.recv = own, everything, send, recv
        self.lined = lined
        self.me, self.sib, self.xn, self.yn = plane_peers()
        self.diag = self.xn + self.yn - self.me
        self.line = line_peers()
        if lined:
            self.home = pltpu.make_async_copy(own, everything.at[:, self.me], local)
        else:
            self.home = pltpu.make_async_copy(own, everything.at[self.line[0], self.me], local)
        self.started = []

    def copy(self, index, own, slot, turn, peer, make):
        target = self.everything.at[self.line[turn], slot]
        return make(
            (self.own.at[self.line[turn]] if self.lined else self.own) if own else target,
            target,
            self.send.at[index],
            self.recv.at[self.line[turn], slot],
            peer,
        )

    def put(self, own, slot, turn, peer, make=remote):
        what = (len(self.started), own, slot, turn, peer, make)
        self.started.append(what)
        self.copy(*what).start()

    def pass_on(self, slot, turn, peer):
        self.put(False, slot, turn, peer)

    def wait(self, slot, turn):
        ref = self.everything.at[self.line[turn], slot]
        remote(ref, ref, self.send.at[0], self.recv.at[self.line[turn], slot], self.sib).wait_recv()

    def start_line(self):
        for turn in (1, 2, 3):
            self.put(True, self.me, 0, self.line[turn], line_remote)

    def start_plane(self):
        for turn in (0, 1, 2, 3) if self.lined else (0,):
            for peer in (self.xn, self.yn, self.sib):
                self.put(True, self.me, turn, peer)

    def near(self, turn):
        self.wait(self.xn, turn)
        if turn % 2 == 0:
            self.pass_on(self.xn, turn, self.yn)
        self.pass_on(self.xn, turn, self.sib)
        self.wait(self.yn, turn)
        if turn % 2 == 1:
            self.pass_on(self.yn, turn, self.xn)
        self.pass_on(self.yn, turn, self.sib)

    def from_line(self, turn):
        self.wait(self.me, turn)
        for peer in (self.xn, self.yn, self.sib):
            self.pass_on(self.me, turn, peer)

    def far(self, turn):
        self.wait(self.diag, turn)
        self.pass_on(self.diag, turn, self.sib)

    def arrived(self):
        for turn in (0, 1, 2, 3):
            for slot in (self.me, self.xn, self.yn, self.diag):
                self.wait(slot + self.sib - self.me, turn)
        self.home.wait()

    def finish(self):
        for what in self.started:
            self.copy(*what).wait_send()


def gather_scratch(rows, columns):
    return [
        pltpu.VMEM((4, 8, rows, columns), jnp.bfloat16),
        pltpu.SemaphoreType.DMA((32,)),
        pltpu.SemaphoreType.DMA((4, 8)),
        pltpu.SemaphoreType.DMA((2,)),
    ]


class LineScatter:
    def __init__(self, sums, scratch):
        self.sums = sums
        self.other, self.send, self.recv = scratch
        self.line = line_peers()

    def copy(self, turn):
        target = self.line[turn]
        return line_remote(
            self.sums(target),
            self.other.at[turn - 1],
            self.send.at[turn - 1],
            self.recv.at[turn - 1],
            target,
        )

    def begin(self):
        for turn in (1, 2, 3):
            self.copy(turn).start()

    def finish(self, outs):
        rows_all = self.other.shape[1]
        for turn in (1, 2, 3):
            self.copy(turn).wait_recv()
        own = self.sums(self.line[0])

        def one(index, carry):
            rows = pl.ds(pl.multiple_of(index * 16, 16), 16)
            total = own[rows, :].astype(jnp.float32)
            for turn in (0, 1, 2):
                total = total + self.other[turn, rows, :].astype(jnp.float32)
            first = 0
            for out, place, columns in outs:
                out[rows, place : place + columns] = total[:, first : first + columns]
                first += columns
            return carry

        lax.fori_loop(0, rows_all // 16, one, 0)
        for turn in (1, 2, 3):
            self.copy(turn).wait_send()


class DenseScatter:
    def __init__(self, total, scratch):
        def block(place, slot, half):
            return total.at[half, :, slot]

        self.plane = Scatter(block, block, scratch[:SCATTER_REFS])
        me = self.plane.me
        self.line = LineScatter(
            lambda line: total.at[lax.div(line, 2), lax.rem(line, 2), me], scratch[SCATTER_REFS:]
        )

    def begin(self):
        self.plane.send_theirs()

    def own(self):
        self.plane.send_mine()

    def forward(self):
        self.plane.forward()

    def turn(self):
        def write(half, part, rows, total):
            home = self.plane.mine(0, half)
            home[part, rows, :] = total.astype(home.dtype)

        self.plane.finish(write)
        self.line.begin()

    def finish(self, outs):
        self.line.finish(outs)
        self.plane.drain()


DENSE_REFS = SCATTER_REFS + 3


def dense_scratch(rows, columns):
    return scatter_scratch(2, rows, columns) + [
        pltpu.VMEM((3, rows, columns), jnp.bfloat16),
        pltpu.SemaphoreType.DMA((3,)),
        pltpu.SemaphoreType.DMA((3,)),
    ]


def rope(values, cosine, sine):
    return values * cosine + pltpu.roll(values, HD // 2, 1) * sine


def gain_rows(misc, out):
    for index in range(out.shape[1] // 128):
        rows = pl.ds(index * 128, 128)
        out[:, rows] = jnp.transpose(misc(rows).astype(jnp.float32))


def inverse_rms(values):
    return lax.rsqrt(jnp.mean(values * values, axis=1, keepdims=True) + EPS)


def row_loop(count, chunk, body):
    def one(index, carry):
        body(pl.ds(pl.multiple_of(index * chunk, chunk), chunk))
        return carry

    lax.fori_loop(0, count // chunk, one, 0)


def tile_loop(count, tile, body):
    row_loop(count, tile, body)


ROW_CHUNK = 16
TILE = 256


def attend_kernel(q_heads, kv_heads, experts, tokens, qkv_own, out_own, cosine, sine, segments, routes, rows_out, resid, heads, mixed, lse, prob, bias, picked, qkv_hbm, out_hbm, gains, hidden, *scratch):
    num_rows, width = tokens.shape
    group = q_heads // kv_heads
    qkv_cols = (q_heads + 2 * kv_heads) * HD
    qkv_w, out_w = scratch[0], scratch[4]
    first = DenseGather(qkv_own, qkv_w, scratch[1], scratch[2], scratch[3].at[0], True)
    second = DenseGather(out_own, out_w, scratch[5], scratch[6], scratch[7].at[0], False)
    stores = (
        pltpu.make_async_copy(qkv_w, qkv_hbm, scratch[3].at[1]),
        pltpu.make_async_copy(out_w, out_hbm, scratch[7].at[1]),
    )
    for gather in (first, second):
        gather.home.start()
    full_barrier((first.sib, first.xn, first.yn), first.line[1:])
    first.start_plane()
    second.start_line()
    picked[...] = jnp.zeros_like(picked)
    lane_ids = lax.broadcasted_iota(jnp.int32, picked.shape, 1)
    for index in range(routes.shape[1]):
        picked[...] = picked[...] + jnp.where(lane_ids == routes[:, index : index + 1], 1.0, 0.0)
    seg_row = segments[0:1, :]
    for index in range(num_rows // 128):
        rows = slice(index * 128, (index + 1) * 128)
        wide = jnp.broadcast_to(seg_row[:, rows].astype(jnp.float32), (128, 128))
        seg_col = jnp.transpose(wide)[:, 0:1].astype(jnp.int32)
        keys = lax.broadcasted_iota(jnp.int32, (128, num_rows), 1)
        queries = lax.broadcasted_iota(jnp.int32, (128, num_rows), 0) + index * 128
        visible = (keys <= queries) & ((seg_row == 0) | (seg_row == seg_col))
        bias[rows, :] = jnp.where(visible, 0.0, NEG_BIG)
    for turn in (0, 1, 2, 3):
        first.near(turn)
        if turn > 0:
            first.far(turn - 1)
    first.far(3)
    second.start_plane()
    first.arrived()
    stores[0].start()

    def flat(ref, cols):
        return ref[:, :, :, cols].reshape(-1, cols.size)

    misc = flat(qkv_w, pl.ds(qkv_cols, 128))
    for index in range(width // 128):
        rows = slice(index * 128, (index + 1) * 128)
        gains[:, rows] = jnp.transpose(misc[rows, :].astype(jnp.float32))

    def norm_one(rows):
        value = tokens[rows, :].astype(jnp.float32)
        normed = value * inverse_rms(value)
        hidden[rows, :] = (normed * gains[experts : experts + 1, :]).astype(jnp.bfloat16)

    row_loop(num_rows, ROW_CHUNK, norm_one)

    for turn in (1, 2, 3):
        second.from_line(turn)

    def project(index, carry):
        cols = pl.ds(pl.multiple_of(index * TILE, TILE), TILE)
        raw = nn_dot(hidden[...], flat(qkv_w, cols))
        turned = index < (q_heads + kv_heads) // 2
        cos_now = jnp.where(turned, cosine[...], 1.0)
        sin_now = jnp.where(turned, sine[...], 0.0)
        for part in (0, 1):
            value = rope(raw[:, part * HD : (part + 1) * HD], cos_now, sin_now)
            heads[2 * index + part] = value.astype(jnp.bfloat16)
        return carry

    lax.fori_loop(0, (q_heads + 2 * kv_heads) // 2, project, 0)
    second.near(0)
    lse[...] = jnp.zeros_like(lse)

    def head_step(head, carry):
        kv_head = q_heads + lax.div(head, group)
        cols = pl.ds(pl.multiple_of(head * HD, HD), HD)
        for first, keys in ((0, PROMPT), (PROMPT, num_rows)):
            rows = pl.ds(first, keys - first)
            query = heads[head, rows, :]
            score = nt_dot(query, heads[kv_head, :keys, :]) * HD ** (-0.5) + bias[rows, :keys]
            top = jnp.max(score, axis=1, keepdims=True)
            weight = jnp.exp(score - top)
            total = jnp.sum(weight, axis=1, keepdims=True)
            value = nn_dot(weight.astype(jnp.bfloat16), heads[kv_head + kv_heads, :keys, :])
            mixed[rows, cols] = (value / total).astype(jnp.bfloat16)
            lanes = lax.broadcasted_iota(jnp.int32, (keys - first, 128), 1)
            lse[rows, :] = jnp.where(lanes == head, top + jnp.log(total), lse[rows, :])

        for turn in (1, 2, 3):

            @pl.when(head == 2 * turn - 1)
            def _():
                second.near(turn)

        for turn in (0, 1, 2):

            @pl.when(head == 6 + turn)
            def _():
                second.far(turn)

        return carry

    lax.fori_loop(0, q_heads, head_step, 0)

    second.far(3)
    second.arrived()
    stores[1].start()

    def out_tile(cols):
        resid[:, cols] = tokens[:, cols].astype(jnp.float32) + nn_dot(mixed[...], flat(out_w, cols))

    tile_loop(width, TILE, out_tile)

    def norm_two(rows):
        value = resid[rows, :]
        normed = value * inverse_rms(value)
        rows_out[rows, :width] = (normed * gains[experts + 1 : experts + 2, :]).astype(jnp.bfloat16)

    row_loop(num_rows, ROW_CHUNK, norm_two)
    logits = nn_dot(rows_out[:, :width], flat(qkv_w, pl.ds(qkv_cols, 128)))
    lanes = lax.broadcasted_iota(jnp.int32, logits.shape, 1)
    logits = jnp.where(lanes < experts, logits, NEG_BIG)
    weight = jnp.exp(logits - jnp.max(logits, axis=1, keepdims=True))
    value = weight / jnp.sum(weight, axis=1, keepdims=True)
    prob[...] = value
    chosen = value * picked[...]
    rows_out[:, width:] = (chosen / jnp.sum(chosen, axis=1, keepdims=True)).astype(jnp.bfloat16)
    for gather, store in zip((first, second), stores):
        store.wait()
        gather.finish()


def attend(tokens, qkv_own, out_own, cosine, sine, segments, routes, q_heads, kv_heads, experts):
    num_rows, width = tokens.shape
    bf = jnp.bfloat16
    all_heads = q_heads + 2 * kv_heads
    return pl.pallas_call(
        functools.partial(attend_kernel, q_heads, kv_heads, experts),
        out_shape=(
            jax.ShapeDtypeStruct((num_rows, width + 128), bf),
            jax.ShapeDtypeStruct((num_rows, width), jnp.float32),
            jax.ShapeDtypeStruct((all_heads, num_rows, HD), bf),
            jax.ShapeDtypeStruct((num_rows, q_heads * HD), bf),
            jax.ShapeDtypeStruct((num_rows, 128), jnp.float32),
            jax.ShapeDtypeStruct((num_rows, 128), jnp.float32),
            jax.ShapeDtypeStruct((num_rows, num_rows), jnp.float32),
            jax.ShapeDtypeStruct((num_rows, 128), jnp.float32),
            jax.ShapeDtypeStruct((4, 8, *qkv_own.shape[1:]), bf),
            jax.ShapeDtypeStruct((4, 8, *out_own.shape), bf),
        ),
        in_specs=[VMEM, ANY, ANY] + [VMEM] * 4,
        out_specs=(VMEM,) * 8 + (ANY, ANY),
        scratch_shapes=[
            pltpu.VMEM((128, width), jnp.float32),
            pltpu.VMEM((num_rows, width), bf),
        ]
        + gather_scratch(*qkv_own.shape[1:])
        + gather_scratch(*out_own.shape),
        compiler_params=pltpu.CompilerParams(
            collective_id=5, has_side_effects=True, vmem_limit_bytes=VMEM_BYTES
        ),
        name="attend",
    )(tokens, qkv_own, out_own, cosine, sine, segments.reshape(1, num_rows), routes)


def attend_back_kernel(q_heads, kv_heads, experts, back_hbm, grad_hbm, resid_hbm, rows_hbm, prob_hbm, picked_hbm, qkv_hbm, out_hbm, mixed_hbm, heads_hbm, lse_hbm, bias_hbm, cos_hbm, sin_hbm, tokens_hbm, grad_in, out_sum, q_sum, k_sum, v_sum, misc_sum, back, grad, resid, hidden_two, prob, picked, qkv_w, out_w, mixed, heads, lse, bias, cosine, sine, tokens, gains, gain_sums, grad_logit, grad_proj, grad_mixed, grad_qkv, grad_kv, hidden, load, *scratch):
    num_rows, width = tokens.shape
    group = q_heads // kv_heads
    q_cols = q_heads * HD
    k_cols = kv_heads * HD
    qkv_cols = q_cols + 2 * k_cols
    near_cols = group * HD
    bf = jnp.bfloat16
    parts, scatters = [], []
    for index in range(4):
        some = scratch[index * (1 + DENSE_REFS) : (index + 1) * (1 + DENSE_REFS)]
        parts.append(some[0])
        scatters.append(DenseScatter(some[0], some[1:]))
    out_part, near_part, rest_part, misc_part = parts
    out_scatter, near_scatter, rest_scatter, misc_scatter = scatters
    pairs = (
        (prob_hbm, prob),
        (picked_hbm, picked),
        (back_hbm, back),
        (qkv_hbm, qkv_w),
        (resid_hbm, resid),
        (grad_hbm, grad),
        (rows_hbm, hidden_two),
        (out_hbm, out_w),
        (mixed_hbm, mixed),
        (heads_hbm, heads),
        (lse_hbm, lse),
        (bias_hbm, bias),
        (cos_hbm, cosine),
        (sin_hbm, sine),
        (tokens_hbm, tokens),
    )
    loads = [pltpu.make_async_copy(src, dst, load.at[i]) for i, (src, dst) in enumerate(pairs)]
    for copy in loads:
        copy.start()
    full_barrier(out_scatter.plane.peers(), out_scatter.line.line[1:])
    for copy in loads[:3]:
        copy.wait()
    gain_sums[...] = jnp.zeros_like(gain_sums)

    def router_rows(rows):
        value = prob[rows, :]
        chosen = value * picked[rows, :]
        total = jnp.sum(chosen, axis=1, keepdims=True)
        comb = chosen / total
        grad_comb = back[rows, width:]
        grad_chosen = (
            picked[rows, :] * (grad_comb - jnp.sum(grad_comb * comb, axis=1, keepdims=True)) / total
        )
        logit = value * (grad_chosen - jnp.sum(value * grad_chosen, axis=1, keepdims=True))
        grad_logit[rows, :] = logit.astype(bf)

    row_loop(num_rows, 64, router_rows)
    loads[3].wait()
    misc = qkv_w.at[:, pl.ds(qkv_cols, 128)]
    gain_rows(lambda rows: misc[rows, :], gains)
    lanes = lax.broadcasted_iota(jnp.int32, (TILE, 128), 1)

    def hidden_tile(cols):
        router = jnp.where(lanes < experts, misc[cols, :], jnp.zeros((), bf))
        back[:, cols] = back[:, cols] + nt_dot(grad_logit[...], router)

    tile_loop(width, TILE, hidden_tile)
    for copy in loads[4:]:
        copy.wait()

    def fold(values):
        return jnp.sum(values.reshape(-1, 8, width), axis=0)

    def norm_two(rows):
        value = resid[rows, :]
        inverse = inverse_rms(value)
        normed = value * inverse
        grad_hidden = back[rows, :width]
        gain_sums[8:16, :] = gain_sums[8:16, :] + fold(grad_hidden * normed)
        grad_norm = grad_hidden * gains[experts + 1 : experts + 2, :]
        mean = jnp.mean(grad_norm * normed, axis=1, keepdims=True)
        total = grad[rows, :] + inverse * (grad_norm - normed * mean)
        grad[rows, :] = total
        grad_proj[rows, :] = total.astype(bf)

    row_loop(num_rows, ROW_CHUNK, norm_two)

    def weight_loop(part, left, right):
        _, _, blocks, rows_each, columns = part.shape
        span = blocks * rows_each

        def one(line, carry):
            cols = pl.ds(pl.multiple_of(line * span, 128), span)
            total = tn_dot(left[:, cols], right[...]).astype(bf)
            part[lax.div(line, 2), lax.rem(line, 2)] = total.reshape(blocks, rows_each, columns)
            return carry

        lax.fori_loop(0, 4, one, 0)

    weight_loop(out_part, mixed, grad_proj)
    out_scatter.begin()

    def mixed_tile(cols):
        grad_mixed[:, cols] = nt_dot(
            grad_proj[...], out_w[cols, :]
        ).astype(bf)

    tile_loop(q_cols, TILE, mixed_tile)
    out_scatter.own()

    def norm_one(rows):
        value = tokens[rows, :].astype(jnp.float32)
        normed = value * inverse_rms(value)
        hidden[rows, :] = (normed * gains[experts : experts + 1, :]).astype(bf)

    row_loop(num_rows, ROW_CHUNK, norm_one)
    scale = HD ** (-0.5)

    def head_step(head, carry):
        kv_head = lax.div(head, group)
        cols = pl.ds(pl.multiple_of(head * HD, HD), HD)

        @pl.when(lax.rem(head, group) == 0)
        def _():
            grad_kv[...] = jnp.zeros_like(grad_kv)

        for first, keys in ((0, PROMPT), (PROMPT, num_rows)):
            rows = pl.ds(first, keys - first)
            key = heads[q_heads + kv_head, :keys, :]
            query = heads[head, rows, :]
            up = grad_mixed[rows, cols]
            lane = lax.broadcasted_iota(jnp.int32, (keys - first, 128), 1)
            total = jnp.sum(jnp.where(lane == head, lse[rows, :], 0.0), axis=1, keepdims=True)
            weight = jnp.exp(nt_dot(query, key) * scale + bias[rows, :keys] - total)
            grad_weight = nt_dot(up, heads[q_heads + kv_heads + kv_head, :keys, :])
            delta = jnp.sum(weight * grad_weight, axis=1, keepdims=True)
            score = (weight * (grad_weight - delta)).astype(bf)
            grad_kv[1, :keys, :] = grad_kv[1, :keys, :] + tn_dot(weight.astype(bf), up)
            grad_kv[0, :keys, :] = grad_kv[0, :keys, :] + tn_dot(score, query) * scale
            value = rope(nn_dot(score, key) * scale, cosine[rows, :], -sine[rows, :])
            grad_qkv[rows, cols] = value.astype(bf)

        @pl.when(lax.rem(head, group) == group - 1)
        def _():
            key_cols = pl.ds(pl.multiple_of(q_cols + kv_head * HD, HD), HD)
            value_cols = pl.ds(pl.multiple_of(q_cols + (kv_heads + kv_head) * HD, HD), HD)
            grad_qkv[:, key_cols] = rope(grad_kv[0], cosine[...], -sine[...]).astype(bf)
            grad_qkv[:, value_cols] = grad_kv[1].astype(bf)

        @pl.when(head == 2)
        def _():
            out_scatter.forward()

        @pl.when(head == group - 1)
        def _():
            weight_loop(near_part, hidden, grad_qkv.at[:, pl.ds(0, near_cols)])
            near_scatter.begin()

        @pl.when(head == group)
        def _():
            near_scatter.own()

        @pl.when(head == group + 1)
        def _():
            out_scatter.turn()

        @pl.when(head == group + 3)
        def _():
            near_scatter.forward()

        return carry

    lax.fori_loop(0, q_heads, head_step, 0)
    weight_loop(rest_part, hidden, grad_qkv.at[:, pl.ds(near_cols, qkv_cols - near_cols)])
    rest_scatter.begin()
    near_scatter.turn()

    def hidden_back_tile(cols):
        back[:, cols] = nt_dot(grad_qkv[...], qkv_w[cols, pl.ds(0, qkv_cols)])

    tile_loop(width // 2, TILE, hidden_back_tile)
    rest_scatter.own()

    def late_tile(index, carry):
        hidden_back_tile(pl.ds(pl.multiple_of(width // 2 + index * TILE, TILE), TILE))
        return carry

    lax.fori_loop(0, width // 2 // TILE, late_tile, 0)

    def last_rows(rows):
        value = tokens[rows, :].astype(jnp.float32)
        inverse = inverse_rms(value)
        normed = value * inverse
        grad_hidden = back[rows, :width]
        gain_sums[0:8, :] = gain_sums[0:8, :] + fold(grad_hidden * normed)
        grad_norm = grad_hidden * gains[experts : experts + 1, :]
        mean = jnp.mean(grad_norm * normed, axis=1, keepdims=True)
        grad[rows, :] = grad[rows, :] + inverse * (grad_norm - normed * mean)

    row_loop(num_rows, ROW_CHUNK, last_rows)
    rest_scatter.forward()
    store = pltpu.make_async_copy(grad, grad_in, load.at[0])
    store.start()
    gains[0:16, :] = gain_sums[...]
    _, _, blocks, rows_each, _ = misc_part.shape
    span = blocks * rows_each

    def misc_line(line, carry):
        cols = pl.ds(pl.multiple_of(line * span, 128), span)
        router = tn_dot(hidden_two[:, cols], grad_logit[...])
        one = jnp.sum(gains[0:8, cols], axis=0, keepdims=True)
        two = jnp.sum(gains[8:16, cols], axis=0, keepdims=True)
        place = lax.broadcasted_iota(jnp.int32, (128, span), 0)
        block = jnp.where(place == experts, one, jnp.where(place == experts + 1, two, 0.0))
        total = (router + jnp.transpose(block)).astype(bf)
        misc_part[lax.div(line, 2), lax.rem(line, 2)] = total.reshape(blocks, rows_each, 128)
        return carry

    lax.fori_loop(0, 4, misc_line, 0)
    misc_scatter.begin()
    misc_scatter.own()
    rest_scatter.turn()
    misc_scatter.forward()
    misc_scatter.turn()
    out_scatter.finish(((out_sum, 0, width),))
    near_scatter.finish(((q_sum, 0, near_cols),))
    rest_scatter.finish(
        ((q_sum, near_cols, q_cols - near_cols), (k_sum, 0, k_cols), (v_sum, 0, k_cols))
    )
    misc_scatter.finish(((misc_sum, 0, 128),))
    store.wait()


def attend_back(back, grad, resid, rows_own, prob, picked, qkv_w, out_w, mixed, heads, lse, bias, cosine, sine, tokens, q_heads, kv_heads, experts):
    num_rows, width = tokens.shape
    bf = jnp.bfloat16
    arrays = (back, grad, resid, rows_own, prob, picked, qkv_w, out_w, mixed, heads, lse, bias, cosine, sine, tokens)
    k_cols = kv_heads * HD
    q_cols = q_heads * HD
    qkv_cols = q_cols + 2 * k_cols
    near_cols = q_cols // kv_heads
    block_rows = width // 32
    scratch = []
    for columns in (width, near_cols, qkv_cols - near_cols, 128):
        scratch += [pltpu.VMEM((2, 2, 8, block_rows, columns), bf)]
        scratch += dense_scratch(block_rows, columns)
    return pl.pallas_call(
        functools.partial(attend_back_kernel, q_heads, kv_heads, experts),
        out_shape=(jax.ShapeDtypeStruct((num_rows, width), jnp.float32),)
        + tuple(
            jax.ShapeDtypeStruct((block_rows, columns), jnp.float32)
            for columns in (width, q_cols, k_cols, k_cols, 128)
        ),
        in_specs=[ANY] * len(arrays),
        out_specs=(ANY,) + (VMEM,) * 5,
        scratch_shapes=[pltpu.VMEM(array.shape, array.dtype) for array in arrays]
        + [
            pltpu.VMEM((128, width), jnp.float32),
            pltpu.VMEM((16, width), jnp.float32),
            pltpu.VMEM((num_rows, 128), bf),
            pltpu.VMEM((num_rows, width), bf),
            pltpu.VMEM((num_rows, q_cols), bf),
            pltpu.VMEM((num_rows, qkv_cols), bf),
            pltpu.VMEM((2, num_rows, HD), jnp.float32),
            pltpu.VMEM((num_rows, width), bf),
            pltpu.SemaphoreType.DMA((len(arrays),)),
        ]
        + scratch,
        compiler_params=pltpu.CompilerParams(
            collective_id=6, has_side_effects=True, vmem_limit_bytes=67043328
        ),
        name="attend_back",
    )(*arrays)


def body_plane(
    tokens,
    targets,
    valid_count,
    segments,
    routes,
    gain_attn,
    w_query,
    w_key,
    w_value,
    w_out,
    gain_moe,
    w_router,
    w_gate,
    w_up,
    w_down,
):
    bf = jnp.bfloat16
    num_rows, width = tokens.shape
    half = num_rows // 2
    q_cols, k_cols = w_query.shape[1], w_key.shape[1]
    num_experts = w_router.shape[1]
    num_heads = q_cols // HD
    kv_heads = k_cols // HD
    pad_cols = 128 - 2 - num_experts
    qkv_own = jnp.concatenate(
        [
            w_query,
            w_key,
            w_value,
            w_router,
            gain_attn[:, None],
            gain_moe[:, None],
            jnp.zeros((gain_attn.shape[0], pad_cols), bf),
        ],
        axis=1,
    )
    qkv_line, w_gate, w_up = lax.optimization_barrier((line_gather(qkv_own), w_gate, w_up))
    gate_w = lax.all_gather(w_gate, "dp", axis=1, tiled=True)[0]
    up_w = lax.all_gather(w_up, "dp", axis=1, tiled=True)[0]
    tok_pos = positions(segments)
    freq = THETA ** (-2.0 * jnp.arange(HD // 2, dtype=jnp.float32) / HD)
    angle = tok_pos.astype(jnp.float32)[:, None] * freq[None, :]
    cosine, sine_part = jnp.cos(angle), jnp.sin(angle)
    cosine = jnp.concatenate([cosine, cosine], axis=1)
    sine = jnp.concatenate([-sine_part, sine_part], axis=1)
    rows_own, resid_mid, heads, mixed, lse, prob, bias, picked, qkv_w, out_w = attend(
        tokens, qkv_line, w_out, cosine, sine, segments, routes, num_heads, kv_heads, num_experts
    )
    rows_all, gate_val, down_w = expert_in(
        rows_own.reshape(2, half, width + 128), gate_w, w_down[0]
    )
    down_w = down_w.reshape(-1, width)
    total_rows = num_rows * lax.axis_size(("dp", "exp"))
    global_row = lax.axis_index(("dp", "exp")) * num_rows + jnp.arange(num_rows, dtype=jnp.int32)
    loss_scale = total_rows / valid_count[0].astype(jnp.float32)
    scales = jnp.broadcast_to(
        jnp.where(global_row < valid_count[0], loss_scale, 0.0)[:, None], (num_rows, 128)
    )
    layer_out, grad_out, grad_out_b, ua = expert_out(
        rows_all, gate_val, up_w, down_w, resid_mid, targets, scales
    )
    layer_out = layer_out.reshape(num_rows, width)
    dgu, tails, gate_part, up_part, down_part = expert_back(
        grad_out_b, rows_all, gate_val, ua, down_w
    )
    back = expert_rows(dgu, tails, gate_w, up_w)
    expert_sums = tuple(
        lax.psum_scatter(grad[None], "dp", scatter_dimension=1, tiled=True).astype(jnp.float32)
        for grad in (gate_part, up_part, down_part)
    )
    grad_in, out_sum, q_sum, k_sum, v_sum, misc_sum = attend_back(
        back.reshape(num_rows, width + 128),
        grad_out.reshape(num_rows, width),
        resid_mid,
        rows_own,
        prob,
        picked,
        qkv_w.reshape(width, -1),
        out_w.reshape(q_cols, width),
        mixed,
        heads,
        lse,
        bias,
        cosine,
        sine,
        tokens,
        num_heads,
        kv_heads,
        num_experts,
    )
    return (
        layer_out,
        grad_in,
        misc_sum[:, num_experts],
        q_sum,
        k_sum,
        v_sum,
        out_sum,
        misc_sum[:, num_experts + 1],
        misc_sum[:, :num_experts],
        *expert_sums,
    )


def solution(mesh):
    in_specs = (
        P(("dp", "exp"), None),
        P(("dp", "exp"), None),
        P(),
        P(("dp", "exp")),
        P(("dp", "exp"), None),
        P(("dp", "exp")),
        P(("dp", "exp"), None),
        P(("dp", "exp"), None),
        P(("dp", "exp"), None),
        P(("dp", "exp"), None),
        P(("dp", "exp")),
        P(("dp", "exp"), None),
        P("exp", "dp", None),
        P("exp", "dp", None),
        P("exp", "dp", None),
    )
    out_specs = (
        P(("dp", "exp"), None),
        P(("dp", "exp"), None),
        P(("dp", "exp")),
        P(("dp", "exp"), None),
        P(("dp", "exp"), None),
        P(("dp", "exp"), None),
        P(("dp", "exp"), None),
        P(("dp", "exp")),
        P(("dp", "exp"), None),
        P("exp", "dp", None),
        P("exp", "dp", None),
        P("exp", "dp", None),
    )
    body = body_plane if (mesh.shape["dp"], mesh.shape["exp"]) == (4, 8) else body_general
    return jax.shard_map(body, mesh=mesh, in_specs=in_specs, out_specs=out_specs, check_vma=False)
```

```python
import functools

import jax
import jax.numpy as jnp
from jax import lax
from jax.experimental import pallas as pl
from jax.experimental.pallas import tpu as pltpu
from jax.sharding import PartitionSpec as P

HD = 128
PROMPT = 256
NCONT = 2


EPS = 1e-06
THETA = 10000.0
HIGH = lax.Precision.HIGHEST
NEG_BIG = -1e30


def positions(segments):
    count_rows = segments.shape[0]
    row_ids = jnp.arange(count_rows, dtype=jnp.int32)
    labels = jnp.arange(NCONT + 1, dtype=jnp.int32)
    member = segments[:, None] == labels[None, :]
    first_row = jnp.min(jnp.where(member, row_ids[:, None], count_rows), axis=0)
    start_row = jnp.sum(jnp.where(member, first_row[None, :], 0), axis=1)
    return jnp.where(segments == 0, row_ids, PROMPT + row_ids - start_row)


def key_mask(segments):
    row_ids = jnp.arange(segments.shape[0], dtype=jnp.int32)
    causal = row_ids[None, :] <= row_ids[:, None]
    visible = (segments[None, :] == 0) | (segments[None, :] == segments[:, None])
    return causal & visible


def rotate(values, pos_rows, sign_value):
    half_size = HD // 2
    freq = THETA ** (-2.0 * jnp.arange(half_size, dtype=jnp.float32) / HD)
    angle = pos_rows.astype(jnp.float32)[:, None] * freq[None, :]
    cosine = jnp.cos(angle)[:, None, :]
    sine_part = sign_value * jnp.sin(angle)[:, None, :]
    first_half = values[..., :half_size]
    second = values[..., half_size:]
    return jnp.concatenate(
        [first_half * cosine - second * sine_part, second * cosine + first_half * sine_part],
        axis=-1,
    )


def attention_scores(query_b, key_b, allowed):
    logits = jnp.einsum(
        "qkgd,pkd->kgqp", query_b, key_b, preferred_element_type=jnp.float32
    ) * HD ** (-0.5)
    return jnp.where(allowed[None, None], logits, NEG_BIG)


def expert_gates(rows_in, gate_w, up_w):
    gate_val = jnp.einsum("sacd,adf->sacf", rows_in, gate_w, preferred_element_type=jnp.float32)
    up_val = jnp.einsum("sacd,adf->sacf", rows_in, up_w, preferred_element_type=jnp.float32)
    return (gate_val, up_val)


def body_general(
    tokens,
    targets,
    valid_count,
    segments,
    routes,
    gain_attn,
    w_query,
    w_key,
    w_value,
    w_out,
    gain_moe,
    w_router,
    w_gate,
    w_up,
    w_down,
):
    gain_one, query_w, key_w, value_w, out_w, gain_two, router_w = (
        lax.all_gather(gain_attn, ("dp", "exp"), axis=0, tiled=True),
        lax.all_gather(w_query, ("dp", "exp"), axis=0, tiled=True),
        lax.all_gather(w_key, ("dp", "exp"), axis=0, tiled=True),
        lax.all_gather(w_value, ("dp", "exp"), axis=0, tiled=True),
        lax.all_gather(w_out, ("dp", "exp"), axis=0, tiled=True),
        lax.all_gather(gain_moe, ("dp", "exp"), axis=0, tiled=True),
        lax.all_gather(w_router, ("dp", "exp"), axis=0, tiled=True),
    )
    gate_w, up_w, down_w = (
        lax.all_gather(w_gate, "dp", axis=1, tiled=True),
        lax.all_gather(w_up, "dp", axis=1, tiled=True),
        lax.all_gather(w_down, "dp", axis=1, tiled=True),
    )
    num_rows = tokens.shape[0]
    width = tokens.shape[1]
    num_heads = query_w.shape[1] // HD
    kv_heads = key_w.shape[1] // HD
    group_size = num_heads // kv_heads
    num_experts = router_w.shape[1]
    top_count = routes.shape[1]
    exp_local = gate_w.shape[0]
    exp_ranks = lax.axis_size("exp")
    capacity = 5 * num_rows * top_count // (4 * num_experts)
    tok_pos = positions(segments)
    allowed = key_mask(segments)
    resid_in = tokens.astype(jnp.float32)
    inv_one = lax.rsqrt(jnp.mean(resid_in * resid_in, axis=-1, keepdims=True) + EPS)
    normed_one = resid_in * inv_one
    hidden_one = (normed_one * gain_one.astype(jnp.float32)).astype(jnp.bfloat16)
    query_raw = jnp.dot(hidden_one, query_w, preferred_element_type=jnp.float32)
    key_raw = jnp.dot(hidden_one, key_w, preferred_element_type=jnp.float32)
    value_b = jnp.dot(hidden_one, value_w, preferred_element_type=jnp.float32).astype(jnp.bfloat16)
    query_b = rotate(query_raw.reshape(num_rows, num_heads, HD), tok_pos, 1.0).astype(jnp.bfloat16)
    query_b = query_b.reshape(num_rows, kv_heads, group_size, HD)
    key_b = rotate(key_raw.reshape(num_rows, kv_heads, HD), tok_pos, 1.0).astype(jnp.bfloat16)
    value_h = value_b.reshape(num_rows, kv_heads, HD)
    logit_att = attention_scores(query_b, key_b, allowed)
    row_max = jnp.max(logit_att, axis=-1, keepdims=True)
    log_total = row_max + jnp.log(jnp.sum(jnp.exp(logit_att - row_max), axis=-1, keepdims=True))
    probs_b = jnp.exp(logit_att - log_total).astype(jnp.bfloat16)
    attn_vals = jnp.einsum("kgqp,pkd->qkgd", probs_b, value_h, preferred_element_type=jnp.float32)
    attn_vals = attn_vals.reshape(num_rows, num_heads * HD).astype(jnp.bfloat16)
    resid_mid = resid_in + jnp.dot(attn_vals, out_w, preferred_element_type=jnp.float32)
    inv_two = lax.rsqrt(jnp.mean(resid_mid * resid_mid, axis=-1, keepdims=True) + EPS)
    normed_two = resid_mid * inv_two
    gain_two_f = gain_two.astype(jnp.float32)
    hidden_two = (normed_two * gain_two_f).astype(jnp.bfloat16)
    router_prob = jax.nn.softmax(
        jnp.dot(hidden_two, router_w, preferred_element_type=jnp.float32), axis=-1
    )
    expert_ids = jnp.arange(num_experts, dtype=jnp.int32)
    route_hot = routes[:, :, None] == expert_ids[None, None, :]
    chosen = jnp.sum(jnp.where(route_hot, router_prob[:, None, :], 0.0), axis=-1)
    weight_sum = jnp.sum(chosen, axis=1, keepdims=True)
    combine = chosen / weight_sum
    flat_hot = route_hot.reshape(num_rows * top_count, num_experts).astype(jnp.int32)
    slot_index = jnp.sum((jnp.cumsum(flat_hot, axis=0) - flat_hot) * flat_hot, axis=1)
    dest_index = routes.reshape(-1) * capacity + slot_index
    send_shape = (exp_ranks, exp_local, capacity, width)
    send_rows = jnp.zeros((num_experts * capacity, width), jnp.bfloat16)
    send_rows = (
        send_rows.at[dest_index].set(jnp.repeat(hidden_two, top_count, axis=0)).reshape(send_shape)
    )
    gate_val, up_val = expert_gates(
        lax.all_to_all(send_rows, "exp", split_axis=0, concat_axis=0, tiled=True), gate_w, up_w
    )
    act_b = (jax.nn.relu(gate_val) * up_val).astype(jnp.bfloat16)
    out_b = jnp.einsum("sacf,afd->sacd", act_b, down_w, preferred_element_type=jnp.float32).astype(
        jnp.bfloat16
    )
    returned = lax.all_to_all(out_b, "exp", split_axis=0, concat_axis=0, tiled=True)
    route_out = returned.reshape(num_experts * capacity, width)[dest_index].reshape(
        num_rows, top_count, width
    )
    route_out_f = route_out.astype(jnp.float32)
    resid_out = resid_mid + jnp.sum(combine[:, :, None] * route_out_f, axis=1)
    layer_out = resid_out.astype(jnp.bfloat16)
    total_rows = num_rows * lax.axis_size(("dp", "exp"))
    global_row = lax.axis_index(("dp", "exp")) * num_rows + jnp.arange(num_rows, dtype=jnp.int32)
    loss_scale = total_rows / valid_count[0].astype(jnp.float32)
    grad_out = jnp.where(
        (global_row < valid_count[0])[:, None],
        (resid_out - targets.astype(jnp.float32)) * loss_scale,
        0.0,
    )
    gain_one, query_w, key_w, value_w, out_w, gain_two, router_w = (
        lax.all_gather(gain_attn, ("dp", "exp"), axis=0, tiled=True),
        lax.all_gather(w_query, ("dp", "exp"), axis=0, tiled=True),
        lax.all_gather(w_key, ("dp", "exp"), axis=0, tiled=True),
        lax.all_gather(w_value, ("dp", "exp"), axis=0, tiled=True),
        lax.all_gather(w_out, ("dp", "exp"), axis=0, tiled=True),
        lax.all_gather(gain_moe, ("dp", "exp"), axis=0, tiled=True),
        lax.all_gather(w_router, ("dp", "exp"), axis=0, tiled=True),
    )
    gain_two_f = gain_two.astype(jnp.float32)
    grad_route = (combine[:, :, None] * grad_out[:, None, :]).astype(jnp.bfloat16)
    grad_comb = jnp.sum(grad_out[:, None, :] * route_out_f, axis=-1)
    grad_send = jnp.zeros((num_experts * capacity, width), jnp.bfloat16)
    grad_send = (
        grad_send.at[dest_index]
        .set(grad_route.reshape(num_rows * top_count, width))
        .reshape(send_shape)
    )
    expert_rows, grad_recv = (
        lax.all_to_all(send_rows, "exp", split_axis=0, concat_axis=0, tiled=True),
        lax.all_to_all(grad_send, "exp", split_axis=0, concat_axis=0, tiled=True),
    )
    gate_val, up_val = expert_gates(expert_rows, gate_w, up_w)
    gate_relu = jax.nn.relu(gate_val)
    act_b = (gate_relu * up_val).astype(jnp.bfloat16)
    grad_act = jnp.einsum("sacd,afd->sacf", grad_recv, down_w, preferred_element_type=jnp.float32)
    grad_down_w = jnp.einsum("sacf,sacd->afd", act_b, grad_recv, preferred_element_type=jnp.float32)
    grad_gate_b = jnp.where(gate_val > 0, grad_act * up_val, 0.0).astype(jnp.bfloat16)
    grad_up_b = (grad_act * gate_relu).astype(jnp.bfloat16)
    grad_gate_w = jnp.einsum(
        "sacd,sacf->adf", expert_rows, grad_gate_b, preferred_element_type=jnp.float32
    )
    grad_up_w = jnp.einsum(
        "sacd,sacf->adf", expert_rows, grad_up_b, preferred_element_type=jnp.float32
    )
    grad_rows = (
        jnp.einsum("sacf,adf->sacd", grad_gate_b, gate_w, preferred_element_type=jnp.float32)
        + jnp.einsum("sacf,adf->sacd", grad_up_b, up_w, preferred_element_type=jnp.float32)
    ).astype(jnp.bfloat16)
    grad_back = lax.all_to_all(grad_rows, "exp", split_axis=0, concat_axis=0, tiled=True)
    grad_copies = grad_back.reshape(num_experts * capacity, width)[dest_index].reshape(
        num_rows, top_count, width
    )
    grad_hidden_two = jnp.sum(grad_copies.astype(jnp.float32), axis=1)
    grad_chosen = (grad_comb - jnp.sum(grad_comb * combine, axis=1, keepdims=True)) / weight_sum
    grad_prob = jnp.sum(jnp.where(route_hot, grad_chosen[:, :, None], 0.0), axis=1)
    grad_logit = router_prob * (
        grad_prob - jnp.sum(router_prob * grad_prob, axis=-1, keepdims=True)
    )
    router_f = router_w.astype(jnp.float32)
    grad_hidden_two = grad_hidden_two + jnp.einsum(
        "re,de->rd", grad_logit, router_f, precision=HIGH
    )
    grad_router = jnp.einsum(
        "rd,re->de", hidden_two.astype(jnp.float32), grad_logit, precision=HIGH
    )
    grad_gain_two = jnp.sum(grad_hidden_two * normed_two, axis=0)
    grad_norm_two = grad_hidden_two * gain_two_f
    grad_mid = grad_out + inv_two * (
        grad_norm_two - normed_two * jnp.mean(grad_norm_two * normed_two, axis=-1, keepdims=True)
    )
    grad_proj_b = grad_mid.astype(jnp.bfloat16)
    grad_out_w = jnp.einsum("rh,rd->hd", attn_vals, grad_proj_b, preferred_element_type=jnp.float32)
    grad_vals_b = jnp.einsum(
        "rd,hd->rh", grad_proj_b, out_w, preferred_element_type=jnp.float32
    ).astype(jnp.bfloat16)
    grad_vals_b = grad_vals_b.reshape(num_rows, kv_heads, group_size, HD)
    logit_att = attention_scores(query_b, key_b, allowed)
    probs = jnp.exp(logit_att - log_total)
    probs_b = probs.astype(jnp.bfloat16)
    grad_value = jnp.einsum(
        "kgqp,qkgd->pkd", probs_b, grad_vals_b, preferred_element_type=jnp.float32
    )
    grad_prob_att = jnp.einsum(
        "qkgd,pkd->kgqp", grad_vals_b, value_h, preferred_element_type=jnp.float32
    )
    delta_row = jnp.sum(probs * grad_prob_att, axis=-1, keepdims=True)
    grad_score_b = (probs * (grad_prob_att - delta_row)).astype(jnp.bfloat16)
    grad_query = jnp.einsum(
        "kgqp,pkd->qkgd", grad_score_b, key_b, preferred_element_type=jnp.float32
    ) * HD ** (-0.5)
    grad_key = jnp.einsum(
        "kgqp,qkgd->pkd", grad_score_b, query_b, preferred_element_type=jnp.float32
    ) * HD ** (-0.5)
    grad_query_b = rotate(grad_query.reshape(num_rows, num_heads, HD), tok_pos, -1.0).astype(
        jnp.bfloat16
    )
    grad_query_b = grad_query_b.reshape(num_rows, num_heads * HD)
    grad_key_b = (
        rotate(grad_key, tok_pos, -1.0).astype(jnp.bfloat16).reshape(num_rows, kv_heads * HD)
    )
    grad_value_b = grad_value.astype(jnp.bfloat16).reshape(num_rows, kv_heads * HD)
    grad_query_w = jnp.einsum(
        "rd,rh->dh", hidden_one, grad_query_b, preferred_element_type=jnp.float32
    )
    grad_key_w = jnp.einsum("rd,rh->dh", hidden_one, grad_key_b, preferred_element_type=jnp.float32)
    grad_value_w = jnp.einsum(
        "rd,rh->dh", hidden_one, grad_value_b, preferred_element_type=jnp.float32
    )
    grad_hidden_one = (
        jnp.einsum("rh,dh->rd", grad_query_b, query_w, preferred_element_type=jnp.float32)
        + jnp.einsum("rh,dh->rd", grad_key_b, key_w, preferred_element_type=jnp.float32)
        + jnp.einsum("rh,dh->rd", grad_value_b, value_w, preferred_element_type=jnp.float32)
    )
    grad_gain_one = jnp.sum(grad_hidden_one * normed_one, axis=0)
    grad_norm_one = grad_hidden_one * gain_one.astype(jnp.float32)
    grad_in = grad_mid + inv_one * (
        grad_norm_one - normed_one * jnp.mean(grad_norm_one * normed_one, axis=-1, keepdims=True)
    )
    dense_sums = (
        lax.psum_scatter(grad_gain_one, ("dp", "exp"), scatter_dimension=0, tiled=True),
        lax.psum_scatter(grad_query_w, ("dp", "exp"), scatter_dimension=0, tiled=True),
        lax.psum_scatter(grad_key_w, ("dp", "exp"), scatter_dimension=0, tiled=True),
        lax.psum_scatter(grad_value_w, ("dp", "exp"), scatter_dimension=0, tiled=True),
        lax.psum_scatter(grad_out_w, ("dp", "exp"), scatter_dimension=0, tiled=True),
        lax.psum_scatter(grad_gain_two, ("dp", "exp"), scatter_dimension=0, tiled=True),
        lax.psum_scatter(grad_router, ("dp", "exp"), scatter_dimension=0, tiled=True),
    )
    expert_sums = (
        lax.psum_scatter(
            grad_gate_w.astype(jnp.bfloat16), "dp", scatter_dimension=1, tiled=True
        ).astype(jnp.float32),
        lax.psum_scatter(
            grad_up_w.astype(jnp.bfloat16), "dp", scatter_dimension=1, tiled=True
        ).astype(jnp.float32),
        lax.psum_scatter(
            grad_down_w.astype(jnp.bfloat16), "dp", scatter_dimension=1, tiled=True
        ).astype(jnp.float32),
    )
    return (
        layer_out,
        grad_in,
        dense_sums[0],
        dense_sums[1],
        dense_sums[2],
        dense_sums[3],
        dense_sums[4],
        dense_sums[5],
        dense_sums[6],
        expert_sums[0],
        expert_sums[1],
        expert_sums[2],
    )


MESH = pl.DeviceIdType.MESH
ANY = pl.BlockSpec(memory_space=pl.ANY)
VMEM = pl.BlockSpec(memory_space=pltpu.VMEM)
VMEM_BYTES = 62 * 2**20


def nn_dot(left, right):
    return jnp.dot(left, right, preferred_element_type=jnp.float32)


def nt_dot(left, right):
    return lax.dot_general(
        left, right, (((1,), (1,)), ((), ())), preferred_element_type=jnp.float32
    )


def tn_dot(left, right):
    return lax.dot_general(
        left, right, (((0,), (0,)), ((), ())), preferred_element_type=jnp.float32
    )


def plane_peers():
    me = lax.axis_index("exp")
    core = lax.rem(me, 2)
    x_pos = lax.rem(lax.div(me, 2), 2)
    y_pos = lax.div(me, 4)
    return me, me + 1 - 2 * core, me + 2 - 4 * x_pos, me + 4 - 8 * y_pos


def remote(src, dst, send_sem, recv_sem, peer):
    return pltpu.make_async_remote_copy(
        src_ref=src,
        dst_ref=dst,
        send_sem=send_sem,
        recv_sem=recv_sem,
        device_id={"exp": peer},
        device_id_type=MESH,
    )


def plane_barrier(peers):
    barrier = pltpu.get_barrier_semaphore()
    for peer in peers:
        pl.semaphore_signal(barrier, inc=1, device_id={"exp": peer}, device_id_type=MESH)
    pl.semaphore_wait(barrier, len(peers))


def step_place(step, quad):
    odd = lax.rem(step, 2)
    last = lax.div(quad, 3)
    mid = lax.rem(lax.div(quad + 1, 2), 2)
    return mid * (1 - odd) + last, mid * odd + last


class Gather:
    def __init__(self, own, buf, send, recv):
        self.own, self.buf, self.send, self.recv = own, buf, send, recv
        self.me, self.sib, self.xn, self.yn = plane_peers()
        self.diag = self.xn + self.yn - self.me

    def own_copy(self, half, peer, sem):
        return remote(
            self.own.at[half],
            self.buf.at[self.me, half],
            self.send.at[sem],
            self.recv.at[self.me, half],
            peer,
        )

    def pass_copy(self, slot, half, peer, sem):
        return remote(
            self.buf.at[slot, half],
            self.buf.at[slot, half],
            self.send.at[sem],
            self.recv.at[slot, half],
            peer,
        )

    def own_copies(self):
        return (
            self.own_copy(0, self.xn, 0),
            self.own_copy(1, self.yn, 1),
            self.own_copy(0, self.sib, 2),
            self.own_copy(1, self.sib, 3),
            self.own_copy(1, self.xn, 4),
            self.own_copy(0, self.yn, 5),
        )

    def near_copies(self):
        return (
            self.pass_copy(self.xn, 0, self.yn, 6),
            self.pass_copy(self.yn, 1, self.xn, 7),
            self.pass_copy(self.xn, 0, self.sib, 8),
            self.pass_copy(self.yn, 1, self.sib, 9),
        )

    def late_copies(self):
        return (
            self.pass_copy(self.xn, 1, self.sib, 10),
            self.pass_copy(self.yn, 0, self.sib, 11),
        )

    def far_copies(self):
        return (
            self.pass_copy(self.diag, 0, self.sib, 12),
            self.pass_copy(self.diag, 1, self.sib, 13),
        )

    def wait_block(self, slot, half):
        self.pass_copy(slot, half, self.sib, 0).wait_recv()

    def begin(self):
        plane_barrier((self.sib, self.xn, self.yn))
        for copy in self.own_copies():
            copy.start()

    def place(self, step):
        quad = lax.div(step, 4)
        far_x, far_y = step_place(step, quad)
        odd = lax.rem(step, 2)
        third = lax.div(quad, 2) * (1 - lax.div(quad, 3))
        other = lax.div(lax.rem(step, 4), 2)
        slot = (
            self.me
            + far_x * (self.xn - self.me)
            + far_y * (self.yn - self.me)
            + other * (self.sib - self.me)
        )
        return slot, odd + third * (1 - 2 * odd), other

    def arrive(self, step):
        @pl.when(step == 4)
        def _():
            self.wait_block(self.xn, 0)
            self.wait_block(self.yn, 1)
            for copy in self.near_copies():
                copy.start()

        @pl.when(step == 8)
        def _():
            self.wait_block(self.xn, 1)
            self.wait_block(self.yn, 0)
            for copy in self.late_copies():
                copy.start()

        @pl.when(step == 12)
        def _():
            self.wait_block(self.diag, 0)
            self.wait_block(self.diag, 1)
            for copy in self.far_copies():
                copy.start()

        slot, half, other = self.place(step)

        @pl.when(other == 1)
        def _():
            self.wait_block(slot, half)

        return slot, half

    def finish(self):
        for copies in (self.own_copies(), self.near_copies(), self.late_copies(), self.far_copies()):
            for copy in copies:
                copy.wait_send()


def line_peers():
    line = lax.axis_index("dp")
    return (
        line,
        line + 1 - 2 * lax.rem(line, 2),
        line + 2 - 4 * lax.div(line, 2),
        3 - line,
    )


def line_remote(src, dst, send_sem, recv_sem, peer):
    return pltpu.make_async_remote_copy(
        src_ref=src,
        dst_ref=dst,
        send_sem=send_sem,
        recv_sem=recv_sem,
        device_id={"dp": peer},
        device_id_type=MESH,
    )


def full_barrier(plane, line):
    barrier = pltpu.get_barrier_semaphore()
    for peer in plane:
        pl.semaphore_signal(barrier, inc=1, device_id={"exp": peer}, device_id_type=MESH)
    for peer in line:
        pl.semaphore_signal(barrier, inc=1, device_id={"dp": peer}, device_id_type=MESH)
    pl.semaphore_wait(barrier, len(plane) + len(line))


def expert_in_kernel(own, gate_hbm, down_own, rows_out, gate_out, down_out, buf, gate, gate_w, down_stage, send, recv, load, store_a, store_b, line_send, line_recv):
    width = gate_w.shape[0]
    gather = Gather(own, buf, send, recv)
    line = line_peers()
    loads = (
        pltpu.make_async_copy(own.at[0], buf.at[gather.me, 0], load.at[0]),
        pltpu.make_async_copy(own.at[1], buf.at[gather.me, 1], load.at[1]),
        pltpu.make_async_copy(gate_hbm, gate_w, load.at[2]),
        pltpu.make_async_copy(down_own, down_stage, load.at[3]),
    )
    for copy in loads:
        copy.start()
    full_barrier((gather.sib, gather.xn, gather.yn), line[1:])
    for copy in gather.own_copies():
        copy.start()

    def down_copy(turn):
        return line_remote(
            down_own,
            down_out.at[line[0]],
            line_send.at[turn - 1],
            line_recv.at[turn - 1],
            line[turn],
        )

    for turn in (1, 2, 3):
        down_copy(turn).start()
    for copy in loads:
        copy.wait()
    down_store = pltpu.make_async_copy(down_stage, down_out.at[line[0]], load.at[4])
    down_store.start()

    def row_store(slot, half, step):
        return pltpu.make_async_copy(buf.at[slot, half], rows_out.at[slot, half], store_a.at[step])

    def gate_store(slot, half, step):
        return pltpu.make_async_copy(gate.at[slot, half], gate_out.at[slot, half], store_b.at[step])

    def one(step, carry):
        slot, half = gather.arrive(step)
        row_store(slot, half, step).start()
        gate[slot, half] = nn_dot(buf[slot, half, :, :width], gate_w[...]).astype(jnp.bfloat16)
        gate_store(slot, half, step).start()
        return carry

    lax.fori_loop(0, 16, one, 0)
    gather.finish()

    def drain(step, carry):
        slot, half, _ = gather.place(step)
        row_store(slot, half, step).wait()
        gate_store(slot, half, step).wait()
        return carry

    lax.fori_loop(0, 16, drain, 0)
    down_store.wait()
    for turn in (1, 2, 3):
        line_remote(
            down_own,
            down_out.at[line[turn]],
            line_send.at[turn - 1],
            line_recv.at[turn - 1],
            line[turn],
        ).wait()


def expert_in(own, gate_w, down_own):
    _, half, columns = own.shape
    width, hidden = gate_w.shape
    bf = jnp.bfloat16
    return pl.pallas_call(
        expert_in_kernel,
        out_shape=(
            jax.ShapeDtypeStruct((8, 2, half, columns), bf),
            jax.ShapeDtypeStruct((8, 2, half, hidden), bf),
            jax.ShapeDtypeStruct((4, *down_own.shape), bf),
        ),
        in_specs=[ANY] * 3,
        out_specs=(ANY, ANY, ANY),
        scratch_shapes=[
            pltpu.VMEM((8, 2, half, columns), bf),
            pltpu.VMEM((8, 2, half, hidden), bf),
            pltpu.VMEM((width, hidden), bf),
            pltpu.VMEM(down_own.shape, bf),
            pltpu.SemaphoreType.DMA((14,)),
            pltpu.SemaphoreType.DMA((8, 2)),
            pltpu.SemaphoreType.DMA((5,)),
            pltpu.SemaphoreType.DMA((16,)),
            pltpu.SemaphoreType.DMA((16,)),
            pltpu.SemaphoreType.DMA((3,)),
            pltpu.SemaphoreType.DMA((3,)),
        ],
        compiler_params=pltpu.CompilerParams(
            collective_id=1, has_side_effects=True, vmem_limit_bytes=VMEM_BYTES
        ),
        name="expert_in",
    )(own, gate_w, down_own)


def row_chunk(rows):
    return 64 if rows % 64 == 0 else 16


def add_rows(target, others):
    parts, rows_all, _ = target.shape
    chunk = row_chunk(rows_all)
    for part in range(parts):

        def one(index, carry):
            rows = pl.ds(pl.multiple_of(index * chunk, chunk), chunk)
            total = target[part, rows, :].astype(jnp.float32)
            for other in others:
                total = total + other[part, rows, :].astype(jnp.float32)
            target[part, rows, :] = total.astype(target.dtype)
            return carry

        lax.fori_loop(0, rows_all // chunk, one, 0)


class Scatter:
    def __init__(self, mine, theirs, scratch):
        self.mine_of, self.theirs = mine, theirs
        self.side, self.relay, self.final = scratch[:3]
        self.send, self.side_sem, self.relay_sem, self.final_sem = scratch[3:]
        self.me, self.sib, self.xn, self.yn = plane_peers()

    def mine(self, place, half):
        slot = (self.me, self.xn, self.yn, self.xn + self.yn - self.me)[place]
        return self.mine_of(place, slot, half)

    def peers(self):
        return self.sib, self.xn, self.yn

    def place(self, step):
        quad = lax.div(step, 4)
        odd = lax.div(lax.rem(step, 4), 2)
        far_x, far_y = step_place(odd, 3 - quad)
        third = lax.div(quad, 2) * (1 - lax.div(quad, 3))
        other = 1 - lax.rem(step, 2)
        slot = (
            self.me
            + far_x * (self.xn - self.me)
            + far_y * (self.yn - self.me)
            + other * (self.sib - self.me)
        )
        return slot, odd + third * (1 - 2 * odd), other, far_x + 2 * far_y

    def side_copy(self, step):
        slot, half, _, place = self.place(step)
        return remote(
            self.theirs(place, slot, half),
            self.side.at[place, half],
            self.send.at[step],
            self.side_sem.at[place, half],
            self.sib,
        )

    def side_wait(self, place, half):
        remote(
            self.side.at[place, half],
            self.side.at[place, half],
            self.send.at[0],
            self.side_sem.at[place, half],
            self.sib,
        ).wait_recv()

    def relay_copy(self, step, way):
        return remote(
            self.mine(3, way),
            self.relay.at[way],
            self.send.at[step],
            self.relay_sem.at[way],
            (self.xn, self.yn)[way],
        )

    def final_copy(self, step, way, half):
        return remote(
            self.mine(1 + way, half),
            self.final.at[way, half],
            self.send.at[step],
            self.final_sem.at[way, half],
            (self.xn, self.yn)[way],
        )

    def depart(self, step):
        @pl.when(self.place(step)[2] == 1)
        def _():
            self.side_copy(step).start()

        for way in (0, 1):

            @pl.when(step == 1 + 2 * way)
            def _():
                self.side_wait(3, way)
                add_rows(self.mine(3, way), (self.side.at[3, way],))
                self.relay_copy(1 + 2 * way, way).start()

            @pl.when(step == 5 + 2 * way)
            def _():
                self.side_wait(1 + way, way)
                add_rows(self.mine(1 + way, way), (self.side.at[1 + way, way],))
                self.final_copy(5 + 2 * way, way, way).start()

    def send_theirs(self):
        def one(index, carry):
            self.side_copy(2 * index).start()
            return carry

        lax.fori_loop(0, 8, one, 0)

    def send_mine(self):
        for way in (0, 1):
            self.side_wait(3, way)
            add_rows(self.mine(3, way), (self.side.at[3, way],))
            self.relay_copy(1 + 2 * way, way).start()
        for way in (0, 1):
            self.side_wait(1 + way, way)
            add_rows(self.mine(1 + way, way), (self.side.at[1 + way, way],))
            self.final_copy(5 + 2 * way, way, way).start()

    def forward(self):
        for way in (0, 1):
            self.side_wait(1 + way, 1 - way)
            self.relay_copy(0, 1 - way).wait_recv()
            add_rows(
                self.mine(1 + way, 1 - way),
                (self.side.at[1 + way, 1 - way], self.relay.at[1 - way]),
            )
            self.final_copy(9 + 2 * way, way, 1 - way).start()

    def finish(self, write):
        parts, rows_all = self.relay.shape[1:3]
        chunk = row_chunk(rows_all)
        for half in (0, 1):
            home = self.mine(0, half)
            self.side_wait(0, half)
            self.final_copy(0, 0, half).wait_recv()
            self.final_copy(0, 1, half).wait_recv()
            for part in range(parts):

                def one(index, carry, half=half, home=home, part=part):
                    rows = pl.ds(pl.multiple_of(index * chunk, chunk), chunk)
                    total = home[part, rows, :].astype(jnp.float32)
                    total = total + self.side[0, half, part, rows, :].astype(jnp.float32)
                    total = total + self.final[0, half, part, rows, :].astype(jnp.float32)
                    total = total + self.final[1, half, part, rows, :].astype(jnp.float32)
                    write(half, part, rows, total)
                    return carry

                lax.fori_loop(0, rows_all // chunk, one, 0)

    def drain(self):
        for way in (0, 1):
            self.relay_copy(1 + 2 * way, way).wait_send()
            self.final_copy(5 + 2 * way, way, way).wait_send()
            self.final_copy(9 + 2 * way, way, 1 - way).wait_send()

        def one(step, carry):
            @pl.when(self.place(step)[2] == 1)
            def _():
                self.side_copy(step).wait_send()

            return carry

        lax.fori_loop(0, 16, one, 0)


SCATTER_REFS = 7


def scatter_scratch(parts, rows, columns):
    bf = jnp.bfloat16
    return [
        pltpu.VMEM((4, 2, parts, rows, columns), bf),
        pltpu.VMEM((2, parts, rows, columns), bf),
        pltpu.VMEM((2, 2, parts, rows, columns), bf),
        pltpu.SemaphoreType.DMA((16,)),
        pltpu.SemaphoreType.DMA((4, 2)),
        pltpu.SemaphoreType.DMA((2,)),
        pltpu.SemaphoreType.DMA((2, 2)),
    ]


OUT_SLOTS = 4


def expert_out_kernel(rows_hbm, gate_hbm, up_hbm, down_hbm, resid, targets, scales, layer, grad, grad_b, ua_out, rows, gate, ua, up_w, down_w, mine, away, load_w, load_rows, load_gate, store_ua, *scratch):
    hidden, width = down_w.shape
    scatter = Scatter(
        lambda place, slot, half: mine.at[place, half],
        lambda place, slot, half: away.at[place, half],
        scratch,
    )
    weights = (
        pltpu.make_async_copy(up_hbm, up_w, load_w.at[0]),
        pltpu.make_async_copy(down_hbm, down_w, load_w.at[1]),
    )

    def loads(step):
        slot, half, _, _ = scatter.place(step)
        spot = lax.rem(step, OUT_SLOTS)
        return (
            pltpu.make_async_copy(rows_hbm.at[slot, half], rows.at[spot], load_rows.at[step]),
            pltpu.make_async_copy(gate_hbm.at[slot, half], gate.at[spot], load_gate.at[step]),
        )

    def ua_store(step):
        slot, half, _, _ = scatter.place(step)
        return pltpu.make_async_copy(
            ua.at[lax.rem(step, OUT_SLOTS)], ua_out.at[slot, half], store_ua.at[step]
        )

    weights[0].start()
    for step in (0, 1):
        for copy in loads(step):
            copy.start()
    weights[1].start()
    plane_barrier(scatter.peers())
    for copy in weights:
        copy.wait()

    def one(step, carry):
        _, _, other, place = scatter.place(step)
        spot = lax.rem(step, OUT_SLOTS)
        for copy in loads(step):
            copy.wait()

        @pl.when(step < 14)
        def _():
            for copy in loads(step + 2):
                copy.start()

        @pl.when(step >= OUT_SLOTS)
        def _():
            ua_store(step - OUT_SLOTS).wait()

        lanes = lax.broadcasted_iota(jnp.int32, (rows.shape[1], 128), 1)
        tail = rows[spot, :, width:].astype(jnp.float32)
        weight = jnp.sum(jnp.where(lanes == scatter.me, tail, 0.0), axis=1, keepdims=True)
        up_val = nn_dot(rows[spot, :, :width], up_w[...])
        act_val = jnp.maximum(gate[spot].astype(jnp.float32), 0.0) * up_val * weight
        ua[spot, :, :hidden] = up_val.astype(jnp.bfloat16)
        ua[spot, :, hidden:] = act_val.astype(jnp.bfloat16)
        ua_store(step).start()
        partial = nn_dot(ua[spot, :, hidden:], down_w[...]).astype(jnp.bfloat16)

        @pl.when(other == 1)
        def _():
            away[place, half_of(scatter, step), 0] = partial

        @pl.when(other == 0)
        def _():
            mine[place, half_of(scatter, step), 0] = partial

        scatter.depart(step)

        @pl.when(step == 12)
        def _():
            scatter.forward()

        return carry

    lax.fori_loop(0, 16, one, 0)

    def write(half, part, rows, total):
        value = resid[half, rows, :] + total
        layer[half, rows, :] = value.astype(layer.dtype)
        error = (value - targets[half, rows, :].astype(jnp.float32)) * scales[half, rows, 0:1]
        grad[half, rows, :] = error
        grad_b[half, rows, :] = error.astype(grad_b.dtype)

    scatter.finish(write)
    scatter.drain()

    def drain(step, carry):
        ua_store(step).wait()
        return carry

    lax.fori_loop(16 - OUT_SLOTS, 16, drain, 0)


def half_of(scatter, step):
    return scatter.place(step)[1]


def expert_out(rows_all, gate_val, up_w, down_w, resid, targets, scales):
    half, columns = rows_all.shape[2:]
    hidden, width = down_w.shape
    bf = jnp.bfloat16
    return pl.pallas_call(
        expert_out_kernel,
        out_shape=(
            jax.ShapeDtypeStruct((2, half, width), bf),
            jax.ShapeDtypeStruct((2, half, width), jnp.float32),
            jax.ShapeDtypeStruct((2, half, width), bf),
            jax.ShapeDtypeStruct((8, 2, half, 2 * hidden), bf),
        ),
        in_specs=[ANY] * 4 + [VMEM] * 3,
        out_specs=(VMEM, VMEM, VMEM, ANY),
        scratch_shapes=[
            pltpu.VMEM((OUT_SLOTS, half, columns), bf),
            pltpu.VMEM((OUT_SLOTS, half, hidden), bf),
            pltpu.VMEM((OUT_SLOTS, half, 2 * hidden), bf),
            pltpu.VMEM((width, hidden), bf),
            pltpu.VMEM((hidden, width), bf),
            pltpu.VMEM((4, 2, 1, half, width), bf),
            pltpu.VMEM((4, 2, 1, half, width), bf),
            pltpu.SemaphoreType.DMA((2,)),
            pltpu.SemaphoreType.DMA((16,)),
            pltpu.SemaphoreType.DMA((16,)),
            pltpu.SemaphoreType.DMA((16,)),
        ]
        + scatter_scratch(1, half, width),
        compiler_params=pltpu.CompilerParams(
            collective_id=2, has_side_effects=True, vmem_limit_bytes=VMEM_BYTES
        ),
        name="expert_out",
    )(
        rows_all,
        gate_val,
        up_w,
        down_w,
        resid.reshape(2, half, width),
        targets.reshape(2, half, width),
        scales.reshape(2, half, 128),
    )


BACK_SLOTS = 8


def expert_back_kernel(own, rows_hbm, g_hbm, ua_hbm, down_hbm, dgu_out, tail_out, parts_out, buf, gua, rows, tails, down_w, acc, down_acc, send, recv, load, load_g, load_ua, load_rows, store_dgu, store_tail):
    hidden, width = down_w.shape
    gather = Gather(own, buf, send, recv)
    loads = (
        pltpu.make_async_copy(own.at[0], buf.at[gather.me, 0], load.at[0]),
        pltpu.make_async_copy(own.at[1], buf.at[gather.me, 1], load.at[1]),
        pltpu.make_async_copy(down_hbm, down_w, load.at[2]),
    )
    for copy in loads:
        copy.start()

    def block_loads(step):
        slot, half, _ = gather.place(step)
        spot = lax.rem(step, BACK_SLOTS)
        return (
            pltpu.make_async_copy(
                g_hbm.at[slot, half], gua.at[spot, :, pl.ds(0, hidden)], load_g.at[step]
            ),
            pltpu.make_async_copy(
                ua_hbm.at[slot, half], gua.at[spot, :, pl.ds(hidden, 2 * hidden)], load_ua.at[step]
            ),
            pltpu.make_async_copy(rows_hbm.at[slot, half], rows.at[spot], load_rows.at[step]),
        )

    def block_stores(step):
        slot, half, _ = gather.place(step)
        spot = lax.rem(step, BACK_SLOTS)
        return (
            pltpu.make_async_copy(
                gua.at[spot, :, pl.ds(0, 2 * hidden)], dgu_out.at[slot, half], store_dgu.at[step]
            ),
            pltpu.make_async_copy(tails.at[spot], tail_out.at[slot, half], store_tail.at[step]),
        )

    def fetch(step, carry):
        for copy in block_loads(step):
            copy.start()
        return carry

    lax.fori_loop(0, BACK_SLOTS, fetch, 0)
    gather.begin()
    for copy in loads:
        copy.wait()

    def weight_grads(step):
        first = 4 * lax.rem(lax.div(step, 4), 2)
        spots = pl.ds(first, 4)
        places = [gather.place(step - 3 + index)[:2] for index in range(4)]

        def add(ref, index, total):
            at = pl.ds(pl.multiple_of(index * 256, 256), 256)

            @pl.when(step == 3)
            def _():
                ref[at, :] = total

            @pl.when(step > 3)
            def _():
                ref[at, :] = ref[at, :] + total

        def gate_up_tile(index, carry):
            cols = pl.ds(pl.multiple_of(index * 256, 256), 256)
            left = rows[spots, :, cols].reshape(-1, 256)
            right = gua[spots, :, : 2 * hidden].reshape(-1, 2 * hidden)
            add(acc, index, tn_dot(left, right))
            return carry

        def down_tile(index, carry):
            cols = pl.ds(pl.multiple_of(2 * hidden + index * 256, 256), 256)
            total = jnp.zeros((256, width), jnp.float32)
            for place, (slot, half) in enumerate(places):
                total = total + tn_dot(gua[first + place, :, cols], buf[slot, half])
            add(down_acc, index, total)
            return carry

        lax.fori_loop(0, width // 256, gate_up_tile, 0)
        lax.fori_loop(0, hidden // 256, down_tile, 0)

    def one(step, carry):
        slot, half = gather.arrive(step)
        spot = lax.rem(step, BACK_SLOTS)
        for copy in block_loads(step):
            copy.wait()

        lanes = lax.broadcasted_iota(jnp.int32, (buf.shape[2], 128), 1)
        tail = rows[spot, :, width:].astype(jnp.float32)
        weight = jnp.sum(jnp.where(lanes == gather.me, tail, 0.0), axis=1, keepdims=True)
        grad_act = nt_dot(buf[slot, half], down_w[...])
        gate_val = gua[spot, :, :hidden].astype(jnp.float32)
        up_val = gua[spot, :, hidden : 2 * hidden].astype(jnp.float32)
        gate_relu = jnp.maximum(gate_val, 0.0)
        grad_comb = jnp.sum(gate_relu * up_val * grad_act, axis=1, keepdims=True)
        grad_act = grad_act * weight
        grad_gate = jnp.where(gate_val > 0, grad_act * up_val, 0.0).astype(jnp.bfloat16)
        grad_up = (grad_act * gate_relu).astype(jnp.bfloat16)
        gua[spot, :, :hidden] = grad_gate
        gua[spot, :, hidden : 2 * hidden] = grad_up
        tails[spot] = jnp.where(lanes == gather.me, grad_comb, 0.0).astype(jnp.bfloat16)
        for copy in block_stores(step):
            copy.start()

        @pl.when(lax.rem(step, 4) == 3)
        def _():
            weight_grads(step)

            @pl.when(step < 8)
            def _():
                for index in range(4):
                    for copy in block_stores(step - 3 + index):
                        copy.wait()
                    for copy in block_loads(step + 5 + index):
                        copy.start()

        return carry

    lax.fori_loop(0, 16, one, 0)
    gather.finish()

    def round_rows(source, rows_each, first):
        chunks = rows_each // 64

        def one(index, carry):
            rows = pl.ds(pl.multiple_of(index * 64, 64), 64)
            place = pl.ds(pl.multiple_of(first + lax.rem(index, chunks) * 64, 64), 64)
            parts_out[lax.div(index, chunks), place, :] = source[rows, :].astype(jnp.bfloat16)
            return carry

        lax.fori_loop(0, 4 * chunks, one, 0)

    round_rows(acc, width // 4, 0)
    round_rows(down_acc, hidden // 4, width // 4)

    def drain(step, carry):
        for copy in block_stores(step):
            copy.wait()
        return carry

    lax.fori_loop(8, 16, drain, 0)


def expert_back(own, rows_all, gate_val, ua, down_w):
    half, columns = rows_all.shape[2:]
    hidden, width = down_w.shape
    bf = jnp.bfloat16
    return pl.pallas_call(
        expert_back_kernel,
        out_shape=(
            jax.ShapeDtypeStruct((8, 2, half, 2 * hidden), bf),
            jax.ShapeDtypeStruct((8, 2, half, 128), bf),
            jax.ShapeDtypeStruct((4, (width + hidden) // 4, width), bf),
        ),
        in_specs=[ANY] * 5,
        out_specs=(ANY, ANY, VMEM),
        scratch_shapes=[
            pltpu.VMEM((8, 2, half, width), bf),
            pltpu.VMEM((BACK_SLOTS, half, 3 * hidden), bf),
            pltpu.VMEM((BACK_SLOTS, half, columns), bf),
            pltpu.VMEM((BACK_SLOTS, half, 128), bf),
            pltpu.VMEM((hidden, width), bf),
            pltpu.VMEM((width, 2 * hidden), jnp.float32),
            pltpu.VMEM((hidden, width), jnp.float32),
            pltpu.SemaphoreType.DMA((14,)),
            pltpu.SemaphoreType.DMA((8, 2)),
            pltpu.SemaphoreType.DMA((3,)),
        ]
        + [pltpu.SemaphoreType.DMA((16,))] * 5,
        compiler_params=pltpu.CompilerParams(
            collective_id=3, has_side_effects=True, vmem_limit_bytes=VMEM_BYTES
        ),
        name="expert_back",
    )(own, rows_all, gate_val, ua, down_w)


def expert_rows_kernel(dgu_hbm, tail_hbm, gate_hbm, up_hbm, out, dgu, tails, gate_w, up_w, mine, away, load_w, load_dgu, load_tail, *scratch):
    width, hidden = gate_w.shape
    scatter = Scatter(
        lambda place, slot, half: mine.at[place, half],
        lambda place, slot, half: away.at[place, half],
        scratch,
    )
    weights = (
        pltpu.make_async_copy(gate_hbm, gate_w, load_w.at[0]),
        pltpu.make_async_copy(up_hbm, up_w, load_w.at[1]),
    )

    def loads(step):
        slot, half, _, _ = scatter.place(step)
        spot = lax.rem(step, OUT_SLOTS)
        return (
            pltpu.make_async_copy(dgu_hbm.at[slot, half], dgu.at[spot], load_dgu.at[step]),
            pltpu.make_async_copy(tail_hbm.at[slot, half], tails.at[spot], load_tail.at[step]),
        )

    for copy in weights:
        copy.start()
    for step in (0, 1):
        for copy in loads(step):
            copy.start()
    plane_barrier(scatter.peers())
    for copy in weights:
        copy.wait()

    def one(step, carry):
        _, half, other, place = scatter.place(step)
        spot = lax.rem(step, OUT_SLOTS)
        for copy in loads(step):
            copy.wait()

        @pl.when(step < 14)
        def _():
            for copy in loads(step + 2):
                copy.start()

        total = nt_dot(dgu[spot, :, :hidden], gate_w[...]) + nt_dot(dgu[spot, :, hidden:], up_w[...])
        partial = total.astype(jnp.bfloat16)

        @pl.when(other == 1)
        def _():
            away[place, half, 0, :, :width] = partial
            away[place, half, 0, :, width:] = tails[spot]

        @pl.when(other == 0)
        def _():
            mine[place, half, 0, :, :width] = partial
            mine[place, half, 0, :, width:] = tails[spot]

        scatter.depart(step)

        @pl.when(step == 12)
        def _():
            scatter.forward()

        return carry

    lax.fori_loop(0, 16, one, 0)

    def write(half, part, rows, total):
        out[half, rows, :] = total

    scatter.finish(write)
    scatter.drain()


def expert_rows(dgu, tails, gate_w, up_w):
    half = dgu.shape[2]
    width, hidden = gate_w.shape
    columns = width + 128
    bf = jnp.bfloat16
    return pl.pallas_call(
        expert_rows_kernel,
        out_shape=jax.ShapeDtypeStruct((2, half, columns), jnp.float32),
        in_specs=[ANY] * 4,
        out_specs=VMEM,
        scratch_shapes=[
            pltpu.VMEM((OUT_SLOTS, half, 2 * hidden), bf),
            pltpu.VMEM((OUT_SLOTS, half, 128), bf),
            pltpu.VMEM((width, hidden), bf),
            pltpu.VMEM((width, hidden), bf),
            pltpu.VMEM((4, 2, 1, half, columns), bf),
            pltpu.VMEM((4, 2, 1, half, columns), bf),
            pltpu.SemaphoreType.DMA((2,)),
            pltpu.SemaphoreType.DMA((16,)),
            pltpu.SemaphoreType.DMA((16,)),
        ]
        + scatter_scratch(1, half, columns),
        compiler_params=pltpu.CompilerParams(
            collective_id=4, has_side_effects=True, vmem_limit_bytes=VMEM_BYTES
        ),
        name="expert_rows",
    )(dgu, tails, gate_w, up_w)


def line_gather_kernel(own, everything, stage, send, recv, local):
    line = line_peers()
    into = pltpu.make_async_copy(own, stage, local.at[0])
    into.start()
    full_barrier((), line[1:])

    def copy(turn, block):
        return line_remote(
            own, everything.at[block], send.at[turn - 1], recv.at[turn - 1], line[turn]
        )

    for turn in (1, 2, 3):
        copy(turn, line[0]).start()
    into.wait()
    out = pltpu.make_async_copy(stage, everything.at[line[0]], local.at[1])
    out.start()
    out.wait()
    for turn in (1, 2, 3):
        copy(turn, line[turn]).wait()


def line_gather(own):
    return pl.pallas_call(
        line_gather_kernel,
        out_shape=jax.ShapeDtypeStruct((4, *own.shape), own.dtype),
        in_specs=[ANY],
        out_specs=ANY,
        scratch_shapes=[
            pltpu.VMEM(own.shape, own.dtype),
            pltpu.SemaphoreType.DMA((3,)),
            pltpu.SemaphoreType.DMA((3,)),
            pltpu.SemaphoreType.DMA((2,)),
        ],
        compiler_params=pltpu.CompilerParams(
            collective_id=7, has_side_effects=True, vmem_limit_bytes=VMEM_BYTES
        ),
        name="line_gather",
    )(own)


class DenseGather:
    def __init__(self, own, everything, send, recv, local, lined):
        self.own, self.everything, self.send, self.recv = own, everything, send, recv
        self.lined = lined
        self.me, self.sib, self.xn, self.yn = plane_peers()
        self.diag = self.xn + self.yn - self.me
        self.line = line_peers()
        if lined:
            self.home = pltpu.make_async_copy(own, everything.at[:, self.me], local)
        else:
            self.home = pltpu.make_async_copy(own, everything.at[self.line[0], self.me], local)
        self.started = []

    def copy(self, index, own, slot, turn, peer, make):
        target = self.everything.at[self.line[turn], slot]
        return make(
            (self.own.at[self.line[turn]] if self.lined else self.own) if own else target,
            target,
            self.send.at[index],
            self.recv.at[self.line[turn], slot],
            peer,
        )

    def put(self, own, slot, turn, peer, make=remote):
        what = (len(self.started), own, slot, turn, peer, make)
        self.started.append(what)
        self.copy(*what).start()

    def pass_on(self, slot, turn, peer):
        self.put(False, slot, turn, peer)

    def wait(self, slot, turn):
        ref = self.everything.at[self.line[turn], slot]
        remote(ref, ref, self.send.at[0], self.recv.at[self.line[turn], slot], self.sib).wait_recv()

    def start_line(self):
        for turn in (1, 2, 3):
            self.put(True, self.me, 0, self.line[turn], line_remote)

    def start_plane(self):
        for turn in (0, 1, 2, 3) if self.lined else (0,):
            for peer in (self.xn, self.yn, self.sib):
                self.put(True, self.me, turn, peer)

    def near(self, turn):
        self.wait(self.xn, turn)
        if turn % 2 == 0:
            self.pass_on(self.xn, turn, self.yn)
        self.pass_on(self.xn, turn, self.sib)
        self.wait(self.yn, turn)
        if turn % 2 == 1:
            self.pass_on(self.yn, turn, self.xn)
        self.pass_on(self.yn, turn, self.sib)

    def from_line(self, turn):
        self.wait(self.me, turn)
        for peer in (self.xn, self.yn, self.sib):
            self.pass_on(self.me, turn, peer)

    def far(self, turn):
        self.wait(self.diag, turn)
        self.pass_on(self.diag, turn, self.sib)

    def arrived(self):
        for turn in (0, 1, 2, 3):
            for slot in (self.me, self.xn, self.yn, self.diag):
                self.wait(slot + self.sib - self.me, turn)
        self.home.wait()

    def finish(self):
        for what in self.started:
            self.copy(*what).wait_send()


def gather_scratch(rows, columns):
    return [
        pltpu.VMEM((4, 8, rows, columns), jnp.bfloat16),
        pltpu.SemaphoreType.DMA((32,)),
        pltpu.SemaphoreType.DMA((4, 8)),
        pltpu.SemaphoreType.DMA((2,)),
    ]


class LineScatter:
    def __init__(self, sums, scratch):
        self.sums = sums
        self.other, self.send, self.recv = scratch
        self.line = line_peers()

    def copy(self, turn):
        target = self.line[turn]
        return line_remote(
            self.sums(target),
            self.other.at[turn - 1],
            self.send.at[turn - 1],
            self.recv.at[turn - 1],
            target,
        )

    def begin(self):
        for turn in (1, 2, 3):
            self.copy(turn).start()

    def finish(self, outs):
        rows_all = self.other.shape[1]
        for turn in (1, 2, 3):
            self.copy(turn).wait_recv()
        own = self.sums(self.line[0])

        def one(index, carry):
            rows = pl.ds(pl.multiple_of(index * 16, 16), 16)
            total = own[rows, :].astype(jnp.float32)
            for turn in (0, 1, 2):
                total = total + self.other[turn, rows, :].astype(jnp.float32)
            first = 0
            for out, place, columns in outs:
                out[rows, place : place + columns] = total[:, first : first + columns]
                first += columns
            return carry

        lax.fori_loop(0, rows_all // 16, one, 0)
        for turn in (1, 2, 3):
            self.copy(turn).wait_send()


class DenseScatter:
    def __init__(self, total, scratch):
        def block(place, slot, half):
            return total.at[half, :, slot]

        self.plane = Scatter(block, block, scratch[:SCATTER_REFS])
        me = self.plane.me
        self.line = LineScatter(
            lambda line: total.at[lax.div(line, 2), lax.rem(line, 2), me], scratch[SCATTER_REFS:]
        )

    def begin(self):
        self.plane.send_theirs()

    def own(self):
        self.plane.send_mine()

    def forward(self):
        self.plane.forward()

    def turn(self):
        def write(half, part, rows, total):
            home = self.plane.mine(0, half)
            home[part, rows, :] = total.astype(home.dtype)

        self.plane.finish(write)
        self.line.begin()

    def finish(self, outs):
        self.line.finish(outs)
        self.plane.drain()


DENSE_REFS = SCATTER_REFS + 3


def dense_scratch(rows, columns):
    return scatter_scratch(2, rows, columns) + [
        pltpu.VMEM((3, rows, columns), jnp.bfloat16),
        pltpu.SemaphoreType.DMA((3,)),
        pltpu.SemaphoreType.DMA((3,)),
    ]


def rope(values, cosine, sine):
    return values * cosine + pltpu.roll(values, HD // 2, 1) * sine


def gain_rows(misc, out):
    for index in range(out.shape[1] // 128):
        rows = pl.ds(index * 128, 128)
        out[:, rows] = jnp.transpose(misc(rows).astype(jnp.float32))


def inverse_rms(values):
    return lax.rsqrt(jnp.mean(values * values, axis=1, keepdims=True) + EPS)


def row_loop(count, chunk, body):
    def one(index, carry):
        body(pl.ds(pl.multiple_of(index * chunk, chunk), chunk))
        return carry

    lax.fori_loop(0, count // chunk, one, 0)


def tile_loop(count, tile, body):
    row_loop(count, tile, body)


ROW_CHUNK = 16
TILE = 256


def attend_kernel(q_heads, kv_heads, experts, tokens, qkv_own, out_own, cosine, sine, segments, routes, rows_out, resid, heads, mixed, lse, prob, bias, picked, qkv_hbm, out_hbm, gains, hidden, *scratch):
    num_rows, width = tokens.shape
    group = q_heads // kv_heads
    qkv_cols = (q_heads + 2 * kv_heads) * HD
    qkv_w, out_w = scratch[0], scratch[4]
    first = DenseGather(qkv_own, qkv_w, scratch[1], scratch[2], scratch[3].at[0], True)
    second = DenseGather(out_own, out_w, scratch[5], scratch[6], scratch[7].at[0], False)
    stores = (
        pltpu.make_async_copy(qkv_w, qkv_hbm, scratch[3].at[1]),
        pltpu.make_async_copy(out_w, out_hbm, scratch[7].at[1]),
    )
    for gather in (first, second):
        gather.home.start()
    full_barrier((first.sib, first.xn, first.yn), first.line[1:])
    first.start_plane()
    second.start_line()
    picked[...] = jnp.zeros_like(picked)
    lane_ids = lax.broadcasted_iota(jnp.int32, picked.shape, 1)
    for index in range(routes.shape[1]):
        picked[...] = picked[...] + jnp.where(lane_ids == routes[:, index : index + 1], 1.0, 0.0)
    seg_row = segments[0:1, :]
    for index in range(num_rows // 128):
        rows = slice(index * 128, (index + 1) * 128)
        wide = jnp.broadcast_to(seg_row[:, rows].astype(jnp.float32), (128, 128))
        seg_col = jnp.transpose(wide)[:, 0:1].astype(jnp.int32)
        keys = lax.broadcasted_iota(jnp.int32, (128, num_rows), 1)
        queries = lax.broadcasted_iota(jnp.int32, (128, num_rows), 0) + index * 128
        visible = (keys <= queries) & ((seg_row == 0) | (seg_row == seg_col))
        bias[rows, :] = jnp.where(visible, 0.0, NEG_BIG)
    for turn in (0, 1, 2, 3):
        first.near(turn)
        if turn > 0:
            first.far(turn - 1)
    first.far(3)
    second.start_plane()
    first.arrived()
    stores[0].start()

    def flat(ref, cols):
        return ref[:, :, :, cols].reshape(-1, cols.size)

    misc = flat(qkv_w, pl.ds(qkv_cols, 128))
    for index in range(width // 128):
        rows = slice(index * 128, (index + 1) * 128)
        gains[:, rows] = jnp.transpose(misc[rows, :].astype(jnp.float32))

    def norm_one(rows):
        value = tokens[rows, :].astype(jnp.float32)
        normed = value * inverse_rms(value)
        hidden[rows, :] = (normed * gains[experts : experts + 1, :]).astype(jnp.bfloat16)

    row_loop(num_rows, ROW_CHUNK, norm_one)

    for turn in (1, 2, 3):
        second.from_line(turn)

    def project(index, carry):
        cols = pl.ds(pl.multiple_of(index * TILE, TILE), TILE)
        raw = nn_dot(hidden[...], flat(qkv_w, cols))
        turned = index < (q_heads + kv_heads) // 2
        cos_now = jnp.where(turned, cosine[...], 1.0)
        sin_now = jnp.where(turned, sine[...], 0.0)
        for part in (0, 1):
            value = rope(raw[:, part * HD : (part + 1) * HD], cos_now, sin_now)
            heads[2 * index + part] = value.astype(jnp.bfloat16)
        return carry

    lax.fori_loop(0, (q_heads + 2 * kv_heads) // 2, project, 0)
    second.near(0)
    lse[...] = jnp.zeros_like(lse)

    def head_step(head, carry):
        kv_head = q_heads + lax.div(head, group)
        cols = pl.ds(pl.multiple_of(head * HD, HD), HD)
        for first, keys in ((0, PROMPT), (PROMPT, num_rows)):
            rows = pl.ds(first, keys - first)
            query = heads[head, rows, :]
            score = nt_dot(query, heads[kv_head, :keys, :]) * HD ** (-0.5) + bias[rows, :keys]
            top = jnp.max(score, axis=1, keepdims=True)
            weight = jnp.exp(score - top)
            total = jnp.sum(weight, axis=1, keepdims=True)
            value = nn_dot(weight.astype(jnp.bfloat16), heads[kv_head + kv_heads, :keys, :])
            mixed[rows, cols] = (value / total).astype(jnp.bfloat16)
            lanes = lax.broadcasted_iota(jnp.int32, (keys - first, 128), 1)
            lse[rows, :] = jnp.where(lanes == head, top + jnp.log(total), lse[rows, :])

        for turn in (1, 2, 3):

            @pl.when(head == 2 * turn - 1)
            def _():
                second.near(turn)

        for turn in (0, 1, 2):

            @pl.when(head == 6 + turn)
            def _():
                second.far(turn)

        return carry

    lax.fori_loop(0, q_heads, head_step, 0)

    second.far(3)
    second.arrived()
    stores[1].start()

    def out_tile(cols):
        resid[:, cols] = tokens[:, cols].astype(jnp.float32) + nn_dot(mixed[...], flat(out_w, cols))

    tile_loop(width, TILE, out_tile)

    def norm_two(rows):
        value = resid[rows, :]
        normed = value * inverse_rms(value)
        rows_out[rows, :width] = (normed * gains[experts + 1 : experts + 2, :]).astype(jnp.bfloat16)

    row_loop(num_rows, ROW_CHUNK, norm_two)
    logits = nn_dot(rows_out[:, :width], flat(qkv_w, pl.ds(qkv_cols, 128)))
    lanes = lax.broadcasted_iota(jnp.int32, logits.shape, 1)
    logits = jnp.where(lanes < experts, logits, NEG_BIG)
    weight = jnp.exp(logits - jnp.max(logits, axis=1, keepdims=True))
    value = weight / jnp.sum(weight, axis=1, keepdims=True)
    prob[...] = value
    chosen = value * picked[...]
    rows_out[:, width:] = (chosen / jnp.sum(chosen, axis=1, keepdims=True)).astype(jnp.bfloat16)
    for gather, store in zip((first, second), stores):
        store.wait()
        gather.finish()


def attend(tokens, qkv_own, out_own, cosine, sine, segments, routes, q_heads, kv_heads, experts):
    num_rows, width = tokens.shape
    bf = jnp.bfloat16
    all_heads = q_heads + 2 * kv_heads
    return pl.pallas_call(
        functools.partial(attend_kernel, q_heads, kv_heads, experts),
        out_shape=(
            jax.ShapeDtypeStruct((num_rows, width + 128), bf),
            jax.ShapeDtypeStruct((num_rows, width), jnp.float32),
            jax.ShapeDtypeStruct((all_heads, num_rows, HD), bf),
            jax.ShapeDtypeStruct((num_rows, q_heads * HD), bf),
            jax.ShapeDtypeStruct((num_rows, 128), jnp.float32),
            jax.ShapeDtypeStruct((num_rows, 128), jnp.float32),
            jax.ShapeDtypeStruct((num_rows, num_rows), jnp.float32),
            jax.ShapeDtypeStruct((num_rows, 128), jnp.float32),
            jax.ShapeDtypeStruct((4, 8, *qkv_own.shape[1:]), bf),
            jax.ShapeDtypeStruct((4, 8, *out_own.shape), bf),
        ),
        in_specs=[VMEM, ANY, ANY] + [VMEM] * 4,
        out_specs=(VMEM,) * 8 + (ANY, ANY),
        scratch_shapes=[
            pltpu.VMEM((128, width), jnp.float32),
            pltpu.VMEM((num_rows, width), bf),
        ]
        + gather_scratch(*qkv_own.shape[1:])
        + gather_scratch(*out_own.shape),
        compiler_params=pltpu.CompilerParams(
            collective_id=5, has_side_effects=True, vmem_limit_bytes=VMEM_BYTES
        ),
        name="attend",
    )(tokens, qkv_own, out_own, cosine, sine, segments.reshape(1, num_rows), routes)


def attend_back_kernel(q_heads, kv_heads, experts, back_hbm, grad_hbm, resid_hbm, rows_hbm, prob_hbm, picked_hbm, qkv_hbm, out_hbm, mixed_hbm, heads_hbm, lse_hbm, bias_hbm, cos_hbm, sin_hbm, tokens_hbm, grad_in, out_sum, q_sum, k_sum, v_sum, misc_sum, back, grad, resid, hidden_two, prob, picked, qkv_w, out_w, mixed, heads, lse, bias, cosine, sine, tokens, gains, gain_sums, grad_logit, grad_proj, grad_mixed, grad_qkv, grad_kv, hidden, load, *scratch):
    num_rows, width = tokens.shape
    group = q_heads // kv_heads
    q_cols = q_heads * HD
    k_cols = kv_heads * HD
    qkv_cols = q_cols + 2 * k_cols
    near_cols = group * HD
    bf = jnp.bfloat16
    parts, scatters = [], []
    for index in range(4):
        some = scratch[index * (1 + DENSE_REFS) : (index + 1) * (1 + DENSE_REFS)]
        parts.append(some[0])
        scatters.append(DenseScatter(some[0], some[1:]))
    out_part, near_part, rest_part, misc_part = parts
    out_scatter, near_scatter, rest_scatter, misc_scatter = scatters
    pairs = (
        (prob_hbm, prob),
        (picked_hbm, picked),
        (back_hbm, back),
        (qkv_hbm, qkv_w),
        (resid_hbm, resid),
        (grad_hbm, grad),
        (rows_hbm, hidden_two),
        (out_hbm, out_w),
        (mixed_hbm, mixed),
        (heads_hbm, heads),
        (lse_hbm, lse),
        (bias_hbm, bias),
        (cos_hbm, cosine),
        (sin_hbm, sine),
        (tokens_hbm, tokens),
    )
    loads = [pltpu.make_async_copy(src, dst, load.at[i]) for i, (src, dst) in enumerate(pairs)]
    for copy in loads:
        copy.start()
    full_barrier(out_scatter.plane.peers(), out_scatter.line.line[1:])
    for copy in loads[:3]:
        copy.wait()
    gain_sums[...] = jnp.zeros_like(gain_sums)

    def router_rows(rows):
        value = prob[rows, :]
        chosen = value * picked[rows, :]
        total = jnp.sum(chosen, axis=1, keepdims=True)
        comb = chosen / total
        grad_comb = back[rows, width:]
        grad_chosen = (
            picked[rows, :] * (grad_comb - jnp.sum(grad_comb * comb, axis=1, keepdims=True)) / total
        )
        logit = value * (grad_chosen - jnp.sum(value * grad_chosen, axis=1, keepdims=True))
        grad_logit[rows, :] = logit.astype(bf)

    row_loop(num_rows, 64, router_rows)
    loads[3].wait()
    misc = qkv_w.at[:, pl.ds(qkv_cols, 128)]
    gain_rows(lambda rows: misc[rows, :], gains)
    lanes = lax.broadcasted_iota(jnp.int32, (TILE, 128), 1)

    def hidden_tile(cols):
        router = jnp.where(lanes < experts, misc[cols, :], jnp.zeros((), bf))
        back[:, cols] = back[:, cols] + nt_dot(grad_logit[...], router)

    tile_loop(width, TILE, hidden_tile)
    for copy in loads[4:]:
        copy.wait()

    def fold(values):
        return jnp.sum(values.reshape(-1, 8, width), axis=0)

    def norm_two(rows):
        value = resid[rows, :]
        inverse = inverse_rms(value)
        normed = value * inverse
        grad_hidden = back[rows, :width]
        gain_sums[8:16, :] = gain_sums[8:16, :] + fold(grad_hidden * normed)
        grad_norm = grad_hidden * gains[experts + 1 : experts + 2, :]
        mean = jnp.mean(grad_norm * normed, axis=1, keepdims=True)
        total = grad[rows, :] + inverse * (grad_norm - normed * mean)
        grad[rows, :] = total
        grad_proj[rows, :] = total.astype(bf)

    row_loop(num_rows, ROW_CHUNK, norm_two)

    def weight_loop(part, left, right):
        _, _, blocks, rows_each, columns = part.shape
        span = blocks * rows_each

        def one(line, carry):
            cols = pl.ds(pl.multiple_of(line * span, 128), span)
            total = tn_dot(left[:, cols], right[...]).astype(bf)
            part[lax.div(line, 2), lax.rem(line, 2)] = total.reshape(blocks, rows_each, columns)
            return carry

        lax.fori_loop(0, 4, one, 0)

    weight_loop(out_part, mixed, grad_proj)
    out_scatter.begin()

    def mixed_tile(cols):
        grad_mixed[:, cols] = nt_dot(
            grad_proj[...], out_w[cols, :]
        ).astype(bf)

    tile_loop(q_cols, TILE, mixed_tile)
    out_scatter.own()

    def norm_one(rows):
        value = tokens[rows, :].astype(jnp.float32)
        normed = value * inverse_rms(value)
        hidden[rows, :] = (normed * gains[experts : experts + 1, :]).astype(bf)

    row_loop(num_rows, ROW_CHUNK, norm_one)
    scale = HD ** (-0.5)

    def head_step(head, carry):
        kv_head = lax.div(head, group)
        cols = pl.ds(pl.multiple_of(head * HD, HD), HD)

        @pl.when(lax.rem(head, group) == 0)
        def _():
            grad_kv[...] = jnp.zeros_like(grad_kv)

        for first, keys in ((0, PROMPT), (PROMPT, num_rows)):
            rows = pl.ds(first, keys - first)
            key = heads[q_heads + kv_head, :keys, :]
            query = heads[head, rows, :]
            up = grad_mixed[rows, cols]
            lane = lax.broadcasted_iota(jnp.int32, (keys - first, 128), 1)
            total = jnp.sum(jnp.where(lane == head, lse[rows, :], 0.0), axis=1, keepdims=True)
            weight = jnp.exp(nt_dot(query, key) * scale + bias[rows, :keys] - total)
            grad_weight = nt_dot(up, heads[q_heads + kv_heads + kv_head, :keys, :])
            delta = jnp.sum(weight * grad_weight, axis=1, keepdims=True)
            score = (weight * (grad_weight - delta)).astype(bf)
            grad_kv[1, :keys, :] = grad_kv[1, :keys, :] + tn_dot(weight.astype(bf), up)
            grad_kv[0, :keys, :] = grad_kv[0, :keys, :] + tn_dot(score, query) * scale
            value = rope(nn_dot(score, key) * scale, cosine[rows, :], -sine[rows, :])
            grad_qkv[rows, cols] = value.astype(bf)

        @pl.when(lax.rem(head, group) == group - 1)
        def _():
            key_cols = pl.ds(pl.multiple_of(q_cols + kv_head * HD, HD), HD)
            value_cols = pl.ds(pl.multiple_of(q_cols + (kv_heads + kv_head) * HD, HD), HD)
            grad_qkv[:, key_cols] = rope(grad_kv[0], cosine[...], -sine[...]).astype(bf)
            grad_qkv[:, value_cols] = grad_kv[1].astype(bf)

        @pl.when(head == 2)
        def _():
            out_scatter.forward()

        @pl.when(head == group - 1)
        def _():
            weight_loop(near_part, hidden, grad_qkv.at[:, pl.ds(0, near_cols)])
            near_scatter.begin()

        @pl.when(head == group)
        def _():
            near_scatter.own()

        @pl.when(head == group + 1)
        def _():
            out_scatter.turn()

        @pl.when(head == group + 3)
        def _():
            near_scatter.forward()

        return carry

    lax.fori_loop(0, q_heads, head_step, 0)
    weight_loop(rest_part, hidden, grad_qkv.at[:, pl.ds(near_cols, qkv_cols - near_cols)])
    rest_scatter.begin()
    near_scatter.turn()

    def hidden_back_tile(cols):
        back[:, cols] = nt_dot(grad_qkv[...], qkv_w[cols, pl.ds(0, qkv_cols)])

    tile_loop(width // 2, TILE, hidden_back_tile)
    rest_scatter.own()

    def late_tile(index, carry):
        hidden_back_tile(pl.ds(pl.multiple_of(width // 2 + index * TILE, TILE), TILE))
        return carry

    lax.fori_loop(0, width // 2 // TILE, late_tile, 0)

    def last_rows(rows):
        value = tokens[rows, :].astype(jnp.float32)
        inverse = inverse_rms(value)
        normed = value * inverse
        grad_hidden = back[rows, :width]
        gain_sums[0:8, :] = gain_sums[0:8, :] + fold(grad_hidden * normed)
        grad_norm = grad_hidden * gains[experts : experts + 1, :]
        mean = jnp.mean(grad_norm * normed, axis=1, keepdims=True)
        grad[rows, :] = grad[rows, :] + inverse * (grad_norm - normed * mean)

    row_loop(num_rows, ROW_CHUNK, last_rows)
    rest_scatter.forward()
    store = pltpu.make_async_copy(grad, grad_in, load.at[0])
    store.start()
    gains[0:16, :] = gain_sums[...]
    _, _, blocks, rows_each, _ = misc_part.shape
    span = blocks * rows_each

    def misc_line(line, carry):
        cols = pl.ds(pl.multiple_of(line * span, 128), span)
        router = tn_dot(hidden_two[:, cols], grad_logit[...])
        one = jnp.sum(gains[0:8, cols], axis=0, keepdims=True)
        two = jnp.sum(gains[8:16, cols], axis=0, keepdims=True)
        place = lax.broadcasted_iota(jnp.int32, (128, span), 0)
        block = jnp.where(place == experts, one, jnp.where(place == experts + 1, two, 0.0))
        total = (router + jnp.transpose(block)).astype(bf)
        misc_part[lax.div(line, 2), lax.rem(line, 2)] = total.reshape(blocks, rows_each, 128)
        return carry

    lax.fori_loop(0, 4, misc_line, 0)
    misc_scatter.begin()
    misc_scatter.own()
    rest_scatter.turn()
    misc_scatter.forward()
    misc_scatter.turn()
    out_scatter.finish(((out_sum, 0, width),))
    near_scatter.finish(((q_sum, 0, near_cols),))
    rest_scatter.finish(
        ((q_sum, near_cols, q_cols - near_cols), (k_sum, 0, k_cols), (v_sum, 0, k_cols))
    )
    misc_scatter.finish(((misc_sum, 0, 128),))
    store.wait()


def attend_back(back, grad, resid, rows_own, prob, picked, qkv_w, out_w, mixed, heads, lse, bias, cosine, sine, tokens, q_heads, kv_heads, experts):
    num_rows, width = tokens.shape
    bf = jnp.bfloat16
    arrays = (back, grad, resid, rows_own, prob, picked, qkv_w, out_w, mixed, heads, lse, bias, cosine, sine, tokens)
    k_cols = kv_heads * HD
    q_cols = q_heads * HD
    qkv_cols = q_cols + 2 * k_cols
    near_cols = q_cols // kv_heads
    block_rows = width // 32
    scratch = []
    for columns in (width, near_cols, qkv_cols - near_cols, 128):
        scratch += [pltpu.VMEM((2, 2, 8, block_rows, columns), bf)]
        scratch += dense_scratch(block_rows, columns)
    return pl.pallas_call(
        functools.partial(attend_back_kernel, q_heads, kv_heads, experts),
        out_shape=(jax.ShapeDtypeStruct((num_rows, width), jnp.float32),)
        + tuple(
            jax.ShapeDtypeStruct((block_rows, columns), jnp.float32)
            for columns in (width, q_cols, k_cols, k_cols, 128)
        ),
        in_specs=[ANY] * len(arrays),
        out_specs=(ANY,) + (VMEM,) * 5,
        scratch_shapes=[pltpu.VMEM(array.shape, array.dtype) for array in arrays]
        + [
            pltpu.VMEM((128, width), jnp.float32),
            pltpu.VMEM((16, width), jnp.float32),
            pltpu.VMEM((num_rows, 128), bf),
            pltpu.VMEM((num_rows, width), bf),
            pltpu.VMEM((num_rows, q_cols), bf),
            pltpu.VMEM((num_rows, qkv_cols), bf),
            pltpu.VMEM((2, num_rows, HD), jnp.float32),
            pltpu.VMEM((num_rows, width), bf),
            pltpu.SemaphoreType.DMA((len(arrays),)),
        ]
        + scratch,
        compiler_params=pltpu.CompilerParams(
            collective_id=6, has_side_effects=True, vmem_limit_bytes=67043328
        ),
        name="attend_back",
    )(*arrays)


def body_plane(
    tokens,
    targets,
    valid_count,
    segments,
    routes,
    gain_attn,
    w_query,
    w_key,
    w_value,
    w_out,
    gain_moe,
    w_router,
    w_gate,
    w_up,
    w_down,
):
    bf = jnp.bfloat16
    num_rows, width = tokens.shape
    half = num_rows // 2
    q_cols, k_cols = w_query.shape[1], w_key.shape[1]
    num_experts = w_router.shape[1]
    num_heads = q_cols // HD
    kv_heads = k_cols // HD
    pad_cols = 128 - 2 - num_experts
    qkv_own = jnp.concatenate(
        [
            w_query,
            w_key,
            w_value,
            w_router,
            gain_attn[:, None],
            gain_moe[:, None],
            jnp.zeros((gain_attn.shape[0], pad_cols), bf),
        ],
        axis=1,
    )
    qkv_line, w_gate, w_up = lax.optimization_barrier((line_gather(qkv_own), w_gate, w_up))
    gate_w = lax.all_gather(w_gate, "dp", axis=1, tiled=True)[0]
    up_w = lax.all_gather(w_up, "dp", axis=1, tiled=True)[0]
    tok_pos = positions(segments)
    freq = THETA ** (-2.0 * jnp.arange(HD // 2, dtype=jnp.float32) / HD)
    angle = tok_pos.astype(jnp.float32)[:, None] * freq[None, :]
    cosine, sine_part = jnp.cos(angle), jnp.sin(angle)
    cosine = jnp.concatenate([cosine, cosine], axis=1)
    sine = jnp.concatenate([-sine_part, sine_part], axis=1)
    rows_own, resid_mid, heads, mixed, lse, prob, bias, picked, qkv_w, out_w = attend(
        tokens, qkv_line, w_out, cosine, sine, segments, routes, num_heads, kv_heads, num_experts
    )
    rows_all, gate_val, down_w = expert_in(
        rows_own.reshape(2, half, width + 128), gate_w, w_down[0]
    )
    down_w = down_w.reshape(-1, width)
    total_rows = num_rows * lax.axis_size(("dp", "exp"))
    global_row = lax.axis_index(("dp", "exp")) * num_rows + jnp.arange(num_rows, dtype=jnp.int32)
    loss_scale = total_rows / valid_count[0].astype(jnp.float32)
    scales = jnp.broadcast_to(
        jnp.where(global_row < valid_count[0], loss_scale, 0.0)[:, None], (num_rows, 128)
    )
    layer_out, grad_out, grad_out_b, ua = expert_out(
        rows_all, gate_val, up_w, down_w, resid_mid, targets, scales
    )
    layer_out = layer_out.reshape(num_rows, width)
    dgu, tails, expert_parts = expert_back(
        grad_out_b, rows_all, gate_val, ua, down_w
    )
    back = expert_rows(dgu, tails, gate_w, up_w)
    expert_sum = lax.psum_scatter(expert_parts, "dp", scatter_dimension=0, tiled=True)
    hidden, shard = w_gate.shape[2], w_gate.shape[1]
    expert_sums = (
        expert_sum[:, :shard, :hidden].astype(jnp.float32),
        expert_sum[:, :shard, hidden:].astype(jnp.float32),
        expert_sum[:, shard:].astype(jnp.float32),
    )
    grad_in, out_sum, q_sum, k_sum, v_sum, misc_sum = attend_back(
        back.reshape(num_rows, width + 128),
        grad_out.reshape(num_rows, width),
        resid_mid,
        rows_own,
        prob,
        picked,
        qkv_w.reshape(width, -1),
        out_w.reshape(q_cols, width),
        mixed,
        heads,
        lse,
        bias,
        cosine,
        sine,
        tokens,
        num_heads,
        kv_heads,
        num_experts,
    )
    return (
        layer_out,
        grad_in,
        misc_sum[:, num_experts],
        q_sum,
        k_sum,
        v_sum,
        out_sum,
        misc_sum[:, num_experts + 1],
        misc_sum[:, :num_experts],
        *expert_sums,
    )


def solution(mesh):
    in_specs = (
        P(("dp", "exp"), None),
        P(("dp", "exp"), None),
        P(),
        P(("dp", "exp")),
        P(("dp", "exp"), None),
        P(("dp", "exp")),
        P(("dp", "exp"), None),
        P(("dp", "exp"), None),
        P(("dp", "exp"), None),
        P(("dp", "exp"), None),
        P(("dp", "exp")),
        P(("dp", "exp"), None),
        P("exp", "dp", None),
        P("exp", "dp", None),
        P("exp", "dp", None),
    )
    out_specs = (
        P(("dp", "exp"), None),
        P(("dp", "exp"), None),
        P(("dp", "exp")),
        P(("dp", "exp"), None),
        P(("dp", "exp"), None),
        P(("dp", "exp"), None),
        P(("dp", "exp"), None),
        P(("dp", "exp")),
        P(("dp", "exp"), None),
        P("exp", "dp", None),
        P("exp", "dp", None),
        P("exp", "dp", None),
    )
    body = body_plane if (mesh.shape["dp"], mesh.shape["exp"]) == (4, 8) else body_general
    return jax.shard_map(body, mesh=mesh, in_specs=in_specs, out_specs=out_specs, check_vma=False)
```

```python
import functools

import jax
import jax.numpy as jnp
from jax import lax
from jax.experimental import pallas as pl
from jax.experimental.pallas import tpu as pltpu
from jax.sharding import PartitionSpec as P

HD = 128
PROMPT = 256
NCONT = 2


EPS = 1e-06
THETA = 10000.0
HIGH = lax.Precision.HIGHEST
NEG_BIG = -1e30


def positions(segments):
    count_rows = segments.shape[0]
    row_ids = jnp.arange(count_rows, dtype=jnp.int32)
    labels = jnp.arange(NCONT + 1, dtype=jnp.int32)
    member = segments[:, None] == labels[None, :]
    first_row = jnp.min(jnp.where(member, row_ids[:, None], count_rows), axis=0)
    start_row = jnp.sum(jnp.where(member, first_row[None, :], 0), axis=1)
    return jnp.where(segments == 0, row_ids, PROMPT + row_ids - start_row)


def key_mask(segments):
    row_ids = jnp.arange(segments.shape[0], dtype=jnp.int32)
    causal = row_ids[None, :] <= row_ids[:, None]
    visible = (segments[None, :] == 0) | (segments[None, :] == segments[:, None])
    return causal & visible


def rotate(values, pos_rows, sign_value):
    half_size = HD // 2
    freq = THETA ** (-2.0 * jnp.arange(half_size, dtype=jnp.float32) / HD)
    angle = pos_rows.astype(jnp.float32)[:, None] * freq[None, :]
    cosine = jnp.cos(angle)[:, None, :]
    sine_part = sign_value * jnp.sin(angle)[:, None, :]
    first_half = values[..., :half_size]
    second = values[..., half_size:]
    return jnp.concatenate(
        [first_half * cosine - second * sine_part, second * cosine + first_half * sine_part],
        axis=-1,
    )


def attention_scores(query_b, key_b, allowed):
    logits = jnp.einsum(
        "qkgd,pkd->kgqp", query_b, key_b, preferred_element_type=jnp.float32
    ) * HD ** (-0.5)
    return jnp.where(allowed[None, None], logits, NEG_BIG)


def expert_gates(rows_in, gate_w, up_w):
    gate_val = jnp.einsum("sacd,adf->sacf", rows_in, gate_w, preferred_element_type=jnp.float32)
    up_val = jnp.einsum("sacd,adf->sacf", rows_in, up_w, preferred_element_type=jnp.float32)
    return (gate_val, up_val)


def body_general(
    tokens,
    targets,
    valid_count,
    segments,
    routes,
    gain_attn,
    w_query,
    w_key,
    w_value,
    w_out,
    gain_moe,
    w_router,
    w_gate,
    w_up,
    w_down,
):
    gain_one, query_w, key_w, value_w, out_w, gain_two, router_w = (
        lax.all_gather(gain_attn, ("dp", "exp"), axis=0, tiled=True),
        lax.all_gather(w_query, ("dp", "exp"), axis=0, tiled=True),
        lax.all_gather(w_key, ("dp", "exp"), axis=0, tiled=True),
        lax.all_gather(w_value, ("dp", "exp"), axis=0, tiled=True),
        lax.all_gather(w_out, ("dp", "exp"), axis=0, tiled=True),
        lax.all_gather(gain_moe, ("dp", "exp"), axis=0, tiled=True),
        lax.all_gather(w_router, ("dp", "exp"), axis=0, tiled=True),
    )
    gate_w, up_w, down_w = (
        lax.all_gather(w_gate, "dp", axis=1, tiled=True),
        lax.all_gather(w_up, "dp", axis=1, tiled=True),
        lax.all_gather(w_down, "dp", axis=1, tiled=True),
    )
    num_rows = tokens.shape[0]
    width = tokens.shape[1]
    num_heads = query_w.shape[1] // HD
    kv_heads = key_w.shape[1] // HD
    group_size = num_heads // kv_heads
    num_experts = router_w.shape[1]
    top_count = routes.shape[1]
    exp_local = gate_w.shape[0]
    exp_ranks = lax.axis_size("exp")
    capacity = 5 * num_rows * top_count // (4 * num_experts)
    tok_pos = positions(segments)
    allowed = key_mask(segments)
    resid_in = tokens.astype(jnp.float32)
    inv_one = lax.rsqrt(jnp.mean(resid_in * resid_in, axis=-1, keepdims=True) + EPS)
    normed_one = resid_in * inv_one
    hidden_one = (normed_one * gain_one.astype(jnp.float32)).astype(jnp.bfloat16)
    query_raw = jnp.dot(hidden_one, query_w, preferred_element_type=jnp.float32)
    key_raw = jnp.dot(hidden_one, key_w, preferred_element_type=jnp.float32)
    value_b = jnp.dot(hidden_one, value_w, preferred_element_type=jnp.float32).astype(jnp.bfloat16)
    query_b = rotate(query_raw.reshape(num_rows, num_heads, HD), tok_pos, 1.0).astype(jnp.bfloat16)
    query_b = query_b.reshape(num_rows, kv_heads, group_size, HD)
    key_b = rotate(key_raw.reshape(num_rows, kv_heads, HD), tok_pos, 1.0).astype(jnp.bfloat16)
    value_h = value_b.reshape(num_rows, kv_heads, HD)
    logit_att = attention_scores(query_b, key_b, allowed)
    row_max = jnp.max(logit_att, axis=-1, keepdims=True)
    log_total = row_max + jnp.log(jnp.sum(jnp.exp(logit_att - row_max), axis=-1, keepdims=True))
    probs_b = jnp.exp(logit_att - log_total).astype(jnp.bfloat16)
    attn_vals = jnp.einsum("kgqp,pkd->qkgd", probs_b, value_h, preferred_element_type=jnp.float32)
    attn_vals = attn_vals.reshape(num_rows, num_heads * HD).astype(jnp.bfloat16)
    resid_mid = resid_in + jnp.dot(attn_vals, out_w, preferred_element_type=jnp.float32)
    inv_two = lax.rsqrt(jnp.mean(resid_mid * resid_mid, axis=-1, keepdims=True) + EPS)
    normed_two = resid_mid * inv_two
    gain_two_f = gain_two.astype(jnp.float32)
    hidden_two = (normed_two * gain_two_f).astype(jnp.bfloat16)
    router_prob = jax.nn.softmax(
        jnp.dot(hidden_two, router_w, preferred_element_type=jnp.float32), axis=-1
    )
    expert_ids = jnp.arange(num_experts, dtype=jnp.int32)
    route_hot = routes[:, :, None] == expert_ids[None, None, :]
    chosen = jnp.sum(jnp.where(route_hot, router_prob[:, None, :], 0.0), axis=-1)
    weight_sum = jnp.sum(chosen, axis=1, keepdims=True)
    combine = chosen / weight_sum
    flat_hot = route_hot.reshape(num_rows * top_count, num_experts).astype(jnp.int32)
    slot_index = jnp.sum((jnp.cumsum(flat_hot, axis=0) - flat_hot) * flat_hot, axis=1)
    dest_index = routes.reshape(-1) * capacity + slot_index
    send_shape = (exp_ranks, exp_local, capacity, width)
    send_rows = jnp.zeros((num_experts * capacity, width), jnp.bfloat16)
    send_rows = (
        send_rows.at[dest_index].set(jnp.repeat(hidden_two, top_count, axis=0)).reshape(send_shape)
    )
    gate_val, up_val = expert_gates(
        lax.all_to_all(send_rows, "exp", split_axis=0, concat_axis=0, tiled=True), gate_w, up_w
    )
    act_b = (jax.nn.relu(gate_val) * up_val).astype(jnp.bfloat16)
    out_b = jnp.einsum("sacf,afd->sacd", act_b, down_w, preferred_element_type=jnp.float32).astype(
        jnp.bfloat16
    )
    returned = lax.all_to_all(out_b, "exp", split_axis=0, concat_axis=0, tiled=True)
    route_out = returned.reshape(num_experts * capacity, width)[dest_index].reshape(
        num_rows, top_count, width
    )
    route_out_f = route_out.astype(jnp.float32)
    resid_out = resid_mid + jnp.sum(combine[:, :, None] * route_out_f, axis=1)
    layer_out = resid_out.astype(jnp.bfloat16)
    total_rows = num_rows * lax.axis_size(("dp", "exp"))
    global_row = lax.axis_index(("dp", "exp")) * num_rows + jnp.arange(num_rows, dtype=jnp.int32)
    loss_scale = total_rows / valid_count[0].astype(jnp.float32)
    grad_out = jnp.where(
        (global_row < valid_count[0])[:, None],
        (resid_out - targets.astype(jnp.float32)) * loss_scale,
        0.0,
    )
    gain_one, query_w, key_w, value_w, out_w, gain_two, router_w = (
        lax.all_gather(gain_attn, ("dp", "exp"), axis=0, tiled=True),
        lax.all_gather(w_query, ("dp", "exp"), axis=0, tiled=True),
        lax.all_gather(w_key, ("dp", "exp"), axis=0, tiled=True),
        lax.all_gather(w_value, ("dp", "exp"), axis=0, tiled=True),
        lax.all_gather(w_out, ("dp", "exp"), axis=0, tiled=True),
        lax.all_gather(gain_moe, ("dp", "exp"), axis=0, tiled=True),
        lax.all_gather(w_router, ("dp", "exp"), axis=0, tiled=True),
    )
    gain_two_f = gain_two.astype(jnp.float32)
    grad_route = (combine[:, :, None] * grad_out[:, None, :]).astype(jnp.bfloat16)
    grad_comb = jnp.sum(grad_out[:, None, :] * route_out_f, axis=-1)
    grad_send = jnp.zeros((num_experts * capacity, width), jnp.bfloat16)
    grad_send = (
        grad_send.at[dest_index]
        .set(grad_route.reshape(num_rows * top_count, width))
        .reshape(send_shape)
    )
    expert_rows, grad_recv = (
        lax.all_to_all(send_rows, "exp", split_axis=0, concat_axis=0, tiled=True),
        lax.all_to_all(grad_send, "exp", split_axis=0, concat_axis=0, tiled=True),
    )
    gate_val, up_val = expert_gates(expert_rows, gate_w, up_w)
    gate_relu = jax.nn.relu(gate_val)
    act_b = (gate_relu * up_val).astype(jnp.bfloat16)
    grad_act = jnp.einsum("sacd,afd->sacf", grad_recv, down_w, preferred_element_type=jnp.float32)
    grad_down_w = jnp.einsum("sacf,sacd->afd", act_b, grad_recv, preferred_element_type=jnp.float32)
    grad_gate_b = jnp.where(gate_val > 0, grad_act * up_val, 0.0).astype(jnp.bfloat16)
    grad_up_b = (grad_act * gate_relu).astype(jnp.bfloat16)
    grad_gate_w = jnp.einsum(
        "sacd,sacf->adf", expert_rows, grad_gate_b, preferred_element_type=jnp.float32
    )
    grad_up_w = jnp.einsum(
        "sacd,sacf->adf", expert_rows, grad_up_b, preferred_element_type=jnp.float32
    )
    grad_rows = (
        jnp.einsum("sacf,adf->sacd", grad_gate_b, gate_w, preferred_element_type=jnp.float32)
        + jnp.einsum("sacf,adf->sacd", grad_up_b, up_w, preferred_element_type=jnp.float32)
    ).astype(jnp.bfloat16)
    grad_back = lax.all_to_all(grad_rows, "exp", split_axis=0, concat_axis=0, tiled=True)
    grad_copies = grad_back.reshape(num_experts * capacity, width)[dest_index].reshape(
        num_rows, top_count, width
    )
    grad_hidden_two = jnp.sum(grad_copies.astype(jnp.float32), axis=1)
    grad_chosen = (grad_comb - jnp.sum(grad_comb * combine, axis=1, keepdims=True)) / weight_sum
    grad_prob = jnp.sum(jnp.where(route_hot, grad_chosen[:, :, None], 0.0), axis=1)
    grad_logit = router_prob * (
        grad_prob - jnp.sum(router_prob * grad_prob, axis=-1, keepdims=True)
    )
    router_f = router_w.astype(jnp.float32)
    grad_hidden_two = grad_hidden_two + jnp.einsum(
        "re,de->rd", grad_logit, router_f, precision=HIGH
    )
    grad_router = jnp.einsum(
        "rd,re->de", hidden_two.astype(jnp.float32), grad_logit, precision=HIGH
    )
    grad_gain_two = jnp.sum(grad_hidden_two * normed_two, axis=0)
    grad_norm_two = grad_hidden_two * gain_two_f
    grad_mid = grad_out + inv_two * (
        grad_norm_two - normed_two * jnp.mean(grad_norm_two * normed_two, axis=-1, keepdims=True)
    )
    grad_proj_b = grad_mid.astype(jnp.bfloat16)
    grad_out_w = jnp.einsum("rh,rd->hd", attn_vals, grad_proj_b, preferred_element_type=jnp.float32)
    grad_vals_b = jnp.einsum(
        "rd,hd->rh", grad_proj_b, out_w, preferred_element_type=jnp.float32
    ).astype(jnp.bfloat16)
    grad_vals_b = grad_vals_b.reshape(num_rows, kv_heads, group_size, HD)
    logit_att = attention_scores(query_b, key_b, allowed)
    probs = jnp.exp(logit_att - log_total)
    probs_b = probs.astype(jnp.bfloat16)
    grad_value = jnp.einsum(
        "kgqp,qkgd->pkd", probs_b, grad_vals_b, preferred_element_type=jnp.float32
    )
    grad_prob_att = jnp.einsum(
        "qkgd,pkd->kgqp", grad_vals_b, value_h, preferred_element_type=jnp.float32
    )
    delta_row = jnp.sum(probs * grad_prob_att, axis=-1, keepdims=True)
    grad_score_b = (probs * (grad_prob_att - delta_row)).astype(jnp.bfloat16)
    grad_query = jnp.einsum(
        "kgqp,pkd->qkgd", grad_score_b, key_b, preferred_element_type=jnp.float32
    ) * HD ** (-0.5)
    grad_key = jnp.einsum(
        "kgqp,qkgd->pkd", grad_score_b, query_b, preferred_element_type=jnp.float32
    ) * HD ** (-0.5)
    grad_query_b = rotate(grad_query.reshape(num_rows, num_heads, HD), tok_pos, -1.0).astype(
        jnp.bfloat16
    )
    grad_query_b = grad_query_b.reshape(num_rows, num_heads * HD)
    grad_key_b = (
        rotate(grad_key, tok_pos, -1.0).astype(jnp.bfloat16).reshape(num_rows, kv_heads * HD)
    )
    grad_value_b = grad_value.astype(jnp.bfloat16).reshape(num_rows, kv_heads * HD)
    grad_query_w = jnp.einsum(
        "rd,rh->dh", hidden_one, grad_query_b, preferred_element_type=jnp.float32
    )
    grad_key_w = jnp.einsum("rd,rh->dh", hidden_one, grad_key_b, preferred_element_type=jnp.float32)
    grad_value_w = jnp.einsum(
        "rd,rh->dh", hidden_one, grad_value_b, preferred_element_type=jnp.float32
    )
    grad_hidden_one = (
        jnp.einsum("rh,dh->rd", grad_query_b, query_w, preferred_element_type=jnp.float32)
        + jnp.einsum("rh,dh->rd", grad_key_b, key_w, preferred_element_type=jnp.float32)
        + jnp.einsum("rh,dh->rd", grad_value_b, value_w, preferred_element_type=jnp.float32)
    )
    grad_gain_one = jnp.sum(grad_hidden_one * normed_one, axis=0)
    grad_norm_one = grad_hidden_one * gain_one.astype(jnp.float32)
    grad_in = grad_mid + inv_one * (
        grad_norm_one - normed_one * jnp.mean(grad_norm_one * normed_one, axis=-1, keepdims=True)
    )
    dense_sums = (
        lax.psum_scatter(grad_gain_one, ("dp", "exp"), scatter_dimension=0, tiled=True),
        lax.psum_scatter(grad_query_w, ("dp", "exp"), scatter_dimension=0, tiled=True),
        lax.psum_scatter(grad_key_w, ("dp", "exp"), scatter_dimension=0, tiled=True),
        lax.psum_scatter(grad_value_w, ("dp", "exp"), scatter_dimension=0, tiled=True),
        lax.psum_scatter(grad_out_w, ("dp", "exp"), scatter_dimension=0, tiled=True),
        lax.psum_scatter(grad_gain_two, ("dp", "exp"), scatter_dimension=0, tiled=True),
        lax.psum_scatter(grad_router, ("dp", "exp"), scatter_dimension=0, tiled=True),
    )
    expert_sums = (
        lax.psum_scatter(
            grad_gate_w.astype(jnp.bfloat16), "dp", scatter_dimension=1, tiled=True
        ).astype(jnp.float32),
        lax.psum_scatter(
            grad_up_w.astype(jnp.bfloat16), "dp", scatter_dimension=1, tiled=True
        ).astype(jnp.float32),
        lax.psum_scatter(
            grad_down_w.astype(jnp.bfloat16), "dp", scatter_dimension=1, tiled=True
        ).astype(jnp.float32),
    )
    return (
        layer_out,
        grad_in,
        dense_sums[0],
        dense_sums[1],
        dense_sums[2],
        dense_sums[3],
        dense_sums[4],
        dense_sums[5],
        dense_sums[6],
        expert_sums[0],
        expert_sums[1],
        expert_sums[2],
    )


MESH = pl.DeviceIdType.MESH
ANY = pl.BlockSpec(memory_space=pl.ANY)
VMEM = pl.BlockSpec(memory_space=pltpu.VMEM)
VMEM_BYTES = 62 * 2**20


def nn_dot(left, right):
    return jnp.dot(left, right, preferred_element_type=jnp.float32)


def nt_dot(left, right):
    return lax.dot_general(
        left, right, (((1,), (1,)), ((), ())), preferred_element_type=jnp.float32
    )


def tn_dot(left, right):
    return lax.dot_general(
        left, right, (((0,), (0,)), ((), ())), preferred_element_type=jnp.float32
    )


def plane_peers():
    me = lax.axis_index("exp")
    core = lax.rem(me, 2)
    x_pos = lax.rem(lax.div(me, 2), 2)
    y_pos = lax.div(me, 4)
    return me, me + 1 - 2 * core, me + 2 - 4 * x_pos, me + 4 - 8 * y_pos


def remote(src, dst, send_sem, recv_sem, peer):
    return pltpu.make_async_remote_copy(
        src_ref=src,
        dst_ref=dst,
        send_sem=send_sem,
        recv_sem=recv_sem,
        device_id={"exp": peer},
        device_id_type=MESH,
    )


def plane_barrier(peers):
    barrier = pltpu.get_barrier_semaphore()
    for peer in peers:
        pl.semaphore_signal(barrier, inc=1, device_id={"exp": peer}, device_id_type=MESH)
    pl.semaphore_wait(barrier, len(peers))


def step_place(step, quad):
    odd = lax.rem(step, 2)
    last = lax.div(quad, 3)
    mid = lax.rem(lax.div(quad + 1, 2), 2)
    return mid * (1 - odd) + last, mid * odd + last


class Gather:
    def __init__(self, own, buf, send, recv):
        self.own, self.buf, self.send, self.recv = own, buf, send, recv
        self.me, self.sib, self.xn, self.yn = plane_peers()
        self.diag = self.xn + self.yn - self.me

    def own_copy(self, half, peer, sem):
        return remote(
            self.own.at[half],
            self.buf.at[self.me, half],
            self.send.at[sem],
            self.recv.at[self.me, half],
            peer,
        )

    def pass_copy(self, slot, half, peer, sem):
        return remote(
            self.buf.at[slot, half],
            self.buf.at[slot, half],
            self.send.at[sem],
            self.recv.at[slot, half],
            peer,
        )

    def own_copies(self):
        return (
            self.own_copy(0, self.xn, 0),
            self.own_copy(1, self.yn, 1),
            self.own_copy(0, self.sib, 2),
            self.own_copy(1, self.sib, 3),
            self.own_copy(1, self.xn, 4),
            self.own_copy(0, self.yn, 5),
        )

    def near_copies(self):
        return (
            self.pass_copy(self.xn, 0, self.yn, 6),
            self.pass_copy(self.yn, 1, self.xn, 7),
            self.pass_copy(self.xn, 0, self.sib, 8),
            self.pass_copy(self.yn, 1, self.sib, 9),
        )

    def late_copies(self):
        return (
            self.pass_copy(self.xn, 1, self.sib, 10),
            self.pass_copy(self.yn, 0, self.sib, 11),
        )

    def far_copies(self):
        return (
            self.pass_copy(self.diag, 0, self.sib, 12),
            self.pass_copy(self.diag, 1, self.sib, 13),
        )

    def wait_block(self, slot, half):
        self.pass_copy(slot, half, self.sib, 0).wait_recv()

    def begin(self):
        plane_barrier((self.sib, self.xn, self.yn))
        for copy in self.own_copies():
            copy.start()

    def place(self, step):
        quad = lax.div(step, 4)
        far_x, far_y = step_place(step, quad)
        odd = lax.rem(step, 2)
        third = lax.div(quad, 2) * (1 - lax.div(quad, 3))
        other = lax.div(lax.rem(step, 4), 2)
        slot = (
            self.me
            + far_x * (self.xn - self.me)
            + far_y * (self.yn - self.me)
            + other * (self.sib - self.me)
        )
        return slot, odd + third * (1 - 2 * odd), other

    def arrive(self, step):
        @pl.when(step == 4)
        def _():
            self.wait_block(self.xn, 0)
            self.wait_block(self.yn, 1)
            for copy in self.near_copies():
                copy.start()

        @pl.when(step == 8)
        def _():
            self.wait_block(self.xn, 1)
            self.wait_block(self.yn, 0)
            for copy in self.late_copies():
                copy.start()

        @pl.when(step == 12)
        def _():
            self.wait_block(self.diag, 0)
            self.wait_block(self.diag, 1)
            for copy in self.far_copies():
                copy.start()

        slot, half, other = self.place(step)

        @pl.when(other == 1)
        def _():
            self.wait_block(slot, half)

        return slot, half

    def finish(self):
        for copies in (self.own_copies(), self.near_copies(), self.late_copies(), self.far_copies()):
            for copy in copies:
                copy.wait_send()


def line_peers():
    line = lax.axis_index("dp")
    return (
        line,
        line + 1 - 2 * lax.rem(line, 2),
        line + 2 - 4 * lax.div(line, 2),
        3 - line,
    )


def line_remote(src, dst, send_sem, recv_sem, peer):
    return pltpu.make_async_remote_copy(
        src_ref=src,
        dst_ref=dst,
        send_sem=send_sem,
        recv_sem=recv_sem,
        device_id={"dp": peer},
        device_id_type=MESH,
    )


def full_barrier(plane, line):
    barrier = pltpu.get_barrier_semaphore()
    for peer in plane:
        pl.semaphore_signal(barrier, inc=1, device_id={"exp": peer}, device_id_type=MESH)
    for peer in line:
        pl.semaphore_signal(barrier, inc=1, device_id={"dp": peer}, device_id_type=MESH)
    pl.semaphore_wait(barrier, len(plane) + len(line))


def expert_in_kernel(own, gate_hbm, down_own, rows_out, gate_out, down_out, buf, gate, gate_w, down_stage, send, recv, load, store_a, store_b, line_send, line_recv):
    width = gate_w.shape[0]
    gather = Gather(own, buf, send, recv)
    line = line_peers()
    loads = (
        pltpu.make_async_copy(own.at[0], buf.at[gather.me, 0], load.at[0]),
        pltpu.make_async_copy(own.at[1], buf.at[gather.me, 1], load.at[1]),
        pltpu.make_async_copy(gate_hbm, gate_w, load.at[2]),
        pltpu.make_async_copy(down_own, down_stage, load.at[3]),
    )
    for copy in loads:
        copy.start()
    full_barrier((gather.sib, gather.xn, gather.yn), line[1:])
    for copy in gather.own_copies():
        copy.start()

    def down_copy(turn):
        return line_remote(
            down_own,
            down_out.at[line[0]],
            line_send.at[turn - 1],
            line_recv.at[turn - 1],
            line[turn],
        )

    for turn in (1, 2, 3):
        down_copy(turn).start()
    for copy in loads:
        copy.wait()
    down_store = pltpu.make_async_copy(down_stage, down_out.at[line[0]], load.at[4])
    down_store.start()

    def row_store(slot, half, step):
        return pltpu.make_async_copy(buf.at[slot, half], rows_out.at[slot, half], store_a.at[step])

    def gate_store(slot, half, step):
        return pltpu.make_async_copy(gate.at[slot, half], gate_out.at[slot, half], store_b.at[step])

    def one(step, carry):
        slot, half = gather.arrive(step)
        row_store(slot, half, step).start()
        gate[slot, half] = nn_dot(buf[slot, half, :, :width], gate_w[...]).astype(jnp.bfloat16)
        gate_store(slot, half, step).start()
        return carry

    lax.fori_loop(0, 16, one, 0)
    gather.finish()

    def drain(step, carry):
        slot, half, _ = gather.place(step)
        row_store(slot, half, step).wait()
        gate_store(slot, half, step).wait()
        return carry

    lax.fori_loop(0, 16, drain, 0)
    down_store.wait()
    for turn in (1, 2, 3):
        line_remote(
            down_own,
            down_out.at[line[turn]],
            line_send.at[turn - 1],
            line_recv.at[turn - 1],
            line[turn],
        ).wait()


def expert_in(own, gate_w, down_own):
    _, half, columns = own.shape
    width, hidden = gate_w.shape
    bf = jnp.bfloat16
    return pl.pallas_call(
        expert_in_kernel,
        out_shape=(
            jax.ShapeDtypeStruct((8, 2, half, columns), bf),
            jax.ShapeDtypeStruct((8, 2, half, hidden), bf),
            jax.ShapeDtypeStruct((4, *down_own.shape), bf),
        ),
        in_specs=[ANY] * 3,
        out_specs=(ANY, ANY, ANY),
        scratch_shapes=[
            pltpu.VMEM((8, 2, half, columns), bf),
            pltpu.VMEM((8, 2, half, hidden), bf),
            pltpu.VMEM((width, hidden), bf),
            pltpu.VMEM(down_own.shape, bf),
            pltpu.SemaphoreType.DMA((14,)),
            pltpu.SemaphoreType.DMA((8, 2)),
            pltpu.SemaphoreType.DMA((5,)),
            pltpu.SemaphoreType.DMA((16,)),
            pltpu.SemaphoreType.DMA((16,)),
            pltpu.SemaphoreType.DMA((3,)),
            pltpu.SemaphoreType.DMA((3,)),
        ],
        compiler_params=pltpu.CompilerParams(
            collective_id=1, has_side_effects=True, vmem_limit_bytes=VMEM_BYTES
        ),
        name="expert_in",
    )(own, gate_w, down_own)


def row_chunk(rows):
    return 64 if rows % 64 == 0 else 16


def add_rows(target, others):
    parts, rows_all, _ = target.shape
    chunk = row_chunk(rows_all)
    for part in range(parts):

        def one(index, carry):
            rows = pl.ds(pl.multiple_of(index * chunk, chunk), chunk)
            total = target[part, rows, :].astype(jnp.float32)
            for other in others:
                total = total + other[part, rows, :].astype(jnp.float32)
            target[part, rows, :] = total.astype(target.dtype)
            return carry

        lax.fori_loop(0, rows_all // chunk, one, 0)


class Scatter:
    def __init__(self, mine, theirs, scratch):
        self.mine_of, self.theirs = mine, theirs
        self.side, self.relay, self.final = scratch[:3]
        self.send, self.side_sem, self.relay_sem, self.final_sem = scratch[3:]
        self.me, self.sib, self.xn, self.yn = plane_peers()

    def mine(self, place, half):
        slot = (self.me, self.xn, self.yn, self.xn + self.yn - self.me)[place]
        return self.mine_of(place, slot, half)

    def peers(self):
        return self.sib, self.xn, self.yn

    def place(self, step):
        quad = lax.div(step, 4)
        odd = lax.div(lax.rem(step, 4), 2)
        far_x, far_y = step_place(odd, 3 - quad)
        third = lax.div(quad, 2) * (1 - lax.div(quad, 3))
        other = 1 - lax.rem(step, 2)
        slot = (
            self.me
            + far_x * (self.xn - self.me)
            + far_y * (self.yn - self.me)
            + other * (self.sib - self.me)
        )
        return slot, odd + third * (1 - 2 * odd), other, far_x + 2 * far_y

    def side_copy(self, step):
        slot, half, _, place = self.place(step)
        return remote(
            self.theirs(place, slot, half),
            self.side.at[place, half],
            self.send.at[step],
            self.side_sem.at[place, half],
            self.sib,
        )

    def side_wait(self, place, half):
        remote(
            self.side.at[place, half],
            self.side.at[place, half],
            self.send.at[0],
            self.side_sem.at[place, half],
            self.sib,
        ).wait_recv()

    def relay_copy(self, step, way):
        return remote(
            self.mine(3, way),
            self.relay.at[way],
            self.send.at[step],
            self.relay_sem.at[way],
            (self.xn, self.yn)[way],
        )

    def final_copy(self, step, way, half):
        return remote(
            self.mine(1 + way, half),
            self.final.at[way, half],
            self.send.at[step],
            self.final_sem.at[way, half],
            (self.xn, self.yn)[way],
        )

    def depart(self, step):
        @pl.when(self.place(step)[2] == 1)
        def _():
            self.side_copy(step).start()

        for way in (0, 1):

            @pl.when(step == 1 + 2 * way)
            def _():
                self.side_wait(3, way)
                add_rows(self.mine(3, way), (self.side.at[3, way],))
                self.relay_copy(1 + 2 * way, way).start()

            @pl.when(step == 5 + 2 * way)
            def _():
                self.side_wait(1 + way, way)
                add_rows(self.mine(1 + way, way), (self.side.at[1 + way, way],))
                self.final_copy(5 + 2 * way, way, way).start()

    def send_theirs(self):
        def one(index, carry):
            self.side_copy(2 * index).start()
            return carry

        lax.fori_loop(0, 8, one, 0)

    def send_mine(self):
        for way in (0, 1):
            self.side_wait(3, way)
            add_rows(self.mine(3, way), (self.side.at[3, way],))
            self.relay_copy(1 + 2 * way, way).start()
        for way in (0, 1):
            self.side_wait(1 + way, way)
            add_rows(self.mine(1 + way, way), (self.side.at[1 + way, way],))
            self.final_copy(5 + 2 * way, way, way).start()

    def forward(self):
        for way in (0, 1):
            self.side_wait(1 + way, 1 - way)
            self.relay_copy(0, 1 - way).wait_recv()
            add_rows(
                self.mine(1 + way, 1 - way),
                (self.side.at[1 + way, 1 - way], self.relay.at[1 - way]),
            )
            self.final_copy(9 + 2 * way, way, 1 - way).start()

    def finish(self, write):
        parts, rows_all = self.relay.shape[1:3]
        chunk = row_chunk(rows_all)
        for half in (0, 1):
            home = self.mine(0, half)
            self.side_wait(0, half)
            self.final_copy(0, 0, half).wait_recv()
            self.final_copy(0, 1, half).wait_recv()
            for part in range(parts):

                def one(index, carry, half=half, home=home, part=part):
                    rows = pl.ds(pl.multiple_of(index * chunk, chunk), chunk)
                    total = home[part, rows, :].astype(jnp.float32)
                    total = total + self.side[0, half, part, rows, :].astype(jnp.float32)
                    total = total + self.final[0, half, part, rows, :].astype(jnp.float32)
                    total = total + self.final[1, half, part, rows, :].astype(jnp.float32)
                    write(half, part, rows, total)
                    return carry

                lax.fori_loop(0, rows_all // chunk, one, 0)

    def drain(self):
        for way in (0, 1):
            self.relay_copy(1 + 2 * way, way).wait_send()
            self.final_copy(5 + 2 * way, way, way).wait_send()
            self.final_copy(9 + 2 * way, way, 1 - way).wait_send()

        def one(step, carry):
            @pl.when(self.place(step)[2] == 1)
            def _():
                self.side_copy(step).wait_send()

            return carry

        lax.fori_loop(0, 16, one, 0)


SCATTER_REFS = 7


def scatter_scratch(parts, rows, columns):
    bf = jnp.bfloat16
    return [
        pltpu.VMEM((4, 2, parts, rows, columns), bf),
        pltpu.VMEM((2, parts, rows, columns), bf),
        pltpu.VMEM((2, 2, parts, rows, columns), bf),
        pltpu.SemaphoreType.DMA((16,)),
        pltpu.SemaphoreType.DMA((4, 2)),
        pltpu.SemaphoreType.DMA((2,)),
        pltpu.SemaphoreType.DMA((2, 2)),
    ]


OUT_SLOTS = 4


def expert_out_kernel(rows_hbm, gate_hbm, up_hbm, down_hbm, resid, targets, scales, layer, grad, grad_b, ua_out, rows, gate, ua, up_w, down_w, mine, away, load_w, load_rows, load_gate, store_ua, *scratch):
    hidden, width = down_w.shape
    scatter = Scatter(
        lambda place, slot, half: mine.at[place, half],
        lambda place, slot, half: away.at[place, half],
        scratch,
    )
    weights = (
        pltpu.make_async_copy(up_hbm, up_w, load_w.at[0]),
        pltpu.make_async_copy(down_hbm, down_w, load_w.at[1]),
    )

    def loads(step):
        slot, half, _, _ = scatter.place(step)
        spot = lax.rem(step, OUT_SLOTS)
        return (
            pltpu.make_async_copy(rows_hbm.at[slot, half], rows.at[spot], load_rows.at[step]),
            pltpu.make_async_copy(gate_hbm.at[slot, half], gate.at[spot], load_gate.at[step]),
        )

    def ua_store(step):
        slot, half, _, _ = scatter.place(step)
        return pltpu.make_async_copy(
            ua.at[lax.rem(step, OUT_SLOTS)], ua_out.at[slot, half], store_ua.at[step]
        )

    weights[0].start()
    for step in (0, 1):
        for copy in loads(step):
            copy.start()
    weights[1].start()
    plane_barrier(scatter.peers())
    weights[0].wait()

    def one(step, carry):
        _, _, other, place = scatter.place(step)
        spot = lax.rem(step, OUT_SLOTS)
        for copy in loads(step):
            copy.wait()

        @pl.when(step < 14)
        def _():
            for copy in loads(step + 2):
                copy.start()

        @pl.when(step >= OUT_SLOTS)
        def _():
            ua_store(step - OUT_SLOTS).wait()

        lanes = lax.broadcasted_iota(jnp.int32, (rows.shape[1], 128), 1)
        tail = rows[spot, :, width:].astype(jnp.float32)
        weight = jnp.sum(jnp.where(lanes == scatter.me, tail, 0.0), axis=1, keepdims=True)
        up_val = nn_dot(rows[spot, :, :width], up_w[...])
        act_val = jnp.maximum(gate[spot].astype(jnp.float32), 0.0) * up_val * weight
        ua[spot, :, :hidden] = up_val.astype(jnp.bfloat16)
        ua[spot, :, hidden:] = act_val.astype(jnp.bfloat16)
        ua_store(step).start()

        @pl.when(step == 0)
        def _():
            weights[1].wait()

        partial = nn_dot(ua[spot, :, hidden:], down_w[...]).astype(jnp.bfloat16)

        @pl.when(other == 1)
        def _():
            away[place, half_of(scatter, step), 0] = partial

        @pl.when(other == 0)
        def _():
            mine[place, half_of(scatter, step), 0] = partial

        scatter.depart(step)

        @pl.when(step == 12)
        def _():
            scatter.forward()

        return carry

    lax.fori_loop(0, 16, one, 0)

    def write(half, part, rows, total):
        value = resid[half, rows, :] + total
        layer[half, rows, :] = value.astype(layer.dtype)
        error = (value - targets[half, rows, :].astype(jnp.float32)) * scales[half, rows, 0:1]
        grad[half, rows, :] = error
        grad_b[half, rows, :] = error.astype(grad_b.dtype)

    scatter.finish(write)
    scatter.drain()

    def drain(step, carry):
        ua_store(step).wait()
        return carry

    lax.fori_loop(16 - OUT_SLOTS, 16, drain, 0)


def half_of(scatter, step):
    return scatter.place(step)[1]


def expert_out(rows_all, gate_val, up_w, down_w, resid, targets, scales):
    half, columns = rows_all.shape[2:]
    hidden, width = down_w.shape
    bf = jnp.bfloat16
    return pl.pallas_call(
        expert_out_kernel,
        out_shape=(
            jax.ShapeDtypeStruct((2, half, width), bf),
            jax.ShapeDtypeStruct((2, half, width), jnp.float32),
            jax.ShapeDtypeStruct((2, half, width), bf),
            jax.ShapeDtypeStruct((8, 2, half, 2 * hidden), bf),
        ),
        in_specs=[ANY] * 4 + [VMEM] * 3,
        out_specs=(VMEM, VMEM, VMEM, ANY),
        scratch_shapes=[
            pltpu.VMEM((OUT_SLOTS, half, columns), bf),
            pltpu.VMEM((OUT_SLOTS, half, hidden), bf),
            pltpu.VMEM((OUT_SLOTS, half, 2 * hidden), bf),
            pltpu.VMEM((width, hidden), bf),
            pltpu.VMEM((hidden, width), bf),
            pltpu.VMEM((4, 2, 1, half, width), bf),
            pltpu.VMEM((4, 2, 1, half, width), bf),
            pltpu.SemaphoreType.DMA((2,)),
            pltpu.SemaphoreType.DMA((16,)),
            pltpu.SemaphoreType.DMA((16,)),
            pltpu.SemaphoreType.DMA((16,)),
        ]
        + scatter_scratch(1, half, width),
        compiler_params=pltpu.CompilerParams(
            collective_id=2, has_side_effects=True, vmem_limit_bytes=VMEM_BYTES
        ),
        name="expert_out",
    )(
        rows_all,
        gate_val,
        up_w,
        down_w,
        resid.reshape(2, half, width),
        targets.reshape(2, half, width),
        scales.reshape(2, half, 128),
    )


BACK_SLOTS = 8


def expert_back_kernel(own, rows_hbm, g_hbm, ua_hbm, down_hbm, dgu_out, tail_out, parts_out, buf, gua, rows, tails, down_w, acc, down_acc, send, recv, load, load_g, load_ua, load_rows, store_dgu, store_tail):
    hidden, width = down_w.shape
    gather = Gather(own, buf, send, recv)
    loads = (
        pltpu.make_async_copy(own.at[0], buf.at[gather.me, 0], load.at[0]),
        pltpu.make_async_copy(own.at[1], buf.at[gather.me, 1], load.at[1]),
        pltpu.make_async_copy(down_hbm, down_w, load.at[2]),
    )
    for copy in loads:
        copy.start()

    def block_loads(step):
        slot, half, _ = gather.place(step)
        spot = lax.rem(step, BACK_SLOTS)
        return (
            pltpu.make_async_copy(
                g_hbm.at[slot, half], gua.at[spot, :, pl.ds(0, hidden)], load_g.at[step]
            ),
            pltpu.make_async_copy(
                ua_hbm.at[slot, half], gua.at[spot, :, pl.ds(hidden, 2 * hidden)], load_ua.at[step]
            ),
            pltpu.make_async_copy(rows_hbm.at[slot, half], rows.at[spot], load_rows.at[step]),
        )

    def block_stores(step):
        slot, half, _ = gather.place(step)
        spot = lax.rem(step, BACK_SLOTS)
        return (
            pltpu.make_async_copy(
                gua.at[spot, :, pl.ds(0, 2 * hidden)], dgu_out.at[slot, half], store_dgu.at[step]
            ),
            pltpu.make_async_copy(tails.at[spot], tail_out.at[slot, half], store_tail.at[step]),
        )

    def fetch(step, carry):
        for copy in block_loads(step):
            copy.start()
        return carry

    lax.fori_loop(0, BACK_SLOTS, fetch, 0)
    gather.begin()
    for copy in loads:
        copy.wait()

    def weight_grads(step):
        first = 4 * lax.rem(lax.div(step, 4), 2)
        spots = pl.ds(first, 4)
        places = [gather.place(step - 3 + index)[:2] for index in range(4)]

        def add(ref, index, total):
            at = pl.ds(pl.multiple_of(index * 256, 256), 256)

            @pl.when(step == 3)
            def _():
                ref[at, :] = total

            @pl.when(step > 3)
            def _():
                ref[at, :] = ref[at, :] + total

        def gate_up_tile(index, carry):
            cols = pl.ds(pl.multiple_of(index * 256, 256), 256)
            left = rows[spots, :, cols].reshape(-1, 256)
            right = gua[spots, :, : 2 * hidden].reshape(-1, 2 * hidden)
            add(acc, index, tn_dot(left, right))
            return carry

        def down_tile(index, carry):
            cols = pl.ds(pl.multiple_of(2 * hidden + index * 256, 256), 256)
            total = jnp.zeros((256, width), jnp.float32)
            for place, (slot, half) in enumerate(places):
                total = total + tn_dot(gua[first + place, :, cols], buf[slot, half])
            add(down_acc, index, total)
            return carry

        lax.fori_loop(0, width // 256, gate_up_tile, 0)
        lax.fori_loop(0, hidden // 256, down_tile, 0)

    def one(step, carry):
        slot, half = gather.arrive(step)
        spot = lax.rem(step, BACK_SLOTS)
        for copy in block_loads(step):
            copy.wait()

        lanes = lax.broadcasted_iota(jnp.int32, (buf.shape[2], 128), 1)
        tail = rows[spot, :, width:].astype(jnp.float32)
        weight = jnp.sum(jnp.where(lanes == gather.me, tail, 0.0), axis=1, keepdims=True)
        grad_act = nt_dot(buf[slot, half], down_w[...])
        gate_val = gua[spot, :, :hidden].astype(jnp.float32)
        up_val = gua[spot, :, hidden : 2 * hidden].astype(jnp.float32)
        gate_relu = jnp.maximum(gate_val, 0.0)
        grad_comb = jnp.sum(gate_relu * up_val * grad_act, axis=1, keepdims=True)
        grad_act = grad_act * weight
        grad_gate = jnp.where(gate_val > 0, grad_act * up_val, 0.0).astype(jnp.bfloat16)
        grad_up = (grad_act * gate_relu).astype(jnp.bfloat16)
        gua[spot, :, :hidden] = grad_gate
        gua[spot, :, hidden : 2 * hidden] = grad_up
        tails[spot] = jnp.where(lanes == gather.me, grad_comb, 0.0).astype(jnp.bfloat16)
        for copy in block_stores(step):
            copy.start()

        @pl.when(lax.rem(step, 4) == 3)
        def _():
            weight_grads(step)

            @pl.when(step < 8)
            def _():
                for index in range(4):
                    for copy in block_stores(step - 3 + index):
                        copy.wait()
                    for copy in block_loads(step + 5 + index):
                        copy.start()

        return carry

    lax.fori_loop(0, 16, one, 0)
    gather.finish()

    def round_rows(source, rows_each, first):
        chunks = rows_each // 64

        def one(index, carry):
            rows = pl.ds(pl.multiple_of(index * 64, 64), 64)
            place = pl.ds(pl.multiple_of(first + lax.rem(index, chunks) * 64, 64), 64)
            parts_out[lax.div(index, chunks), place, :] = source[rows, :].astype(jnp.bfloat16)
            return carry

        lax.fori_loop(0, 4 * chunks, one, 0)

    round_rows(acc, width // 4, 0)
    round_rows(down_acc, hidden // 4, width // 4)

    def drain(step, carry):
        for copy in block_stores(step):
            copy.wait()
        return carry

    lax.fori_loop(8, 16, drain, 0)


def expert_back(own, rows_all, gate_val, ua, down_w):
    half, columns = rows_all.shape[2:]
    hidden, width = down_w.shape
    bf = jnp.bfloat16
    return pl.pallas_call(
        expert_back_kernel,
        out_shape=(
            jax.ShapeDtypeStruct((8, 2, half, 2 * hidden), bf),
            jax.ShapeDtypeStruct((8, 2, half, 128), bf),
            jax.ShapeDtypeStruct((4, (width + hidden) // 4, width), bf),
        ),
        in_specs=[ANY] * 5,
        out_specs=(ANY, ANY, VMEM),
        scratch_shapes=[
            pltpu.VMEM((8, 2, half, width), bf),
            pltpu.VMEM((BACK_SLOTS, half, 3 * hidden), bf),
            pltpu.VMEM((BACK_SLOTS, half, columns), bf),
            pltpu.VMEM((BACK_SLOTS, half, 128), bf),
            pltpu.VMEM((hidden, width), bf),
            pltpu.VMEM((width, 2 * hidden), jnp.float32),
            pltpu.VMEM((hidden, width), jnp.float32),
            pltpu.SemaphoreType.DMA((14,)),
            pltpu.SemaphoreType.DMA((8, 2)),
            pltpu.SemaphoreType.DMA((3,)),
        ]
        + [pltpu.SemaphoreType.DMA((16,))] * 5,
        compiler_params=pltpu.CompilerParams(
            collective_id=3, has_side_effects=True, vmem_limit_bytes=VMEM_BYTES
        ),
        name="expert_back",
    )(own, rows_all, gate_val, ua, down_w)


def expert_rows_kernel(dgu_hbm, tail_hbm, gate_hbm, up_hbm, out, dgu, tails, gate_w, up_w, mine, away, load_w, load_dgu, load_tail, *scratch):
    width, hidden = gate_w.shape
    scatter = Scatter(
        lambda place, slot, half: mine.at[place, half],
        lambda place, slot, half: away.at[place, half],
        scratch,
    )
    weights = (
        pltpu.make_async_copy(gate_hbm, gate_w, load_w.at[0]),
        pltpu.make_async_copy(up_hbm, up_w, load_w.at[1]),
    )

    def loads(step):
        slot, half, _, _ = scatter.place(step)
        spot = lax.rem(step, OUT_SLOTS)
        return (
            pltpu.make_async_copy(dgu_hbm.at[slot, half], dgu.at[spot], load_dgu.at[step]),
            pltpu.make_async_copy(tail_hbm.at[slot, half], tails.at[spot], load_tail.at[step]),
        )

    for copy in weights:
        copy.start()
    for step in (0, 1):
        for copy in loads(step):
            copy.start()
    plane_barrier(scatter.peers())
    for copy in weights:
        copy.wait()

    def one(step, carry):
        _, half, other, place = scatter.place(step)
        spot = lax.rem(step, OUT_SLOTS)
        for copy in loads(step):
            copy.wait()

        @pl.when(step < 14)
        def _():
            for copy in loads(step + 2):
                copy.start()

        total = nt_dot(dgu[spot, :, :hidden], gate_w[...]) + nt_dot(dgu[spot, :, hidden:], up_w[...])
        partial = total.astype(jnp.bfloat16)

        @pl.when(other == 1)
        def _():
            away[place, half, 0, :, :width] = partial
            away[place, half, 0, :, width:] = tails[spot]

        @pl.when(other == 0)
        def _():
            mine[place, half, 0, :, :width] = partial
            mine[place, half, 0, :, width:] = tails[spot]

        scatter.depart(step)

        @pl.when(step == 12)
        def _():
            scatter.forward()

        return carry

    lax.fori_loop(0, 16, one, 0)

    def write(half, part, rows, total):
        out[half, rows, :] = total

    scatter.finish(write)
    scatter.drain()


def expert_rows(dgu, tails, gate_w, up_w):
    half = dgu.shape[2]
    width, hidden = gate_w.shape
    columns = width + 128
    bf = jnp.bfloat16
    return pl.pallas_call(
        expert_rows_kernel,
        out_shape=jax.ShapeDtypeStruct((2, half, columns), jnp.float32),
        in_specs=[ANY] * 4,
        out_specs=VMEM,
        scratch_shapes=[
            pltpu.VMEM((OUT_SLOTS, half, 2 * hidden), bf),
            pltpu.VMEM((OUT_SLOTS, half, 128), bf),
            pltpu.VMEM((width, hidden), bf),
            pltpu.VMEM((width, hidden), bf),
            pltpu.VMEM((4, 2, 1, half, columns), bf),
            pltpu.VMEM((4, 2, 1, half, columns), bf),
            pltpu.SemaphoreType.DMA((2,)),
            pltpu.SemaphoreType.DMA((16,)),
            pltpu.SemaphoreType.DMA((16,)),
        ]
        + scatter_scratch(1, half, columns),
        compiler_params=pltpu.CompilerParams(
            collective_id=4, has_side_effects=True, vmem_limit_bytes=VMEM_BYTES
        ),
        name="expert_rows",
    )(dgu, tails, gate_w, up_w)


def line_gather_kernel(own, everything, stage, send, recv, local):
    line = line_peers()
    into = pltpu.make_async_copy(own, stage, local.at[0])
    into.start()
    full_barrier((), line[1:])

    def copy(turn, block):
        return line_remote(
            own, everything.at[block], send.at[turn - 1], recv.at[turn - 1], line[turn]
        )

    for turn in (1, 2, 3):
        copy(turn, line[0]).start()
    into.wait()
    out = pltpu.make_async_copy(stage, everything.at[line[0]], local.at[1])
    out.start()
    out.wait()
    for turn in (1, 2, 3):
        copy(turn, line[turn]).wait()


def line_gather(own):
    return pl.pallas_call(
        line_gather_kernel,
        out_shape=jax.ShapeDtypeStruct((4, *own.shape), own.dtype),
        in_specs=[ANY],
        out_specs=ANY,
        scratch_shapes=[
            pltpu.VMEM(own.shape, own.dtype),
            pltpu.SemaphoreType.DMA((3,)),
            pltpu.SemaphoreType.DMA((3,)),
            pltpu.SemaphoreType.DMA((2,)),
        ],
        compiler_params=pltpu.CompilerParams(
            collective_id=7, has_side_effects=True, vmem_limit_bytes=VMEM_BYTES
        ),
        name="line_gather",
    )(own)


class DenseGather:
    def __init__(self, own, everything, send, recv, local, lined):
        self.own, self.everything, self.send, self.recv = own, everything, send, recv
        self.lined = lined
        self.me, self.sib, self.xn, self.yn = plane_peers()
        self.diag = self.xn + self.yn - self.me
        self.line = line_peers()
        if lined:
            self.home = pltpu.make_async_copy(own, everything.at[:, self.me], local)
        else:
            self.home = pltpu.make_async_copy(own, everything.at[self.line[0], self.me], local)
        self.started = []

    def copy(self, index, own, slot, turn, peer, make):
        target = self.everything.at[self.line[turn], slot]
        return make(
            (self.own.at[self.line[turn]] if self.lined else self.own) if own else target,
            target,
            self.send.at[index],
            self.recv.at[self.line[turn], slot],
            peer,
        )

    def put(self, own, slot, turn, peer, make=remote):
        what = (len(self.started), own, slot, turn, peer, make)
        self.started.append(what)
        self.copy(*what).start()

    def pass_on(self, slot, turn, peer):
        self.put(False, slot, turn, peer)

    def wait(self, slot, turn):
        ref = self.everything.at[self.line[turn], slot]
        remote(ref, ref, self.send.at[0], self.recv.at[self.line[turn], slot], self.sib).wait_recv()

    def start_line(self):
        for turn in (1, 2, 3):
            self.put(True, self.me, 0, self.line[turn], line_remote)

    def start_plane(self):
        for turn in (0, 1, 2, 3) if self.lined else (0,):
            for peer in (self.xn, self.yn, self.sib):
                self.put(True, self.me, turn, peer)

    def near(self, turn):
        self.wait(self.xn, turn)
        if turn % 2 == 0:
            self.pass_on(self.xn, turn, self.yn)
        self.pass_on(self.xn, turn, self.sib)
        self.wait(self.yn, turn)
        if turn % 2 == 1:
            self.pass_on(self.yn, turn, self.xn)
        self.pass_on(self.yn, turn, self.sib)

    def from_line(self, turn):
        self.wait(self.me, turn)
        for peer in (self.xn, self.yn, self.sib):
            self.pass_on(self.me, turn, peer)

    def far(self, turn):
        self.wait(self.diag, turn)
        self.pass_on(self.diag, turn, self.sib)

    def arrived(self):
        for turn in (0, 1, 2, 3):
            for slot in (self.me, self.xn, self.yn, self.diag):
                self.wait(slot + self.sib - self.me, turn)
        self.home.wait()

    def finish(self):
        for what in self.started:
            self.copy(*what).wait_send()


def gather_scratch(rows, columns):
    return [
        pltpu.VMEM((4, 8, rows, columns), jnp.bfloat16),
        pltpu.SemaphoreType.DMA((32,)),
        pltpu.SemaphoreType.DMA((4, 8)),
        pltpu.SemaphoreType.DMA((2,)),
    ]


class LineScatter:
    def __init__(self, sums, scratch):
        self.sums = sums
        self.other, self.send, self.recv = scratch
        self.line = line_peers()

    def copy(self, turn):
        target = self.line[turn]
        return line_remote(
            self.sums(target),
            self.other.at[turn - 1],
            self.send.at[turn - 1],
            self.recv.at[turn - 1],
            target,
        )

    def begin(self):
        for turn in (1, 2, 3):
            self.copy(turn).start()

    def finish(self, outs):
        rows_all = self.other.shape[1]
        for turn in (1, 2, 3):
            self.copy(turn).wait_recv()
        own = self.sums(self.line[0])

        def one(index, carry):
            rows = pl.ds(pl.multiple_of(index * 16, 16), 16)
            total = own[rows, :].astype(jnp.float32)
            for turn in (0, 1, 2):
                total = total + self.other[turn, rows, :].astype(jnp.float32)
            first = 0
            for out, place, columns in outs:
                out[rows, place : place + columns] = total[:, first : first + columns]
                first += columns
            return carry

        lax.fori_loop(0, rows_all // 16, one, 0)
        for turn in (1, 2, 3):
            self.copy(turn).wait_send()


class DenseScatter:
    def __init__(self, total, scratch):
        def block(place, slot, half):
            return total.at[half, :, slot]

        self.plane = Scatter(block, block, scratch[:SCATTER_REFS])
        me = self.plane.me
        self.line = LineScatter(
            lambda line: total.at[lax.div(line, 2), lax.rem(line, 2), me], scratch[SCATTER_REFS:]
        )

    def begin(self):
        self.plane.send_theirs()

    def own(self):
        self.plane.send_mine()

    def forward(self):
        self.plane.forward()

    def turn(self):
        def write(half, part, rows, total):
            home = self.plane.mine(0, half)
            home[part, rows, :] = total.astype(home.dtype)

        self.plane.finish(write)
        self.line.begin()

    def finish(self, outs):
        self.line.finish(outs)
        self.plane.drain()


DENSE_REFS = SCATTER_REFS + 3


def dense_scratch(rows, columns):
    return scatter_scratch(2, rows, columns) + [
        pltpu.VMEM((3, rows, columns), jnp.bfloat16),
        pltpu.SemaphoreType.DMA((3,)),
        pltpu.SemaphoreType.DMA((3,)),
    ]


def rope(values, cosine, sine):
    return values * cosine + pltpu.roll(values, HD // 2, 1) * sine


def gain_rows(misc, out):
    for index in range(out.shape[1] // 128):
        rows = pl.ds(index * 128, 128)
        out[:, rows] = jnp.transpose(misc(rows).astype(jnp.float32))


def inverse_rms(values):
    return lax.rsqrt(jnp.mean(values * values, axis=1, keepdims=True) + EPS)


def row_loop(count, chunk, body):
    def one(index, carry):
        body(pl.ds(pl.multiple_of(index * chunk, chunk), chunk))
        return carry

    lax.fori_loop(0, count // chunk, one, 0)


def tile_loop(count, tile, body):
    row_loop(count, tile, body)


ROW_CHUNK = 16
TILE = 256


def attend_kernel(q_heads, kv_heads, experts, tokens, qkv_own, out_own, cosine, sine, segments, routes, rows_out, resid, heads, mixed, lse, prob, bias, picked, qkv_hbm, out_hbm, gains, hidden, *scratch):
    num_rows, width = tokens.shape
    group = q_heads // kv_heads
    qkv_cols = (q_heads + 2 * kv_heads) * HD
    qkv_w, out_w = scratch[0], scratch[4]
    first = DenseGather(qkv_own, qkv_w, scratch[1], scratch[2], scratch[3].at[0], True)
    second = DenseGather(out_own, out_w, scratch[5], scratch[6], scratch[7].at[0], False)
    stores = (
        pltpu.make_async_copy(qkv_w, qkv_hbm, scratch[3].at[1]),
        pltpu.make_async_copy(out_w, out_hbm, scratch[7].at[1]),
    )
    for gather in (first, second):
        gather.home.start()
    full_barrier((first.sib, first.xn, first.yn), first.line[1:])
    first.start_plane()
    second.start_line()
    picked[...] = jnp.zeros_like(picked)
    lane_ids = lax.broadcasted_iota(jnp.int32, picked.shape, 1)
    for index in range(routes.shape[1]):
        picked[...] = picked[...] + jnp.where(lane_ids == routes[:, index : index + 1], 1.0, 0.0)
    seg_row = segments[0:1, :]
    for index in range(num_rows // 128):
        rows = slice(index * 128, (index + 1) * 128)
        wide = jnp.broadcast_to(seg_row[:, rows].astype(jnp.float32), (128, 128))
        seg_col = jnp.transpose(wide)[:, 0:1].astype(jnp.int32)
        keys = lax.broadcasted_iota(jnp.int32, (128, num_rows), 1)
        queries = lax.broadcasted_iota(jnp.int32, (128, num_rows), 0) + index * 128
        visible = (keys <= queries) & ((seg_row == 0) | (seg_row == seg_col))
        bias[rows, :] = jnp.where(visible, 0.0, NEG_BIG)
    for turn in (0, 1, 2, 3):
        first.near(turn)
        if turn > 0:
            first.far(turn - 1)
    first.far(3)
    second.start_plane()
    first.arrived()
    stores[0].start()

    def flat(ref, cols):
        return ref[:, :, :, cols].reshape(-1, cols.size)

    misc = flat(qkv_w, pl.ds(qkv_cols, 128))
    for index in range(width // 128):
        rows = slice(index * 128, (index + 1) * 128)
        gains[:, rows] = jnp.transpose(misc[rows, :].astype(jnp.float32))

    def norm_one(rows):
        value = tokens[rows, :].astype(jnp.float32)
        normed = value * inverse_rms(value)
        hidden[rows, :] = (normed * gains[experts : experts + 1, :]).astype(jnp.bfloat16)

    row_loop(num_rows, ROW_CHUNK, norm_one)

    for turn in (1, 2, 3):
        second.from_line(turn)

    def project(index, carry):
        cols = pl.ds(pl.multiple_of(index * TILE, TILE), TILE)
        raw = nn_dot(hidden[...], flat(qkv_w, cols))
        for part in (0, 1):
            slot = 2 * index + part
            turned = lax.rem(slot, group + 2) != group + 1
            cos_now = jnp.where(turned, cosine[...], 1.0)
            sin_now = jnp.where(turned, sine[...], 0.0)
            value = rope(raw[:, part * HD : (part + 1) * HD], cos_now, sin_now)
            heads[slot] = value.astype(jnp.bfloat16)
        return carry

    lax.fori_loop(0, (q_heads + 2 * kv_heads) // 2, project, 0)
    second.near(0)
    lse[...] = jnp.zeros_like(lse)

    def head_step(head, carry):
        key_slot = lax.div(head, group) * (group + 2) + group
        query_slot = head + 2 * lax.div(head, group)
        cols = pl.ds(pl.multiple_of(head * HD, HD), HD)
        for first, keys in ((0, PROMPT), (PROMPT, num_rows)):
            rows = pl.ds(first, keys - first)
            query = heads[query_slot, rows, :]
            score = nt_dot(query, heads[key_slot, :keys, :]) * HD ** (-0.5) + bias[rows, :keys]
            top = jnp.max(score, axis=1, keepdims=True)
            weight = jnp.exp(score - top)
            total = jnp.sum(weight, axis=1, keepdims=True)
            value = nn_dot(weight.astype(jnp.bfloat16), heads[key_slot + 1, :keys, :])
            mixed[rows, cols] = (value / total).astype(jnp.bfloat16)
            lanes = lax.broadcasted_iota(jnp.int32, (keys - first, 128), 1)
            lse[rows, :] = jnp.where(lanes == head, top + jnp.log(total), lse[rows, :])

        for turn in (1, 2, 3):

            @pl.when(head == 2 * turn - 1)
            def _():
                second.near(turn)

        for turn in (0, 1, 2):

            @pl.when(head == 6 + turn)
            def _():
                second.far(turn)

        return carry

    lax.fori_loop(0, q_heads, head_step, 0)

    second.far(3)
    second.arrived()
    stores[1].start()

    def out_tile(cols):
        resid[:, cols] = tokens[:, cols].astype(jnp.float32) + nn_dot(mixed[...], flat(out_w, cols))

    tile_loop(width, TILE, out_tile)

    def norm_two(rows):
        value = resid[rows, :]
        normed = value * inverse_rms(value)
        rows_out[rows, :width] = (normed * gains[experts + 1 : experts + 2, :]).astype(jnp.bfloat16)

    row_loop(num_rows, ROW_CHUNK, norm_two)
    logits = nn_dot(rows_out[:, :width], flat(qkv_w, pl.ds(qkv_cols, 128)))
    lanes = lax.broadcasted_iota(jnp.int32, logits.shape, 1)
    logits = jnp.where(lanes < experts, logits, NEG_BIG)
    weight = jnp.exp(logits - jnp.max(logits, axis=1, keepdims=True))
    value = weight / jnp.sum(weight, axis=1, keepdims=True)
    prob[...] = value
    chosen = value * picked[...]
    rows_out[:, width:] = (chosen / jnp.sum(chosen, axis=1, keepdims=True)).astype(jnp.bfloat16)
    for gather, store in zip((first, second), stores):
        store.wait()
        gather.finish()


def attend(tokens, qkv_own, out_own, cosine, sine, segments, routes, q_heads, kv_heads, experts):
    num_rows, width = tokens.shape
    bf = jnp.bfloat16
    all_heads = q_heads + 2 * kv_heads
    return pl.pallas_call(
        functools.partial(attend_kernel, q_heads, kv_heads, experts),
        out_shape=(
            jax.ShapeDtypeStruct((num_rows, width + 128), bf),
            jax.ShapeDtypeStruct((num_rows, width), jnp.float32),
            jax.ShapeDtypeStruct((all_heads, num_rows, HD), bf),
            jax.ShapeDtypeStruct((num_rows, q_heads * HD), bf),
            jax.ShapeDtypeStruct((num_rows, 128), jnp.float32),
            jax.ShapeDtypeStruct((num_rows, 128), jnp.float32),
            jax.ShapeDtypeStruct((num_rows, num_rows), jnp.float32),
            jax.ShapeDtypeStruct((num_rows, 128), jnp.float32),
            jax.ShapeDtypeStruct((4, 8, *qkv_own.shape[1:]), bf),
            jax.ShapeDtypeStruct((4, 8, *out_own.shape), bf),
        ),
        in_specs=[VMEM, ANY, ANY] + [VMEM] * 4,
        out_specs=(VMEM,) * 8 + (ANY, ANY),
        scratch_shapes=[
            pltpu.VMEM((128, width), jnp.float32),
            pltpu.VMEM((num_rows, width), bf),
        ]
        + gather_scratch(*qkv_own.shape[1:])
        + gather_scratch(*out_own.shape),
        compiler_params=pltpu.CompilerParams(
            collective_id=5, has_side_effects=True, vmem_limit_bytes=VMEM_BYTES
        ),
        name="attend",
    )(tokens, qkv_own, out_own, cosine, sine, segments.reshape(1, num_rows), routes)


def attend_back_kernel(q_heads, kv_heads, experts, back_hbm, grad_hbm, resid_hbm, rows_hbm, prob_hbm, picked_hbm, qkv_hbm, out_hbm, mixed_hbm, heads_hbm, lse_hbm, bias_hbm, cos_hbm, sin_hbm, tokens_hbm, grad_in, out_sum, q_sum, k_sum, v_sum, misc_sum, back, grad, resid, hidden_two, prob, picked, qkv_w, out_w, mixed, heads, lse, bias, cosine, sine, tokens, misc, gains, gain_sums, grad_logit, grad_proj, grad_mixed, grad_qkv, grad_kv, hidden, load, *scratch):
    num_rows, width = tokens.shape
    group = q_heads // kv_heads
    q_cols = q_heads * HD
    k_cols = kv_heads * HD
    qkv_cols = q_cols + 2 * k_cols
    near_cols = (group + 2) * HD
    bf = jnp.bfloat16
    parts, scatters = [], []
    for index in range(4):
        some = scratch[index * (1 + DENSE_REFS) : (index + 1) * (1 + DENSE_REFS)]
        parts.append(some[0])
        scatters.append(DenseScatter(some[0], some[1:]))
    out_part, near_part, rest_part, misc_part = parts
    out_scatter, near_scatter, rest_scatter, misc_scatter = scatters
    pairs = (
        (prob_hbm, prob),
        (picked_hbm, picked),
        (back_hbm, back),
        (qkv_hbm.at[:, pl.ds(qkv_cols, 128)], misc),
        (resid_hbm, resid),
        (grad_hbm, grad),
        (mixed_hbm, mixed),
        (out_hbm, out_w),
        (tokens_hbm, tokens),
        (heads_hbm, heads),
        (lse_hbm, lse),
        (bias_hbm, bias),
        (cos_hbm, cosine),
        (sin_hbm, sine),
        (qkv_hbm, qkv_w),
        (rows_hbm, hidden_two),
    )
    loads = [pltpu.make_async_copy(src, dst, load.at[i]) for i, (src, dst) in enumerate(pairs)]

    def start(first, last):
        for copy in loads[first:last]:
            copy.start()

    def wait(first, last):
        for copy in loads[first:last]:
            copy.wait()

    start(0, 6)
    full_barrier(out_scatter.plane.peers(), out_scatter.line.line[1:])
    wait(0, 3)
    start(6, 9)
    gain_sums[...] = jnp.zeros_like(gain_sums)

    def router_rows(rows):
        value = prob[rows, :]
        chosen = value * picked[rows, :]
        total = jnp.sum(chosen, axis=1, keepdims=True)
        comb = chosen / total
        grad_comb = back[rows, width:]
        grad_chosen = (
            picked[rows, :] * (grad_comb - jnp.sum(grad_comb * comb, axis=1, keepdims=True)) / total
        )
        logit = value * (grad_chosen - jnp.sum(value * grad_chosen, axis=1, keepdims=True))
        grad_logit[rows, :] = logit.astype(bf)

    row_loop(num_rows, 64, router_rows)
    wait(3, 4)
    gain_rows(lambda rows: misc[rows, :], gains)
    lanes = lax.broadcasted_iota(jnp.int32, (TILE, 128), 1)

    def hidden_tile(cols):
        router = jnp.where(lanes < experts, misc[cols, :], jnp.zeros((), bf))
        back[:, cols] = back[:, cols] + nt_dot(grad_logit[...], router)

    tile_loop(width, TILE, hidden_tile)
    wait(4, 6)
    start(9, 16)

    def fold(values):
        return jnp.sum(values.reshape(-1, 8, width), axis=0)

    def norm_two(rows):
        value = resid[rows, :]
        inverse = inverse_rms(value)
        normed = value * inverse
        grad_hidden = back[rows, :width]
        gain_sums[8:16, :] = gain_sums[8:16, :] + fold(grad_hidden * normed)
        grad_norm = grad_hidden * gains[experts + 1 : experts + 2, :]
        mean = jnp.mean(grad_norm * normed, axis=1, keepdims=True)
        total = grad[rows, :] + inverse * (grad_norm - normed * mean)
        grad[rows, :] = total
        grad_proj[rows, :] = total.astype(bf)

    row_loop(num_rows, ROW_CHUNK, norm_two)

    def weight_loop(part, left, right):
        _, _, blocks, rows_each, columns = part.shape
        span = blocks * rows_each

        def one(line, carry):
            cols = pl.ds(pl.multiple_of(line * span, 128), span)
            total = tn_dot(left[:, cols], right[...]).astype(bf)
            part[lax.div(line, 2), lax.rem(line, 2)] = total.reshape(blocks, rows_each, columns)
            return carry

        lax.fori_loop(0, 4, one, 0)

    wait(6, 7)
    weight_loop(out_part, mixed, grad_proj)
    out_scatter.begin()

    def mixed_tile(cols):
        grad_mixed[:, cols] = nt_dot(
            grad_proj[...], out_w[cols, :]
        ).astype(bf)

    wait(7, 9)
    tile_loop(q_cols, TILE, mixed_tile)
    out_scatter.own()

    def norm_one(rows):
        value = tokens[rows, :].astype(jnp.float32)
        normed = value * inverse_rms(value)
        hidden[rows, :] = (normed * gains[experts : experts + 1, :]).astype(bf)

    row_loop(num_rows, ROW_CHUNK, norm_one)
    scale = HD ** (-0.5)
    wait(9, 14)

    def head_step(head, carry):
        key_slot = lax.div(head, group) * (group + 2) + group
        query_slot = head + 2 * lax.div(head, group)
        cols = pl.ds(pl.multiple_of(head * HD, HD), HD)
        query_cols = pl.ds(pl.multiple_of(query_slot * HD, HD), HD)

        @pl.when(lax.rem(head, group) == 0)
        def _():
            grad_kv[...] = jnp.zeros_like(grad_kv)

        for first, keys in ((0, PROMPT), (PROMPT, num_rows)):
            rows = pl.ds(first, keys - first)
            key = heads[key_slot, :keys, :]
            query = heads[query_slot, rows, :]
            up = grad_mixed[rows, cols]
            lane = lax.broadcasted_iota(jnp.int32, (keys - first, 128), 1)
            total = jnp.sum(jnp.where(lane == head, lse[rows, :], 0.0), axis=1, keepdims=True)
            weight = jnp.exp(nt_dot(query, key) * scale + bias[rows, :keys] - total)
            grad_weight = nt_dot(up, heads[key_slot + 1, :keys, :])
            delta = jnp.sum(weight * grad_weight, axis=1, keepdims=True)
            score = (weight * (grad_weight - delta)).astype(bf)
            grad_kv[1, :keys, :] = grad_kv[1, :keys, :] + tn_dot(weight.astype(bf), up)
            grad_kv[0, :keys, :] = grad_kv[0, :keys, :] + tn_dot(score, query) * scale
            value = rope(nn_dot(score, key) * scale, cosine[rows, :], -sine[rows, :])
            grad_qkv[rows, query_cols] = value.astype(bf)

        @pl.when(lax.rem(head, group) == group - 1)
        def _():
            key_cols = pl.ds(pl.multiple_of(key_slot * HD, HD), HD)
            value_cols = pl.ds(pl.multiple_of((key_slot + 1) * HD, HD), HD)
            grad_qkv[:, key_cols] = rope(grad_kv[0], cosine[...], -sine[...]).astype(bf)
            grad_qkv[:, value_cols] = grad_kv[1].astype(bf)

        @pl.when(head == 2)
        def _():
            out_scatter.forward()

        @pl.when(head == group - 1)
        def _():
            weight_loop(near_part, hidden, grad_qkv.at[:, pl.ds(0, near_cols)])
            near_scatter.begin()

        @pl.when(head == group)
        def _():
            near_scatter.own()

        @pl.when(head == group + 1)
        def _():
            out_scatter.turn()

        @pl.when(head == group + 3)
        def _():
            near_scatter.forward()

        return carry

    lax.fori_loop(0, q_heads, head_step, 0)
    weight_loop(rest_part, hidden, grad_qkv.at[:, pl.ds(near_cols, qkv_cols - near_cols)])
    rest_scatter.begin()
    near_scatter.turn()

    def hidden_back_tile(cols):
        back[:, cols] = nt_dot(grad_qkv[...], qkv_w[cols, pl.ds(0, qkv_cols)])

    wait(14, 16)
    tile_loop(width // 2, TILE, hidden_back_tile)
    rest_scatter.own()

    def late_tile(index, carry):
        hidden_back_tile(pl.ds(pl.multiple_of(width // 2 + index * TILE, TILE), TILE))
        return carry

    lax.fori_loop(0, width // 2 // TILE, late_tile, 0)

    def last_rows(rows):
        value = tokens[rows, :].astype(jnp.float32)
        inverse = inverse_rms(value)
        normed = value * inverse
        grad_hidden = back[rows, :width]
        gain_sums[0:8, :] = gain_sums[0:8, :] + fold(grad_hidden * normed)
        grad_norm = grad_hidden * gains[experts : experts + 1, :]
        mean = jnp.mean(grad_norm * normed, axis=1, keepdims=True)
        grad[rows, :] = grad[rows, :] + inverse * (grad_norm - normed * mean)

    row_loop(num_rows, ROW_CHUNK, last_rows)
    rest_scatter.forward()
    store = pltpu.make_async_copy(grad, grad_in, load.at[0])
    store.start()
    gains[0:16, :] = gain_sums[...]
    _, _, blocks, rows_each, _ = misc_part.shape
    span = blocks * rows_each

    def misc_line(line, carry):
        cols = pl.ds(pl.multiple_of(line * span, 128), span)
        router = tn_dot(hidden_two[:, cols], grad_logit[...])
        one = jnp.sum(gains[0:8, cols], axis=0, keepdims=True)
        two = jnp.sum(gains[8:16, cols], axis=0, keepdims=True)
        place = lax.broadcasted_iota(jnp.int32, (128, span), 0)
        block = jnp.where(place == experts, one, jnp.where(place == experts + 1, two, 0.0))
        total = (router + jnp.transpose(block)).astype(bf)
        misc_part[lax.div(line, 2), lax.rem(line, 2)] = total.reshape(blocks, rows_each, 128)
        return carry

    lax.fori_loop(0, 4, misc_line, 0)
    misc_scatter.begin()
    misc_scatter.own()
    rest_scatter.turn()
    misc_scatter.forward()
    misc_scatter.turn()
    out_scatter.finish(((out_sum, 0, width),))
    half_cols = group * HD
    near_scatter.finish(((q_sum, 0, half_cols), (k_sum, 0, HD), (v_sum, 0, HD)))
    rest_scatter.finish(((q_sum, half_cols, half_cols), (k_sum, HD, HD), (v_sum, HD, HD)))
    misc_scatter.finish(((misc_sum, 0, 128),))
    store.wait()


def attend_back(back, grad, resid, rows_own, prob, picked, qkv_w, out_w, mixed, heads, lse, bias, cosine, sine, tokens, q_heads, kv_heads, experts):
    num_rows, width = tokens.shape
    bf = jnp.bfloat16
    arrays = (back, grad, resid, rows_own, prob, picked, qkv_w, out_w, mixed, heads, lse, bias, cosine, sine, tokens)
    k_cols = kv_heads * HD
    q_cols = q_heads * HD
    qkv_cols = q_cols + 2 * k_cols
    near_cols = qkv_cols // kv_heads
    block_rows = width // 32
    scratch = []
    for columns in (width, near_cols, qkv_cols - near_cols, 128):
        scratch += [pltpu.VMEM((2, 2, 8, block_rows, columns), bf)]
        scratch += dense_scratch(block_rows, columns)
    return pl.pallas_call(
        functools.partial(attend_back_kernel, q_heads, kv_heads, experts),
        out_shape=(jax.ShapeDtypeStruct((num_rows, width), jnp.float32),)
        + tuple(
            jax.ShapeDtypeStruct((block_rows, columns), jnp.float32)
            for columns in (width, q_cols, k_cols, k_cols, 128)
        ),
        in_specs=[ANY] * len(arrays),
        out_specs=(ANY,) + (VMEM,) * 5,
        scratch_shapes=[pltpu.VMEM(array.shape, array.dtype) for array in arrays]
        + [
            pltpu.VMEM((width, 128), bf),
            pltpu.VMEM((128, width), jnp.float32),
            pltpu.VMEM((16, width), jnp.float32),
            pltpu.VMEM((num_rows, 128), bf),
            pltpu.VMEM((num_rows, width), bf),
            pltpu.VMEM((num_rows, q_cols), bf),
            pltpu.VMEM((num_rows, qkv_cols), bf),
            pltpu.VMEM((2, num_rows, HD), jnp.float32),
            pltpu.VMEM((num_rows, width), bf),
            pltpu.SemaphoreType.DMA((len(arrays) + 1,)),
        ]
        + scratch,
        compiler_params=pltpu.CompilerParams(
            collective_id=6, has_side_effects=True, vmem_limit_bytes=67043328
        ),
        name="attend_back",
    )(*arrays)


def body_plane(
    tokens,
    targets,
    valid_count,
    segments,
    routes,
    gain_attn,
    w_query,
    w_key,
    w_value,
    w_out,
    gain_moe,
    w_router,
    w_gate,
    w_up,
    w_down,
):
    bf = jnp.bfloat16
    num_rows, width = tokens.shape
    half = num_rows // 2
    q_cols, k_cols = w_query.shape[1], w_key.shape[1]
    num_experts = w_router.shape[1]
    num_heads = q_cols // HD
    kv_heads = k_cols // HD
    pad_cols = 128 - 2 - num_experts
    qkv_own = jnp.concatenate(
        [
            *(
                weight[:, index * columns : (index + 1) * columns]
                for index in range(kv_heads)
                for weight, columns in ((w_query, q_cols // kv_heads), (w_key, HD), (w_value, HD))
            ),
            w_router,
            gain_attn[:, None],
            gain_moe[:, None],
            jnp.zeros((gain_attn.shape[0], pad_cols), bf),
        ],
        axis=1,
    )
    qkv_line, w_gate, w_up = lax.optimization_barrier((line_gather(qkv_own), w_gate, w_up))
    gate_w = lax.all_gather(w_gate, "dp", axis=1, tiled=True)[0]
    up_w = lax.all_gather(w_up, "dp", axis=1, tiled=True)[0]
    tok_pos = positions(segments)
    freq = THETA ** (-2.0 * jnp.arange(HD // 2, dtype=jnp.float32) / HD)
    angle = tok_pos.astype(jnp.float32)[:, None] * freq[None, :]
    cosine, sine_part = jnp.cos(angle), jnp.sin(angle)
    cosine = jnp.concatenate([cosine, cosine], axis=1)
    sine = jnp.concatenate([-sine_part, sine_part], axis=1)
    rows_own, resid_mid, heads, mixed, lse, prob, bias, picked, qkv_w, out_w = attend(
        tokens, qkv_line, w_out, cosine, sine, segments, routes, num_heads, kv_heads, num_experts
    )
    rows_all, gate_val, down_w = expert_in(
        rows_own.reshape(2, half, width + 128), gate_w, w_down[0]
    )
    down_w = down_w.reshape(-1, width)
    total_rows = num_rows * lax.axis_size(("dp", "exp"))
    global_row = lax.axis_index(("dp", "exp")) * num_rows + jnp.arange(num_rows, dtype=jnp.int32)
    loss_scale = total_rows / valid_count[0].astype(jnp.float32)
    scales = jnp.broadcast_to(
        jnp.where(global_row < valid_count[0], loss_scale, 0.0)[:, None], (num_rows, 128)
    )
    layer_out, grad_out, grad_out_b, ua = expert_out(
        rows_all, gate_val, up_w, down_w, resid_mid, targets, scales
    )
    layer_out = layer_out.reshape(num_rows, width)
    dgu, tails, expert_parts = expert_back(
        grad_out_b, rows_all, gate_val, ua, down_w
    )
    back = expert_rows(dgu, tails, gate_w, up_w)
    expert_sum = lax.psum_scatter(expert_parts, "dp", scatter_dimension=0, tiled=True)
    hidden, shard = w_gate.shape[2], w_gate.shape[1]
    expert_sums = (
        expert_sum[:, :shard, :hidden].astype(jnp.float32),
        expert_sum[:, :shard, hidden:].astype(jnp.float32),
        expert_sum[:, shard:].astype(jnp.float32),
    )
    grad_in, out_sum, q_sum, k_sum, v_sum, misc_sum = attend_back(
        back.reshape(num_rows, width + 128),
        grad_out.reshape(num_rows, width),
        resid_mid,
        rows_own,
        prob,
        picked,
        qkv_w.reshape(width, -1),
        out_w.reshape(q_cols, width),
        mixed,
        heads,
        lse,
        bias,
        cosine,
        sine,
        tokens,
        num_heads,
        kv_heads,
        num_experts,
    )
    return (
        layer_out,
        grad_in,
        misc_sum[:, num_experts],
        q_sum,
        k_sum,
        v_sum,
        out_sum,
        misc_sum[:, num_experts + 1],
        misc_sum[:, :num_experts],
        *expert_sums,
    )


def solution(mesh):
    in_specs = (
        P(("dp", "exp"), None),
        P(("dp", "exp"), None),
        P(),
        P(("dp", "exp")),
        P(("dp", "exp"), None),
        P(("dp", "exp")),
        P(("dp", "exp"), None),
        P(("dp", "exp"), None),
        P(("dp", "exp"), None),
        P(("dp", "exp"), None),
        P(("dp", "exp")),
        P(("dp", "exp"), None),
        P("exp", "dp", None),
        P("exp", "dp", None),
        P("exp", "dp", None),
    )
    out_specs = (
        P(("dp", "exp"), None),
        P(("dp", "exp"), None),
        P(("dp", "exp")),
        P(("dp", "exp"), None),
        P(("dp", "exp"), None),
        P(("dp", "exp"), None),
        P(("dp", "exp"), None),
        P(("dp", "exp")),
        P(("dp", "exp"), None),
        P("exp", "dp", None),
        P("exp", "dp", None),
        P("exp", "dp", None),
    )
    body = body_plane if (mesh.shape["dp"], mesh.shape["exp"]) == (4, 8) else body_general
    return jax.shard_map(body, mesh=mesh, in_specs=in_specs, out_specs=out_specs, check_vma=False)
```
